32 devices in a mesh: fsdp: 4 (over y, x), tensor: 8 (over z, core).
Axes of the slice: x: 2, y: 2, z: 4, core: 2. Of those that a mesh axis runs over, the one named last changes fastest.
Arguments:
- block_input: bfloat16 [8, 1536, 1152], P('fsdp', 'tensor'), may hold values from -6 to 6
- segment_ids: int32 [8, 1536], P('fsdp'), may hold values from -1 to 15, as said below
- norm_gains: float32 [2, 1152], replicated, may hold values from 0.5 to 1.5
- row_biases: float32 [4, 1152], replicated, may hold values from -0.15 to 0.15
- in_projection: bfloat16 [3, 1152, 1152], P(None, 'fsdp', 'tensor'), may hold values from -0.1875 to 0.1875
- query_value_bias: float32 [2, 1152], P(None, 'tensor'), may hold values from -0.12 to 0.12
- out_projection: bfloat16 [1152, 1152], P('tensor', 'fsdp'), may hold values from -4 to 4
- up_weight: bfloat16 [1152, 4304], P('fsdp', 'tensor'), may hold values from -0.1875 to 0.1875
- unit_bias: bfloat16 [4304], P('tensor'), may hold values from -3 to 3
- down_weight: bfloat16 [4304, 1152], P('tensor', 'fsdp'), may hold values from -0.1875 to 0.1875
- cotangent: bfloat16 [8, 1536, 1152], P('fsdp', 'tensor'), may hold values from -6 to 6
Outputs:
- block_output: bfloat16 [8, 1536, 1152], P('fsdp', 'tensor')
- input_grad: float32 [8, 1536, 1152], P('fsdp', 'tensor')
- norm_gains_grad: float32 [2, 1152], replicated
- row_biases_grad: float32 [4, 1152], replicated
- in_projection_grad: float32 [3, 1152, 1152], P(None, 'fsdp', 'tensor')
- query_value_bias_grad: float32 [2, 1152], P(None, 'tensor')
- out_projection_grad: float32 [1152, 1152], P('tensor', 'fsdp')
- up_weight_grad: float32 [1152, 4304], P('fsdp', 'tensor')
- unit_bias_grad: float32 [4304], P('tensor')
- down_weight_grad: float32 [4304, 1152], P('tensor', 'fsdp')
The draws below stay inside these ranges and needn't reach their ends.
Inputs may be any that keep to these rules, and one draw needn't show every extreme that they name: `segment_ids`: row block b holds 2 images in order; image j is a run of 729 consecutive rows with the id b * 2 + j, and every other row is padding with the id -1.
All inputs are finite; a program needn't handle non-finite values.
Results may differ from the reference program's by a relative error of at most 0.012.
Values may be sent and summed in bfloat16 or wider, within the bound.
A program may use at most 192 MiB of HBM per device.

```python
import jax
import jax.numpy as jnp
from jax import lax

D = 1152
H = 16
DH = 72
FF = 4304
IMG = 729
IMG_MB = 2
ROWS_MB = 1536
BATCHES = 8


def draw_segment_ids(key, part):
    padding = ROWS_MB - IMG_MB * IMG
    batch_keys = jax.random.split(key, BATCHES)

    def single_batch(batch_key, batch_index):
        offsets = jnp.sort(jax.random.randint(batch_key, (IMG_MB,), 0, padding + 1)).astype(jnp.int32)
        starts = offsets + jnp.arange(IMG_MB, dtype=jnp.int32) * IMG
        positions = jnp.arange(ROWS_MB, dtype=jnp.int32)[:, None]
        inside = (positions >= starts[None, :]) & (positions < starts[None, :] + IMG)
        image_ids = batch_index * IMG_MB + jnp.arange(IMG_MB, dtype=jnp.int32)[None, :]
        return jnp.max(jnp.where(inside, image_ids, -1), axis=1).astype(jnp.int32)
    return jax.vmap(single_batch)(batch_keys, jnp.arange(BATCHES, dtype=jnp.int32))


def steps_of(stream_key, extent, cuts, low, largest):
    loudness = 1.0
    for position, shards_of in cuts:
        draws = jax.random.uniform(jax.random.fold_in(jax.random.fold_in(stream_key, 6), position), (shards_of,), jnp.float32, low / len(cuts), largest / len(cuts))
        loudness = loudness * jnp.repeat(jnp.exp(draws), extent[position] // shards_of).reshape((-1,) + (1,) * (len(extent) - 1 - position))
    return loudness


def gaussian(rng, extent, width, bound, shards=(), held_as=jnp.bfloat16):
    entries = width * jax.random.normal(rng, extent, jnp.float32)
    if shards:
        entries = entries * steps_of(rng, extent, shards, -0.22, 0.18)
    return jnp.clip(entries, -bound, bound).astype(held_as)


def setup_inputs(seed: int = 0) -> dict:
    key_list = jax.random.split(jax.random.key(seed), 12)
    block_input = gaussian(key_list[0], (BATCHES, ROWS_MB, D), 1.0, 6.0, ((0, 4), (1, 8)))
    segment_ids = draw_segment_ids(jax.random.fold_in(key_list[11], 71), 0)
    norm_gains = jnp.clip(1.0 + 0.1 * jax.random.normal(key_list[2], (2, D), jnp.float32), 0.5, 1.5)
    row_biases = gaussian(key_list[3], (4, D), 0.025, 0.15, (), jnp.float32)
    in_projection = gaussian(key_list[4], (3, D, H * DH), D ** -0.5, 0.1875, ((1, 4), (2, 8)))
    query_value_bias = gaussian(key_list[5], (2, H * DH), 0.02, 0.12, ((1, 8),), jnp.float32)
    out_projection = gaussian(key_list[6], (H * DH, D), 2 ** -0.5, 4.0, ((0, 8), (1, 4)))
    up_weight = gaussian(key_list[7], (D, FF), D ** -0.5, 0.1875, ((0, 4), (1, 8)))
    unit_bias = gaussian(key_list[8], (FF,), 0.5, 3.0, ((0, 8),))
    down_weight = gaussian(key_list[9], (FF, D), D ** -0.5, 0.1875, ((0, 8), (1, 4)))
    cotangent = gaussian(key_list[10], (BATCHES, ROWS_MB, D), 1.0, 6.0, ((0, 4), (1, 8)))
    return dict(block_input=block_input, segment_ids=segment_ids, norm_gains=norm_gains, row_biases=row_biases, in_projection=in_projection, query_value_bias=query_value_bias, out_projection=out_projection, up_weight=up_weight, unit_bias=unit_bias, down_weight=down_weight, cotangent=cotangent)


EPS = 1e-06
GELU_C = 0.7978845608028654

def norm_forward(values, norm_gain, norm_shift):
    center = values - lax.optimization_barrier(jnp.mean(values, axis=-1, keepdims=True))
    factor = lax.rsqrt(lax.optimization_barrier(jnp.mean(center * center, axis=-1, keepdims=True)) + EPS)
    scaled = center * factor
    return (scaled * norm_gain + norm_shift, scaled, factor)

def norm_backward(upstream, scaled, factor, norm_gain):
    inside = upstream * norm_gain
    return factor * (inside - lax.optimization_barrier(jnp.mean(inside, axis=-1, keepdims=True)) - scaled * lax.optimization_barrier(jnp.mean(inside * scaled, axis=-1, keepdims=True)))

def gelu(pre_act):
    return 0.5 * pre_act * (1.0 + jnp.tanh(GELU_C * (pre_act + 0.044715 * pre_act * pre_act * pre_act)))

def gelu_back(pre_act, upstream):
    return jax.vjp(gelu, pre_act)[1](upstream)[0]

def allowed(segments):
    return (segments[:, None] == segments[None, :])[None]

def attention_forward(queries, key_rows, value_rows, segments):
    rows_count = queries.shape[0]
    score_scale = DH ** (-0.5)
    query_float = queries.astype(jnp.float32).reshape(rows_count, -1, DH)
    key_float = key_rows.astype(jnp.float32).reshape(rows_count, -1, DH)
    value_float = value_rows.astype(jnp.float32).reshape(rows_count, -1, DH)
    scores = jnp.einsum('qhd,khd->hqk', query_float, key_float) * score_scale
    allowed_pairs = allowed(segments)
    log_total = jnp.log(lax.optimization_barrier(jnp.sum(jnp.where(allowed_pairs, jnp.exp(scores), 0.0), axis=2, keepdims=True)))
    probs = jnp.where(allowed_pairs, jnp.exp(scores - log_total), 0.0).astype(jnp.bfloat16)
    probs_float = lax.optimization_barrier(probs).astype(jnp.float32)
    context = jnp.einsum('hqk,khd->qhd', probs_float, value_float).astype(jnp.bfloat16)
    return (context.reshape(rows_count, -1), log_total)

def attention_backward(queries, key_rows, value_rows, context, context_grad, log_total, segments):
    rows_count = queries.shape[0]
    score_scale = DH ** (-0.5)
    query_float = queries.astype(jnp.float32).reshape(rows_count, -1, DH)
    key_float = key_rows.astype(jnp.float32).reshape(rows_count, -1, DH)
    value_float = value_rows.astype(jnp.float32).reshape(rows_count, -1, DH)
    context_float = context.astype(jnp.float32).reshape(rows_count, -1, DH)
    back_float = context_grad.astype(jnp.float32).reshape(rows_count, -1, DH)
    scores = jnp.einsum('qhd,khd->hqk', query_float, key_float) * score_scale
    allowed_pairs = allowed(segments)
    exact = jnp.where(allowed_pairs, jnp.exp(scores - log_total), 0.0)
    probs_float = lax.optimization_barrier(exact.astype(jnp.bfloat16)).astype(jnp.float32)
    value_grad = jnp.einsum('hqk,qhd->khd', probs_float, back_float)
    prob_grad = jnp.einsum('qhd,khd->hqk', back_float, value_float)
    delta = jnp.einsum('qhd,qhd->hq', back_float, context_float)[:, :, None]
    score_half = (exact * (prob_grad - delta) * score_scale).astype(jnp.bfloat16)
    score_grad = lax.optimization_barrier(score_half).astype(jnp.float32)
    query_grad = jnp.einsum('hqk,khd->qhd', score_grad, key_float)
    key_grad = jnp.einsum('hqk,qhd->khd', score_grad, query_float)
    return (query_grad.reshape(rows_count, -1), key_grad.reshape(rows_count, -1), value_grad.reshape(rows_count, -1))

def reference(block_input, segment_ids, norm_gains, row_biases, in_projection, query_value_bias, out_projection, up_weight, unit_bias, down_weight, cotangent):

    def one_batch(carry, inputs):
        rows_in, segments, grad_rows = inputs
        input_float = rows_in.astype(jnp.float32)
        first_out, first_scaled, first_factor = norm_forward(input_float, norm_gains[0], row_biases[0])
        first_norm = first_out.astype(jnp.bfloat16)
        queries = (jnp.dot(first_norm, in_projection[0], preferred_element_type=jnp.float32) + query_value_bias[0]).astype(jnp.bfloat16)
        key_rows = jnp.dot(first_norm, in_projection[1], preferred_element_type=jnp.float32).astype(jnp.bfloat16)
        value_rows = (jnp.dot(first_norm, in_projection[2], preferred_element_type=jnp.float32) + query_value_bias[1]).astype(jnp.bfloat16)
        context, log_total = attention_forward(queries, key_rows, value_rows, segments)
        residual = input_float + jnp.dot(context, out_projection, preferred_element_type=jnp.float32) + row_biases[2]
        second_out, second_scaled, second_factor = norm_forward(residual, norm_gains[1], row_biases[1])
        second_norm = second_out.astype(jnp.bfloat16)
        pre_act = jnp.dot(second_norm, up_weight, preferred_element_type=jnp.float32) + unit_bias
        hidden = gelu(pre_act).astype(jnp.bfloat16)
        block_output = (residual + jnp.dot(hidden, down_weight, preferred_element_type=jnp.float32) + row_biases[3]).astype(jnp.bfloat16)
        upstream = grad_rows.astype(jnp.float32)
        down_grad = jnp.dot(hidden.T, grad_rows, preferred_element_type=jnp.float32)
        pre_grad = gelu_back(pre_act, jnp.dot(grad_rows, down_weight.T, preferred_element_type=jnp.float32))
        pre_half = pre_grad.astype(jnp.bfloat16)
        up_grad = jnp.dot(second_norm.T, pre_half, preferred_element_type=jnp.float32)
        second_grad = jnp.dot(pre_half, up_weight.T, preferred_element_type=jnp.float32)
        residual_grad = upstream + norm_backward(second_grad, second_scaled, second_factor, norm_gains[1])
        residual_half = residual_grad.astype(jnp.bfloat16)
        out_grad = jnp.dot(context.T, residual_half, preferred_element_type=jnp.float32)
        context_grad = jnp.dot(residual_half, out_projection.T, preferred_element_type=jnp.float32).astype(jnp.bfloat16)
        query_grad, key_grad, value_grad = attention_backward(queries, key_rows, value_rows, context, context_grad, log_total, segments)
        triple_half = [query_grad.astype(jnp.bfloat16), key_grad.astype(jnp.bfloat16), value_grad.astype(jnp.bfloat16)]
        in_grad = jnp.stack([jnp.dot(first_norm.T, member, preferred_element_type=jnp.float32) for member in triple_half])
        first_grad = jnp.dot(triple_half[0], in_projection[0].T, preferred_element_type=jnp.float32)
        first_grad = first_grad + jnp.dot(triple_half[1], in_projection[1].T, preferred_element_type=jnp.float32)
        first_grad = first_grad + jnp.dot(triple_half[2], in_projection[2].T, preferred_element_type=jnp.float32)
        input_grad = residual_grad + norm_backward(first_grad, first_scaled, first_factor, norm_gains[0])
        gains_grad = jnp.stack([lax.optimization_barrier(jnp.sum(first_grad * first_scaled, axis=0)), lax.optimization_barrier(jnp.sum(second_grad * second_scaled, axis=0))])
        shifts_grad = jnp.stack([lax.optimization_barrier(jnp.sum(first_grad, axis=0)), lax.optimization_barrier(jnp.sum(second_grad, axis=0)), lax.optimization_barrier(jnp.sum(residual_grad, axis=0)), lax.optimization_barrier(jnp.sum(upstream, axis=0))])
        bias_grad = jnp.stack([lax.optimization_barrier(jnp.sum(query_grad, axis=0)), lax.optimization_barrier(jnp.sum(value_grad, axis=0))])
        unit_grad = lax.optimization_barrier(jnp.sum(pre_grad, axis=0))
        terms = (gains_grad, shifts_grad, in_grad, bias_grad, out_grad, up_grad, unit_grad, down_grad)
        return (jax.tree.map(jnp.add, carry, terms), (block_output, input_grad))
    zeros = (jnp.zeros((2, D), jnp.float32), jnp.zeros((4, D), jnp.float32), jnp.zeros((3, D, H * DH), jnp.float32), jnp.zeros((2, H * DH), jnp.float32), jnp.zeros((H * DH, D), jnp.float32), jnp.zeros((D, FF), jnp.float32), jnp.zeros((FF,), jnp.float32), jnp.zeros((FF, D), jnp.float32))
    totals, stacked = lax.scan(one_batch, zeros, (block_input, segment_ids, cotangent))
    return (stacked[0], stacked[1], totals[0], totals[1], totals[2], totals[3], totals[4], totals[5], totals[6], totals[7])
```

```python
import functools
import math

import jax
import jax.numpy as jnp
from jax import lax
from jax.experimental import pallas as pl
from jax.experimental.pallas import tpu as pltpu
from jax.sharding import Mesh
from jax.sharding import PartitionSpec as P

DH = 72
IMG = 729
IMG_MB = 2
EPS = 1e-06
GELU_C = 0.7978845608028654
F32 = jnp.float32
BF16 = jnp.bfloat16
FSDP = ("fy", "fx")
SCALE = DH ** (-0.5)
LOG2E = math.log2(math.e)


def norm_forward(values, norm_gain, norm_shift):
    center = values - jnp.mean(values, axis=-1, keepdims=True)
    factor = lax.rsqrt(jnp.mean(center * center, axis=-1, keepdims=True) + EPS)
    scaled = center * factor
    return (scaled * norm_gain + norm_shift, scaled, factor)


def norm_backward(upstream, scaled, factor, norm_gain):
    inside = upstream * norm_gain
    return factor * (
        inside
        - jnp.mean(inside, axis=-1, keepdims=True)
        - scaled * jnp.mean(inside * scaled, axis=-1, keepdims=True)
    )


def gelu(pre_act):
    return (
        0.5
        * pre_act
        * (1.0 + jnp.tanh(GELU_C * (pre_act + 0.044715 * pre_act * pre_act * pre_act)))
    )


def gelu_back(pre_act, upstream):
    return jax.vjp(gelu, pre_act)[1](upstream)[0]


def dot_nn(left, right):
    return lax.dot_general(left, right, (((1,), (0,)), ((), ())), preferred_element_type=F32)


def dot_nt(left, right):
    return lax.dot_general(left, right, (((1,), (1,)), ((), ())), preferred_element_type=F32)


def dot_tn(left, right):
    return lax.dot_general(left, right, (((0,), (0,)), ((), ())), preferred_element_type=F32)


def sum_products(lefts, rights):
    total = dot_nt(lefts[0], rights[0])
    for left, right in zip(lefts[1:], rights[1:]):
        total = total + dot_nt(left, right)
    return total


def round_up(value, unit):
    return -(-value // unit) * unit


def swap(value, axis):
    return lax.ppermute(value, axis, [(0, 1), (1, 0)])


def slot_swap(value, stride, slots):
    return lax.ppermute(value, "slot", [(s, s ^ stride) for s in range(slots)])


def part_sum(value, parts):
    value = value.astype(BF16)
    if parts == 2:
        return value.astype(F32) + swap(value, "part").astype(F32)
    return lax.psum(value.astype(F32), "part")


def part_gather(value, parts):
    if parts == 2:
        other = swap(value, "part")
        first = lax.axis_index("part") == 0
        return jnp.stack([jnp.where(first, value, other), jnp.where(first, other, value)])
    return lax.all_gather(value, "part", axis=0)


def add_half(left, right):
    return (left.astype(F32) + right.astype(F32)).astype(BF16)


MESH = pl.DeviceIdType.MESH


class Place:
    def __init__(self):
        self.y, self.x = lax.axis_index("fy"), lax.axis_index("fx")
        self.z = lax.axis_index("slot")
        self.f = 2 * self.y + self.x
        self.across_x, self.across_y = {"fx": 1 - self.x}, {"fy": 1 - self.y}
        self.above = {"slot": jnp.minimum(self.z + 1, 3)}
        self.below = {"slot": jnp.maximum(self.z - 1, 0)}

    def barrier(self):
        z, sem = self.z, pltpu.get_barrier_semaphore()
        signal = lambda device: pl.semaphore_signal(sem, inc=1, device_id=device, device_id_type=MESH)
        signal(self.across_x)
        signal(self.across_y)

        @pl.when(z < 3)
        def _():
            signal(self.above)

        @pl.when(z > 0)
        def _():
            signal(self.below)

        pl.semaphore_wait(sem, 2 + jnp.where(z < 3, 1, 0) + jnp.where(z > 0, 1, 0))

    def far_first(self, i):
        low = self.z < 2
        near = jnp.where(low, self.z, 3 - self.z)
        at = jnp.where(i == 0, 3, jnp.where(i == 1, 2, jnp.where(i == 2, 1 - near, near)))
        return jnp.where(low, at, 3 - at)


def send(src, dst, send_sem, recv_sem, device):
    return pltpu.make_async_remote_copy(
        src_ref=src, dst_ref=dst, send_sem=send_sem, recv_sem=recv_sem, device_id=device, device_id_type=MESH
    )


class Gather:
    SEMS = 11

    def __init__(self, place, shards, w, sems, local_sem, rows):
        self.p, self.shards, self.w, self.rows = place, shards, w, rows
        (self.zr, self.zu, self.zd, self.xr, self.xs, self.yr, self.ys, self.ar, self.asn, self.br, self.bs) = sems
        self.local_sem = local_sem

    def block(self, k, slot, owner, half=None):
        at, count = owner * self.rows, self.rows
        if half is not None:
            count = count // 2
            at = at + half * count
        return self.w[k].at[slot, pl.ds(pl.multiple_of(at, 16), count), :]

    def mine(self, k, slot, shard):
        return self.shards[k] if shard else self.block(k, slot, self.p.f)

    def up(self, k, slot, shard=False):
        dst = self.block(k, slot, self.p.f)
        return send(self.mine(k, slot, shard), dst, self.zu.at[k, slot], self.zr.at[k, slot], self.p.above)

    def down(self, k, slot, shard=False):
        dst = self.block(k, slot, self.p.f)
        return send(self.mine(k, slot, shard), dst, self.zd.at[k, slot], self.zr.at[k, slot], self.p.below)

    def to_x(self, k, slot, shard=False):
        dst = self.block(k, slot, self.p.f)
        return send(self.mine(k, slot, shard), dst, self.xs.at[k, slot], self.xr.at[k, slot], self.p.across_x)

    def to_y(self, k, slot, shard=False):
        dst = self.block(k, slot, self.p.f)
        return send(self.mine(k, slot, shard), dst, self.ys.at[k, slot], self.yr.at[k, slot], self.p.across_y)

    def from_x(self, k, slot):
        ref = self.block(k, slot, self.p.f ^ 1)
        return send(ref, ref, self.xs.at[k, slot], self.xr.at[k, slot], self.p.across_x)

    def from_y(self, k, slot):
        ref = self.block(k, slot, self.p.f ^ 2)
        return send(ref, ref, self.ys.at[k, slot], self.yr.at[k, slot], self.p.across_y)

    def corner_y(self, k, slot):
        ref = self.block(k, slot, self.p.f ^ 1, 0)
        return send(ref, ref, self.asn.at[k, slot], self.ar.at[k, slot], self.p.across_y)

    def corner_x(self, k, slot):
        ref = self.block(k, slot, self.p.f ^ 2, 1)
        return send(ref, ref, self.bs.at[k, slot], self.br.at[k, slot], self.p.across_x)

    def wait_corner(self, k, slot):
        ref = self.block(k, slot, self.p.f ^ 3, 0)
        send(ref, ref, self.asn.at[k, slot], self.ar.at[k, slot], self.p.across_y).wait_recv()
        ref = self.block(k, slot, self.p.f ^ 3, 1)
        send(ref, ref, self.bs.at[k, slot], self.br.at[k, slot], self.p.across_x).wait_recv()

    def local(self, k):
        return pltpu.make_async_copy(self.shards[k], self.block(k, self.p.z, self.p.f), self.local_sem.at[k])

    def start_z(self, k):
        @pl.when(self.p.z < 3)
        def _():
            self.up(k, self.p.z, True).start()

        @pl.when(self.p.z > 0)
        def _():
            self.down(k, self.p.z, True).start()

    def start_xy(self, k):
        self.to_x(k, self.p.z, True).start()
        self.to_y(k, self.p.z, True).start()
        self.local(k).start()

    def pass_on(self, k, d):
        z = self.p.z

        @pl.when(z >= d)
        def _():
            self.up(k, z - d).wait_recv()

            @pl.when(z < 3)
            def _():
                self.up(k, z - d).start()

            self.to_x(k, z - d).start()
            self.to_y(k, z - d).start()

        @pl.when(z + d <= 3)
        def _():
            self.down(k, z + d).wait_recv()

            @pl.when(z > 0)
            def _():
                self.down(k, z + d).start()

            self.to_x(k, z + d).start()
            self.to_y(k, z + d).start()

    def corner(self, k, d):
        def one(slot):
            self.from_x(k, slot).wait_recv()
            self.corner_y(k, slot).start()
            self.from_y(k, slot).wait_recv()
            self.corner_x(k, slot).start()

        z = self.p.z
        if d == 0:
            one(z)
        else:
            pl.when(z >= d)(lambda: one(z - d))
            pl.when(z + d <= 3)(lambda: one(z + d))

    def arrive(self, k):
        self.local(k).wait()
        for slot in range(4):
            self.wait_corner(k, slot)

    def drain(self, k):
        z = self.p.z
        for slot in range(4):
            self.to_x(k, slot).wait_send()
            self.to_y(k, slot).wait_send()
            self.corner_y(k, slot).wait_send()
            self.corner_x(k, slot).wait_send()

            @pl.when((z < 3) & (slot <= z))
            def _(slot=slot):
                self.up(k, slot).wait_send()

            @pl.when((z > 0) & (slot >= z))
            def _(slot=slot):
                self.down(k, slot).wait_send()


def gather_kernel(*refs, count, rows):
    shards, w = refs[:count], refs[count : 2 * count]
    sems = refs[2 * count :]
    place = Place()
    place.barrier()
    g = Gather(place, shards, w, sems[:-1], sems[-1], rows)
    g.start_z(0)
    for k in range(count):
        g.start_xy(k)
        g.pass_on(k, 1)
        g.corner(k, 0)
        g.pass_on(k, 2)
        g.corner(k, 1)
        g.pass_on(k, 3)
        if k + 1 < count:
            g.start_z(k + 1)
        g.corner(k, 2)
        g.corner(k, 3)
    for k in range(count):
        g.arrive(k)
        g.drain(k)


def gather_weights(shards, paired):
    if not paired:
        slots = lax.axis_size("slot")
        whole = [lax.all_gather(s, ("slot",) + FSDP, axis=0) for s in shards]
        return [w.reshape(slots, -1, w.shape[-1]) for w in whole]
    count, rows = len(shards), shards[0].shape[0]
    return pl.pallas_call(
        functools.partial(gather_kernel, count=count, rows=rows),
        in_specs=[pl.BlockSpec(memory_space=pltpu.VMEM)] * count,
        out_specs=[pl.BlockSpec(memory_space=pl.ANY)] * count,
        out_shape=[jax.ShapeDtypeStruct((4, 4 * rows, s.shape[1]), BF16) for s in shards],
        scratch_shapes=[pltpu.SemaphoreType.DMA((count, 4))] * Gather.SEMS + [pltpu.SemaphoreType.DMA((count,))],
        compiler_params=pltpu.CompilerParams(collective_id=1, has_side_effects=True),
        name="gather",
    )(*shards)


class Reduce:
    SEMS = 16

    def __init__(self, place, g, out, bufs, sems, rows):
        self.p, self.g, self.out, self.rows = place, g, out, rows
        self.bufs, self.sems = bufs, sems

    def grad(self, k, slot, owner, half=None):
        at, count = owner * self.rows, self.rows
        if half is not None:
            count = count // 2
            at = at + half * count
        return self.g[k].at[slot, pl.ds(pl.multiple_of(at, 16), count), :]

    def half(self, ref, slot, half):
        count = self.rows // 2
        return ref.at[slot, half * count : (half + 1) * count, :]

    def copy(self, k, slot, src, dst, index, device):
        return send(src, dst, self.sems[2 * index].at[k, slot], self.sems[2 * index + 1].at[k, slot], device)

    def corner_y(self, k, s):
        return self.copy(k, s, self.grad(k, s, self.p.f ^ 3, 0), self.bufs[k][0].at[s], 0, self.p.across_y)

    def corner_x(self, k, s):
        return self.copy(k, s, self.grad(k, s, self.p.f ^ 3, 1), self.bufs[k][1].at[s], 1, self.p.across_x)

    def x_low(self, k, s):
        return self.copy(k, s, self.bufs[k][0].at[s], self.half(self.bufs[k][2], s, 0), 2, self.p.across_x)

    def x_high(self, k, s):
        dst = self.half(self.bufs[k][2], s, 1)
        return self.copy(k, s, self.grad(k, s, self.p.f ^ 1, 1), dst, 3, self.p.across_x)

    def y_low(self, k, s):
        dst = self.half(self.bufs[k][3], s, 0)
        return self.copy(k, s, self.grad(k, s, self.p.f ^ 2, 0), dst, 4, self.p.across_y)

    def y_high(self, k, s):
        return self.copy(k, s, self.bufs[k][1].at[s], self.half(self.bufs[k][3], s, 1), 5, self.p.across_y)

    def up(self, k, s):
        return self.copy(k, s, self.bufs[k][2].at[s], self.bufs[k][4].at[s], 6, self.p.above)

    def down(self, k, s):
        return self.copy(k, s, self.bufs[k][2].at[s], self.bufs[k][5].at[s], 7, self.p.below)

    def start(self, k):
        def one(i, carry):
            s = self.p.far_first(i)
            self.corner_y(k, s).start()
            self.corner_x(k, s).start()
            self.y_low(k, s).start()
            self.x_high(k, s).start()
            return carry

        lax.fori_loop(0, 4, one, 0)

    def tiles(self, rows, body):
        step = 48 if rows % 48 == 0 else 16

        def one(t, carry):
            body(pl.ds(pl.multiple_of(t * step, 16), step))
            return carry

        lax.fori_loop(0, rows // step, one, 0)

    def middle(self, k):
        count = self.rows // 2

        def one(i, carry):
            s = self.p.far_first(i)
            low, high = self.bufs[k][0], self.bufs[k][1]
            self.corner_y(k, s).wait_recv()
            own = self.grad(k, s, self.p.f ^ 1, 0)

            def add_low(span):
                low[s, span, :] = add_half(low[s, span, :], own[span, :])

            self.tiles(count, add_low)
            self.x_low(k, s).start()
            self.corner_x(k, s).wait_recv()
            other = self.grad(k, s, self.p.f ^ 2, 1)

            def add_high(span):
                high[s, span, :] = add_half(high[s, span, :], other[span, :])

            self.tiles(count, add_high)
            self.y_high(k, s).start()
            return carry

        lax.fori_loop(0, 4, one, 0)

    def line(self, k):
        z, acc, side = self.p.z, self.bufs[k][2], self.bufs[k][3]
        lower, upper = self.bufs[k][4], self.bufs[k][5]

        def one(i, carry):
            s = self.p.far_first(i)
            self.x_low(k, s).wait_recv()
            self.x_high(k, s).wait_recv()
            self.y_low(k, s).wait_recv()
            self.y_high(k, s).wait_recv()
            own = self.grad(k, s, self.p.f)

            def add(span):
                total = own[span, :].astype(F32) + acc[s, span, :].astype(F32) + side[s, span, :].astype(F32)
                acc[s, span, :] = total.astype(BF16)

            def add_from(ref):
                def body(span):
                    acc[s, span, :] = add_half(acc[s, span, :], ref[s, span, :])

                return body

            self.tiles(self.rows, add)

            @pl.when((z > 0) & (s >= z))
            def _():
                self.up(k, s).wait_recv()
                self.tiles(self.rows, add_from(lower))

            @pl.when((z < 3) & (s <= z))
            def _():
                self.down(k, s).wait_recv()
                self.tiles(self.rows, add_from(upper))

            @pl.when(s > z)
            def _():
                self.up(k, s).start()

            @pl.when(s < z)
            def _():
                self.down(k, s).start()

            @pl.when(s == z)
            def _():
                def final(span):
                    self.out[k][span, :] = acc[s, span, :].astype(F32)

                self.tiles(self.rows, final)

            return carry

        lax.fori_loop(0, 4, one, 0)

    def drain(self, k):
        def one(s, carry):
            for copy in (self.corner_y, self.corner_x, self.x_low, self.x_high, self.y_low, self.y_high):
                copy(k, s).wait_send()

            @pl.when(s > self.p.z)
            def _():
                self.up(k, s).wait_send()

            @pl.when(s < self.p.z)
            def _():
                self.down(k, s).wait_send()

            return carry

        lax.fori_loop(0, 4, one, 0)


def reduce_buffers(rows, lanes):
    return [
        pltpu.VMEM((4, rows // 2, lanes), BF16),
        pltpu.VMEM((4, rows // 2, lanes), BF16),
        pltpu.VMEM((4, rows, lanes), BF16),
        pltpu.VMEM((4, rows, lanes), BF16),
        pltpu.VMEM((4, rows, lanes), BF16),
        pltpu.VMEM((4, rows, lanes), BF16),
    ]


def reduce_kernel(*refs, count, rows):
    g, out = refs[:count], refs[count : 2 * count]
    bufs = [refs[2 * count + 6 * k : 2 * count + 6 * k + 6] for k in range(count)]
    sems = refs[8 * count :]
    place = Place()
    place.barrier()
    r = Reduce(place, g, out, bufs, sems, rows)
    r.start(0)
    for k in range(count):
        r.middle(k)
        if k + 1 < count:
            r.start(k + 1)
        r.line(k)
    for k in range(count):
        r.drain(k)


def scatter_grads(chunks, paired):
    if not paired:
        count = lax.axis_size("fy") * lax.axis_size("fx")
        split = [c.reshape(c.shape[0] * count, c.shape[1] // count, c.shape[2]) for c in chunks]
        return [lax.psum_scatter(c, ("slot",) + FSDP, scatter_dimension=0).astype(F32) for c in split]
    count, rows = len(chunks), chunks[0].shape[1] // 4
    scratch = [b for c in chunks for b in reduce_buffers(rows, c.shape[2])]
    return pl.pallas_call(
        functools.partial(reduce_kernel, count=count, rows=rows),
        in_specs=[pl.BlockSpec(memory_space=pltpu.VMEM)] * count,
        out_specs=[pl.BlockSpec(memory_space=pltpu.VMEM)] * count,
        out_shape=[jax.ShapeDtypeStruct((rows, c.shape[2]), F32) for c in chunks],
        scratch_shapes=scratch + [pltpu.SemaphoreType.DMA((count, 4))] * Reduce.SEMS,
        compiler_params=pltpu.CompilerParams(
            collective_id=2, has_side_effects=True, vmem_limit_bytes=64000000
        ),
        name="reduce",
    )(*chunks)


def attend_kernel(x_ref, w_ref, b_ref, segc_ref, segr_ref, qkv_ref, ctx_ref, inv_ref, part_ref, *, cols, tile):
    rows = x_ref.shape[0]
    heads = cols // DH
    block = pl.program_id(0)
    projected = dot_nn(x_ref[...], w_ref[0, :, : 3 * cols]) + b_ref[0]
    qkv_ref[0] = projected.astype(BF16)
    for head in range(heads):
        lo = head * DH
        keys = qkv_ref[0, :, cols + lo : cols + lo + DH]
        values = qkv_ref[0, :, 2 * cols + lo : 2 * cols + lo + DH]

        def one_tile(t, carry):
            span = pl.ds(pl.multiple_of(t * tile, tile), tile)
            scores = dot_nt(qkv_ref[0, span, lo : lo + DH], keys)
            allowed = segc_ref[span, :] == segr_ref[...]
            exact = jnp.where(allowed, jnp.exp2(scores * (SCALE * LOG2E)), 0.0)
            inverse = 1.0 / jnp.sum(exact, axis=1, keepdims=True)
            context = dot_nn(exact.astype(BF16), values) * inverse
            ctx_ref[0, span, lo : lo + DH] = context.astype(BF16)
            inv_ref[0, span, head : head + 1] = inverse
            return carry

        lax.fori_loop(0, rows // tile, one_tile, 0)
    part = dot_nt(ctx_ref[0], w_ref[0, :, 3 * cols : 4 * cols])

    @pl.when(block == 0)
    def _():
        part_ref[...] = part

    @pl.when(block > 0)
    def _():
        part_ref[...] += part


def attend(first_norm, weights, bias, segments, cols, tile):
    rows, width = first_norm.shape
    slots, _, lanes = weights.shape
    heads = cols // DH
    whole = lambda shape: pl.BlockSpec(shape, lambda s: (0,) * len(shape))
    each = lambda shape: pl.BlockSpec((1,) + shape, lambda s: (s, 0, 0))
    return pl.pallas_call(
        functools.partial(attend_kernel, cols=cols, tile=tile),
        grid=(slots,),
        in_specs=[
            whole((rows, width)),
            each((width, lanes)),
            each((1, 3 * cols)),
            whole((rows, 1)),
            whole((1, rows)),
        ],
        out_specs=[each((rows, 3 * cols)), each((rows, cols)), each((rows, heads)), whole((rows, width))],
        out_shape=[
            jax.ShapeDtypeStruct((slots, rows, 3 * cols), BF16),
            jax.ShapeDtypeStruct((slots, rows, cols), BF16),
            jax.ShapeDtypeStruct((slots, rows, heads), F32),
            jax.ShapeDtypeStruct((rows, width), F32),
        ],
        cost_estimate=pl.CostEstimate(
            flops=slots * (8 * rows * width * cols + 4 * rows * rows * 256 * heads),
            bytes_accessed=slots * width * lanes * 2 + rows * width * 10,
            transcendentals=slots * heads * rows * rows,
        ),
        name="attend",
    )(first_norm, weights, bias, segments[:, None], segments[None, :])


def attend_back_kernel(
    r_ref, w_ref, qkv_ref, ctx_ref, inv_ref, segc_ref, segr_ref, grad_ref, bias_ref, back_ref, key_acc, value_acc, *, cols, tile
):
    rows = r_ref.shape[0]
    heads = cols // DH
    back_ref[...] = dot_nn(r_ref[...], w_ref[0, :, 3 * cols : 4 * cols]).astype(BF16)
    ones = jnp.ones((8, DH), F32)
    for head in range(heads):
        lo = head * DH
        keys = qkv_ref[0, :, cols + lo : cols + lo + DH]
        values = qkv_ref[0, :, 2 * cols + lo : 2 * cols + lo + DH]
        key_acc[...] = jnp.zeros_like(key_acc)
        value_acc[...] = jnp.zeros_like(value_acc)

        def one_tile(t, query_total):
            span = slice(t * tile, (t + 1) * tile)
            queries = qkv_ref[0, span, lo : lo + DH]
            back = (back_ref[span, lo : lo + DH].astype(F32) * inv_ref[0, span, head : head + 1]).astype(BF16)
            along = back.astype(F32) * ctx_ref[0, span, lo : lo + DH].astype(F32)
            delta = lax.dot_general(
                ones, along, (((1,), (1,)), ((), ())), precision=lax.Precision.HIGHEST, preferred_element_type=F32
            )[:1]
            scores = dot_nt(keys, queries)
            allowed = segc_ref[...] == segr_ref[:, span]
            exact = jnp.where(allowed, jnp.exp2(scores * (SCALE * LOG2E)), 0.0)
            value_acc[...] += dot_nn(exact.astype(BF16), back)
            prob_grad = dot_nt(values, back)
            score_grad = (exact * (prob_grad - delta)).astype(BF16)
            key_acc[...] += dot_nn(score_grad, queries)
            query_grad = dot_tn(score_grad, keys) * SCALE
            grad_ref[0, span, lo : lo + DH] = query_grad.astype(BF16)
            return query_total + jnp.sum(query_grad, axis=0, keepdims=True)

        tiles = rows // tile
        query_total = jnp.zeros((1, DH), F32)
        for t in range(tiles):
            query_total = one_tile(t, query_total)
        grad_ref[0, :, cols + lo : cols + lo + DH] = (key_acc[...] * SCALE).astype(BF16)
        grad_ref[0, :, 2 * cols + lo : 2 * cols + lo + DH] = value_acc[...].astype(BF16)
        bias_ref[0, 0:1, lo : lo + DH] = query_total
        bias_ref[0, 1:2, lo : lo + DH] = jnp.sum(value_acc[...], axis=0, keepdims=True)


def attend_back(residual_half, weights, qkv, context, inverse, segments, cols, tile):
    rows, width = residual_half.shape
    slots, _, lanes = weights.shape
    heads = cols // DH
    whole = lambda shape: pl.BlockSpec(shape, lambda s: (0,) * len(shape))
    each = lambda shape: pl.BlockSpec((1,) + shape, lambda s: (s, 0, 0))
    return pl.pallas_call(
        functools.partial(attend_back_kernel, cols=cols, tile=tile),
        grid=(slots,),
        in_specs=[
            whole((rows, width)),
            each((width, lanes)),
            each((rows, 3 * cols)),
            each((rows, cols)),
            each((rows, heads)),
            whole((rows, 1)),
            whole((1, rows)),
        ],
        out_specs=[each((rows, 3 * cols)), each((2, cols))],
        out_shape=[
            jax.ShapeDtypeStruct((slots, rows, 3 * cols), BF16),
            jax.ShapeDtypeStruct((slots, 2, cols), F32),
        ],
        scratch_shapes=[
            pltpu.VMEM((rows, cols), BF16),
            pltpu.VMEM((rows, DH), F32),
            pltpu.VMEM((rows, DH), F32),
        ],
        cost_estimate=pl.CostEstimate(
            flops=slots * (2 * rows * width * cols + 10 * rows * rows * 256 * heads),
            bytes_accessed=slots * width * lanes * 2 + rows * width * 10,
            transcendentals=slots * heads * rows * rows,
        ),
        name="attend_back",
    )(residual_half, weights, qkv, context, inverse, segments[:, None], segments[None, :])


def on_device(
    block_input,
    segment_ids,
    norm_gains,
    row_biases,
    in_projection,
    query_value_bias,
    out_projection,
    up_weight,
    unit_bias,
    down_weight,
    cotangent,
):
    local, rows_each, width = block_input.shape
    rows_mb = segment_ids.shape[1]
    cols = in_projection.shape[2]
    units = up_weight.shape[1]
    shard_rows = up_weight.shape[0]
    slots, parts = lax.axis_size("slot"), lax.axis_size("part")
    paired = lax.axis_size("fy") == 2 and lax.axis_size("fx") == 2 and slots == 4 and shard_rows % 32 == 0
    slot, part = lax.axis_index("slot"), lax.axis_index("part")
    fsdp_index = lax.axis_index("fy") * lax.axis_size("fx") + lax.axis_index("fx")
    batch, image = slot % local, slot // local
    late = image == 1

    half_rows = rows_mb // IMG_MB
    padding = rows_mb - IMG_MB * IMG
    edge = round_up(max(half_rows - IMG, padding - (half_rows - IMG)), 16)
    tail = round_up(padding, 16)
    rows = round_up(half_rows + edge + tail, 128)
    filler = rows - half_rows - edge - tail

    def edges(main):
        near = jnp.where(late, main[:edge], main[half_rows - edge :])
        far = main[half_rows - tail :]
        return jnp.concatenate([near, far])

    def to_slot(value):
        mine = lax.dynamic_index_in_dim(value, batch, 0, keepdims=False)
        send = lax.dynamic_index_in_dim(value, 1 - batch, 0, keepdims=False)
        other = slot_swap(send, 1, slots)
        pair = jnp.where(batch == 0, jnp.stack([mine, other]), jnp.stack([other, mine]))
        main = part_gather(pair, parts).swapaxes(0, 1).reshape(half_rows, width)
        beyond = slot_swap(edges(main), local, slots)
        return jnp.concatenate([main, beyond, jnp.zeros((filler, width), value.dtype)])

    def from_slot(value, owned):
        main = value[:half_rows]
        beyond = slot_swap(value[half_rows : half_rows + edge + tail], local, slots)
        keep = owned[:half_rows, None]
        near, far = beyond[:edge], beyond[edge:]
        blank = lambda count: jnp.zeros((count, width), value.dtype)
        early_fill = jnp.concatenate([blank(half_rows - edge), near])
        late_fill = jnp.concatenate([near, blank(half_rows - edge - tail), far])
        main = jnp.where(keep, main, jnp.where(late, late_fill, early_fill))
        main = main.reshape(local, parts, rows_each, width)
        mine = lax.dynamic_index_in_dim(main, part, 1, keepdims=False)
        stay = lax.dynamic_index_in_dim(mine, batch, 0, keepdims=False)
        other = slot_swap(lax.dynamic_index_in_dim(mine, 1 - batch, 0, keepdims=False), 1, slots)
        return jnp.where(batch == 0, jnp.stack([stay, other]), jnp.stack([other, stay]))

    ids = lax.dynamic_index_in_dim(segment_ids, batch, 0, keepdims=False)
    fill_ids = jnp.full((filler,), -2, jnp.int32)
    early_ids = jnp.concatenate([ids[: half_rows + edge], ids[rows_mb - tail :], fill_ids])
    late_ids = jnp.concatenate(
        [ids[half_rows:], ids[half_rows - edge : half_rows], jnp.full((tail,), -2, jnp.int32), fill_ids]
    )
    segments = jnp.where(late, late_ids, early_ids)
    image_id = (fsdp_index * local + batch) * IMG_MB + image
    owned = (segments == image_id) | (jnp.logical_not(late) & (segments == -1))

    main_units = units // 128 * 128
    rest = units - main_units
    in_lanes = 3 * cols
    small = in_lanes + cols + 2 * rest
    high = query_value_bias.astype(BF16)
    low = (query_value_bias - high.astype(F32)).astype(BF16)
    vectors = jnp.concatenate([high.reshape(-1), low.reshape(-1), unit_bias])
    extra = -(-vectors.shape[0] // shard_rows)
    lanes = round_up(small + extra, 128)
    vectors = jnp.pad(vectors, (0, extra * shard_rows - vectors.shape[0])).reshape(shard_rows, extra)
    down_t = down_weight.T
    small_shard = jnp.concatenate(
        [
            in_projection.transpose(1, 0, 2).reshape(shard_rows, in_lanes),
            out_projection.T,
            up_weight[:, main_units:],
            down_t[:, main_units:],
            vectors,
            jnp.zeros((shard_rows, lanes - small - extra), BF16),
        ],
        axis=1,
    )
    small_all, up_main, down_main = gather_weights(
        [small_shard, up_weight[:, :main_units], down_t[:, :main_units]], paired
    )
    small_blocks, up_blocks, down_blocks = list(small_all), list(up_main), list(down_main)
    vectors = jnp.stack([b[:shard_rows, small : small + extra].reshape(-1) for b in small_blocks])
    qv_all = vectors[:, : 2 * cols].astype(F32) + vectors[:, 2 * cols : 4 * cols].astype(F32)
    unit_all = vectors[:, 4 * cols : 4 * cols + units].astype(F32)

    bias = jnp.concatenate([qv_all[:, :cols], jnp.zeros((slots, cols), F32), qv_all[:, cols:]], axis=1)[:, None]
    rest_lanes = round_up(slots * rest, 128)
    rest_pad = rest_lanes - slots * rest

    def unit_layout(blocks, at):
        extra = [b[:, at : at + rest] for b in small_blocks]
        return blocks + [jnp.concatenate(extra + [jnp.zeros((width, rest_pad), BF16)], axis=1)]

    gains, shifts = norm_gains, row_biases

    x_float = to_slot(block_input).astype(F32)
    grad_rows = jnp.where(owned[:, None], to_slot(cotangent), 0)
    upstream = grad_rows.astype(F32)

    first_out, first_scaled, first_factor = norm_forward(x_float, gains[0], shifts[0])
    first_norm = first_out.astype(BF16)
    qkv, context, inverse, attention_part = attend(
        first_norm, small_all, bias, segments, cols, rows // 2
    )
    residual = x_float + part_sum(attention_part, parts) + shifts[2]
    second_out, second_scaled, second_factor = norm_forward(residual, gains[1], shifts[1])
    second_norm = second_out.astype(BF16)
    up_all = unit_layout(up_blocks, in_lanes + cols)
    down_all = unit_layout(down_blocks, in_lanes + cols + rest)
    unit_rows = [unit_all[s, :main_units] for s in range(slots)]
    unit_rows += [jnp.concatenate([unit_all[:, main_units:].reshape(-1), jnp.zeros((rest_pad,), F32)])]
    pre_acts = [dot_nn(second_norm, w) + b for w, b in zip(up_all, unit_rows)]
    hiddens = [gelu(p).astype(BF16) for p in pre_acts]
    unit_part = sum_products(hiddens, down_all)
    unit_part = part_sum(unit_part, parts)
    output = from_slot((residual + unit_part + shifts[3]).astype(BF16), owned)

    down_sums = [dot_tn(grad_rows, h).astype(BF16) for h in hiddens]
    pre_grads = [gelu_back(p, dot_nn(grad_rows, w)) for p, w in zip(pre_acts, down_all)]
    pre_halves = [p.astype(BF16) for p in pre_grads]
    unit_sums = [jnp.sum(p, axis=0) for p in pre_grads]
    up_sums = [dot_tn(second_norm, p).astype(BF16) for p in pre_halves]
    second_grad = part_sum(sum_products(pre_halves, up_all), parts)
    residual_grad = upstream + norm_backward(second_grad, second_scaled, second_factor, gains[1])
    residual_half = residual_grad.astype(BF16)
    out_sum = [dot_tn(residual_half, context[s]).astype(BF16) for s in range(slots)]
    triple, bias_sum = attend_back(
        residual_half, small_all, qkv, context, inverse, segments, cols, rows // 2
    )
    in_sum = [dot_tn(first_norm, triple[s]).astype(BF16) for s in range(slots)]
    first_part = sum_products([triple[s] for s in range(slots)], [b[:, :in_lanes] for b in small_blocks])
    first_grad = part_sum(first_part, parts)
    input_grad = residual_grad + norm_backward(first_grad, first_scaled, first_factor, gains[0])
    input_grad = from_slot(input_grad.astype(BF16), owned)

    rest_of = lambda sums, s: sums[slots][:, s * rest : (s + 1) * rest]
    blank = jnp.zeros((width, lanes - small), BF16)
    small_sums = [
        jnp.concatenate([in_sum[s], out_sum[s], rest_of(up_sums, s), rest_of(down_sums, s), blank], axis=1)
        for s in range(slots)
    ]
    down_grad, up_grad, small_grad = scatter_grads(
        [jnp.stack(down_sums[:slots]), jnp.stack(up_sums[:slots]), jnp.stack(small_sums)], paired
    )
    in_grad = small_grad[:, :in_lanes].reshape(shard_rows, 3, cols).transpose(1, 0, 2)
    out_grad = small_grad[:, in_lanes : in_lanes + cols].T
    at = in_lanes + cols
    up_grad = jnp.concatenate([up_grad, small_grad[:, at : at + rest]], axis=1)
    down_grad = jnp.concatenate([down_grad, small_grad[:, at + rest : at + 2 * rest]], axis=1).T

    rows_sum = jnp.stack(
        [
            jnp.sum(first_grad * first_scaled, axis=0),
            jnp.sum(second_grad * second_scaled, axis=0),
            jnp.sum(first_grad, axis=0),
            jnp.sum(second_grad, axis=0),
            jnp.sum(residual_grad, axis=0),
            jnp.sum(upstream, axis=0),
        ]
    )
    sums = [rows_sum, bias_sum] + unit_sums
    flat = jnp.concatenate([v.reshape(-1) for v in sums])
    total = jnp.pad(flat, (0, round_up(flat.shape[0], 1024) - flat.shape[0])).reshape(-1, 128)
    if paired:
        total = total + swap(total, "fx")
        total = total + swap(total, "fy")
        stride = 1
        while stride < slots:
            total = total + slot_swap(total, stride, slots)
            stride *= 2
    else:
        total = lax.psum(total, ("slot",) + FSDP)
    total = total.reshape(-1)
    parts_of, at = [], 0
    for v in sums:
        parts_of.append(total[at : at + v.size].reshape(v.shape))
        at += v.size
    rows_total, bias_total = parts_of[:2]
    bias_grad = lax.dynamic_index_in_dim(bias_total, slot, 0, keepdims=False)
    unit_grad = jnp.concatenate(
        [
            lax.dynamic_index_in_dim(jnp.stack(parts_of[2 : 2 + slots]), slot, 0, keepdims=False),
            lax.dynamic_slice_in_dim(parts_of[2 + slots], slot * rest, rest),
        ]
    )
    return (
        output,
        input_grad.astype(F32),
        rows_total[:2],
        rows_total[2:],
        in_grad,
        bias_grad,
        out_grad,
        up_grad,
        unit_grad,
        down_grad,
    )


def solution(mesh):
    fsdp, tensor = mesh.shape["fsdp"], mesh.shape["tensor"]

    def layer(*arrays):
        local = arrays[0].shape[0] // fsdp
        slots = local * IMG_MB
        assert local == 2 and slots == 4 and tensor % slots == 0 and fsdp % 2 == 0
        grid = Mesh(
            mesh.devices.reshape(fsdp // 2, 2, slots, tensor // slots), ("fy", "fx", "slot", "part")
        )
        tens = ("slot", "part")
        return jax.shard_map(
            on_device,
            mesh=grid,
            in_specs=(
                P(FSDP, tens, None),
                P(FSDP, None),
                P(),
                P(),
                P(None, FSDP, tens),
                P(None, tens),
                P(tens, FSDP),
                P(FSDP, tens),
                P(tens),
                P(tens, FSDP),
                P(FSDP, tens, None),
            ),
            out_specs=(
                P(FSDP, tens, None),
                P(FSDP, tens, None),
                P(),
                P(),
                P(None, FSDP, tens),
                P(None, tens),
                P(tens, FSDP),
                P(FSDP, tens),
                P(tens),
                P(tens, FSDP),
            ),
            check_vma=False,
        )(*arrays)

    return layer
```

```python
import functools
import math

import jax
import jax.numpy as jnp
from jax import lax
from jax.experimental import pallas as pl
from jax.experimental.pallas import tpu as pltpu
from jax.sharding import Mesh
from jax.sharding import PartitionSpec as P

DH = 72
IMG = 729
IMG_MB = 2
EPS = 1e-06
GELU_C = 0.7978845608028654
F32 = jnp.float32
BF16 = jnp.bfloat16
FSDP = ("fy", "fx")
SCALE = DH ** (-0.5)
LOG2E = math.log2(math.e)


def norm_forward(values, norm_gain, norm_shift):
    center = values - jnp.mean(values, axis=-1, keepdims=True)
    factor = lax.rsqrt(jnp.mean(center * center, axis=-1, keepdims=True) + EPS)
    scaled = center * factor
    return (scaled * norm_gain + norm_shift, scaled, factor)


def norm_backward(upstream, scaled, factor, norm_gain):
    inside = upstream * norm_gain
    return factor * (
        inside
        - jnp.mean(inside, axis=-1, keepdims=True)
        - scaled * jnp.mean(inside * scaled, axis=-1, keepdims=True)
    )


def gelu(pre_act):
    return (
        0.5
        * pre_act
        * (1.0 + jnp.tanh(GELU_C * (pre_act + 0.044715 * pre_act * pre_act * pre_act)))
    )


def gelu_back(pre_act, upstream):
    return jax.vjp(gelu, pre_act)[1](upstream)[0]


def dot_nn(left, right):
    return lax.dot_general(left, right, (((1,), (0,)), ((), ())), preferred_element_type=F32)


def dot_nt(left, right):
    return lax.dot_general(left, right, (((1,), (1,)), ((), ())), preferred_element_type=F32)


def dot_tn(left, right):
    return lax.dot_general(left, right, (((0,), (0,)), ((), ())), preferred_element_type=F32)


def sum_products(lefts, rights):
    total = dot_nt(lefts[0], rights[0])
    for left, right in zip(lefts[1:], rights[1:]):
        total = total + dot_nt(left, right)
    return total


def round_up(value, unit):
    return -(-value // unit) * unit


def swap(value, axis):
    return lax.ppermute(value, axis, [(0, 1), (1, 0)])


def slot_swap(value, stride, slots):
    return lax.ppermute(value, "slot", [(s, s ^ stride) for s in range(slots)])


def part_sum(value, parts):
    value = value.astype(BF16)
    if parts == 2:
        return value.astype(F32) + swap(value, "part").astype(F32)
    return lax.psum(value.astype(F32), "part")


def part_gather(value, parts):
    if parts == 2:
        other = swap(value, "part")
        first = lax.axis_index("part") == 0
        return jnp.stack([jnp.where(first, value, other), jnp.where(first, other, value)])
    return lax.all_gather(value, "part", axis=0)


def add_half(left, right):
    return (left.astype(F32) + right.astype(F32)).astype(BF16)


MESH = pl.DeviceIdType.MESH


class Place:
    def __init__(self):
        self.y, self.x = lax.axis_index("fy"), lax.axis_index("fx")
        self.z = lax.axis_index("slot")
        self.f = 2 * self.y + self.x
        self.across_x, self.across_y = {"fx": 1 - self.x}, {"fy": 1 - self.y}
        self.c = lax.axis_index("part")
        self.above = {"slot": jnp.minimum(self.z + 1, 3)}
        self.below = {"slot": jnp.maximum(self.z - 1, 0)}
        self.batch, self.image = self.z % 2, self.z // 2
        self.mate = {"part": 1 - self.c}
        self.pair = {"slot": self.z + 1 - 2 * self.batch}
        self.cross = {"slot": self.z + 2 - 4 * self.image}

    def slot_after(self, d):
        return {"slot": (self.z + d) % 4}

    def barrier(self):
        sem = pltpu.get_barrier_semaphore()
        others = [self.across_x, self.across_y, self.mate] + [self.slot_after(d) for d in (1, 2, 3)]
        for device in others:
            pl.semaphore_signal(sem, inc=1, device_id=device, device_id_type=MESH)
        pl.semaphore_wait(sem, len(others))

    def far_first(self, i):
        low = self.z < 2
        near = jnp.where(low, self.z, 3 - self.z)
        at = jnp.where(i == 0, 3, jnp.where(i == 1, 2, jnp.where(i == 2, 1 - near, near)))
        return jnp.where(low, at, 3 - at)


def send(src, dst, send_sem, recv_sem, device):
    return pltpu.make_async_remote_copy(
        src_ref=src, dst_ref=dst, send_sem=send_sem, recv_sem=recv_sem, device_id=device, device_id_type=MESH
    )


class Gather:
    SEMS = 11

    def __init__(self, place, shards, w, sems, local_sem, rows):
        self.p, self.shards, self.w, self.rows = place, shards, w, rows
        (self.zr, self.zu, self.zd, self.xr, self.xs, self.yr, self.ys, self.ar, self.asn, self.br, self.bs) = sems
        self.local_sem = local_sem

    def block(self, k, slot, owner, half=None):
        at, count = owner * self.rows, self.rows
        if half is not None:
            count = count // 2
            at = at + half * count
        return self.w[k].at[slot, pl.ds(pl.multiple_of(at, 16), count), :]

    def mine(self, k, slot, shard):
        return self.shards[k] if shard else self.block(k, slot, self.p.f)

    def up(self, k, slot, shard=False):
        dst = self.block(k, slot, self.p.f)
        return send(self.mine(k, slot, shard), dst, self.zu.at[k, slot], self.zr.at[k, slot], self.p.above)

    def down(self, k, slot, shard=False):
        dst = self.block(k, slot, self.p.f)
        return send(self.mine(k, slot, shard), dst, self.zd.at[k, slot], self.zr.at[k, slot], self.p.below)

    def to_x(self, k, slot, shard=False):
        dst = self.block(k, slot, self.p.f)
        return send(self.mine(k, slot, shard), dst, self.xs.at[k, slot], self.xr.at[k, slot], self.p.across_x)

    def to_y(self, k, slot, shard=False):
        dst = self.block(k, slot, self.p.f)
        return send(self.mine(k, slot, shard), dst, self.ys.at[k, slot], self.yr.at[k, slot], self.p.across_y)

    def from_x(self, k, slot):
        ref = self.block(k, slot, self.p.f ^ 1)
        return send(ref, ref, self.xs.at[k, slot], self.xr.at[k, slot], self.p.across_x)

    def from_y(self, k, slot):
        ref = self.block(k, slot, self.p.f ^ 2)
        return send(ref, ref, self.ys.at[k, slot], self.yr.at[k, slot], self.p.across_y)

    def corner_y(self, k, slot):
        ref = self.block(k, slot, self.p.f ^ 1, 0)
        return send(ref, ref, self.asn.at[k, slot], self.ar.at[k, slot], self.p.across_y)

    def corner_x(self, k, slot):
        ref = self.block(k, slot, self.p.f ^ 2, 1)
        return send(ref, ref, self.bs.at[k, slot], self.br.at[k, slot], self.p.across_x)

    def wait_corner(self, k, slot):
        ref = self.block(k, slot, self.p.f ^ 3, 0)
        send(ref, ref, self.asn.at[k, slot], self.ar.at[k, slot], self.p.across_y).wait_recv()
        ref = self.block(k, slot, self.p.f ^ 3, 1)
        send(ref, ref, self.bs.at[k, slot], self.br.at[k, slot], self.p.across_x).wait_recv()

    def local(self, k):
        return pltpu.make_async_copy(self.shards[k], self.block(k, self.p.z, self.p.f), self.local_sem.at[k])

    def start_z(self, k):
        @pl.when(self.p.z < 3)
        def _():
            self.up(k, self.p.z, True).start()

        @pl.when(self.p.z > 0)
        def _():
            self.down(k, self.p.z, True).start()

    def start_xy(self, k):
        self.to_x(k, self.p.z, True).start()
        self.to_y(k, self.p.z, True).start()
        self.local(k).start()

    def pass_on(self, k, d):
        z = self.p.z

        @pl.when(z >= d)
        def _():
            self.up(k, z - d).wait_recv()

            @pl.when(z < 3)
            def _():
                self.up(k, z - d).start()

            self.to_x(k, z - d).start()
            self.to_y(k, z - d).start()

        @pl.when(z + d <= 3)
        def _():
            self.down(k, z + d).wait_recv()

            @pl.when(z > 0)
            def _():
                self.down(k, z + d).start()

            self.to_x(k, z + d).start()
            self.to_y(k, z + d).start()

    def corner(self, k, d):
        def one(slot):
            self.from_x(k, slot).wait_recv()
            self.corner_y(k, slot).start()
            self.from_y(k, slot).wait_recv()
            self.corner_x(k, slot).start()

        z = self.p.z
        if d == 0:
            one(z)
        else:
            pl.when(z >= d)(lambda: one(z - d))
            pl.when(z + d <= 3)(lambda: one(z + d))

    def arrive(self, k):
        self.local(k).wait()
        for slot in range(4):
            self.wait_corner(k, slot)

    def drain(self, k):
        z = self.p.z
        for slot in range(4):
            self.to_x(k, slot).wait_send()
            self.to_y(k, slot).wait_send()
            self.corner_y(k, slot).wait_send()
            self.corner_x(k, slot).wait_send()

            @pl.when((z < 3) & (slot <= z))
            def _(slot=slot):
                self.up(k, slot).wait_send()

            @pl.when((z > 0) & (slot >= z))
            def _(slot=slot):
                self.down(k, slot).wait_send()


def gather_weights(shards):
    slots = lax.axis_size("slot")
    whole = [lax.all_gather(s, ("slot",) + FSDP, axis=0) for s in shards]
    return [w.reshape(slots, -1, w.shape[-1]) for w in whole]


class Rows:
    SEMS = 11

    def __init__(self, place, index, src, dst, sems, rows_each, edge, tail):
        self.p, self.src, self.dst, self.each = place, src, dst, rows_each
        self.half = 4 * rows_each
        self.edge, self.tail = edge, tail
        self.sems = [sem.at[index] for sem in sems]

    def at(self, row, count):
        return self.dst.at[pl.ds(pl.multiple_of(row, 16), count), :]

    def block(self, near, core):
        batch = self.p.batch if near else 1 - self.p.batch
        return self.at((2 * batch + core) * self.each, self.each)

    def own(self):
        return pltpu.make_async_copy(self.src.at[self.p.batch], self.block(True, self.p.c), self.sems[0])

    def to_mate(self):
        return send(self.src.at[self.p.batch], self.block(True, self.p.c), self.sems[1], self.sems[2], self.p.mate)

    def to_pair(self):
        return send(self.src.at[1 - self.p.batch], self.block(True, self.p.c), self.sems[3], self.sems[4], self.p.pair)

    def pass_on(self):
        ref = self.block(False, self.p.c)
        return send(ref, ref, self.sems[5], self.sems[6], self.p.mate)

    def edge_out(self):
        src = self.at(jnp.where(self.p.image == 0, self.half - self.edge, 0), self.edge)
        return send(src, self.at(self.half, self.edge), self.sems[7], self.sems[8], self.p.cross)

    def tail_out(self):
        src = self.at(self.half - self.tail, self.tail)
        dst = self.at(self.half + self.edge, self.tail)
        return send(src, dst, self.sems[7], self.sems[8], self.p.cross)

    def edge_mate(self):
        ref = self.at(self.half, self.edge)
        return send(ref, ref, self.sems[9], self.sems[10], self.p.mate)

    def tail_mate(self):
        ref = self.at(self.half + self.edge, self.tail)
        return send(ref, ref, self.sems[9], self.sems[10], self.p.mate)

    def start(self):
        self.to_pair().start()
        self.to_mate().start()
        self.own().start()

    def forward(self):
        ref = self.block(False, self.p.c)
        send(ref, ref, self.sems[3], self.sems[4], self.p.pair).wait_recv()
        self.pass_on().start()

    def main_ready(self):
        self.own().wait()
        ref = self.block(True, 1 - self.p.c)
        send(ref, ref, self.sems[1], self.sems[2], self.p.mate).wait_recv()
        ref = self.block(False, 1 - self.p.c)
        send(ref, ref, self.sems[5], self.sems[6], self.p.mate).wait_recv()

    def edges(self):
        pl.when(self.p.c == 0)(lambda: self.edge_out().start())
        pl.when(self.p.c == 1)(lambda: self.tail_out().start())

    def edges_forward(self):
        @pl.when(self.p.c == 0)
        def _():
            self.edge_out().wait_recv()
            self.edge_mate().start()

        @pl.when(self.p.c == 1)
        def _():
            self.tail_out().wait_recv()
            self.tail_mate().start()

    def edges_ready(self):
        pl.when(self.p.c == 0)(lambda: self.tail_mate().wait_recv())
        pl.when(self.p.c == 1)(lambda: self.edge_mate().wait_recv())

    def drain(self):
        self.to_mate().wait_send()
        self.to_pair().wait_send()
        self.pass_on().wait_send()

        @pl.when(self.p.c == 0)
        def _():
            self.edge_out().wait_send()
            self.edge_mate().wait_send()

        @pl.when(self.p.c == 1)
        def _():
            self.tail_out().wait_send()
            self.tail_mate().wait_send()


def row_tiles(rows, step, body):
    def one(t, carry):
        body(pl.ds(pl.multiple_of(t * step, 16), step))
        return carry

    lax.fori_loop(0, rows // step, one, 0)


def forward_kernel(*refs, cols, edge, tail, tile):
    (small_ref, up_ref, down_ref, vec_ref, x_src, c_src, gain_ref, shift_ref, segc_ref, segr_ref) = refs[:10]
    (ws, wu, wd, x_ref, c_ref, vec_all, first_ref, qkv_ref, ctx_ref, inv_ref, res_ref, second_ref) = refs[10:22]
    (blocks, part, part_out, part_in) = refs[22:26]
    gather_sems, local_sem = refs[26 : 26 + Gather.SEMS], refs[26 + Gather.SEMS]
    rest = refs[27 + Gather.SEMS :]
    row_sems, (vec_s, vec_r, load_sem, part_s, part_r) = rest[: Rows.SEMS], rest[Rows.SEMS :]
    rows, width = x_ref.shape
    place = Place()
    place.barrier()
    shards = (small_ref, up_ref, down_ref)
    g = Gather(place, shards, (ws, wu, wd), gather_sems, local_sem, small_ref.shape[0])
    each = x_src.shape[1]
    x_rows = Rows(place, 0, x_src, x_ref, row_sems, each, edge, tail)
    c_rows = Rows(place, 1, c_src, c_ref, row_sems, each, edge, tail)

    def vec_to(d):
        device = place.slot_after(d)
        return send(vec_ref, vec_all.at[place.z], vec_s.at[d], vec_r.at[d], device)

    def vec_from(d):
        ref = vec_all.at[(place.z + 4 - d) % 4]
        return send(ref, ref, vec_s.at[d], vec_r.at[d], place.slot_after(d))

    g.start_z(0)
    g.start_xy(0)
    for d in (1, 2, 3):
        vec_to(d).start()
    x_rows.start()
    vec_all[place.z] = vec_ref[...]
    g.pass_on(0, 1)
    g.corner(0, 0)
    x_rows.forward()
    g.pass_on(0, 2)
    x_rows.main_ready()
    x_rows.edges()
    g.corner(0, 1)
    x_rows.edges_forward()
    g.pass_on(0, 3)
    g.start_z(1)
    x_rows.edges_ready()

    def first(span):
        value = x_ref[span, :].astype(F32)
        out, _, _ = norm_forward(value, gain_ref[0:1, :], shift_ref[0:1, :])
        first_ref[span, :] = out.astype(BF16)

    row_tiles(rows, 128, first)
    g.corner(0, 2)
    g.corner(0, 3)
    for d in (1, 2, 3):
        vec_from(d).wait_recv()
    g.arrive(0)

    later = []
    for k in (1, 2):
        later.append(lambda k=k: g.start_xy(k))
        if k == 1:
            later.append(lambda: c_rows.start())
        for d in (1, 2, 3):
            later.append(lambda k=k, d=d: g.pass_on(k, d))
            later.append(lambda k=k, d=d: g.corner(k, d - 1))
        if k == 1:
            later.append(lambda: g.start_z(2))
            later.append(lambda: c_rows.forward())
            later.append(lambda: (c_rows.main_ready(), c_rows.edges()))
        later.append(lambda k=k: g.corner(k, 3))
        if k == 1:
            later.append(lambda: c_rows.edges_forward())

    def step(count=1):
        for _ in range(count):
            if later:
                later.pop(0)()

    step(2)

    def load(s):
        return pltpu.make_async_copy(ws.at[s], blocks.at[s % 2], load_sem.at[s % 2])

    heads = cols // DH
    load(0).start()
    for s in range(4):
        load(s).wait()
        if s < 3:
            load(s + 1).start()
        w = blocks.at[s % 2]
        bias = vec_all[s, 0:1, : 3 * cols].astype(F32) + vec_all[s, 1:2, : 3 * cols].astype(F32)
        projected = dot_nn(first_ref[...], w[:, : 3 * cols]) + bias
        qkv_ref[s] = projected.astype(BF16)
        step()
        for head in range(heads):
            attend_head(qkv_ref, ctx_ref, inv_ref, segc_ref, segr_ref, s, head, cols, tile)
            step()
        product = dot_nt(ctx_ref[s], w[:, 3 * cols : 4 * cols])
        if s == 0:
            part[...] = product
        else:
            part[...] += product

    def halves(h):
        return pl.ds(h * (rows // 2), rows // 2)

    def exchange(h):
        src, dst = part_out.at[halves(h), :], part_in.at[halves(h), :]
        return send(src, dst, part_s.at[h], part_r.at[h], place.mate)

    for h in (0, 1):
        part_out[halves(h), :] = part[halves(h), :].astype(BF16)
        exchange(h).start()
    step()
    for h in (0, 1):
        exchange(h).wait_recv()

    def second(span):
        value = x_ref[span, :].astype(F32) + (part_out[span, :].astype(F32) + part_in[span, :].astype(F32))
        value = value + shift_ref[2:3, :]
        res_ref[span, :] = value
        out, _, _ = norm_forward(value, gain_ref[1:2, :], shift_ref[1:2, :])
        second_ref[span, :] = out.astype(BF16)

    row_tiles(rows, 128, second)
    step(len(later))
    for k in (1, 2):
        g.arrive(k)
    c_rows.edges_ready()
    for k in (0, 1, 2):
        g.drain(k)
    x_rows.drain()
    c_rows.drain()
    for d in (1, 2, 3):
        vec_to(d).wait_send()
    for h in (0, 1):
        exchange(h).wait_send()


def forward_stage(small, up, down, vectors, x_src, c_src, gains, shifts, segments, cols, rows, edge, tail):
    width, shard_rows = x_src.shape[2], small.shape[0]
    heads = cols // DH
    vmem = pl.BlockSpec(memory_space=pltpu.VMEM)
    far = pl.BlockSpec(memory_space=pl.ANY)
    shape = jax.ShapeDtypeStruct
    dma = pltpu.SemaphoreType.DMA
    return pl.pallas_call(
        functools.partial(forward_kernel, cols=cols, edge=edge, tail=tail, tile=rows // 2),
        in_specs=[vmem] * 10,
        out_specs=[far] * 3 + [vmem, far] + [vmem] * 7,
        out_shape=[
            shape((4, 4 * shard_rows, small.shape[1]), BF16),
            shape((4, 4 * shard_rows, up.shape[1]), BF16),
            shape((4, 4 * shard_rows, down.shape[1]), BF16),
            shape((rows, width), BF16),
            shape((rows, width), BF16),
            shape((4,) + vectors.shape, BF16),
            shape((rows, width), BF16),
            shape((4, rows, 3 * cols), BF16),
            shape((4, rows, cols), BF16),
            shape((4, rows, heads), F32),
            shape((rows, width), F32),
            shape((rows, width), BF16),
        ],
        scratch_shapes=[
            pltpu.VMEM((2, width, small.shape[1]), BF16),
            pltpu.VMEM((rows, width), F32),
            pltpu.VMEM((rows, width), BF16),
            pltpu.VMEM((rows, width), BF16),
        ]
        + [dma((3, 4))] * Gather.SEMS
        + [dma((3,))]
        + [dma((2,))] * Rows.SEMS
        + [dma((4,)), dma((4,)), dma((2,)), dma((2,)), dma((2,))],
        compiler_params=pltpu.CompilerParams(collective_id=1, has_side_effects=True, vmem_limit_bytes=64000000),
        name="forward",
    )(small, up, down, vectors, x_src, c_src, gains, shifts, segments[:, None], segments[None, :])


class Reduce:
    SEMS = 16

    def __init__(self, place, g, out, bufs, sems, rows):
        self.p, self.g, self.out, self.rows = place, g, out, rows
        self.bufs, self.sems = bufs, sems

    def grad(self, k, slot, owner, half=None):
        at, count = owner * self.rows, self.rows
        if half is not None:
            count = count // 2
            at = at + half * count
        return self.g[k].at[slot, pl.ds(pl.multiple_of(at, 16), count), :]

    def half(self, ref, slot, half):
        count = self.rows // 2
        return ref.at[slot, half * count : (half + 1) * count, :]

    def copy(self, k, slot, src, dst, index, device):
        return send(src, dst, self.sems[2 * index].at[k, slot], self.sems[2 * index + 1].at[k, slot], device)

    def corner_y(self, k, s):
        return self.copy(k, s, self.grad(k, s, self.p.f ^ 3, 0), self.bufs[k][0].at[s], 0, self.p.across_y)

    def corner_x(self, k, s):
        return self.copy(k, s, self.grad(k, s, self.p.f ^ 3, 1), self.bufs[k][1].at[s], 1, self.p.across_x)

    def x_low(self, k, s):
        return self.copy(k, s, self.bufs[k][0].at[s], self.half(self.bufs[k][2], s, 0), 2, self.p.across_x)

    def x_high(self, k, s):
        dst = self.half(self.bufs[k][2], s, 1)
        return self.copy(k, s, self.grad(k, s, self.p.f ^ 1, 1), dst, 3, self.p.across_x)

    def y_low(self, k, s):
        dst = self.half(self.bufs[k][3], s, 0)
        return self.copy(k, s, self.grad(k, s, self.p.f ^ 2, 0), dst, 4, self.p.across_y)

    def y_high(self, k, s):
        return self.copy(k, s, self.bufs[k][1].at[s], self.half(self.bufs[k][3], s, 1), 5, self.p.across_y)

    def up(self, k, s):
        return self.copy(k, s, self.bufs[k][2].at[s], self.bufs[k][4].at[s], 6, self.p.above)

    def down(self, k, s):
        return self.copy(k, s, self.bufs[k][2].at[s], self.bufs[k][5].at[s], 7, self.p.below)

    def start(self, k):
        def one(i, carry):
            s = self.p.far_first(i)
            self.corner_y(k, s).start()
            self.corner_x(k, s).start()
            self.y_low(k, s).start()
            self.x_high(k, s).start()
            return carry

        lax.fori_loop(0, 4, one, 0)

    def tiles(self, rows, body):
        step = 48 if rows % 48 == 0 else 16

        def one(t, carry):
            body(pl.ds(pl.multiple_of(t * step, 16), step))
            return carry

        lax.fori_loop(0, rows // step, one, 0)

    def middle(self, k):
        count = self.rows // 2

        def one(i, carry):
            s = self.p.far_first(i)
            low, high = self.bufs[k][0], self.bufs[k][1]
            self.corner_y(k, s).wait_recv()
            own = self.grad(k, s, self.p.f ^ 1, 0)

            def add_low(span):
                low[s, span, :] = add_half(low[s, span, :], own[span, :])

            self.tiles(count, add_low)
            self.x_low(k, s).start()
            self.corner_x(k, s).wait_recv()
            other = self.grad(k, s, self.p.f ^ 2, 1)

            def add_high(span):
                high[s, span, :] = add_half(high[s, span, :], other[span, :])

            self.tiles(count, add_high)
            self.y_high(k, s).start()
            return carry

        lax.fori_loop(0, 4, one, 0)

    def line(self, k):
        z, acc, side = self.p.z, self.bufs[k][2], self.bufs[k][3]
        lower, upper = self.bufs[k][4], self.bufs[k][5]

        def one(i, carry):
            s = self.p.far_first(i)
            self.x_low(k, s).wait_recv()
            self.x_high(k, s).wait_recv()
            self.y_low(k, s).wait_recv()
            self.y_high(k, s).wait_recv()
            own = self.grad(k, s, self.p.f)

            def add(span):
                total = own[span, :].astype(F32) + acc[s, span, :].astype(F32) + side[s, span, :].astype(F32)
                acc[s, span, :] = total.astype(BF16)

            def add_from(ref):
                def body(span):
                    acc[s, span, :] = add_half(acc[s, span, :], ref[s, span, :])

                return body

            self.tiles(self.rows, add)

            @pl.when((z > 0) & (s >= z))
            def _():
                self.up(k, s).wait_recv()
                self.tiles(self.rows, add_from(lower))

            @pl.when((z < 3) & (s <= z))
            def _():
                self.down(k, s).wait_recv()
                self.tiles(self.rows, add_from(upper))

            @pl.when(s > z)
            def _():
                self.up(k, s).start()

            @pl.when(s < z)
            def _():
                self.down(k, s).start()

            @pl.when(s == z)
            def _():
                def final(span):
                    self.out[k][span, :] = acc[s, span, :].astype(F32)

                self.tiles(self.rows, final)

            return carry

        lax.fori_loop(0, 4, one, 0)

    def drain(self, k):
        def one(s, carry):
            for copy in (self.corner_y, self.corner_x, self.x_low, self.x_high, self.y_low, self.y_high):
                copy(k, s).wait_send()

            @pl.when(s > self.p.z)
            def _():
                self.up(k, s).wait_send()

            @pl.when(s < self.p.z)
            def _():
                self.down(k, s).wait_send()

            return carry

        lax.fori_loop(0, 4, one, 0)


def reduce_buffers(rows, lanes):
    return [
        pltpu.VMEM((4, rows // 2, lanes), BF16),
        pltpu.VMEM((4, rows // 2, lanes), BF16),
        pltpu.VMEM((4, rows, lanes), BF16),
        pltpu.VMEM((4, rows, lanes), BF16),
        pltpu.VMEM((4, rows, lanes), BF16),
        pltpu.VMEM((4, rows, lanes), BF16),
    ]


def reduce_kernel(*refs, count, rows):
    g, out = refs[:count], refs[count : 2 * count]
    bufs = [refs[2 * count + 6 * k : 2 * count + 6 * k + 6] for k in range(count)]
    sems = refs[8 * count :]
    place = Place()
    place.barrier()
    r = Reduce(place, g, out, bufs, sems, rows)
    r.start(0)
    for k in range(count):
        r.middle(k)
        if k + 1 < count:
            r.start(k + 1)
        r.line(k)
    for k in range(count):
        r.drain(k)


def scatter_grads(chunks, paired):
    if not paired:
        count = lax.axis_size("fy") * lax.axis_size("fx")
        split = [c.reshape(c.shape[0] * count, c.shape[1] // count, c.shape[2]) for c in chunks]
        return [lax.psum_scatter(c, ("slot",) + FSDP, scatter_dimension=0).astype(F32) for c in split]
    count, rows = len(chunks), chunks[0].shape[1] // 4
    scratch = [b for c in chunks for b in reduce_buffers(rows, c.shape[2])]
    return pl.pallas_call(
        functools.partial(reduce_kernel, count=count, rows=rows),
        in_specs=[pl.BlockSpec(memory_space=pltpu.VMEM)] * count,
        out_specs=[pl.BlockSpec(memory_space=pltpu.VMEM)] * count,
        out_shape=[jax.ShapeDtypeStruct((rows, c.shape[2]), F32) for c in chunks],
        scratch_shapes=scratch + [pltpu.SemaphoreType.DMA((count, 4))] * Reduce.SEMS,
        compiler_params=pltpu.CompilerParams(
            collective_id=2, has_side_effects=True, vmem_limit_bytes=64000000
        ),
        name="reduce",
    )(*chunks)


def attend_head(qkv_ref, ctx_ref, inv_ref, segc_ref, segr_ref, s, head, cols, tile):
    lo = head * DH
    keys = qkv_ref[s, :, cols + lo : cols + lo + DH]
    values = qkv_ref[s, :, 2 * cols + lo : 2 * cols + lo + DH]

    def one_tile(t, carry):
        span = pl.ds(pl.multiple_of(t * tile, tile), tile)
        scores = dot_nt(qkv_ref[s, span, lo : lo + DH], keys)
        allowed = segc_ref[span, :] == segr_ref[...]
        exact = jnp.where(allowed, jnp.exp2(scores * (SCALE * LOG2E)), 0.0)
        inverse = 1.0 / jnp.sum(exact, axis=1, keepdims=True)
        context = dot_nn(exact.astype(BF16), values) * inverse
        ctx_ref[s, span, lo : lo + DH] = context.astype(BF16)
        inv_ref[s, span, head : head + 1] = inverse
        return carry

    lax.fori_loop(0, qkv_ref.shape[1] // tile, one_tile, 0)


def attend_kernel(x_ref, w_ref, b_ref, segc_ref, segr_ref, qkv_ref, ctx_ref, inv_ref, part_ref, *, cols, tile):
    block = pl.program_id(0)
    projected = dot_nn(x_ref[...], w_ref[0, :, : 3 * cols]) + b_ref[0]
    qkv_ref[0] = projected.astype(BF16)
    for head in range(cols // DH):
        attend_head(qkv_ref, ctx_ref, inv_ref, segc_ref, segr_ref, 0, head, cols, tile)
    part = dot_nt(ctx_ref[0], w_ref[0, :, 3 * cols : 4 * cols])

    @pl.when(block == 0)
    def _():
        part_ref[...] = part

    @pl.when(block > 0)
    def _():
        part_ref[...] += part


def attend(first_norm, weights, bias, segments, cols, tile):
    rows, width = first_norm.shape
    slots, _, lanes = weights.shape
    heads = cols // DH
    whole = lambda shape: pl.BlockSpec(shape, lambda s: (0,) * len(shape))
    each = lambda shape: pl.BlockSpec((1,) + shape, lambda s: (s, 0, 0))
    return pl.pallas_call(
        functools.partial(attend_kernel, cols=cols, tile=tile),
        grid=(slots,),
        in_specs=[
            whole((rows, width)),
            each((width, lanes)),
            each((1, 3 * cols)),
            whole((rows, 1)),
            whole((1, rows)),
        ],
        out_specs=[each((rows, 3 * cols)), each((rows, cols)), each((rows, heads)), whole((rows, width))],
        out_shape=[
            jax.ShapeDtypeStruct((slots, rows, 3 * cols), BF16),
            jax.ShapeDtypeStruct((slots, rows, cols), BF16),
            jax.ShapeDtypeStruct((slots, rows, heads), F32),
            jax.ShapeDtypeStruct((rows, width), F32),
        ],
        cost_estimate=pl.CostEstimate(
            flops=slots * (8 * rows * width * cols + 4 * rows * rows * 256 * heads),
            bytes_accessed=slots * width * lanes * 2 + rows * width * 10,
            transcendentals=slots * heads * rows * rows,
        ),
        name="attend",
    )(first_norm, weights, bias, segments[:, None], segments[None, :])


def attend_back_kernel(
    r_ref, w_ref, qkv_ref, ctx_ref, inv_ref, segc_ref, segr_ref, grad_ref, bias_ref, back_ref, key_acc, value_acc, *, cols, tile
):
    rows = r_ref.shape[0]
    heads = cols // DH
    back_ref[...] = dot_nn(r_ref[...], w_ref[0, :, 3 * cols : 4 * cols]).astype(BF16)
    ones = jnp.ones((8, DH), F32)
    for head in range(heads):
        lo = head * DH
        keys = qkv_ref[0, :, cols + lo : cols + lo + DH]
        values = qkv_ref[0, :, 2 * cols + lo : 2 * cols + lo + DH]
        key_acc[...] = jnp.zeros_like(key_acc)
        value_acc[...] = jnp.zeros_like(value_acc)

        def one_tile(t, query_total):
            span = slice(t * tile, (t + 1) * tile)
            queries = qkv_ref[0, span, lo : lo + DH]
            back = (back_ref[span, lo : lo + DH].astype(F32) * inv_ref[0, span, head : head + 1]).astype(BF16)
            along = back.astype(F32) * ctx_ref[0, span, lo : lo + DH].astype(F32)
            delta = lax.dot_general(
                ones, along, (((1,), (1,)), ((), ())), precision=lax.Precision.HIGHEST, preferred_element_type=F32
            )[:1]
            scores = dot_nt(keys, queries)
            allowed = segc_ref[...] == segr_ref[:, span]
            exact = jnp.where(allowed, jnp.exp2(scores * (SCALE * LOG2E)), 0.0)
            value_acc[...] += dot_nn(exact.astype(BF16), back)
            prob_grad = dot_nt(values, back)
            score_grad = (exact * (prob_grad - delta)).astype(BF16)
            key_acc[...] += dot_nn(score_grad, queries)
            query_grad = dot_tn(score_grad, keys) * SCALE
            grad_ref[0, span, lo : lo + DH] = query_grad.astype(BF16)
            return query_total + jnp.sum(query_grad, axis=0, keepdims=True)

        tiles = rows // tile
        query_total = jnp.zeros((1, DH), F32)
        for t in range(tiles):
            query_total = one_tile(t, query_total)
        grad_ref[0, :, cols + lo : cols + lo + DH] = (key_acc[...] * SCALE).astype(BF16)
        grad_ref[0, :, 2 * cols + lo : 2 * cols + lo + DH] = value_acc[...].astype(BF16)
        bias_ref[0, 0:1, lo : lo + DH] = query_total
        bias_ref[0, 1:2, lo : lo + DH] = jnp.sum(value_acc[...], axis=0, keepdims=True)


def attend_back(residual_half, weights, qkv, context, inverse, segments, cols, tile):
    rows, width = residual_half.shape
    slots, _, lanes = weights.shape
    heads = cols // DH
    whole = lambda shape: pl.BlockSpec(shape, lambda s: (0,) * len(shape))
    each = lambda shape: pl.BlockSpec((1,) + shape, lambda s: (s, 0, 0))
    return pl.pallas_call(
        functools.partial(attend_back_kernel, cols=cols, tile=tile),
        grid=(slots,),
        in_specs=[
            whole((rows, width)),
            each((width, lanes)),
            each((rows, 3 * cols)),
            each((rows, cols)),
            each((rows, heads)),
            whole((rows, 1)),
            whole((1, rows)),
        ],
        out_specs=[each((rows, 3 * cols)), each((2, cols))],
        out_shape=[
            jax.ShapeDtypeStruct((slots, rows, 3 * cols), BF16),
            jax.ShapeDtypeStruct((slots, 2, cols), F32),
        ],
        scratch_shapes=[
            pltpu.VMEM((rows, cols), BF16),
            pltpu.VMEM((rows, DH), F32),
            pltpu.VMEM((rows, DH), F32),
        ],
        cost_estimate=pl.CostEstimate(
            flops=slots * (2 * rows * width * cols + 10 * rows * rows * 256 * heads),
            bytes_accessed=slots * width * lanes * 2 + rows * width * 10,
            transcendentals=slots * heads * rows * rows,
        ),
        name="attend_back",
    )(residual_half, weights, qkv, context, inverse, segments[:, None], segments[None, :])


def on_device(
    block_input,
    segment_ids,
    norm_gains,
    row_biases,
    in_projection,
    query_value_bias,
    out_projection,
    up_weight,
    unit_bias,
    down_weight,
    cotangent,
):
    local, rows_each, width = block_input.shape
    rows_mb = segment_ids.shape[1]
    cols = in_projection.shape[2]
    units = up_weight.shape[1]
    shard_rows = up_weight.shape[0]
    slots, parts = lax.axis_size("slot"), lax.axis_size("part")
    slot, part = lax.axis_index("slot"), lax.axis_index("part")
    fsdp_index = lax.axis_index("fy") * lax.axis_size("fx") + lax.axis_index("fx")
    batch, image = slot % local, slot // local
    late = image == 1

    half_rows = rows_mb // IMG_MB
    padding = rows_mb - IMG_MB * IMG
    edge = round_up(max(half_rows - IMG, padding - (half_rows - IMG)), 16)
    tail = round_up(padding, 16)
    rows = round_up(half_rows + edge + tail, 128)
    filler = rows - half_rows - edge - tail
    paired = lax.axis_size("fy") == 2 and lax.axis_size("fx") == 2 and slots == 4 and parts == 2
    paired = paired and shard_rows % 32 == 0 and filler == 0

    def edges(main):
        near = jnp.where(late, main[:edge], main[half_rows - edge :])
        far = main[half_rows - tail :]
        return jnp.concatenate([near, far])

    def to_slot(value):
        mine = lax.dynamic_index_in_dim(value, batch, 0, keepdims=False)
        send = lax.dynamic_index_in_dim(value, 1 - batch, 0, keepdims=False)
        other = slot_swap(send, 1, slots)
        pair = jnp.where(batch == 0, jnp.stack([mine, other]), jnp.stack([other, mine]))
        main = part_gather(pair, parts).swapaxes(0, 1).reshape(half_rows, width)
        beyond = slot_swap(edges(main), local, slots)
        return jnp.concatenate([main, beyond, jnp.zeros((filler, width), value.dtype)])

    def from_slot(value, owned):
        main = value[:half_rows]
        beyond = slot_swap(value[half_rows : half_rows + edge + tail], local, slots)
        keep = owned[:half_rows, None]
        near, far = beyond[:edge], beyond[edge:]
        blank = lambda count: jnp.zeros((count, width), value.dtype)
        early_fill = jnp.concatenate([blank(half_rows - edge), near])
        late_fill = jnp.concatenate([near, blank(half_rows - edge - tail), far])
        main = jnp.where(keep, main, jnp.where(late, late_fill, early_fill))
        main = main.reshape(local, parts, rows_each, width)
        mine = lax.dynamic_index_in_dim(main, part, 1, keepdims=False)
        stay = lax.dynamic_index_in_dim(mine, batch, 0, keepdims=False)
        other = slot_swap(lax.dynamic_index_in_dim(mine, 1 - batch, 0, keepdims=False), 1, slots)
        return jnp.where(batch == 0, jnp.stack([stay, other]), jnp.stack([other, stay]))

    ids = lax.dynamic_index_in_dim(segment_ids, batch, 0, keepdims=False)
    fill_ids = jnp.full((filler,), -2, jnp.int32)
    early_ids = jnp.concatenate([ids[: half_rows + edge], ids[rows_mb - tail :], fill_ids])
    late_ids = jnp.concatenate(
        [ids[half_rows:], ids[half_rows - edge : half_rows], jnp.full((tail,), -2, jnp.int32), fill_ids]
    )
    segments = jnp.where(late, late_ids, early_ids)
    image_id = (fsdp_index * local + batch) * IMG_MB + image
    owned = (segments == image_id) | (jnp.logical_not(late) & (segments == -1))

    main_units = units // 128 * 128
    rest = units - main_units
    in_lanes = 3 * cols
    small = in_lanes + cols + 2 * rest
    lanes = round_up(small, 128)
    down_t = down_weight.T
    small_shard = jnp.concatenate(
        [
            in_projection.transpose(1, 0, 2).reshape(shard_rows, in_lanes),
            out_projection.T,
            up_weight[:, main_units:],
            down_t[:, main_units:],
            jnp.zeros((shard_rows, lanes - small), BF16),
        ],
        axis=1,
    )
    shards = [small_shard, up_weight[:, :main_units], down_t[:, :main_units]]
    triple_bias = jnp.concatenate([query_value_bias[0], jnp.zeros((cols,), F32), query_value_bias[1]])
    high = triple_bias.astype(BF16)
    low = (triple_bias - high.astype(F32)).astype(BF16)
    wide = round_up(max(in_lanes, units), 128)
    vectors = [jnp.pad(v, (0, wide - v.shape[0])) for v in (high, low, unit_bias)]
    vectors = jnp.concatenate([jnp.stack(vectors), jnp.zeros((13, wide), BF16)])
    gains, shifts = norm_gains, row_biases
    if paired:
        (small_all, up_main, down_main, x_half, cot_half, vec_all, first_norm, qkv, context, inverse, residual, second_norm) = (
            forward_stage(
                *shards, vectors, block_input, cotangent, gains, shifts, segments, cols, rows, edge, tail
            )
        )
        x_float = x_half.astype(F32)
        first_out, first_scaled, first_factor = norm_forward(x_float, gains[0], shifts[0])
    else:
        small_all, up_main, down_main = gather_weights(shards)
        vec_all = lax.all_gather(vectors, "slot", axis=0)
        cot_half = to_slot(cotangent)
        x_float = to_slot(block_input).astype(F32)
        first_out, first_scaled, first_factor = norm_forward(x_float, gains[0], shifts[0])
        first_norm = first_out.astype(BF16)
        bias = vec_all[:, :1, :in_lanes].astype(F32) + vec_all[:, 1:2, :in_lanes].astype(F32)
        qkv, context, inverse, attention_part = attend(
            first_norm, small_all, bias, segments, cols, rows // 2
        )
        residual = x_float + part_sum(attention_part, parts) + shifts[2]
    second_out, second_scaled, second_factor = norm_forward(residual, gains[1], shifts[1])
    if not paired:
        second_norm = second_out.astype(BF16)
    grad_rows = jnp.where(owned[:, None], cot_half, 0)
    upstream = grad_rows.astype(F32)
    small_blocks, up_blocks, down_blocks = list(small_all), list(up_main), list(down_main)
    unit_all = vec_all[:, 2, :units].astype(F32)
    rest_lanes = round_up(slots * rest, 128)
    rest_pad = rest_lanes - slots * rest

    def unit_layout(blocks, at):
        extra = [b[:, at : at + rest] for b in small_blocks]
        return blocks + [jnp.concatenate(extra + [jnp.zeros((width, rest_pad), BF16)], axis=1)]

    up_all = unit_layout(up_blocks, in_lanes + cols)
    down_all = unit_layout(down_blocks, in_lanes + cols + rest)
    unit_rows = [unit_all[s, :main_units] for s in range(slots)]
    unit_rows += [jnp.concatenate([unit_all[:, main_units:].reshape(-1), jnp.zeros((rest_pad,), F32)])]
    pre_acts = [dot_nn(second_norm, w) + b for w, b in zip(up_all, unit_rows)]
    hiddens = [gelu(p).astype(BF16) for p in pre_acts]
    unit_part = sum_products(hiddens, down_all)
    unit_part = part_sum(unit_part, parts)
    output = from_slot((residual + unit_part + shifts[3]).astype(BF16), owned)

    down_sums = [dot_tn(grad_rows, h).astype(BF16) for h in hiddens]
    pre_grads = [gelu_back(p, dot_nn(grad_rows, w)) for p, w in zip(pre_acts, down_all)]
    pre_halves = [p.astype(BF16) for p in pre_grads]
    unit_sums = [jnp.sum(p, axis=0) for p in pre_grads]
    up_sums = [dot_tn(second_norm, p).astype(BF16) for p in pre_halves]
    second_grad = part_sum(sum_products(pre_halves, up_all), parts)
    residual_grad = upstream + norm_backward(second_grad, second_scaled, second_factor, gains[1])
    residual_half = residual_grad.astype(BF16)
    out_sum = [dot_tn(residual_half, context[s]).astype(BF16) for s in range(slots)]
    triple, bias_sum = attend_back(
        residual_half, small_all, qkv, context, inverse, segments, cols, rows // 2
    )
    in_sum = [dot_tn(first_norm, triple[s]).astype(BF16) for s in range(slots)]
    first_part = sum_products([triple[s] for s in range(slots)], [b[:, :in_lanes] for b in small_blocks])
    first_grad = part_sum(first_part, parts)
    input_grad = residual_grad + norm_backward(first_grad, first_scaled, first_factor, gains[0])
    input_grad = from_slot(input_grad.astype(BF16), owned)

    rest_of = lambda sums, s: sums[slots][:, s * rest : (s + 1) * rest]
    blank = jnp.zeros((width, lanes - small), BF16)
    small_sums = [
        jnp.concatenate([in_sum[s], out_sum[s], rest_of(up_sums, s), rest_of(down_sums, s), blank], axis=1)
        for s in range(slots)
    ]
    down_grad, up_grad, small_grad = scatter_grads(
        [jnp.stack(down_sums[:slots]), jnp.stack(up_sums[:slots]), jnp.stack(small_sums)], paired
    )
    in_grad = small_grad[:, :in_lanes].reshape(shard_rows, 3, cols).transpose(1, 0, 2)
    out_grad = small_grad[:, in_lanes : in_lanes + cols].T
    at = in_lanes + cols
    up_grad = jnp.concatenate([up_grad, small_grad[:, at : at + rest]], axis=1)
    down_grad = jnp.concatenate([down_grad, small_grad[:, at + rest : at + 2 * rest]], axis=1).T

    rows_sum = jnp.stack(
        [
            jnp.sum(first_grad * first_scaled, axis=0),
            jnp.sum(second_grad * second_scaled, axis=0),
            jnp.sum(first_grad, axis=0),
            jnp.sum(second_grad, axis=0),
            jnp.sum(residual_grad, axis=0),
            jnp.sum(upstream, axis=0),
        ]
    )
    sums = [rows_sum, bias_sum] + unit_sums
    flat = jnp.concatenate([v.reshape(-1) for v in sums])
    total = jnp.pad(flat, (0, round_up(flat.shape[0], 1024) - flat.shape[0])).reshape(-1, 128)
    if paired:
        total = total + swap(total, "fx")
        total = total + swap(total, "fy")
        stride = 1
        while stride < slots:
            total = total + slot_swap(total, stride, slots)
            stride *= 2
    else:
        total = lax.psum(total, ("slot",) + FSDP)
    total = total.reshape(-1)
    parts_of, at = [], 0
    for v in sums:
        parts_of.append(total[at : at + v.size].reshape(v.shape))
        at += v.size
    rows_total, bias_total = parts_of[:2]
    bias_grad = lax.dynamic_index_in_dim(bias_total, slot, 0, keepdims=False)
    unit_grad = jnp.concatenate(
        [
            lax.dynamic_index_in_dim(jnp.stack(parts_of[2 : 2 + slots]), slot, 0, keepdims=False),
            lax.dynamic_slice_in_dim(parts_of[2 + slots], slot * rest, rest),
        ]
    )
    return (
        output,
        input_grad.astype(F32),
        rows_total[:2],
        rows_total[2:],
        in_grad,
        bias_grad,
        out_grad,
        up_grad,
        unit_grad,
        down_grad,
    )


def solution(mesh):
    fsdp, tensor = mesh.shape["fsdp"], mesh.shape["tensor"]

    def layer(*arrays):
        local = arrays[0].shape[0] // fsdp
        slots = local * IMG_MB
        assert local == 2 and slots == 4 and tensor % slots == 0 and fsdp % 2 == 0
        grid = Mesh(
            mesh.devices.reshape(fsdp // 2, 2, slots, tensor // slots), ("fy", "fx", "slot", "part")
        )
        tens = ("slot", "part")
        return jax.shard_map(
            on_device,
            mesh=grid,
            in_specs=(
                P(FSDP, tens, None),
                P(FSDP, None),
                P(),
                P(),
                P(None, FSDP, tens),
                P(None, tens),
                P(tens, FSDP),
                P(FSDP, tens),
                P(tens),
                P(tens, FSDP),
                P(FSDP, tens, None),
            ),
            out_specs=(
                P(FSDP, tens, None),
                P(FSDP, tens, None),
                P(),
                P(),
                P(None, FSDP, tens),
                P(None, tens),
                P(tens, FSDP),
                P(FSDP, tens),
                P(tens),
                P(tens, FSDP),
            ),
            check_vma=False,
        )(*arrays)

    return layer
```

```python
import functools
import math

import jax
import jax.numpy as jnp
from jax import lax
from jax.experimental import pallas as pl
from jax.experimental.pallas import tpu as pltpu
from jax.sharding import Mesh
from jax.sharding import PartitionSpec as P

DH = 72
IMG = 729
IMG_MB = 2
EPS = 1e-06
GELU_C = 0.7978845608028654
F32 = jnp.float32
BF16 = jnp.bfloat16
FSDP = ("fy", "fx")
SCALE = DH ** (-0.5)
LOG2E = math.log2(math.e)


def norm_forward(values, norm_gain, norm_shift):
    center = values - jnp.mean(values, axis=-1, keepdims=True)
    factor = lax.rsqrt(jnp.mean(center * center, axis=-1, keepdims=True) + EPS)
    scaled = center * factor
    return (scaled * norm_gain + norm_shift, scaled, factor)


def norm_backward(upstream, scaled, factor, norm_gain):
    inside = upstream * norm_gain
    return factor * (
        inside
        - jnp.mean(inside, axis=-1, keepdims=True)
        - scaled * jnp.mean(inside * scaled, axis=-1, keepdims=True)
    )


def gelu(pre_act):
    return (
        0.5
        * pre_act
        * (1.0 + jnp.tanh(GELU_C * (pre_act + 0.044715 * pre_act * pre_act * pre_act)))
    )


def gelu_both(pre_act):
    square = pre_act * pre_act
    curve = jnp.tanh(GELU_C * pre_act * (1.0 + 0.044715 * square))
    rise = 0.5 * (1.0 + curve)
    slope = rise + 0.5 * pre_act * (1.0 - curve * curve) * GELU_C * (1.0 + 3.0 * 0.044715 * square)
    return pre_act * rise, slope


def gelu_back(pre_act, upstream):
    return jax.vjp(gelu, pre_act)[1](upstream)[0]


def dot_nn(left, right):
    return lax.dot_general(left, right, (((1,), (0,)), ((), ())), preferred_element_type=F32)


def dot_nt(left, right):
    return lax.dot_general(left, right, (((1,), (1,)), ((), ())), preferred_element_type=F32)


def dot_tn(left, right):
    return lax.dot_general(left, right, (((0,), (0,)), ((), ())), preferred_element_type=F32)


def sum_products(lefts, rights):
    total = dot_nt(lefts[0], rights[0])
    for left, right in zip(lefts[1:], rights[1:]):
        total = total + dot_nt(left, right)
    return total


def round_up(value, unit):
    return -(-value // unit) * unit


def swap(value, axis):
    return lax.ppermute(value, axis, [(0, 1), (1, 0)])


def slot_swap(value, stride, slots):
    return lax.ppermute(value, "slot", [(s, s ^ stride) for s in range(slots)])


def part_sum(value, parts):
    value = value.astype(BF16)
    if parts == 2:
        return value.astype(F32) + swap(value, "part").astype(F32)
    return lax.psum(value.astype(F32), "part")


def part_gather(value, parts):
    if parts == 2:
        other = swap(value, "part")
        first = lax.axis_index("part") == 0
        return jnp.stack([jnp.where(first, value, other), jnp.where(first, other, value)])
    return lax.all_gather(value, "part", axis=0)


def add_half(left, right):
    return (left.astype(F32) + right.astype(F32)).astype(BF16)


MESH = pl.DeviceIdType.MESH


class Place:
    def __init__(self):
        self.y, self.x = lax.axis_index("fy"), lax.axis_index("fx")
        self.z = lax.axis_index("slot")
        self.f = 2 * self.y + self.x
        self.across_x, self.across_y = {"fx": 1 - self.x}, {"fy": 1 - self.y}
        self.c = lax.axis_index("part")
        self.above = {"slot": jnp.minimum(self.z + 1, 3)}
        self.below = {"slot": jnp.maximum(self.z - 1, 0)}
        self.batch, self.image = self.z % 2, self.z // 2
        self.mate = {"part": 1 - self.c}
        self.pair = {"slot": self.z + 1 - 2 * self.batch}
        self.cross = {"slot": self.z + 2 - 4 * self.image}

    def slot_after(self, d):
        return {"slot": (self.z + d) % 4}

    def barrier(self):
        sem = pltpu.get_barrier_semaphore()
        others = [self.across_x, self.across_y, self.mate] + [self.slot_after(d) for d in (1, 2, 3)]
        for device in others:
            pl.semaphore_signal(sem, inc=1, device_id=device, device_id_type=MESH)
        pl.semaphore_wait(sem, len(others))

    def far_first(self, i):
        low = self.z < 2
        near = jnp.where(low, self.z, 3 - self.z)
        at = jnp.where(i == 0, 3, jnp.where(i == 1, 2, jnp.where(i == 2, 1 - near, near)))
        return jnp.where(low, at, 3 - at)


def send(src, dst, send_sem, recv_sem, device):
    return pltpu.make_async_remote_copy(
        src_ref=src, dst_ref=dst, send_sem=send_sem, recv_sem=recv_sem, device_id=device, device_id_type=MESH
    )


class Gather:
    SEMS = 11

    def __init__(self, place, shards, w, sems, local_sem, rows):
        self.p, self.shards, self.w, self.rows = place, shards, w, rows
        (self.zr, self.zu, self.zd, self.xr, self.xs, self.yr, self.ys, self.ar, self.asn, self.br, self.bs) = sems
        self.local_sem = local_sem

    def block(self, k, slot, owner, half=None):
        at, count = owner * self.rows, self.rows
        if half is not None:
            count = count // 2
            at = at + half * count
        return self.w[k].at[slot, pl.ds(pl.multiple_of(at, 16), count), :]

    def mine(self, k, slot, shard):
        return self.shards[k] if shard else self.block(k, slot, self.p.f)

    def up(self, k, slot, shard=False):
        dst = self.block(k, slot, self.p.f)
        return send(self.mine(k, slot, shard), dst, self.zu.at[k, slot], self.zr.at[k, slot], self.p.above)

    def down(self, k, slot, shard=False):
        dst = self.block(k, slot, self.p.f)
        return send(self.mine(k, slot, shard), dst, self.zd.at[k, slot], self.zr.at[k, slot], self.p.below)

    def to_x(self, k, slot, shard=False):
        dst = self.block(k, slot, self.p.f)
        return send(self.mine(k, slot, shard), dst, self.xs.at[k, slot], self.xr.at[k, slot], self.p.across_x)

    def to_y(self, k, slot, shard=False):
        dst = self.block(k, slot, self.p.f)
        return send(self.mine(k, slot, shard), dst, self.ys.at[k, slot], self.yr.at[k, slot], self.p.across_y)

    def from_x(self, k, slot):
        ref = self.block(k, slot, self.p.f ^ 1)
        return send(ref, ref, self.xs.at[k, slot], self.xr.at[k, slot], self.p.across_x)

    def from_y(self, k, slot):
        ref = self.block(k, slot, self.p.f ^ 2)
        return send(ref, ref, self.ys.at[k, slot], self.yr.at[k, slot], self.p.across_y)

    def corner_y(self, k, slot):
        ref = self.block(k, slot, self.p.f ^ 1, 0)
        return send(ref, ref, self.asn.at[k, slot], self.ar.at[k, slot], self.p.across_y)

    def corner_x(self, k, slot):
        ref = self.block(k, slot, self.p.f ^ 2, 1)
        return send(ref, ref, self.bs.at[k, slot], self.br.at[k, slot], self.p.across_x)

    def wait_corner(self, k, slot):
        ref = self.block(k, slot, self.p.f ^ 3, 0)
        send(ref, ref, self.asn.at[k, slot], self.ar.at[k, slot], self.p.across_y).wait_recv()
        ref = self.block(k, slot, self.p.f ^ 3, 1)
        send(ref, ref, self.bs.at[k, slot], self.br.at[k, slot], self.p.across_x).wait_recv()

    def local(self, k):
        return pltpu.make_async_copy(self.shards[k], self.block(k, self.p.z, self.p.f), self.local_sem.at[k])

    def start_z(self, k):
        @pl.when(self.p.z < 3)
        def _():
            self.up(k, self.p.z, True).start()

        @pl.when(self.p.z > 0)
        def _():
            self.down(k, self.p.z, True).start()

    def start_xy(self, k):
        self.to_x(k, self.p.z, True).start()
        self.to_y(k, self.p.z, True).start()
        self.local(k).start()

    def pass_on(self, k, d):
        z = self.p.z

        @pl.when(z >= d)
        def _():
            self.up(k, z - d).wait_recv()

            @pl.when(z < 3)
            def _():
                self.up(k, z - d).start()

            self.to_x(k, z - d).start()
            self.to_y(k, z - d).start()

        @pl.when(z + d <= 3)
        def _():
            self.down(k, z + d).wait_recv()

            @pl.when(z > 0)
            def _():
                self.down(k, z + d).start()

            self.to_x(k, z + d).start()
            self.to_y(k, z + d).start()

    def corner(self, k, d):
        def one(slot):
            self.from_x(k, slot).wait_recv()
            self.corner_y(k, slot).start()
            self.from_y(k, slot).wait_recv()
            self.corner_x(k, slot).start()

        z = self.p.z
        if d == 0:
            one(z)
        else:
            pl.when(z >= d)(lambda: one(z - d))
            pl.when(z + d <= 3)(lambda: one(z + d))

    def arrive(self, k):
        self.local(k).wait()
        for slot in range(4):
            self.wait_corner(k, slot)

    def drain(self, k):
        z = self.p.z
        for slot in range(4):
            self.to_x(k, slot).wait_send()
            self.to_y(k, slot).wait_send()
            self.corner_y(k, slot).wait_send()
            self.corner_x(k, slot).wait_send()

            @pl.when((z < 3) & (slot <= z))
            def _(slot=slot):
                self.up(k, slot).wait_send()

            @pl.when((z > 0) & (slot >= z))
            def _(slot=slot):
                self.down(k, slot).wait_send()


def gather_weights(shards):
    slots = lax.axis_size("slot")
    whole = [lax.all_gather(s, ("slot",) + FSDP, axis=0) for s in shards]
    return [w.reshape(slots, -1, w.shape[-1]) for w in whole]


class Rows:
    SEMS = 11

    def __init__(self, place, index, src, dst, sems, rows_each, edge, tail):
        self.p, self.src, self.dst, self.each = place, src, dst, rows_each
        self.half = 4 * rows_each
        self.edge, self.tail = edge, tail
        self.sems = [sem.at[index] for sem in sems]

    def at(self, row, count):
        return self.dst.at[pl.ds(pl.multiple_of(row, 16), count), :]

    def block(self, near, core):
        batch = self.p.batch if near else 1 - self.p.batch
        return self.at((2 * batch + core) * self.each, self.each)

    def own(self):
        return pltpu.make_async_copy(self.src.at[self.p.batch], self.block(True, self.p.c), self.sems[0])

    def to_mate(self):
        return send(self.src.at[self.p.batch], self.block(True, self.p.c), self.sems[1], self.sems[2], self.p.mate)

    def to_pair(self):
        return send(self.src.at[1 - self.p.batch], self.block(True, self.p.c), self.sems[3], self.sems[4], self.p.pair)

    def pass_on(self):
        ref = self.block(False, self.p.c)
        return send(ref, ref, self.sems[5], self.sems[6], self.p.mate)

    def edge_out(self):
        src = self.at(jnp.where(self.p.image == 0, self.half - self.edge, 0), self.edge)
        return send(src, self.at(self.half, self.edge), self.sems[7], self.sems[8], self.p.cross)

    def tail_out(self):
        src = self.at(self.half - self.tail, self.tail)
        dst = self.at(self.half + self.edge, self.tail)
        return send(src, dst, self.sems[7], self.sems[8], self.p.cross)

    def edge_mate(self):
        ref = self.at(self.half, self.edge)
        return send(ref, ref, self.sems[9], self.sems[10], self.p.mate)

    def tail_mate(self):
        ref = self.at(self.half + self.edge, self.tail)
        return send(ref, ref, self.sems[9], self.sems[10], self.p.mate)

    def start(self):
        self.to_pair().start()
        self.to_mate().start()
        self.own().start()

    def forward(self):
        ref = self.block(False, self.p.c)
        send(ref, ref, self.sems[3], self.sems[4], self.p.pair).wait_recv()
        self.pass_on().start()

    def main_ready(self):
        self.own().wait()
        ref = self.block(True, 1 - self.p.c)
        send(ref, ref, self.sems[1], self.sems[2], self.p.mate).wait_recv()
        ref = self.block(False, 1 - self.p.c)
        send(ref, ref, self.sems[5], self.sems[6], self.p.mate).wait_recv()

    def edges(self):
        pl.when(self.p.c == 0)(lambda: self.edge_out().start())
        pl.when(self.p.c == 1)(lambda: self.tail_out().start())

    def edges_forward(self):
        @pl.when(self.p.c == 0)
        def _():
            self.edge_out().wait_recv()
            self.edge_mate().start()

        @pl.when(self.p.c == 1)
        def _():
            self.tail_out().wait_recv()
            self.tail_mate().start()

    def edges_ready(self):
        pl.when(self.p.c == 0)(lambda: self.tail_mate().wait_recv())
        pl.when(self.p.c == 1)(lambda: self.edge_mate().wait_recv())

    def drain(self):
        self.to_mate().wait_send()
        self.to_pair().wait_send()
        self.pass_on().wait_send()

        @pl.when(self.p.c == 0)
        def _():
            self.edge_out().wait_send()
            self.edge_mate().wait_send()

        @pl.when(self.p.c == 1)
        def _():
            self.tail_out().wait_send()
            self.tail_mate().wait_send()


def row_tiles(rows, step, body):
    def one(t, carry):
        body(pl.ds(pl.multiple_of(t * step, 16), step))
        return carry

    lax.fori_loop(0, rows // step, one, 0)


def forward_kernel(*refs, cols, unit_rest, edge, tail, tile):
    (small_ref, up_ref, down_ref, vec_ref, x_src, c_src, gain_ref, shift_ref, segc_ref, segr_ref) = refs[:10]
    own_ref = refs[10]
    (ws, wu, wd, gd) = refs[11:15]
    (x_ref, c_ref, vec_all, first_ref, qkv_ref, ctx_ref, inv_ref, res_ref, second_ref) = refs[15:24]
    (hidden_ref, slope_ref, hidden_rest, slope_rest, rest_up, rest_down) = refs[24:30]
    (blocks, unit_blocks, grads, part, part_out, part_in, bias_rest) = refs[30:37]
    gather_sems, local_sem = refs[37 : 37 + Gather.SEMS], refs[37 + Gather.SEMS]
    tail_refs = refs[38 + Gather.SEMS :]
    row_sems, (vec_s, vec_r, load_sem, part_s, part_r, unit_sem, grad_sem) = tail_refs[: Rows.SEMS], tail_refs[Rows.SEMS :]
    main, rest = up_ref.shape[1], unit_rest
    rows, width = x_ref.shape
    place = Place()
    place.barrier()
    shards = (small_ref, up_ref, down_ref)
    g = Gather(place, shards, (ws, wu, wd), gather_sems, local_sem, small_ref.shape[0])
    each = x_src.shape[1]
    x_rows = Rows(place, 0, x_src, x_ref, row_sems, each, edge, tail)
    c_rows = Rows(place, 1, c_src, c_ref, row_sems, each, edge, tail)

    def vec_to(d):
        device = place.slot_after(d)
        return send(vec_ref, vec_all.at[place.z], vec_s.at[d], vec_r.at[d], device)

    def vec_from(d):
        ref = vec_all.at[(place.z + 4 - d) % 4]
        return send(ref, ref, vec_s.at[d], vec_r.at[d], place.slot_after(d))

    g.start_z(0)
    g.start_xy(0)
    for d in (1, 2, 3):
        vec_to(d).start()
    x_rows.start()
    vec_all[place.z] = vec_ref[...]
    g.pass_on(0, 1)
    g.corner(0, 0)
    x_rows.forward()
    g.pass_on(0, 2)
    x_rows.main_ready()
    x_rows.edges()
    g.corner(0, 1)
    x_rows.edges_forward()
    g.pass_on(0, 3)
    g.start_z(1)
    x_rows.edges_ready()

    def first(span):
        value = x_ref[span, :].astype(F32)
        out, _, _ = norm_forward(value, gain_ref[0:1, :], shift_ref[0:1, :])
        first_ref[span, :] = out.astype(BF16)

    row_tiles(rows, 128, first)
    g.corner(0, 2)
    g.corner(0, 3)
    for d in (1, 2, 3):
        vec_from(d).wait_recv()
    g.arrive(0)

    later = []
    for k in (1, 2):
        later.append(lambda k=k: g.start_xy(k))
        if k == 1:
            later.append(lambda: c_rows.start())
        for d in (1, 2, 3):
            later.append(lambda k=k, d=d: g.pass_on(k, d))
            later.append(lambda k=k, d=d: g.corner(k, d - 1))
        if k == 1:
            later.append(lambda: g.start_z(2))
            later.append(lambda: c_rows.forward())
            later.append(lambda: (c_rows.main_ready(), c_rows.edges()))
        later.append(lambda k=k: g.corner(k, 3))
        if k == 1:
            later.append(lambda: c_rows.edges_forward())

    def step(count=1):
        for _ in range(count):
            if later:
                later.pop(0)()

    step(2)

    def load(s):
        return pltpu.make_async_copy(ws.at[s], blocks.at[s % 2], load_sem.at[s % 2])

    heads = cols // DH
    rest_up[...] = jnp.zeros_like(rest_up)
    rest_down[...] = jnp.zeros_like(rest_down)
    bias_rest[...] = jnp.zeros_like(bias_rest)
    load(0).start()
    for s in range(4):
        load(s).wait()
        if s < 3:
            load(s + 1).start()
        w = blocks.at[s % 2]
        bias = vec_all[s, 0:1, : 3 * cols].astype(F32) + vec_all[s, 1:2, : 3 * cols].astype(F32)
        projected = dot_nn(first_ref[...], w[:, : 3 * cols]) + bias
        qkv_ref[s] = projected.astype(BF16)
        step()
        for head in range(heads):
            attend_head(qkv_ref, ctx_ref, inv_ref, segc_ref, segr_ref, s, head, cols, tile)
            step()
        product = dot_nt(ctx_ref[s], w[:, 3 * cols : 4 * cols])
        at = 4 * cols
        rest_up[:, s * rest : (s + 1) * rest] = w[:, at : at + rest]
        rest_down[:, s * rest : (s + 1) * rest] = w[:, at + rest : at + 2 * rest]
        bias_rest[:, s * rest : (s + 1) * rest] = vec_all[s, 2:3, main : main + rest].astype(F32)
        if s == 0:
            part[...] = product
        else:
            part[...] += product

    def halves(h):
        return pl.ds(h * (rows // 2), rows // 2)

    def exchange(h):
        src, dst = part_out.at[halves(h), :], part_in.at[halves(h), :]
        return send(src, dst, part_s.at[h], part_r.at[h], place.mate)

    for h in (0, 1):
        part_out[halves(h), :] = part[halves(h), :].astype(BF16)
        exchange(h).start()
    step()
    for h in (0, 1):
        exchange(h).wait_recv()

    def second(span):
        value = x_ref[span, :].astype(F32) + (part_out[span, :].astype(F32) + part_in[span, :].astype(F32))
        value = value + shift_ref[2:3, :]
        res_ref[span, :] = value
        out, _, _ = norm_forward(value, gain_ref[1:2, :], shift_ref[1:2, :])
        second_ref[span, :] = out.astype(BF16)

    row_tiles(rows, 128, second)
    g.arrive(1)

    def unit_load(s):
        return pltpu.make_async_copy(wu.at[s], unit_blocks.at[s % 2], unit_sem.at[s % 2])

    unit_load(0).start()
    for s in range(4):
        unit_load(s).wait()
        if s < 3:
            unit_load(s + 1).start()
        bias = vec_all[s, 2:3, :main].astype(F32)

        def units(span, s=s, bias=bias):
            hidden, slope = gelu_both(dot_nn(second_ref[span, :], unit_blocks[s % 2]) + bias)
            hidden_ref[s, span, :] = hidden.astype(BF16)
            slope_ref[s, span, :] = slope.astype(BF16)

        row_tiles(rows, tile, units)
        step()

    def units_rest(span):
        hidden, slope = gelu_both(dot_nn(second_ref[span, :], rest_up[...]) + bias_rest[...])
        hidden_rest[span, :] = hidden.astype(BF16)
        slope_rest[span, :] = slope.astype(BF16)

    row_tiles(rows, tile, units_rest)
    step()
    c_rows.edges_ready()
    c_rows.drain()
    c_ref[...] = jnp.where(own_ref[...] > 0, c_ref[...], jnp.zeros_like(c_ref))

    def grad_out(s):
        return pltpu.make_async_copy(grads.at[s % 2], gd.at[s], grad_sem.at[s % 2])

    def down_grad(s, carry):
        pl.when(s >= 2)(lambda: grad_out(s - 2).wait())
        grads[s % 2] = dot_tn(c_ref[...], hidden_ref[s]).astype(BF16)
        grad_out(s).start()
        return carry

    lax.fori_loop(0, 2, down_grad, 0)
    step()
    lax.fori_loop(2, 4, down_grad, 0)
    step(len(later))
    for s in (2, 3):
        grad_out(s).wait()
    g.arrive(2)
    for k in (0, 1, 2):
        g.drain(k)
    x_rows.drain()
    for d in (1, 2, 3):
        vec_to(d).wait_send()
    for h in (0, 1):
        exchange(h).wait_send()


def forward_stage(
    small, up, down, vectors, x_src, c_src, gains, shifts, segments, owned, cols, unit_rest, rows, edge, tail
):
    width, shard_rows, main = x_src.shape[2], small.shape[0], up.shape[1]
    heads, rest_lanes = cols // DH, round_up(4 * unit_rest, 128)
    vmem = pl.BlockSpec(memory_space=pltpu.VMEM)
    far = pl.BlockSpec(memory_space=pl.ANY)
    shape = jax.ShapeDtypeStruct
    dma = pltpu.SemaphoreType.DMA
    return pl.pallas_call(
        functools.partial(forward_kernel, cols=cols, unit_rest=unit_rest, edge=edge, tail=tail, tile=rows // 2),
        in_specs=[vmem] * 11,
        out_specs=[far] * 4 + [vmem] * 15,
        out_shape=[
            shape((4, width, small.shape[1]), BF16),
            shape((4, width, main), BF16),
            shape((4, width, main), BF16),
            shape((4, width, main), BF16),
            shape((rows, width), BF16),
            shape((rows, width), BF16),
            shape((4,) + vectors.shape, BF16),
            shape((rows, width), BF16),
            shape((4, rows, 3 * cols), BF16),
            shape((4, rows, cols), BF16),
            shape((4, rows, heads), F32),
            shape((rows, width), F32),
            shape((rows, width), BF16),
            shape((4, rows, main), BF16),
            shape((4, rows, main), BF16),
            shape((rows, rest_lanes), BF16),
            shape((rows, rest_lanes), BF16),
            shape((width, rest_lanes), BF16),
            shape((width, rest_lanes), BF16),
        ],
        scratch_shapes=[
            pltpu.VMEM((2, width, small.shape[1]), BF16),
            pltpu.VMEM((2, width, main), BF16),
            pltpu.VMEM((2, width, main), BF16),
            pltpu.VMEM((rows, width), F32),
            pltpu.VMEM((rows, width), BF16),
            pltpu.VMEM((rows, width), BF16),
            pltpu.VMEM((1, rest_lanes), F32),
        ]
        + [dma((3, 4))] * Gather.SEMS
        + [dma((3,))]
        + [dma((2,))] * Rows.SEMS
        + [dma((4,)), dma((4,)), dma((2,)), dma((2,)), dma((2,)), dma((2,)), dma((2,))],
        compiler_params=pltpu.CompilerParams(collective_id=1, has_side_effects=True, vmem_limit_bytes=64000000),
        name="forward",
    )(
        small, up, down, vectors, x_src, c_src, gains, shifts, segments[:, None], segments[None, :],
        owned[:, None].astype(jnp.int32),
    )


def middle_kernel(*refs, cols, unit_rest):
    (wd, wu, gd) = refs[:3]
    (hidden_ref, slope_ref, hidden_rest, slope_rest, rest_up, rest_down) = refs[3:9]
    (c_ref, second_ref, res_ref, gain_ref, shift_ref) = refs[9:14]
    gu = refs[14]
    (d_out, rest_sums, half_ref, grad_ref, y_ref, sums_ref, unit_ref, unit_rest_ref) = refs[15:23]
    (blocks, grads, pre_half, part, part_out, part_in, part_in2) = refs[23:30]
    d_bufs, d_own = refs[30:35], refs[35:38]
    refs = refs[38:]
    sems, loads = refs[: Reduce.SEMS], refs[Reduce.SEMS : Reduce.SEMS + 3]
    load_sem, grad_sem, part_s, part_r = refs[Reduce.SEMS + 3 :]
    rows, width = c_ref.shape
    rest = unit_rest
    place = Place()
    place.barrier()
    r = Reduce(place, (gd,), (d_own,), (d_out,), (d_bufs,), sems, loads, d_out.shape[0])

    def load(w, slot, buffer):
        return pltpu.make_async_copy(w.at[slot], blocks.at[buffer], load_sem.at[buffer])

    def halves(h):
        return pl.ds(h * (rows // 2), rows // 2)

    def exchange(n, h):
        dst = (part_in, part_in2)[n]
        src, dst = part_out.at[halves(h), :], dst.at[halves(h), :]
        return send(src, dst, part_s.at[n, h], part_r.at[n, h], place.mate)

    load(wd, 0, 0).start()
    r.start(0)
    part[...] = dot_nt(hidden_rest[...], rest_down[...])
    grad_rest = slope_rest[...].astype(F32) * dot_nn(c_ref[...], rest_down[...])
    unit_rest_ref[...] = jnp.sum(grad_rest, axis=0, keepdims=True)
    half_rest = grad_rest.astype(BF16)

    def down_block(s, carry):
        load(wd, s, s % 2).wait()
        pl.when(s < 3)(lambda: load(wd, s + 1, (s + 1) % 2).start())
        pl.when(s == 3)(lambda: load(wu, 0, 0).start())
        w = blocks[s % 2]
        part[...] += dot_nt(hidden_ref[s], w)
        grad = slope_ref[s].astype(F32) * dot_nn(c_ref[...], w)
        pre_half[s] = grad.astype(BF16)
        unit_ref[s] = jnp.broadcast_to(jnp.sum(grad, axis=0, keepdims=True), unit_ref.shape[1:])
        r.middle_one(0, s)
        return carry

    lax.fori_loop(0, 4, down_block, 0)
    for h in (0, 1):
        part_out[halves(h), :] = part[halves(h), :].astype(BF16)
        exchange(0, h).start()
    up_sum = dot_tn(second_ref[...], half_rest).astype(BF16)
    down_sum = dot_tn(c_ref[...], hidden_rest[...]).astype(BF16)
    rest_sums[...] = jnp.zeros_like(rest_sums)
    for s in range(4):
        rest_sums[s, :, :rest] = up_sum[:, s * rest : (s + 1) * rest]
        rest_sums[s, :, rest : 2 * rest] = down_sum[:, s * rest : (s + 1) * rest]
    part[...] = dot_nt(half_rest, rest_up[...])

    def grad_out(s):
        return pltpu.make_async_copy(grads.at[s % 2], gu.at[s], grad_sem.at[s % 2])

    def up_block(s, carry):
        load(wu, s, s % 2).wait()
        pl.when(s < 3)(lambda: load(wu, s + 1, (s + 1) % 2).start())
        part[...] += dot_nt(pre_half[s], blocks[s % 2])
        pl.when(s >= 2)(lambda: grad_out(s - 2).wait())
        grads[s % 2] = dot_tn(second_ref[...], pre_half[s]).astype(BF16)
        grad_out(s).start()
        pl.when(s >= 2)(lambda: r.line_one(0, s - 2))
        return carry

    lax.fori_loop(0, 4, up_block, 0)
    for h in (0, 1):
        exchange(0, h).wait_recv()

    def output(span):
        value = part_out[span, :].astype(F32) + part_in[span, :].astype(F32)
        y_ref[span, :] = (res_ref[span, :] + value + shift_ref[3:4, :]).astype(BF16)

    row_tiles(rows, 128, output)
    for h in (0, 1):
        exchange(0, h).wait_send()
        part_out[halves(h), :] = part[halves(h), :].astype(BF16)
        exchange(1, h).start()
    r.line_one(0, 2)
    r.line_one(0, 3)
    for h in (0, 1):
        exchange(1, h).wait_recv()
    sums_ref[...] = jnp.zeros_like(sums_ref)

    def back(span):
        grad = part_out[span, :].astype(F32) + part_in2[span, :].astype(F32)
        upstream = c_ref[span, :].astype(F32)
        _, scaled, factor = norm_forward(res_ref[span, :], gain_ref[1:2, :], shift_ref[1:2, :])
        value = upstream + norm_backward(grad, scaled, factor, gain_ref[1:2, :])
        grad_ref[span, :] = value
        half_ref[span, :] = value.astype(BF16)
        sums_ref[1:2, :] += jnp.sum(grad * scaled, axis=0, keepdims=True)
        sums_ref[3:4, :] += jnp.sum(grad, axis=0, keepdims=True)
        sums_ref[4:5, :] += jnp.sum(value, axis=0, keepdims=True)
        sums_ref[5:6, :] += jnp.sum(upstream, axis=0, keepdims=True)

    row_tiles(rows, 128, back)
    for s in (2, 3):
        grad_out(s).wait()
    r.drain(0)
    for h in (0, 1):
        exchange(1, h).wait_send()


def middle_stage(
    wd, wu, gd, hidden, slope, hidden_rest, slope_rest, rest_up, rest_down, cot, second, residual, gains, shifts, cols, unit_rest, spare
):
    rows, width = cot.shape
    main, shard_rows = wd.shape[2], width // 4
    vmem = pl.BlockSpec(memory_space=pltpu.VMEM)
    far = pl.BlockSpec(memory_space=pl.ANY)
    shape = jax.ShapeDtypeStruct
    dma = pltpu.SemaphoreType.DMA
    return pl.pallas_call(
        functools.partial(middle_kernel, cols=cols, unit_rest=unit_rest),
        in_specs=[far] * 3 + [vmem] * 11,
        out_specs=[far] + [vmem] * 8,
        out_shape=[
            shape((4, width, main), BF16),
            shape((shard_rows, main), F32),
            shape((4, width, 2 * unit_rest + spare), BF16),
            shape((rows, width), BF16),
            shape((rows, width), F32),
            shape((rows, width), BF16),
            shape((8, width), F32),
            shape((4, 8, main), F32),
            shape((1, rest_up.shape[1]), F32),
        ],
        scratch_shapes=[
            pltpu.VMEM((2, width, main), BF16),
            pltpu.VMEM((2, width, main), BF16),
            pltpu.VMEM((4, rows, main), BF16),
            pltpu.VMEM((rows, width), F32),
            pltpu.VMEM((rows, width), BF16),
            pltpu.VMEM((rows, width), BF16),
            pltpu.VMEM((rows, width), BF16),
        ]
        + reduce_buffers(shard_rows, main)
        + reduce_terms(shard_rows, main)
        + [dma((1, 4))] * Reduce.SEMS
        + [dma((1, 4))] * 3
        + [dma((2,)), dma((2,)), dma((2, 2)), dma((2, 2))],
        compiler_params=pltpu.CompilerParams(collective_id=3, has_side_effects=True, vmem_limit_bytes=64000000),
        name="middle",
    )(wd, wu, gd, hidden, slope, hidden_rest, slope_rest, rest_up, rest_down, cot, second, residual, gains, shifts)


class Reduce:
    SEMS = 16

    def __init__(self, place, g, own, out, bufs, sems, load_sems, rows):
        self.p, self.g, self.own, self.out, self.rows = place, g, own, out, rows
        self.bufs, self.sems, self.load_sems = bufs, sems, load_sems

    def grad(self, k, slot, owner, half=None):
        at, count = owner * self.rows, self.rows
        if half is not None:
            count = count // 2
            at = at + half * count
        return self.g[k].at[slot, pl.ds(pl.multiple_of(at, 16), count), :]

    def terms(self, k, slot):
        f = self.p.f
        if self.own[k] is None:
            return self.grad(k, slot, f ^ 1, 0), self.grad(k, slot, f ^ 2, 1), self.grad(k, slot, f)
        return tuple(ref.at[slot] for ref in self.own[k])

    def loads(self, k, slot):
        f = self.p.f
        src = self.grad(k, slot, f ^ 1, 0), self.grad(k, slot, f ^ 2, 1), self.grad(k, slot, f)
        pairs = zip(src, self.terms(k, slot), self.load_sems)
        return [pltpu.make_async_copy(one, dst, sem.at[k, slot]) for one, dst, sem in pairs]

    def half(self, ref, slot, half):
        count = self.rows // 2
        return ref.at[slot, half * count : (half + 1) * count, :]

    def copy(self, k, slot, src, dst, index, device):
        return send(src, dst, self.sems[2 * index].at[k, slot], self.sems[2 * index + 1].at[k, slot], device)

    def corner_y(self, k, s):
        return self.copy(k, s, self.grad(k, s, self.p.f ^ 3, 0), self.bufs[k][0].at[s], 0, self.p.across_y)

    def corner_x(self, k, s):
        return self.copy(k, s, self.grad(k, s, self.p.f ^ 3, 1), self.bufs[k][1].at[s], 1, self.p.across_x)

    def x_low(self, k, s):
        return self.copy(k, s, self.bufs[k][0].at[s], self.half(self.bufs[k][2], s, 0), 2, self.p.across_x)

    def x_high(self, k, s):
        dst = self.half(self.bufs[k][2], s, 1)
        return self.copy(k, s, self.grad(k, s, self.p.f ^ 1, 1), dst, 3, self.p.across_x)

    def y_low(self, k, s):
        dst = self.half(self.bufs[k][3], s, 0)
        return self.copy(k, s, self.grad(k, s, self.p.f ^ 2, 0), dst, 4, self.p.across_y)

    def y_high(self, k, s):
        return self.copy(k, s, self.bufs[k][1].at[s], self.half(self.bufs[k][3], s, 1), 5, self.p.across_y)

    def up(self, k, s):
        return self.copy(k, s, self.bufs[k][2].at[s], self.bufs[k][4].at[s], 6, self.p.above)

    def down(self, k, s):
        at = jnp.where(s == self.p.z - 1, 4, s)
        return self.copy(k, s, self.bufs[k][2].at[s], self.bufs[k][4].at[at], 7, self.p.below)

    def from_above(self, k, s):
        at = jnp.where(s == self.p.z, 4, s)
        return self.copy(k, s, self.bufs[k][4].at[at], self.bufs[k][4].at[at], 7, self.p.below), at

    def start_one(self, k, s):
        self.corner_y(k, s).start()
        self.corner_x(k, s).start()
        self.y_low(k, s).start()
        self.x_high(k, s).start()

    def start(self, k):
        def one(i, carry):
            self.start_one(k, self.p.far_first(i))
            return carry

        lax.fori_loop(0, 4, one, 0)
        if self.own[k] is not None:
            for slot in range(4):
                for load in self.loads(k, slot):
                    load.start()

    def tiles(self, rows, body):
        row_tiles(rows, 48 if rows % 48 == 0 else 16, body)

    def middle_one(self, k, i):
        s, count = self.p.far_first(i), self.rows // 2
        low, high = self.bufs[k][0], self.bufs[k][1]
        if self.own[k] is not None:
            for load in self.loads(k, s):
                load.wait()
        own_low, own_high, _ = self.terms(k, s)
        self.corner_y(k, s).wait_recv()

        def add_low(span):
            low[s, span, :] = add_half(low[s, span, :], own_low[span, :])

        self.tiles(count, add_low)
        self.corner_x(k, s).wait_recv()

        def add_high(span):
            high[s, span, :] = add_half(high[s, span, :], own_high[span, :])

        self.tiles(count, add_high)
        self.x_low(k, s).start()
        self.y_high(k, s).start()

    def line_one(self, k, i):
        z, acc, side, far = self.p.z, self.bufs[k][2], self.bufs[k][3], self.bufs[k][4]
        s = self.p.far_first(i)
        self.x_low(k, s).wait_recv()
        self.x_high(k, s).wait_recv()
        self.y_low(k, s).wait_recv()
        self.y_high(k, s).wait_recv()
        own = self.terms(k, s)[2]

        def add(span):
            total = own[span, :].astype(F32) + acc[s, span, :].astype(F32) + side[s, span, :].astype(F32)
            acc[s, span, :] = total.astype(BF16)

        self.tiles(self.rows, add)

        def add_far(at):
            def body(span):
                acc[s, span, :] = add_half(acc[s, span, :], far[at, span, :])

            self.tiles(self.rows, body)

        @pl.when((z > 0) & (s >= z))
        def _():
            self.up(k, s).wait_recv()
            add_far(s)

        @pl.when((z < 3) & (s <= z))
        def _():
            copy, at = self.from_above(k, s)
            copy.wait_recv()
            add_far(at)

        @pl.when(s > z)
        def _():
            self.up(k, s).start()

        @pl.when(s < z)
        def _():
            self.down(k, s).start()

        @pl.when(s == z)
        def _():
            def final(span):
                self.out[k][span, :] = acc[s, span, :].astype(F32)

            self.tiles(self.rows, final)

    def loop(self, one):
        def body(i, carry):
            one(i)
            return carry

        lax.fori_loop(0, 4, body, 0)

    def drain(self, k):
        def one(s):
            for copy in (self.corner_y, self.corner_x, self.x_low, self.x_high, self.y_low, self.y_high):
                copy(k, s).wait_send()

            @pl.when(s > self.p.z)
            def _():
                self.up(k, s).wait_send()

            @pl.when(s < self.p.z)
            def _():
                self.down(k, s).wait_send()

        self.loop(one)


def reduce_buffers(rows, lanes):
    half, whole = pltpu.VMEM((4, rows // 2, lanes), BF16), pltpu.VMEM((4, rows, lanes), BF16)
    return [half, half, whole, whole, pltpu.VMEM((5, rows, lanes), BF16)]


def reduce_terms(rows, lanes):
    half, whole = pltpu.VMEM((4, rows // 2, lanes), BF16), pltpu.VMEM((4, rows, lanes), BF16)
    return [half, half, whole]


def scatter_grads(chunks):
    count = lax.axis_size("fy") * lax.axis_size("fx")
    split = [c.reshape(c.shape[0] * count, c.shape[1] // count, c.shape[2]) for c in chunks]
    return [lax.psum_scatter(c, ("slot",) + FSDP, scatter_dimension=0).astype(F32) for c in split]


class RowsBack:
    SEMS = 7

    def __init__(self, place, index, window, inbox, owned, out, sems, rows_each, edge, tail):
        self.p, self.window, self.inbox, self.owned, self.out = place, window, inbox, owned, out
        self.each, self.half, self.edge, self.tail = rows_each, 4 * rows_each, edge, tail
        self.sems = [sem.at[index] for sem in sems]

    def edge_out(self):
        src = self.window.at[self.half : self.half + self.edge, :]
        return send(src, self.inbox.at[: self.edge, :], self.sems[0], self.sems[1], self.p.cross)

    def tail_out(self):
        src = self.window.at[self.half + self.edge :, :]
        return send(src, self.inbox.at[self.edge :, :], self.sems[2], self.sems[3], self.p.cross)

    def block(self, near):
        batch = self.p.batch if near else 1 - self.p.batch
        row = (2 * batch + self.p.c) * self.each
        return self.window.at[pl.ds(pl.multiple_of(row, 16), self.each), :]

    def stay(self):
        return pltpu.make_async_copy(self.block(True), self.out.at[self.p.batch], self.sems[4])

    def to_pair(self):
        return send(self.block(False), self.out.at[self.p.batch], self.sems[5], self.sems[6], self.p.pair)

    def edges(self):
        pl.when(self.p.c == self.p.image)(lambda: self.edge_out().start())
        pl.when((self.p.c == 1) & (self.p.image == 0))(lambda: self.tail_out().start())

    def merge(self, row, count, at):
        keep = self.owned[row : row + count, :] > 0
        value = jnp.where(keep, self.window[row : row + count, :], self.inbox[at : at + count, :])
        self.window[row : row + count, :] = value

    def finish(self):
        p = self.p

        @pl.when((p.c == 1) & (p.image == 0))
        def _():
            self.edge_out().wait_recv()
            self.merge(self.half - self.edge, self.edge, 0)

        @pl.when((p.c == 0) & (p.image == 1))
        def _():
            self.edge_out().wait_recv()
            self.merge(0, self.edge, 0)

        @pl.when((p.c == 1) & (p.image == 1))
        def _():
            self.tail_out().wait_recv()
            self.merge(self.half - self.tail, self.tail, self.edge)

        self.to_pair().start()
        self.stay().start()

    def drain(self):
        pl.when(self.p.c == self.p.image)(lambda: self.edge_out().wait_send())
        pl.when((self.p.c == 1) & (self.p.image == 0))(lambda: self.tail_out().wait_send())
        self.stay().wait()
        self.to_pair().wait_send()
        ref = self.out.at[1 - self.p.batch]
        send(ref, ref, self.sems[5], self.sems[6], self.p.pair).wait_recv()


def backward_kernel(*refs, cols, unit_rest, edge, tail):
    (ws, gu, rest_ref, half_ref, first_ref, triple_ref, ctx_ref, bias_ref) = refs[:8]
    (x_ref, res_grad_ref, y_ref, gain_ref, own_ref, old_sums, unit_ref, unit_rest_ref) = refs[8:16]
    (u_out, s_out, x_out, y_out, sums_ref, vec_ref) = refs[16:22]
    refs = refs[22:]
    (blocks, gs, part, part_out, part_in, inbox_x, inbox_y, y_window) = refs[:8]
    sums_in, vec_sum, vec_in, vec_far = refs[8:12]
    u_bufs, s_bufs, u_own = refs[12:17], refs[17:22], refs[22:25]
    refs = refs[25:]
    sems, loads, back_sems = refs[: Reduce.SEMS], refs[Reduce.SEMS : Reduce.SEMS + 3], refs[Reduce.SEMS + 3 : Reduce.SEMS + 3 + RowsBack.SEMS]
    load_sem, part_s, part_r, y_sems, sum_s, sum_r, vec_s, vec_r = refs[Reduce.SEMS + 3 + RowsBack.SEMS :]
    rows, width = half_ref.shape
    shard_rows = u_out.shape[0]
    place = Place()
    place.barrier()
    each = x_out.shape[1]
    r = Reduce(place, (gu, gs), (u_own, None), (u_out, s_out), (u_bufs, s_bufs), sems, loads, shard_rows)
    x_back = RowsBack(place, 0, part_in, inbox_x, own_ref, x_out, back_sems, each, edge, tail)
    y_back = RowsBack(place, 1, y_window, inbox_y, own_ref, y_out, back_sems, each, edge, tail)

    def load(i):
        return pltpu.make_async_copy(ws.at[place.far_first(i)], blocks.at[i % 2], load_sem.at[i % 2])

    y_load = pltpu.make_async_copy(y_ref, y_window, y_sems.at[0])
    y_load.start()
    load(0).start()
    r.start(0)
    y_load.wait()
    y_back.edges()

    def one_slot(i, carry):
        s = place.far_first(i)
        load(i).wait()

        @pl.when(i < 3)
        def _():
            load(i + 1).start()

        w = blocks.at[i % 2]
        gs[s, :, 3 * cols : 4 * cols] = dot_tn(half_ref[...], ctx_ref[s]).astype(BF16)
        gs[s, :, 4 * cols :] = rest_ref[s]
        pl.when(i > 0)(lambda: r.start_one(1, place.far_first(i - 1)))
        r.middle_one(0, i)
        gs[s, :, : 3 * cols] = dot_tn(first_ref[...], triple_ref[s]).astype(BF16)
        product = dot_nt(triple_ref[s], w[:, : 3 * cols])

        @pl.when(i == 0)
        def _():
            part[...] = product

        @pl.when(i > 0)
        def _():
            part[...] += product

        @pl.when(i > 1)
        def _():
            r.line_one(0, 2 * (i - 2))
            r.line_one(0, 2 * (i - 2) + 1)

        return carry

    lax.fori_loop(0, 4, one_slot, 0)

    def halves(h):
        return pl.ds(h * (rows // 2), rows // 2)

    def exchange(h):
        src, dst = part_out.at[halves(h), :], part_in.at[halves(h), :]
        return send(src, dst, part_s.at[h], part_r.at[h], place.mate)

    for h in (0, 1):
        part_out[halves(h), :] = part[halves(h), :].astype(BF16)
        exchange(h).start()
    res_load = pltpu.make_async_copy(res_grad_ref, part, load_sem.at[0])
    res_load.start()
    r.start_one(1, place.far_first(3))
    y_back.finish()
    for h in (0, 1):
        exchange(h).wait_recv()

    res_load.wait()
    sums_ref[...] = old_sums[...]

    def last(span):
        grad = part_out[span, :].astype(F32) + part_in[span, :].astype(F32)
        value = x_ref[span, :].astype(F32)
        _, scaled, factor = norm_forward(value, gain_ref[0:1, :], gain_ref[0:1, :])
        result = part[span, :] + norm_backward(grad, scaled, factor, gain_ref[0:1, :])
        part_in[span, :] = result.astype(BF16)
        sums_ref[0:1, :] += jnp.sum(grad * scaled, axis=0, keepdims=True)
        sums_ref[2:3, :] += jnp.sum(grad, axis=0, keepdims=True)

    row_tiles(rows, 128, last)
    x_back.edges()

    vec_sum[...] = jnp.zeros_like(vec_sum)
    main = unit_ref.shape[2]
    rest = unit_rest
    for s in range(4):
        vec_sum[s, 0:1, :cols] = bias_ref[s, 0:1, :]
        vec_sum[s, 1:2, :cols] = bias_ref[s, 1:2, :]
        vec_sum[s, 2:3, :main] = unit_ref[s, 0:1, :]
        vec_sum[s, 3:4, :rest] = unit_rest_ref[:, s * rest : (s + 1) * rest]

    def across(n, device):
        return (
            send(sums_ref, sums_in.at[n], sum_s.at[n], sum_r.at[n], device),
            send(vec_sum, vec_in.at[n], vec_s.at[n], vec_r.at[n], device),
        )

    def along(d):
        there = (place.z + d) % 4
        device = place.slot_after(d)
        return (
            send(sums_ref, sums_in.at[1 + d], sum_s.at[1 + d], sum_r.at[1 + d], device),
            send(vec_sum.at[there], vec_far.at[d - 1], vec_s.at[1 + d], vec_r.at[1 + d], device),
        )

    def add_across(n, device):
        for copy in across(n, device):
            copy.wait()
        sums_ref[...] += sums_in[n]
        vec_sum[...] += vec_in[n]

    for copy in across(0, place.across_x):
        copy.start()
    r.loop(lambda i: r.middle_one(1, i))
    add_across(0, place.across_x)
    for copy in across(1, place.across_y):
        copy.start()
    x_back.finish()
    r.line_one(1, 0)
    add_across(1, place.across_y)
    for d in (1, 2, 3):
        for copy in along(d):
            copy.start()
    for i in (1, 2, 3):
        r.line_one(1, i)
    for d in (1, 2, 3):
        for copy in along(d):
            copy.wait()
    sums_ref[...] += sums_in[2] + sums_in[3] + sums_in[4]
    vec_ref[...] = vec_sum[place.z] + vec_far[0] + vec_far[1] + vec_far[2]
    for k in (0, 1):
        r.drain(k)
    x_back.drain()
    y_back.drain()
    for h in (0, 1):
        exchange(h).wait_send()


def backward_stage(
    ws, gu, rest_sums, residual_half, first_norm, triple, context, bias_sum, x_half, residual_grad, y_rows, gains, owned,
    sums, unit_sums, unit_rest_sums, cols, unit_rest, edge, tail, rows_each,
):
    rows, width = residual_half.shape
    shard_rows, lanes, main = width // 4, ws.shape[2], gu.shape[2]
    vmem = pl.BlockSpec(memory_space=pltpu.VMEM)
    far = pl.BlockSpec(memory_space=pl.ANY)
    shape = jax.ShapeDtypeStruct
    dma = pltpu.SemaphoreType.DMA
    wide = max(main, round_up(cols, 128))
    return pl.pallas_call(
        functools.partial(backward_kernel, cols=cols, unit_rest=unit_rest, edge=edge, tail=tail),
        in_specs=[far] * 2 + [vmem] * 7 + [far, far] + [vmem] * 5,
        out_specs=[vmem] * 6,
        out_shape=[
            shape((shard_rows, main), F32),
            shape((shard_rows, lanes), F32),
            shape((2, rows_each, width), BF16),
            shape((2, rows_each, width), BF16),
            shape((8, width), F32),
            shape((8, wide), F32),
        ],
        scratch_shapes=[
            pltpu.VMEM((2, width, lanes), BF16),
            pltpu.VMEM((4, width, lanes), BF16),
            pltpu.VMEM((rows, width), F32),
            pltpu.VMEM((rows, width), BF16),
            pltpu.VMEM((rows, width), BF16),
            pltpu.VMEM((edge + tail, width), BF16),
            pltpu.VMEM((edge + tail, width), BF16),
            pltpu.VMEM((rows, width), BF16),
            pltpu.VMEM((5, 8, width), F32),
            pltpu.VMEM((4, 8, wide), F32),
            pltpu.VMEM((2, 4, 8, wide), F32),
            pltpu.VMEM((3, 8, wide), F32),
        ]
        + reduce_buffers(shard_rows, main)
        + reduce_buffers(shard_rows, lanes)
        + reduce_terms(shard_rows, main)
        + [dma((2, 4))] * Reduce.SEMS
        + [dma((1, 4))] * 3
        + [dma((2,))] * RowsBack.SEMS
        + [dma((2,)), dma((2,)), dma((2,)), dma((1,)), dma((5,)), dma((5,)), dma((5,)), dma((5,))],
        compiler_params=pltpu.CompilerParams(collective_id=2, has_side_effects=True, vmem_limit_bytes=64000000),
        name="backward",
    )(
        ws, gu, rest_sums, residual_half, first_norm, triple, context, bias_sum, x_half, residual_grad, y_rows, gains, owned[:, None].astype(jnp.int32), sums, unit_sums, unit_rest_sums,
    )


def attend_head(qkv_ref, ctx_ref, inv_ref, segc_ref, segr_ref, s, head, cols, tile):
    lo = head * DH
    keys = qkv_ref[s, :, cols + lo : cols + lo + DH]
    values = qkv_ref[s, :, 2 * cols + lo : 2 * cols + lo + DH]

    def one_tile(t, carry):
        span = pl.ds(pl.multiple_of(t * tile, tile), tile)
        scores = dot_nt(qkv_ref[s, span, lo : lo + DH], keys)
        allowed = segc_ref[span, :] == segr_ref[...]
        exact = jnp.where(allowed, jnp.exp2(scores * (SCALE * LOG2E)), 0.0)
        inverse = 1.0 / jnp.sum(exact, axis=1, keepdims=True)
        context = dot_nn(exact.astype(BF16), values) * inverse
        ctx_ref[s, span, lo : lo + DH] = context.astype(BF16)
        inv_ref[s, span, head : head + 1] = inverse
        return carry

    lax.fori_loop(0, qkv_ref.shape[1] // tile, one_tile, 0)


def attend_kernel(x_ref, w_ref, b_ref, segc_ref, segr_ref, qkv_ref, ctx_ref, inv_ref, part_ref, *, cols, tile):
    block = pl.program_id(0)
    projected = dot_nn(x_ref[...], w_ref[0, :, : 3 * cols]) + b_ref[0]
    qkv_ref[0] = projected.astype(BF16)
    for head in range(cols // DH):
        attend_head(qkv_ref, ctx_ref, inv_ref, segc_ref, segr_ref, 0, head, cols, tile)
    part = dot_nt(ctx_ref[0], w_ref[0, :, 3 * cols : 4 * cols])

    @pl.when(block == 0)
    def _():
        part_ref[...] = part

    @pl.when(block > 0)
    def _():
        part_ref[...] += part


def attend(first_norm, weights, bias, segments, cols, tile):
    rows, width = first_norm.shape
    slots, _, lanes = weights.shape
    heads = cols // DH
    whole = lambda shape: pl.BlockSpec(shape, lambda s: (0,) * len(shape))
    each = lambda shape: pl.BlockSpec((1,) + shape, lambda s: (s, 0, 0))
    return pl.pallas_call(
        functools.partial(attend_kernel, cols=cols, tile=tile),
        grid=(slots,),
        in_specs=[
            whole((rows, width)),
            each((width, lanes)),
            each((1, 3 * cols)),
            whole((rows, 1)),
            whole((1, rows)),
        ],
        out_specs=[each((rows, 3 * cols)), each((rows, cols)), each((rows, heads)), whole((rows, width))],
        out_shape=[
            jax.ShapeDtypeStruct((slots, rows, 3 * cols), BF16),
            jax.ShapeDtypeStruct((slots, rows, cols), BF16),
            jax.ShapeDtypeStruct((slots, rows, heads), F32),
            jax.ShapeDtypeStruct((rows, width), F32),
        ],
        cost_estimate=pl.CostEstimate(
            flops=slots * (8 * rows * width * cols + 4 * rows * rows * 256 * heads),
            bytes_accessed=slots * width * lanes * 2 + rows * width * 10,
            transcendentals=slots * heads * rows * rows,
        ),
        name="attend",
    )(first_norm, weights, bias, segments[:, None], segments[None, :])


def attend_back_head(
    qkv_ref, ctx_ref, inv_ref, back_ref, segc_ref, segr_ref, grad_ref, bias_ref, key_acc, value_acc, s, head, cols, tile
):
    lo = head * DH
    rows = back_ref.shape[0]
    ones = jnp.ones((8, DH), F32)
    keys = qkv_ref[s, :, cols + lo : cols + lo + DH]
    values = qkv_ref[s, :, 2 * cols + lo : 2 * cols + lo + DH]
    query_total = jnp.zeros((1, DH), F32)
    for t in range(rows // tile):
        span = slice(t * tile, (t + 1) * tile)
        queries = qkv_ref[s, span, lo : lo + DH]
        back = (back_ref[span, lo : lo + DH].astype(F32) * inv_ref[s, span, head : head + 1]).astype(BF16)
        along = back.astype(F32) * ctx_ref[s, span, lo : lo + DH].astype(F32)
        delta = lax.dot_general(
            ones, along, (((1,), (1,)), ((), ())), precision=lax.Precision.HIGHEST, preferred_element_type=F32
        )[:1]
        scores = dot_nt(keys, queries)
        allowed = segc_ref[...] == segr_ref[:, span]
        exact = jnp.where(allowed, jnp.exp2(scores * (SCALE * LOG2E)), 0.0)
        value_part = dot_nn(exact.astype(BF16), back)
        prob_grad = dot_nt(values, back)
        score_grad = (exact * (prob_grad - delta)).astype(BF16)
        key_part = dot_nn(score_grad, queries)
        query_grad = dot_tn(score_grad, keys) * SCALE
        grad_ref[span, lo : lo + DH] = query_grad.astype(BF16)
        query_total = query_total + jnp.sum(query_grad, axis=0, keepdims=True)
        if t == 0:
            value_acc[...] = value_part
            key_acc[...] = key_part
        else:
            value_acc[...] += value_part
            key_acc[...] += key_part
    grad_ref[:, cols + lo : cols + lo + DH] = (key_acc[...] * SCALE).astype(BF16)
    grad_ref[:, 2 * cols + lo : 2 * cols + lo + DH] = value_acc[...].astype(BF16)
    bias_ref[s, 0:1, lo : lo + DH] = query_total
    bias_ref[s, 1:2, lo : lo + DH] = jnp.sum(value_acc[...], axis=0, keepdims=True)


def attend_back_kernel(
    r_ref, w_ref, qkv_ref, ctx_ref, inv_ref, segc_ref, segr_ref, grad_ref, bias_ref, back_ref, key_acc, value_acc, *, cols, tile
):
    back_ref[...] = dot_nn(r_ref[...], w_ref[0, :, 3 * cols : 4 * cols]).astype(BF16)
    for head in range(cols // DH):
        attend_back_head(
            qkv_ref, ctx_ref, inv_ref, back_ref, segc_ref, segr_ref, grad_ref.at[0], bias_ref, key_acc, value_acc, 0, head, cols, tile
        )


def attend_back(residual_half, weights, qkv, context, inverse, segments, cols, tile):
    rows, width = residual_half.shape
    slots, _, lanes = weights.shape
    heads = cols // DH
    whole = lambda shape: pl.BlockSpec(shape, lambda s: (0,) * len(shape))
    each = lambda shape: pl.BlockSpec((1,) + shape, lambda s: (s, 0, 0))
    return pl.pallas_call(
        functools.partial(attend_back_kernel, cols=cols, tile=tile),
        grid=(slots,),
        in_specs=[
            whole((rows, width)),
            each((width, lanes)),
            each((rows, 3 * cols)),
            each((rows, cols)),
            each((rows, heads)),
            whole((rows, 1)),
            whole((1, rows)),
        ],
        out_specs=[each((rows, 3 * cols)), each((2, cols))],
        out_shape=[
            jax.ShapeDtypeStruct((slots, rows, 3 * cols), BF16),
            jax.ShapeDtypeStruct((slots, 2, cols), F32),
        ],
        scratch_shapes=[
            pltpu.VMEM((rows, cols), BF16),
            pltpu.VMEM((rows, DH), F32),
            pltpu.VMEM((rows, DH), F32),
        ],
        cost_estimate=pl.CostEstimate(
            flops=slots * (2 * rows * width * cols + 10 * rows * rows * 256 * heads),
            bytes_accessed=slots * width * lanes * 2 + rows * width * 10,
            transcendentals=slots * heads * rows * rows,
        ),
        name="attend_back",
    )(residual_half, weights, qkv, context, inverse, segments[:, None], segments[None, :])


def plain_layer(shards, vectors, to_slot, from_slot, block_input, cotangent, gains, shifts, segments, owned, cols, units, parts):
    width, rows = block_input.shape[2], segments.shape[0]
    slots, slot = lax.axis_size("slot"), lax.axis_index("slot")
    main_units, in_lanes = shards[1].shape[1], 3 * cols
    rest = units - main_units
    spare = shards[0].shape[1] - in_lanes - cols - 2 * rest
    small_all, up_main, down_main = gather_weights(shards)
    vec_all = lax.all_gather(vectors, "slot", axis=0)
    grad_rows = jnp.where(owned[:, None], to_slot(cotangent), 0)
    upstream = grad_rows.astype(F32)
    x_float = to_slot(block_input).astype(F32)
    first_out, first_scaled, first_factor = norm_forward(x_float, gains[0], shifts[0])
    first_norm = first_out.astype(BF16)
    bias = vec_all[:, :1, :in_lanes].astype(F32) + vec_all[:, 1:2, :in_lanes].astype(F32)
    qkv, context, inverse, attention_part = attend(first_norm, small_all, bias, segments, cols, rows // 2)
    residual = x_float + part_sum(attention_part, parts) + shifts[2]
    second_out, second_scaled, second_factor = norm_forward(residual, gains[1], shifts[1])
    second_norm = second_out.astype(BF16)
    small_blocks = list(small_all)
    unit_all = vec_all[:, 2, :units].astype(F32)
    at = in_lanes + cols
    ups = list(up_main) + [b[:, at : at + rest] for b in small_blocks]
    downs = list(down_main) + [b[:, at + rest : at + 2 * rest] for b in small_blocks]
    unit_rows = list(unit_all[:, :main_units]) + list(unit_all[:, main_units:])
    pre_acts = [dot_nn(second_norm, w) + b for w, b in zip(ups, unit_rows)]
    hiddens = [gelu(p).astype(BF16) for p in pre_acts]
    output = (residual + part_sum(sum_products(hiddens, downs), parts) + shifts[3]).astype(BF16)
    down_sums = [dot_tn(grad_rows, h).astype(BF16) for h in hiddens]
    pre_grads = [gelu_back(p, dot_nn(grad_rows, w)) for p, w in zip(pre_acts, downs)]
    pre_halves = [p.astype(BF16) for p in pre_grads]
    unit_sums = [jnp.sum(p, axis=0) for p in pre_grads]
    up_sums = [dot_tn(second_norm, p).astype(BF16) for p in pre_halves]
    second_grad = part_sum(sum_products(pre_halves, ups), parts)
    residual_grad = upstream + norm_backward(second_grad, second_scaled, second_factor, gains[1])
    residual_half = residual_grad.astype(BF16)
    triple, bias_sum = attend_back(residual_half, small_all, qkv, context, inverse, segments, cols, rows // 2)
    first_part = sum_products(list(triple), [b[:, :in_lanes] for b in small_blocks])
    first_grad = part_sum(first_part, parts)
    input_grad = residual_grad + norm_backward(first_grad, first_scaled, first_factor, gains[0])
    blank = jnp.zeros((width, spare), BF16)
    small_sums = [
        jnp.concatenate(
            [
                dot_tn(first_norm, triple[s]).astype(BF16),
                dot_tn(residual_half, context[s]).astype(BF16),
                up_sums[slots + s],
                down_sums[slots + s],
                blank,
            ],
            axis=1,
        )
        for s in range(slots)
    ]
    down_grad, up_grad, small_grad = scatter_grads(
        [jnp.stack(down_sums[:slots]), jnp.stack(up_sums[:slots]), jnp.stack(small_sums)]
    )
    rows_sum = jnp.stack(
        [
            jnp.sum(first_grad * first_scaled, axis=0),
            jnp.sum(second_grad * second_scaled, axis=0),
            jnp.sum(first_grad, axis=0),
            jnp.sum(second_grad, axis=0),
            jnp.sum(residual_grad, axis=0),
            jnp.sum(upstream, axis=0),
        ]
    )
    unit_sum = jnp.stack([jnp.concatenate([unit_sums[s], unit_sums[slots + s]]) for s in range(slots)])
    rows_total, bias_total, unit_total = lax.psum((rows_sum, bias_sum, unit_sum), ("slot",) + FSDP)
    bias_grad = lax.dynamic_index_in_dim(bias_total, slot, 0, keepdims=False)
    unit_grad = lax.dynamic_index_in_dim(unit_total, slot, 0, keepdims=False)
    return (
        from_slot(output, owned), from_slot(input_grad.astype(BF16), owned), rows_total, bias_grad, unit_grad,
        down_grad, up_grad, small_grad,
    )


def on_device(
    block_input,
    segment_ids,
    norm_gains,
    row_biases,
    in_projection,
    query_value_bias,
    out_projection,
    up_weight,
    unit_bias,
    down_weight,
    cotangent,
):
    local, rows_each, width = block_input.shape
    rows_mb = segment_ids.shape[1]
    cols = in_projection.shape[2]
    units = up_weight.shape[1]
    shard_rows = up_weight.shape[0]
    slots, parts = lax.axis_size("slot"), lax.axis_size("part")
    slot, part = lax.axis_index("slot"), lax.axis_index("part")
    fsdp_index = lax.axis_index("fy") * lax.axis_size("fx") + lax.axis_index("fx")
    batch, image = slot % local, slot // local
    late = image == 1

    half_rows = rows_mb // IMG_MB
    padding = rows_mb - IMG_MB * IMG
    edge = round_up(max(half_rows - IMG, padding - (half_rows - IMG)), 16)
    tail = round_up(padding, 16)
    rows = round_up(half_rows + edge + tail, 128)
    filler = rows - half_rows - edge - tail
    paired = lax.axis_size("fy") == 2 and lax.axis_size("fx") == 2 and slots == 4 and parts == 2
    paired = paired and shard_rows % 32 == 0 and filler == 0

    def edges(main):
        near = jnp.where(late, main[:edge], main[half_rows - edge :])
        far = main[half_rows - tail :]
        return jnp.concatenate([near, far])

    def to_slot(value):
        mine = lax.dynamic_index_in_dim(value, batch, 0, keepdims=False)
        send = lax.dynamic_index_in_dim(value, 1 - batch, 0, keepdims=False)
        other = slot_swap(send, 1, slots)
        pair = jnp.where(batch == 0, jnp.stack([mine, other]), jnp.stack([other, mine]))
        main = part_gather(pair, parts).swapaxes(0, 1).reshape(half_rows, width)
        beyond = slot_swap(edges(main), local, slots)
        return jnp.concatenate([main, beyond, jnp.zeros((filler, width), value.dtype)])

    def from_slot(value, owned):
        main = value[:half_rows]
        beyond = slot_swap(value[half_rows : half_rows + edge + tail], local, slots)
        keep = owned[:half_rows, None]
        near, far = beyond[:edge], beyond[edge:]
        blank = lambda count: jnp.zeros((count, width), value.dtype)
        early_fill = jnp.concatenate([blank(half_rows - edge), near])
        late_fill = jnp.concatenate([near, blank(half_rows - edge - tail), far])
        main = jnp.where(keep, main, jnp.where(late, late_fill, early_fill))
        main = main.reshape(local, parts, rows_each, width)
        mine = lax.dynamic_index_in_dim(main, part, 1, keepdims=False)
        stay = lax.dynamic_index_in_dim(mine, batch, 0, keepdims=False)
        other = slot_swap(lax.dynamic_index_in_dim(mine, 1 - batch, 0, keepdims=False), 1, slots)
        return jnp.where(batch == 0, jnp.stack([stay, other]), jnp.stack([other, stay]))

    ids = lax.dynamic_index_in_dim(segment_ids, batch, 0, keepdims=False)
    fill_ids = jnp.full((filler,), -2, jnp.int32)
    early_ids = jnp.concatenate([ids[: half_rows + edge], ids[rows_mb - tail :], fill_ids])
    late_ids = jnp.concatenate(
        [ids[half_rows:], ids[half_rows - edge : half_rows], jnp.full((tail,), -2, jnp.int32), fill_ids]
    )
    segments = jnp.where(late, late_ids, early_ids)
    image_id = (fsdp_index * local + batch) * IMG_MB + image
    owned = (segments == image_id) | (jnp.logical_not(late) & (segments == -1))

    main_units = units // 128 * 128
    rest = units - main_units
    in_lanes = 3 * cols
    small = in_lanes + cols + 2 * rest
    lanes = round_up(small, 128)
    down_t = down_weight.T
    small_shard = jnp.concatenate(
        [
            in_projection.transpose(1, 0, 2).reshape(shard_rows, in_lanes),
            out_projection.T,
            up_weight[:, main_units:],
            down_t[:, main_units:],
            jnp.zeros((shard_rows, lanes - small), BF16),
        ],
        axis=1,
    )
    shards = [small_shard, up_weight[:, :main_units], down_t[:, :main_units]]
    triple_bias = jnp.concatenate([query_value_bias[0], jnp.zeros((cols,), F32), query_value_bias[1]])
    high = triple_bias.astype(BF16)
    low = (triple_bias - high.astype(F32)).astype(BF16)
    wide = round_up(max(in_lanes, units), 128)
    vectors = [jnp.pad(v, (0, wide - v.shape[0])) for v in (high, low, unit_bias)]
    vectors = jnp.concatenate([jnp.stack(vectors), jnp.zeros((13, wide), BF16)])
    gains, shifts = norm_gains, row_biases
    if paired:
        (
            small_all, up_main, down_main, gd, x_half, cot, _, first_norm, qkv, context, inverse, residual, second_norm,
            hidden, slope, hidden_rest, slope_rest, rest_up, rest_down,
        ) = forward_stage(
            *shards, vectors, block_input, cotangent, gains, shifts, segments, owned, cols, rest, rows, edge, tail
        )
        gu, down_grad, rest_sums, residual_half, residual_grad, y_rows, sums, unit_sums, unit_rest_sums = middle_stage(
            down_main, up_main, gd, hidden, slope, hidden_rest, slope_rest, rest_up, rest_down, cot, second_norm, residual,
            gains, shifts, cols, rest, lanes - small,
        )
        triple, bias_sum = attend_back(residual_half, small_all, qkv, context, inverse, segments, cols, rows // 2)
        up_grad, small_grad, input_grad, output, rows_total, vec_total = backward_stage(
            small_all, gu, rest_sums, residual_half, first_norm, triple, context, bias_sum, x_half, residual_grad, y_rows,
            gains, owned, sums, unit_sums, unit_rest_sums, cols, rest, edge, tail, rows_each,
        )
        rows_total = rows_total[:6]
        bias_grad = vec_total[:2, :cols]
        unit_grad = jnp.concatenate([vec_total[2, :main_units], vec_total[3, :rest]])
    else:
        output, input_grad, rows_total, bias_grad, unit_grad, down_grad, up_grad, small_grad = plain_layer(
            shards, vectors, to_slot, from_slot, block_input, cotangent, gains, shifts, segments, owned, cols, units, parts
        )
    in_grad = small_grad[:, :in_lanes].reshape(shard_rows, 3, cols).transpose(1, 0, 2)
    out_grad = small_grad[:, in_lanes : in_lanes + cols].T
    at = in_lanes + cols
    up_grad = jnp.concatenate([up_grad, small_grad[:, at : at + rest]], axis=1)
    down_grad = jnp.concatenate([down_grad, small_grad[:, at + rest : at + 2 * rest]], axis=1).T
    return (
        output,
        input_grad.astype(F32),
        rows_total[:2],
        rows_total[2:],
        in_grad,
        bias_grad,
        out_grad,
        up_grad,
        unit_grad,
        down_grad,
    )


def solution(mesh):
    fsdp, tensor = mesh.shape["fsdp"], mesh.shape["tensor"]

    def layer(*arrays):
        local = arrays[0].shape[0] // fsdp
        slots = local * IMG_MB
        assert local == 2 and slots == 4 and tensor % slots == 0 and fsdp % 2 == 0
        grid = Mesh(
            mesh.devices.reshape(fsdp // 2, 2, slots, tensor // slots), ("fy", "fx", "slot", "part")
        )
        tens = ("slot", "part")
        return jax.shard_map(
            on_device,
            mesh=grid,
            in_specs=(
                P(FSDP, tens, None),
                P(FSDP, None),
                P(),
                P(),
                P(None, FSDP, tens),
                P(None, tens),
                P(tens, FSDP),
                P(FSDP, tens),
                P(tens),
                P(tens, FSDP),
                P(FSDP, tens, None),
            ),
            out_specs=(
                P(FSDP, tens, None),
                P(FSDP, tens, None),
                P(),
                P(),
                P(None, FSDP, tens),
                P(None, tens),
                P(tens, FSDP),
                P(FSDP, tens),
                P(tens),
                P(tens, FSDP),
            ),
            check_vma=False,
        )(*arrays)

    return layer
```

```python
import functools
import math

import jax
import jax.numpy as jnp
from jax import lax
from jax.experimental import pallas as pl
from jax.experimental.pallas import tpu as pltpu
from jax.sharding import Mesh
from jax.sharding import PartitionSpec as P

DH = 72
IMG = 729
IMG_MB = 2
EPS = 1e-06
GELU_C = 0.7978845608028654
F32 = jnp.float32
BF16 = jnp.bfloat16
FSDP = ("fy", "fx")
SCALE = DH ** (-0.5)
LOG2E = math.log2(math.e)


def norm_forward(values, norm_gain, norm_shift):
    center = values - jnp.mean(values, axis=-1, keepdims=True)
    factor = lax.rsqrt(jnp.mean(center * center, axis=-1, keepdims=True) + EPS)
    scaled = center * factor
    return (scaled * norm_gain + norm_shift, scaled, factor)


def norm_backward(upstream, scaled, factor, norm_gain):
    inside = upstream * norm_gain
    return factor * (
        inside
        - jnp.mean(inside, axis=-1, keepdims=True)
        - scaled * jnp.mean(inside * scaled, axis=-1, keepdims=True)
    )


def gelu(pre_act):
    return (
        0.5
        * pre_act
        * (1.0 + jnp.tanh(GELU_C * (pre_act + 0.044715 * pre_act * pre_act * pre_act)))
    )


def gelu_both(pre_act):
    square = pre_act * pre_act
    curve = jnp.tanh(GELU_C * pre_act * (1.0 + 0.044715 * square))
    rise = 0.5 * (1.0 + curve)
    slope = rise + 0.5 * pre_act * (1.0 - curve * curve) * GELU_C * (1.0 + 3.0 * 0.044715 * square)
    return pre_act * rise, slope


def gelu_back(pre_act, upstream):
    return jax.vjp(gelu, pre_act)[1](upstream)[0]


def dot_nn(left, right):
    return lax.dot_general(left, right, (((1,), (0,)), ((), ())), preferred_element_type=F32)


def dot_nt(left, right):
    return lax.dot_general(left, right, (((1,), (1,)), ((), ())), preferred_element_type=F32)


def dot_tn(left, right):
    return lax.dot_general(left, right, (((0,), (0,)), ((), ())), preferred_element_type=F32)


def sum_products(lefts, rights):
    total = dot_nt(lefts[0], rights[0])
    for left, right in zip(lefts[1:], rights[1:]):
        total = total + dot_nt(left, right)
    return total


def round_up(value, unit):
    return -(-value // unit) * unit


def swap(value, axis):
    return lax.ppermute(value, axis, [(0, 1), (1, 0)])


def slot_swap(value, stride, slots):
    return lax.ppermute(value, "slot", [(s, s ^ stride) for s in range(slots)])


def part_sum(value, parts):
    value = value.astype(BF16)
    if parts == 2:
        return value.astype(F32) + swap(value, "part").astype(F32)
    return lax.psum(value.astype(F32), "part")


def part_gather(value, parts):
    if parts == 2:
        other = swap(value, "part")
        first = lax.axis_index("part") == 0
        return jnp.stack([jnp.where(first, value, other), jnp.where(first, other, value)])
    return lax.all_gather(value, "part", axis=0)


def add_half(left, right):
    return (left.astype(F32) + right.astype(F32)).astype(BF16)


MESH = pl.DeviceIdType.MESH


class Place:
    def __init__(self):
        self.y, self.x = lax.axis_index("fy"), lax.axis_index("fx")
        self.z = lax.axis_index("slot")
        self.f = 2 * self.y + self.x
        self.across_x, self.across_y = {"fx": 1 - self.x}, {"fy": 1 - self.y}
        self.c = lax.axis_index("part")
        self.above = {"slot": jnp.minimum(self.z + 1, 3)}
        self.below = {"slot": jnp.maximum(self.z - 1, 0)}
        self.batch, self.image = self.z % 2, self.z // 2
        self.mate = {"part": 1 - self.c}
        self.pair = {"slot": self.z + 1 - 2 * self.batch}
        self.cross = {"slot": self.z + 2 - 4 * self.image}

    def slot_after(self, d):
        return {"slot": (self.z + d) % 4}

    def barrier(self):
        sem = pltpu.get_barrier_semaphore()
        others = [self.across_x, self.across_y, self.mate] + [self.slot_after(d) for d in (1, 2, 3)]
        for device in others:
            pl.semaphore_signal(sem, inc=1, device_id=device, device_id_type=MESH)
        pl.semaphore_wait(sem, len(others))

    def far_first(self, i):
        low = self.z < 2
        near = jnp.where(low, self.z, 3 - self.z)
        at = jnp.where(i == 0, 3, jnp.where(i == 1, 2, jnp.where(i == 2, 1 - near, near)))
        return jnp.where(low, at, 3 - at)


def send(src, dst, send_sem, recv_sem, device):
    return pltpu.make_async_remote_copy(
        src_ref=src, dst_ref=dst, send_sem=send_sem, recv_sem=recv_sem, device_id=device, device_id_type=MESH
    )


class Gather:
    SEMS = 11

    def __init__(self, place, shards, w, sems, local_sem, rows):
        self.p, self.shards, self.w, self.rows = place, shards, w, rows
        (self.zr, self.zu, self.zd, self.xr, self.xs, self.yr, self.ys, self.ar, self.asn, self.br, self.bs) = sems
        self.local_sem = local_sem

    def block(self, k, slot, owner, half=None):
        at, count = owner * self.rows, self.rows
        if half is not None:
            count = count // 2
            at = at + half * count
        return self.w[k].at[slot, pl.ds(pl.multiple_of(at, 16), count), :]

    def mine(self, k, slot, shard):
        return self.shards[k] if shard else self.block(k, slot, self.p.f)

    def up(self, k, slot, shard=False):
        dst = self.block(k, slot, self.p.f)
        return send(self.mine(k, slot, shard), dst, self.zu.at[k, slot], self.zr.at[k, slot], self.p.above)

    def down(self, k, slot, shard=False):
        dst = self.block(k, slot, self.p.f)
        return send(self.mine(k, slot, shard), dst, self.zd.at[k, slot], self.zr.at[k, slot], self.p.below)

    def to_x(self, k, slot, shard=False):
        dst = self.block(k, slot, self.p.f)
        return send(self.mine(k, slot, shard), dst, self.xs.at[k, slot], self.xr.at[k, slot], self.p.across_x)

    def to_y(self, k, slot, shard=False):
        dst = self.block(k, slot, self.p.f)
        return send(self.mine(k, slot, shard), dst, self.ys.at[k, slot], self.yr.at[k, slot], self.p.across_y)

    def from_x(self, k, slot):
        ref = self.block(k, slot, self.p.f ^ 1)
        return send(ref, ref, self.xs.at[k, slot], self.xr.at[k, slot], self.p.across_x)

    def from_y(self, k, slot):
        ref = self.block(k, slot, self.p.f ^ 2)
        return send(ref, ref, self.ys.at[k, slot], self.yr.at[k, slot], self.p.across_y)

    def corner_y(self, k, slot):
        ref = self.block(k, slot, self.p.f ^ 1, 0)
        return send(ref, ref, self.asn.at[k, slot], self.ar.at[k, slot], self.p.across_y)

    def corner_x(self, k, slot):
        ref = self.block(k, slot, self.p.f ^ 2, 1)
        return send(ref, ref, self.bs.at[k, slot], self.br.at[k, slot], self.p.across_x)

    def wait_corner(self, k, slot):
        ref = self.block(k, slot, self.p.f ^ 3, 0)
        send(ref, ref, self.asn.at[k, slot], self.ar.at[k, slot], self.p.across_y).wait_recv()
        ref = self.block(k, slot, self.p.f ^ 3, 1)
        send(ref, ref, self.bs.at[k, slot], self.br.at[k, slot], self.p.across_x).wait_recv()

    def local(self, k):
        return pltpu.make_async_copy(self.shards[k], self.block(k, self.p.z, self.p.f), self.local_sem.at[k])

    def start_z(self, k):
        @pl.when(self.p.z < 3)
        def _():
            self.up(k, self.p.z, True).start()

        @pl.when(self.p.z > 0)
        def _():
            self.down(k, self.p.z, True).start()

    def start_xy(self, k):
        self.to_x(k, self.p.z, True).start()
        self.to_y(k, self.p.z, True).start()
        self.local(k).start()

    def pass_on(self, k, d):
        z = self.p.z

        @pl.when(z >= d)
        def _():
            self.up(k, z - d).wait_recv()

            @pl.when(z < 3)
            def _():
                self.up(k, z - d).start()

            self.to_x(k, z - d).start()
            self.to_y(k, z - d).start()

        @pl.when(z + d <= 3)
        def _():
            self.down(k, z + d).wait_recv()

            @pl.when(z > 0)
            def _():
                self.down(k, z + d).start()

            self.to_x(k, z + d).start()
            self.to_y(k, z + d).start()

    def corner(self, k, d):
        def one(slot):
            self.from_x(k, slot).wait_recv()
            self.corner_y(k, slot).start()
            self.from_y(k, slot).wait_recv()
            self.corner_x(k, slot).start()

        z = self.p.z
        if d == 0:
            one(z)
        else:
            pl.when(z >= d)(lambda: one(z - d))
            pl.when(z + d <= 3)(lambda: one(z + d))

    def arrive(self, k):
        self.local(k).wait()
        for slot in range(4):
            self.wait_corner(k, slot)

    def drain(self, k):
        z = self.p.z
        for slot in range(4):
            self.to_x(k, slot).wait_send()
            self.to_y(k, slot).wait_send()
            self.corner_y(k, slot).wait_send()
            self.corner_x(k, slot).wait_send()

            @pl.when((z < 3) & (slot <= z))
            def _(slot=slot):
                self.up(k, slot).wait_send()

            @pl.when((z > 0) & (slot >= z))
            def _(slot=slot):
                self.down(k, slot).wait_send()


def gather_weights(shards):
    slots = lax.axis_size("slot")
    whole = [lax.all_gather(s, ("slot",) + FSDP, axis=0) for s in shards]
    return [w.reshape(slots, -1, w.shape[-1]) for w in whole]


class Rows:
    SEMS = 11

    def __init__(self, place, index, src, dst, sems, rows_each, edge, tail):
        self.p, self.src, self.dst, self.each = place, src, dst, rows_each
        self.half = 4 * rows_each
        self.edge, self.tail = edge, tail
        self.sems = [sem.at[index] for sem in sems]

    def at(self, row, count):
        return self.dst.at[pl.ds(pl.multiple_of(row, 16), count), :]

    def block(self, near, core):
        batch = self.p.batch if near else 1 - self.p.batch
        return self.at((2 * batch + core) * self.each, self.each)

    def own(self):
        return pltpu.make_async_copy(self.src.at[self.p.batch], self.block(True, self.p.c), self.sems[0])

    def to_mate(self):
        return send(self.src.at[self.p.batch], self.block(True, self.p.c), self.sems[1], self.sems[2], self.p.mate)

    def to_pair(self):
        return send(self.src.at[1 - self.p.batch], self.block(True, self.p.c), self.sems[3], self.sems[4], self.p.pair)

    def pass_on(self):
        ref = self.block(False, self.p.c)
        return send(ref, ref, self.sems[5], self.sems[6], self.p.mate)

    def edge_out(self):
        src = self.at(jnp.where(self.p.image == 0, self.half - self.edge, 0), self.edge)
        return send(src, self.at(self.half, self.edge), self.sems[7], self.sems[8], self.p.cross)

    def tail_out(self):
        src = self.at(self.half - self.tail, self.tail)
        dst = self.at(self.half + self.edge, self.tail)
        return send(src, dst, self.sems[7], self.sems[8], self.p.cross)

    def edge_mate(self):
        ref = self.at(self.half, self.edge)
        return send(ref, ref, self.sems[9], self.sems[10], self.p.mate)

    def tail_mate(self):
        ref = self.at(self.half + self.edge, self.tail)
        return send(ref, ref, self.sems[9], self.sems[10], self.p.mate)

    def start(self):
        self.to_pair().start()
        self.to_mate().start()
        self.own().start()

    def forward(self):
        ref = self.block(False, self.p.c)
        send(ref, ref, self.sems[3], self.sems[4], self.p.pair).wait_recv()
        self.pass_on().start()

    def main_ready(self):
        self.own().wait()
        ref = self.block(True, 1 - self.p.c)
        send(ref, ref, self.sems[1], self.sems[2], self.p.mate).wait_recv()
        ref = self.block(False, 1 - self.p.c)
        send(ref, ref, self.sems[5], self.sems[6], self.p.mate).wait_recv()

    def edges(self):
        pl.when(self.p.c == 0)(lambda: self.edge_out().start())
        pl.when(self.p.c == 1)(lambda: self.tail_out().start())

    def edges_forward(self):
        @pl.when(self.p.c == 0)
        def _():
            self.edge_out().wait_recv()
            self.edge_mate().start()

        @pl.when(self.p.c == 1)
        def _():
            self.tail_out().wait_recv()
            self.tail_mate().start()

    def edges_ready(self):
        pl.when(self.p.c == 0)(lambda: self.tail_mate().wait_recv())
        pl.when(self.p.c == 1)(lambda: self.edge_mate().wait_recv())

    def drain(self):
        self.to_mate().wait_send()
        self.to_pair().wait_send()
        self.pass_on().wait_send()

        @pl.when(self.p.c == 0)
        def _():
            self.edge_out().wait_send()
            self.edge_mate().wait_send()

        @pl.when(self.p.c == 1)
        def _():
            self.tail_out().wait_send()
            self.tail_mate().wait_send()


def row_tiles(rows, step, body):
    def one(t, carry):
        body(pl.ds(pl.multiple_of(t * step, 16), step))
        return carry

    lax.fori_loop(0, rows // step, one, 0)


def forward_kernel(*refs, cols, unit_rest, edge, tail, tile):
    (small_ref, up_ref, down_ref, vec_ref, x_src, c_src, gain_ref, shift_ref, segc_ref, segr_ref) = refs[:10]
    own_ref = refs[10]
    (ws, wu, wd, gd) = refs[11:15]
    (x_ref, c_ref, vec_all, first_ref, qkv_ref, ctx_ref, inv_ref, res_ref, second_ref) = refs[15:24]
    (hidden_ref, slope_ref, hidden_rest, slope_rest, rest_up, rest_down) = refs[24:30]
    (blocks, unit_blocks, grads, part, part_out, part_in, bias_rest) = refs[30:37]
    gather_sems, local_sem = refs[37 : 37 + Gather.SEMS], refs[37 + Gather.SEMS]
    tail_refs = refs[38 + Gather.SEMS :]
    row_sems, (vec_s, vec_r, load_sem, part_s, part_r, unit_sem, grad_sem) = tail_refs[: Rows.SEMS], tail_refs[Rows.SEMS :]
    main, rest = up_ref.shape[1], unit_rest
    rows, width = x_ref.shape
    place = Place()
    place.barrier()
    shards = (small_ref, up_ref, down_ref)
    g = Gather(place, shards, (ws, wu, wd), gather_sems, local_sem, small_ref.shape[0])
    each = x_src.shape[1]
    x_rows = Rows(place, 0, x_src, x_ref, row_sems, each, edge, tail)
    c_rows = Rows(place, 1, c_src, c_ref, row_sems, each, edge, tail)

    def vec_to(d):
        device = place.slot_after(d)
        return send(vec_ref, vec_all.at[place.z], vec_s.at[d], vec_r.at[d], device)

    def vec_from(d):
        ref = vec_all.at[(place.z + 4 - d) % 4]
        return send(ref, ref, vec_s.at[d], vec_r.at[d], place.slot_after(d))

    g.start_z(0)
    g.start_xy(0)
    for d in (1, 2, 3):
        vec_to(d).start()
    x_rows.start()
    vec_all[place.z] = vec_ref[...]
    g.pass_on(0, 1)
    g.corner(0, 0)
    x_rows.forward()
    g.pass_on(0, 2)
    x_rows.main_ready()
    x_rows.edges()
    g.corner(0, 1)
    x_rows.edges_forward()
    g.pass_on(0, 3)
    g.start_z(1)
    x_rows.edges_ready()

    def first(span):
        value = x_ref[span, :].astype(F32)
        out, _, _ = norm_forward(value, gain_ref[0:1, :], shift_ref[0:1, :])
        first_ref[span, :] = out.astype(BF16)

    row_tiles(rows, 128, first)
    g.corner(0, 2)
    g.corner(0, 3)
    for d in (1, 2, 3):
        vec_from(d).wait_recv()
    g.arrive(0)

    later = []
    for k in (1, 2):
        later.append(lambda k=k: g.start_xy(k))
        if k == 1:
            later.append(lambda: c_rows.start())
        for d in (1, 2, 3):
            later.append(lambda k=k, d=d: g.pass_on(k, d))
            later.append(lambda k=k, d=d: g.corner(k, d - 1))
        if k == 1:
            later.append(lambda: g.start_z(2))
            later.append(lambda: c_rows.forward())
            later.append(lambda: (c_rows.main_ready(), c_rows.edges()))
        later.append(lambda k=k: g.corner(k, 3))
        if k == 1:
            later.append(lambda: c_rows.edges_forward())

    def step(count=1):
        for _ in range(count):
            if later:
                later.pop(0)()

    step(2)

    def load(s):
        return pltpu.make_async_copy(ws.at[s], blocks.at[s % 2], load_sem.at[s % 2])

    heads = cols // DH
    rest_up[...] = jnp.zeros_like(rest_up)
    rest_down[...] = jnp.zeros_like(rest_down)
    bias_rest[...] = jnp.zeros_like(bias_rest)
    load(0).start()
    for s in range(4):
        load(s).wait()
        if s < 3:
            load(s + 1).start()
        w = blocks.at[s % 2]
        bias = vec_all[s, 0:1, : 3 * cols].astype(F32) + vec_all[s, 1:2, : 3 * cols].astype(F32)
        projected = dot_nn(first_ref[...], w[:, : 3 * cols]) + bias
        qkv_ref[s] = projected.astype(BF16)
        step()
        for head in range(heads):
            attend_head(qkv_ref, ctx_ref, inv_ref, segc_ref, segr_ref, s, head, cols, tile)
            step()
        product = dot_nt(ctx_ref[s], w[:, 3 * cols : 4 * cols])
        at = 4 * cols
        rest_up[:, s * rest : (s + 1) * rest] = w[:, at : at + rest]
        rest_down[:, s * rest : (s + 1) * rest] = w[:, at + rest : at + 2 * rest]
        bias_rest[:, s * rest : (s + 1) * rest] = vec_all[s, 2:3, main : main + rest].astype(F32)
        if s == 0:
            part[...] = product
        else:
            part[...] += product

    def halves(h):
        return pl.ds(h * (rows // 2), rows // 2)

    def exchange(h):
        src, dst = part_out.at[halves(h), :], part_in.at[halves(h), :]
        return send(src, dst, part_s.at[h], part_r.at[h], place.mate)

    for h in (0, 1):
        part_out[halves(h), :] = part[halves(h), :].astype(BF16)
        exchange(h).start()
    step()
    for h in (0, 1):
        exchange(h).wait_recv()

    def second(span):
        value = x_ref[span, :].astype(F32) + (part_out[span, :].astype(F32) + part_in[span, :].astype(F32))
        value = value + shift_ref[2:3, :]
        res_ref[span, :] = value
        out, _, _ = norm_forward(value, gain_ref[1:2, :], shift_ref[1:2, :])
        second_ref[span, :] = out.astype(BF16)

    row_tiles(rows, 128, second)
    g.arrive(1)

    def unit_load(s):
        return pltpu.make_async_copy(wu.at[s], unit_blocks.at[s % 2], unit_sem.at[s % 2])

    unit_load(0).start()
    for s in range(4):
        unit_load(s).wait()
        if s < 3:
            unit_load(s + 1).start()
        bias = vec_all[s, 2:3, :main].astype(F32)

        def units(span, s=s, bias=bias):
            hidden, slope = gelu_both(dot_nn(second_ref[span, :], unit_blocks[s % 2]) + bias)
            hidden_ref[s, span, :] = hidden.astype(BF16)
            slope_ref[s, span, :] = slope.astype(BF16)

        row_tiles(rows, tile, units)
        step()

    def units_rest(span):
        hidden, slope = gelu_both(dot_nn(second_ref[span, :], rest_up[...]) + bias_rest[...])
        hidden_rest[span, :] = hidden.astype(BF16)
        slope_rest[span, :] = slope.astype(BF16)

    row_tiles(rows, tile, units_rest)
    step()
    c_rows.edges_ready()
    c_rows.drain()
    c_ref[...] = jnp.where(own_ref[...] > 0, c_ref[...], jnp.zeros_like(c_ref))

    def grad_out(s):
        return pltpu.make_async_copy(grads.at[s % 2], gd.at[s], grad_sem.at[s % 2])

    def down_grad(s, carry):
        pl.when(s >= 2)(lambda: grad_out(s - 2).wait())
        grads[s % 2] = dot_tn(c_ref[...], hidden_ref[s]).astype(BF16)
        grad_out(s).start()
        return carry

    lax.fori_loop(0, 2, down_grad, 0)
    step()
    lax.fori_loop(2, 4, down_grad, 0)
    step(len(later))
    for s in (2, 3):
        grad_out(s).wait()
    g.arrive(2)
    for k in (0, 1, 2):
        g.drain(k)
    x_rows.drain()
    for d in (1, 2, 3):
        vec_to(d).wait_send()
    for h in (0, 1):
        exchange(h).wait_send()


def forward_stage(
    small, up, down, vectors, x_src, c_src, gains, shifts, segments, owned, cols, unit_rest, rows, edge, tail
):
    width, shard_rows, main = x_src.shape[2], small.shape[0], up.shape[1]
    heads, rest_lanes = cols // DH, round_up(4 * unit_rest, 128)
    vmem = pl.BlockSpec(memory_space=pltpu.VMEM)
    far = pl.BlockSpec(memory_space=pl.ANY)
    shape = jax.ShapeDtypeStruct
    dma = pltpu.SemaphoreType.DMA
    return pl.pallas_call(
        functools.partial(forward_kernel, cols=cols, unit_rest=unit_rest, edge=edge, tail=tail, tile=rows // 2),
        in_specs=[vmem] * 11,
        out_specs=[far] * 4 + [vmem] * 15,
        out_shape=[
            shape((4, width, small.shape[1]), BF16),
            shape((4, width, main), BF16),
            shape((4, width, main), BF16),
            shape((4, width, main), BF16),
            shape((rows, width), BF16),
            shape((rows, width), BF16),
            shape((4,) + vectors.shape, BF16),
            shape((rows, width), BF16),
            shape((4, rows, 3 * cols), BF16),
            shape((4, rows, cols), BF16),
            shape((4, rows, heads), F32),
            shape((rows, width), F32),
            shape((rows, width), BF16),
            shape((4, rows, main), BF16),
            shape((4, rows, main), BF16),
            shape((rows, rest_lanes), BF16),
            shape((rows, rest_lanes), BF16),
            shape((width, rest_lanes), BF16),
            shape((width, rest_lanes), BF16),
        ],
        scratch_shapes=[
            pltpu.VMEM((2, width, small.shape[1]), BF16),
            pltpu.VMEM((2, width, main), BF16),
            pltpu.VMEM((2, width, main), BF16),
            pltpu.VMEM((rows, width), F32),
            pltpu.VMEM((rows, width), BF16),
            pltpu.VMEM((rows, width), BF16),
            pltpu.VMEM((1, rest_lanes), F32),
        ]
        + [dma((3, 4))] * Gather.SEMS
        + [dma((3,))]
        + [dma((2,))] * Rows.SEMS
        + [dma((4,)), dma((4,)), dma((2,)), dma((2,)), dma((2,)), dma((2,)), dma((2,))],
        compiler_params=pltpu.CompilerParams(collective_id=1, has_side_effects=True, vmem_limit_bytes=64000000),
        name="forward",
    )(
        small, up, down, vectors, x_src, c_src, gains, shifts, segments[:, None], segments[None, :],
        owned[:, None].astype(jnp.int32),
    )


def middle_kernel(*refs, cols, unit_rest):
    (wd, wu, gd) = refs[:3]
    (hidden_ref, slope_ref, hidden_rest, slope_rest, rest_up, rest_down) = refs[3:9]
    (c_ref, second_ref, res_ref, gain_ref, shift_ref) = refs[9:14]
    gu = refs[14]
    (d_out, rest_sums, half_ref, grad_ref, y_ref, sums_ref, unit_ref, unit_rest_ref) = refs[15:23]
    (blocks, grads, pre_half, part, part_out, part_in, part_in2) = refs[23:30]
    d_bufs, d_own = refs[30:35], refs[35:38]
    refs = refs[38:]
    sems, loads = refs[: Reduce.SEMS], refs[Reduce.SEMS : Reduce.SEMS + 3]
    load_sem, grad_sem, part_s, part_r = refs[Reduce.SEMS + 3 :]
    rows, width = c_ref.shape
    rest = unit_rest
    place = Place()
    place.barrier()
    r = Reduce(place, (gd,), (d_own,), (d_out,), (d_bufs,), sems, loads, d_out.shape[0])

    def load(w, slot, buffer):
        return pltpu.make_async_copy(w.at[slot], blocks.at[buffer], load_sem.at[buffer])

    def halves(h):
        return pl.ds(h * (rows // 2), rows // 2)

    def exchange(n, h):
        dst = (part_in, part_in2)[n]
        src, dst = part_out.at[halves(h), :], dst.at[halves(h), :]
        return send(src, dst, part_s.at[n, h], part_r.at[n, h], place.mate)

    load(wd, 0, 0).start()
    r.start(0)
    part[...] = dot_nt(hidden_rest[...], rest_down[...])
    grad_rest = slope_rest[...].astype(F32) * dot_nn(c_ref[...], rest_down[...])
    unit_rest_ref[...] = jnp.sum(grad_rest, axis=0, keepdims=True)
    half_rest = grad_rest.astype(BF16)

    def down_block(s, carry):
        load(wd, s, s % 2).wait()
        pl.when(s < 3)(lambda: load(wd, s + 1, (s + 1) % 2).start())
        pl.when(s == 3)(lambda: load(wu, 0, 0).start())
        w = blocks[s % 2]
        part[...] += dot_nt(hidden_ref[s], w)
        grad = slope_ref[s].astype(F32) * dot_nn(c_ref[...], w)
        pre_half[s] = grad.astype(BF16)
        unit_ref[s] = jnp.broadcast_to(jnp.sum(grad, axis=0, keepdims=True), unit_ref.shape[1:])
        r.middle_one(0, s)
        return carry

    lax.fori_loop(0, 4, down_block, 0)
    for h in (0, 1):
        part_out[halves(h), :] = part[halves(h), :].astype(BF16)
        exchange(0, h).start()
    up_sum = dot_tn(second_ref[...], half_rest).astype(BF16)
    down_sum = dot_tn(c_ref[...], hidden_rest[...]).astype(BF16)
    rest_sums[...] = jnp.zeros_like(rest_sums)
    for s in range(4):
        rest_sums[s, :, :rest] = up_sum[:, s * rest : (s + 1) * rest]
        rest_sums[s, :, rest : 2 * rest] = down_sum[:, s * rest : (s + 1) * rest]
    part[...] = dot_nt(half_rest, rest_up[...])

    def grad_out(s):
        return pltpu.make_async_copy(grads.at[s % 2], gu.at[s], grad_sem.at[s % 2])

    def up_block(s, carry):
        load(wu, s, s % 2).wait()
        pl.when(s < 3)(lambda: load(wu, s + 1, (s + 1) % 2).start())
        part[...] += dot_nt(pre_half[s], blocks[s % 2])
        pl.when(s >= 2)(lambda: grad_out(s - 2).wait())
        grads[s % 2] = dot_tn(second_ref[...], pre_half[s]).astype(BF16)
        grad_out(s).start()
        pl.when(s >= 2)(lambda: r.line_one(0, s - 2))
        return carry

    lax.fori_loop(0, 4, up_block, 0)
    for h in (0, 1):
        exchange(0, h).wait_recv()

    def output(span):
        value = part_out[span, :].astype(F32) + part_in[span, :].astype(F32)
        y_ref[span, :] = (res_ref[span, :] + value + shift_ref[3:4, :]).astype(BF16)

    row_tiles(rows, 128, output)
    for h in (0, 1):
        exchange(0, h).wait_send()
        part_out[halves(h), :] = part[halves(h), :].astype(BF16)
        exchange(1, h).start()
    r.line_one(0, 2)
    r.line_one(0, 3)
    for h in (0, 1):
        exchange(1, h).wait_recv()
    sums_ref[...] = jnp.zeros_like(sums_ref)

    def back(span):
        grad = part_out[span, :].astype(F32) + part_in2[span, :].astype(F32)
        upstream = c_ref[span, :].astype(F32)
        _, scaled, factor = norm_forward(res_ref[span, :], gain_ref[1:2, :], shift_ref[1:2, :])
        value = upstream + norm_backward(grad, scaled, factor, gain_ref[1:2, :])
        grad_ref[span, :] = value
        half_ref[span, :] = value.astype(BF16)
        sums_ref[1:2, :] += jnp.sum(grad * scaled, axis=0, keepdims=True)
        sums_ref[3:4, :] += jnp.sum(grad, axis=0, keepdims=True)
        sums_ref[4:5, :] += jnp.sum(value, axis=0, keepdims=True)
        sums_ref[5:6, :] += jnp.sum(upstream, axis=0, keepdims=True)

    row_tiles(rows, 128, back)
    for s in (2, 3):
        grad_out(s).wait()
    r.drain(0)
    for h in (0, 1):
        exchange(1, h).wait_send()


def middle_stage(
    wd, wu, gd, hidden, slope, hidden_rest, slope_rest, rest_up, rest_down, cot, second, residual, gains, shifts, cols, unit_rest, spare
):
    rows, width = cot.shape
    main, shard_rows = wd.shape[2], width // 4
    vmem = pl.BlockSpec(memory_space=pltpu.VMEM)
    far = pl.BlockSpec(memory_space=pl.ANY)
    shape = jax.ShapeDtypeStruct
    dma = pltpu.SemaphoreType.DMA
    return pl.pallas_call(
        functools.partial(middle_kernel, cols=cols, unit_rest=unit_rest),
        in_specs=[far] * 3 + [vmem] * 11,
        out_specs=[far] + [vmem] * 8,
        out_shape=[
            shape((4, width, main), BF16),
            shape((shard_rows, main), F32),
            shape((4, width, 2 * unit_rest + spare), BF16),
            shape((rows, width), BF16),
            shape((rows, width), F32),
            shape((rows, width), BF16),
            shape((8, width), F32),
            shape((4, 8, main), F32),
            shape((1, rest_up.shape[1]), F32),
        ],
        scratch_shapes=[
            pltpu.VMEM((2, width, main), BF16),
            pltpu.VMEM((2, width, main), BF16),
            pltpu.VMEM((4, rows, main), BF16),
            pltpu.VMEM((rows, width), F32),
            pltpu.VMEM((rows, width), BF16),
            pltpu.VMEM((rows, width), BF16),
            pltpu.VMEM((rows, width), BF16),
        ]
        + reduce_buffers(shard_rows, main)
        + reduce_terms(shard_rows, main)
        + [dma((1, 4))] * Reduce.SEMS
        + [dma((1, 4))] * 3
        + [dma((2,)), dma((2,)), dma((2, 2)), dma((2, 2))],
        compiler_params=pltpu.CompilerParams(collective_id=3, has_side_effects=True, vmem_limit_bytes=64000000),
        name="middle",
    )(wd, wu, gd, hidden, slope, hidden_rest, slope_rest, rest_up, rest_down, cot, second, residual, gains, shifts)


class Reduce:
    SEMS = 16

    def __init__(self, place, g, own, out, bufs, sems, load_sems, rows):
        self.p, self.g, self.own, self.out, self.rows = place, g, own, out, rows
        self.bufs, self.sems, self.load_sems = bufs, sems, load_sems

    def grad(self, k, slot, owner, half=None):
        at, count = owner * self.rows, self.rows
        if half is not None:
            count = count // 2
            at = at + half * count
        return self.g[k].at[slot, pl.ds(pl.multiple_of(at, 16), count), :]

    def terms(self, k, slot):
        f = self.p.f
        if self.own[k] is None:
            return self.grad(k, slot, f ^ 1, 0), self.grad(k, slot, f ^ 2, 1), self.grad(k, slot, f)
        return tuple(ref.at[slot] for ref in self.own[k])

    def loads(self, k, slot):
        f = self.p.f
        src = self.grad(k, slot, f ^ 1, 0), self.grad(k, slot, f ^ 2, 1), self.grad(k, slot, f)
        pairs = zip(src, self.terms(k, slot), self.load_sems)
        return [pltpu.make_async_copy(one, dst, sem.at[k, slot]) for one, dst, sem in pairs]

    def half(self, ref, slot, half):
        count = self.rows // 2
        return ref.at[slot, half * count : (half + 1) * count, :]

    def copy(self, k, slot, src, dst, index, device):
        return send(src, dst, self.sems[2 * index].at[k, slot], self.sems[2 * index + 1].at[k, slot], device)

    def corner_y(self, k, s):
        return self.copy(k, s, self.grad(k, s, self.p.f ^ 3, 0), self.bufs[k][0].at[s], 0, self.p.across_y)

    def corner_x(self, k, s):
        return self.copy(k, s, self.grad(k, s, self.p.f ^ 3, 1), self.bufs[k][1].at[s], 1, self.p.across_x)

    def x_low(self, k, s):
        return self.copy(k, s, self.bufs[k][0].at[s], self.half(self.bufs[k][2], s, 0), 2, self.p.across_x)

    def x_high(self, k, s):
        dst = self.half(self.bufs[k][2], s, 1)
        return self.copy(k, s, self.grad(k, s, self.p.f ^ 1, 1), dst, 3, self.p.across_x)

    def y_low(self, k, s):
        dst = self.half(self.bufs[k][3], s, 0)
        return self.copy(k, s, self.grad(k, s, self.p.f ^ 2, 0), dst, 4, self.p.across_y)

    def y_high(self, k, s):
        return self.copy(k, s, self.bufs[k][1].at[s], self.half(self.bufs[k][3], s, 1), 5, self.p.across_y)

    def up(self, k, s):
        return self.copy(k, s, self.bufs[k][2].at[s], self.bufs[k][4].at[s], 6, self.p.above)

    def down(self, k, s):
        at = jnp.where(s == self.p.z - 1, 4, s)
        return self.copy(k, s, self.bufs[k][2].at[s], self.bufs[k][4].at[at], 7, self.p.below)

    def from_above(self, k, s):
        at = jnp.where(s == self.p.z, 4, s)
        return self.copy(k, s, self.bufs[k][4].at[at], self.bufs[k][4].at[at], 7, self.p.below), at

    def start_one(self, k, s):
        self.corner_y(k, s).start()
        self.corner_x(k, s).start()
        self.y_low(k, s).start()
        self.x_high(k, s).start()

    def start(self, k):
        def one(i, carry):
            self.start_one(k, self.p.far_first(i))
            return carry

        lax.fori_loop(0, 4, one, 0)
        if self.own[k] is not None:
            for slot in range(4):
                for load in self.loads(k, slot):
                    load.start()

    def tiles(self, rows, body):
        row_tiles(rows, 48 if rows % 48 == 0 else 16, body)

    def middle_one(self, k, i):
        s, count = self.p.far_first(i), self.rows // 2
        low, high = self.bufs[k][0], self.bufs[k][1]
        if self.own[k] is not None:
            for load in self.loads(k, s):
                load.wait()
        own_low, own_high, _ = self.terms(k, s)
        self.corner_y(k, s).wait_recv()

        def add_low(span):
            low[s, span, :] = add_half(low[s, span, :], own_low[span, :])

        self.tiles(count, add_low)
        self.corner_x(k, s).wait_recv()

        def add_high(span):
            high[s, span, :] = add_half(high[s, span, :], own_high[span, :])

        self.tiles(count, add_high)
        self.x_low(k, s).start()
        self.y_high(k, s).start()

    def line_one(self, k, i):
        z, acc, side, far = self.p.z, self.bufs[k][2], self.bufs[k][3], self.bufs[k][4]
        s = self.p.far_first(i)
        self.x_low(k, s).wait_recv()
        self.x_high(k, s).wait_recv()
        self.y_low(k, s).wait_recv()
        self.y_high(k, s).wait_recv()
        own = self.terms(k, s)[2]

        def add(span):
            total = own[span, :].astype(F32) + acc[s, span, :].astype(F32) + side[s, span, :].astype(F32)
            acc[s, span, :] = total.astype(BF16)

        self.tiles(self.rows, add)

        def add_far(at):
            def body(span):
                acc[s, span, :] = add_half(acc[s, span, :], far[at, span, :])

            self.tiles(self.rows, body)

        @pl.when((z > 0) & (s >= z))
        def _():
            self.up(k, s).wait_recv()
            add_far(s)

        @pl.when((z < 3) & (s <= z))
        def _():
            copy, at = self.from_above(k, s)
            copy.wait_recv()
            add_far(at)

        @pl.when(s > z)
        def _():
            self.up(k, s).start()

        @pl.when(s < z)
        def _():
            self.down(k, s).start()

        @pl.when(s == z)
        def _():
            def final(span):
                self.out[k][span, :] = acc[s, span, :].astype(F32)

            self.tiles(self.rows, final)

    def loop(self, one):
        def body(i, carry):
            one(i)
            return carry

        lax.fori_loop(0, 4, body, 0)

    def drain(self, k):
        def one(s):
            for copy in (self.corner_y, self.corner_x, self.x_low, self.x_high, self.y_low, self.y_high):
                copy(k, s).wait_send()

            @pl.when(s > self.p.z)
            def _():
                self.up(k, s).wait_send()

            @pl.when(s < self.p.z)
            def _():
                self.down(k, s).wait_send()

        self.loop(one)


def reduce_buffers(rows, lanes):
    half, whole = pltpu.VMEM((4, rows // 2, lanes), BF16), pltpu.VMEM((4, rows, lanes), BF16)
    return [half, half, whole, whole, pltpu.VMEM((5, rows, lanes), BF16)]


def reduce_terms(rows, lanes):
    half, whole = pltpu.VMEM((4, rows // 2, lanes), BF16), pltpu.VMEM((4, rows, lanes), BF16)
    return [half, half, whole]


def scatter_grads(chunks):
    count = lax.axis_size("fy") * lax.axis_size("fx")
    split = [c.reshape(c.shape[0] * count, c.shape[1] // count, c.shape[2]) for c in chunks]
    return [lax.psum_scatter(c, ("slot",) + FSDP, scatter_dimension=0).astype(F32) for c in split]


class RowsBack:
    SEMS = 7

    def __init__(self, place, index, window, inbox, owned, out, sems, rows_each, edge, tail):
        self.p, self.window, self.inbox, self.owned, self.out = place, window, inbox, owned, out
        self.each, self.half, self.edge, self.tail = rows_each, 4 * rows_each, edge, tail
        self.sems = [sem.at[index] for sem in sems]

    def edge_out(self):
        src = self.window.at[self.half : self.half + self.edge, :]
        return send(src, self.inbox.at[: self.edge, :], self.sems[0], self.sems[1], self.p.cross)

    def tail_out(self):
        src = self.window.at[self.half + self.edge :, :]
        return send(src, self.inbox.at[self.edge :, :], self.sems[2], self.sems[3], self.p.cross)

    def block(self, near):
        batch = self.p.batch if near else 1 - self.p.batch
        row = (2 * batch + self.p.c) * self.each
        return self.window.at[pl.ds(pl.multiple_of(row, 16), self.each), :]

    def stay(self):
        return pltpu.make_async_copy(self.block(True), self.out.at[self.p.batch], self.sems[4])

    def to_pair(self):
        return send(self.block(False), self.out.at[self.p.batch], self.sems[5], self.sems[6], self.p.pair)

    def edges(self):
        pl.when(self.p.c == self.p.image)(lambda: self.edge_out().start())
        pl.when((self.p.c == 1) & (self.p.image == 0))(lambda: self.tail_out().start())

    def merge(self, row, count, at):
        keep = self.owned[row : row + count, :] > 0
        value = jnp.where(keep, self.window[row : row + count, :], self.inbox[at : at + count, :])
        self.window[row : row + count, :] = value

    def finish(self):
        p = self.p

        @pl.when((p.c == 1) & (p.image == 0))
        def _():
            self.edge_out().wait_recv()
            self.merge(self.half - self.edge, self.edge, 0)

        @pl.when((p.c == 0) & (p.image == 1))
        def _():
            self.edge_out().wait_recv()
            self.merge(0, self.edge, 0)

        @pl.when((p.c == 1) & (p.image == 1))
        def _():
            self.tail_out().wait_recv()
            self.merge(self.half - self.tail, self.tail, self.edge)

        self.to_pair().start()
        self.stay().start()

    def drain(self):
        pl.when(self.p.c == self.p.image)(lambda: self.edge_out().wait_send())
        pl.when((self.p.c == 1) & (self.p.image == 0))(lambda: self.tail_out().wait_send())
        self.stay().wait()
        self.to_pair().wait_send()
        ref = self.out.at[1 - self.p.batch]
        send(ref, ref, self.sems[5], self.sems[6], self.p.pair).wait_recv()


def backward_kernel(*refs, cols, unit_rest, edge, tail, tile):
    (ws, gu, rest_ref, half_ref, first_ref, qkv_ref, ctx_ref, inv_ref, segc_ref, segr_ref) = refs[:10]
    (x_ref, res_grad_ref, y_ref, gain_ref, own_ref, old_sums, unit_ref, unit_rest_ref) = refs[10:18]
    (u_out, s_out, x_out, y_out, sums_ref, vec_ref) = refs[18:24]
    refs = refs[24:]
    (blocks, gs, part, part_out, part_in, back_ref, grad_ref, key_acc, value_acc, inbox_x, inbox_y, y_window) = refs[:12]
    bias_ref, sums_in, vec_sum, vec_in, vec_far = refs[12:17]
    u_bufs, s_bufs, u_own = refs[17:22], refs[22:27], refs[27:30]
    refs = refs[30:]
    sems, loads, back_sems = refs[: Reduce.SEMS], refs[Reduce.SEMS : Reduce.SEMS + 3], refs[Reduce.SEMS + 3 : Reduce.SEMS + 3 + RowsBack.SEMS]
    load_sem, part_s, part_r, y_sems, sum_s, sum_r, vec_s, vec_r = refs[Reduce.SEMS + 3 + RowsBack.SEMS :]
    rows, width = half_ref.shape
    shard_rows = u_out.shape[0]
    heads = cols // DH
    place = Place()
    place.barrier()
    each = x_out.shape[1]
    r = Reduce(place, (gu, gs), (u_own, None), (u_out, s_out), (u_bufs, s_bufs), sems, loads, shard_rows)
    x_back = RowsBack(place, 0, part_in, inbox_x, own_ref, x_out, back_sems, each, edge, tail)
    y_back = RowsBack(place, 1, y_window, inbox_y, own_ref, y_out, back_sems, each, edge, tail)

    def load(i):
        return pltpu.make_async_copy(ws.at[place.far_first(i)], blocks.at[i % 2], load_sem.at[i % 2])

    y_load = pltpu.make_async_copy(y_ref, y_window, y_sems.at[0])
    y_load.start()
    load(0).start()
    r.start(0)
    y_load.wait()
    y_back.edges()

    def one_slot(i, carry):
        s = place.far_first(i)
        load(i).wait()

        @pl.when(i < 3)
        def _():
            load(i + 1).start()

        w = blocks.at[i % 2]
        back_ref[...] = dot_nn(half_ref[...], w[:, 3 * cols : 4 * cols]).astype(BF16)
        gs[s, :, 3 * cols : 4 * cols] = dot_tn(half_ref[...], ctx_ref[s]).astype(BF16)
        gs[s, :, 4 * cols :] = rest_ref[s]
        for head in range(heads):
            attend_back_head(
                qkv_ref, ctx_ref, inv_ref, back_ref, segc_ref, segr_ref, grad_ref, bias_ref, key_acc, value_acc, s, head, cols, tile
            )
            if head == 0:
                pl.when(i > 0)(lambda: r.start_one(1, place.far_first(i - 1)))
                r.middle_one(0, i)
        gs[s, :, : 3 * cols] = dot_tn(first_ref[...], grad_ref[...]).astype(BF16)
        product = dot_nt(grad_ref[...], w[:, : 3 * cols])

        @pl.when(i == 0)
        def _():
            part[...] = product

        @pl.when(i > 0)
        def _():
            part[...] += product

        @pl.when(i > 1)
        def _():
            r.line_one(0, 2 * (i - 2))
            r.line_one(0, 2 * (i - 2) + 1)

        return carry

    lax.fori_loop(0, 4, one_slot, 0)

    def halves(h):
        return pl.ds(h * (rows // 2), rows // 2)

    def exchange(h):
        src, dst = part_out.at[halves(h), :], part_in.at[halves(h), :]
        return send(src, dst, part_s.at[h], part_r.at[h], place.mate)

    for h in (0, 1):
        part_out[halves(h), :] = part[halves(h), :].astype(BF16)
        exchange(h).start()
    res_load = pltpu.make_async_copy(res_grad_ref, part, load_sem.at[0])
    res_load.start()
    r.start_one(1, place.far_first(3))
    y_back.finish()
    for h in (0, 1):
        exchange(h).wait_recv()

    res_load.wait()
    sums_ref[...] = old_sums[...]

    def last(span):
        grad = part_out[span, :].astype(F32) + part_in[span, :].astype(F32)
        value = x_ref[span, :].astype(F32)
        _, scaled, factor = norm_forward(value, gain_ref[0:1, :], gain_ref[0:1, :])
        result = part[span, :] + norm_backward(grad, scaled, factor, gain_ref[0:1, :])
        part_in[span, :] = result.astype(BF16)
        sums_ref[0:1, :] += jnp.sum(grad * scaled, axis=0, keepdims=True)
        sums_ref[2:3, :] += jnp.sum(grad, axis=0, keepdims=True)

    row_tiles(rows, 128, last)
    x_back.edges()

    vec_sum[...] = jnp.zeros_like(vec_sum)
    main = unit_ref.shape[2]
    rest = unit_rest
    for s in range(4):
        vec_sum[s, 0:1, :cols] = bias_ref[s, 0:1, :]
        vec_sum[s, 1:2, :cols] = bias_ref[s, 1:2, :]
        vec_sum[s, 2:3, :main] = unit_ref[s, 0:1, :]
        vec_sum[s, 3:4, :rest] = unit_rest_ref[:, s * rest : (s + 1) * rest]

    def across(n, device):
        return (
            send(sums_ref, sums_in.at[n], sum_s.at[n], sum_r.at[n], device),
            send(vec_sum, vec_in.at[n], vec_s.at[n], vec_r.at[n], device),
        )

    def along(d):
        there = (place.z + d) % 4
        device = place.slot_after(d)
        return (
            send(sums_ref, sums_in.at[1 + d], sum_s.at[1 + d], sum_r.at[1 + d], device),
            send(vec_sum.at[there], vec_far.at[d - 1], vec_s.at[1 + d], vec_r.at[1 + d], device),
        )

    def add_across(n, device):
        for copy in across(n, device):
            copy.wait()
        sums_ref[...] += sums_in[n]
        vec_sum[...] += vec_in[n]

    for copy in across(0, place.across_x):
        copy.start()
    r.loop(lambda i: r.middle_one(1, i))
    add_across(0, place.across_x)
    for copy in across(1, place.across_y):
        copy.start()
    x_back.finish()
    r.line_one(1, 0)
    add_across(1, place.across_y)
    for d in (1, 2, 3):
        for copy in along(d):
            copy.start()
    for i in (1, 2, 3):
        r.line_one(1, i)
    for d in (1, 2, 3):
        for copy in along(d):
            copy.wait()
    sums_ref[...] += sums_in[2] + sums_in[3] + sums_in[4]
    vec_ref[...] = vec_sum[place.z] + vec_far[0] + vec_far[1] + vec_far[2]
    for k in (0, 1):
        r.drain(k)
    x_back.drain()
    y_back.drain()
    for h in (0, 1):
        exchange(h).wait_send()


def backward_stage(
    ws, gu, rest_sums, residual_half, first_norm, qkv, context, inverse, segments, x_half, residual_grad, y_rows, gains, owned,
    sums, unit_sums, unit_rest_sums, cols, unit_rest, edge, tail, rows_each,
):
    rows, width = residual_half.shape
    shard_rows, lanes, main = width // 4, ws.shape[2], gu.shape[2]
    vmem = pl.BlockSpec(memory_space=pltpu.VMEM)
    far = pl.BlockSpec(memory_space=pl.ANY)
    shape = jax.ShapeDtypeStruct
    dma = pltpu.SemaphoreType.DMA
    wide = max(main, round_up(cols, 128))
    return pl.pallas_call(
        functools.partial(backward_kernel, cols=cols, unit_rest=unit_rest, edge=edge, tail=tail, tile=rows // 2),
        in_specs=[far] * 2 + [vmem] * 9 + [far, far] + [vmem] * 5,
        out_specs=[vmem] * 6,
        out_shape=[
            shape((shard_rows, main), F32),
            shape((shard_rows, lanes), F32),
            shape((2, rows_each, width), BF16),
            shape((2, rows_each, width), BF16),
            shape((8, width), F32),
            shape((8, wide), F32),
        ],
        scratch_shapes=[
            pltpu.VMEM((2, width, lanes), BF16),
            pltpu.VMEM((4, width, lanes), BF16),
            pltpu.VMEM((rows, width), F32),
            pltpu.VMEM((rows, width), BF16),
            pltpu.VMEM((rows, width), BF16),
            pltpu.VMEM((rows, cols), BF16),
            pltpu.VMEM((rows, 3 * cols), BF16),
            pltpu.VMEM((rows, DH), F32),
            pltpu.VMEM((rows, DH), F32),
            pltpu.VMEM((edge + tail, width), BF16),
            pltpu.VMEM((edge + tail, width), BF16),
            pltpu.VMEM((rows, width), BF16),
            pltpu.VMEM((4, 2, cols), F32),
            pltpu.VMEM((5, 8, width), F32),
            pltpu.VMEM((4, 8, wide), F32),
            pltpu.VMEM((2, 4, 8, wide), F32),
            pltpu.VMEM((3, 8, wide), F32),
        ]
        + reduce_buffers(shard_rows, main)
        + reduce_buffers(shard_rows, lanes)
        + reduce_terms(shard_rows, main)
        + [dma((2, 4))] * Reduce.SEMS
        + [dma((1, 4))] * 3
        + [dma((2,))] * RowsBack.SEMS
        + [dma((2,)), dma((2,)), dma((2,)), dma((1,)), dma((5,)), dma((5,)), dma((5,)), dma((5,))],
        compiler_params=pltpu.CompilerParams(collective_id=2, has_side_effects=True, vmem_limit_bytes=64000000),
        name="backward",
    )(
        ws, gu, rest_sums, residual_half, first_norm, qkv, context, inverse, segments[:, None], segments.reshape(2, 1, -1),
        x_half, residual_grad, y_rows, gains, owned[:, None].astype(jnp.int32), sums, unit_sums, unit_rest_sums,
    )


def attend_head(qkv_ref, ctx_ref, inv_ref, segc_ref, segr_ref, s, head, cols, tile):
    lo = head * DH
    keys = qkv_ref[s, :, cols + lo : cols + lo + DH]
    values = qkv_ref[s, :, 2 * cols + lo : 2 * cols + lo + DH]

    def one_tile(t, carry):
        span = pl.ds(pl.multiple_of(t * tile, tile), tile)
        scores = dot_nt(qkv_ref[s, span, lo : lo + DH], keys)
        allowed = segc_ref[span, :] == segr_ref[...]
        exact = jnp.where(allowed, jnp.exp2(scores * (SCALE * LOG2E)), 0.0)
        inverse = 1.0 / jnp.sum(exact, axis=1, keepdims=True)
        context = dot_nn(exact.astype(BF16), values) * inverse
        ctx_ref[s, span, lo : lo + DH] = context.astype(BF16)
        inv_ref[s, span, head : head + 1] = inverse
        return carry

    lax.fori_loop(0, qkv_ref.shape[1] // tile, one_tile, 0)


def attend_kernel(x_ref, w_ref, b_ref, segc_ref, segr_ref, qkv_ref, ctx_ref, inv_ref, part_ref, *, cols, tile):
    block = pl.program_id(0)
    projected = dot_nn(x_ref[...], w_ref[0, :, : 3 * cols]) + b_ref[0]
    qkv_ref[0] = projected.astype(BF16)
    for head in range(cols // DH):
        attend_head(qkv_ref, ctx_ref, inv_ref, segc_ref, segr_ref, 0, head, cols, tile)
    part = dot_nt(ctx_ref[0], w_ref[0, :, 3 * cols : 4 * cols])

    @pl.when(block == 0)
    def _():
        part_ref[...] = part

    @pl.when(block > 0)
    def _():
        part_ref[...] += part


def attend(first_norm, weights, bias, segments, cols, tile):
    rows, width = first_norm.shape
    slots, _, lanes = weights.shape
    heads = cols // DH
    whole = lambda shape: pl.BlockSpec(shape, lambda s: (0,) * len(shape))
    each = lambda shape: pl.BlockSpec((1,) + shape, lambda s: (s, 0, 0))
    return pl.pallas_call(
        functools.partial(attend_kernel, cols=cols, tile=tile),
        grid=(slots,),
        in_specs=[
            whole((rows, width)),
            each((width, lanes)),
            each((1, 3 * cols)),
            whole((rows, 1)),
            whole((1, rows)),
        ],
        out_specs=[each((rows, 3 * cols)), each((rows, cols)), each((rows, heads)), whole((rows, width))],
        out_shape=[
            jax.ShapeDtypeStruct((slots, rows, 3 * cols), BF16),
            jax.ShapeDtypeStruct((slots, rows, cols), BF16),
            jax.ShapeDtypeStruct((slots, rows, heads), F32),
            jax.ShapeDtypeStruct((rows, width), F32),
        ],
        cost_estimate=pl.CostEstimate(
            flops=slots * (8 * rows * width * cols + 4 * rows * rows * 256 * heads),
            bytes_accessed=slots * width * lanes * 2 + rows * width * 10,
            transcendentals=slots * heads * rows * rows,
        ),
        name="attend",
    )(first_norm, weights, bias, segments[:, None], segments[None, :])


def attend_back_head(
    qkv_ref, ctx_ref, inv_ref, back_ref, segc_ref, segr_ref, grad_ref, bias_ref, key_acc, value_acc, s, head, cols, tile
):
    lo = head * DH
    rows = back_ref.shape[0]
    ones = jnp.ones((8, DH), F32)
    keys = qkv_ref[s, :, cols + lo : cols + lo + DH]
    values = qkv_ref[s, :, 2 * cols + lo : 2 * cols + lo + DH]
    key_acc[...] = jnp.zeros_like(key_acc)
    value_acc[...] = jnp.zeros_like(value_acc)

    def one_tile(t, query_total):
        span = pl.ds(pl.multiple_of(t * tile, tile), tile)
        queries = qkv_ref[s, span, lo : lo + DH]
        back = (back_ref[span, lo : lo + DH].astype(F32) * inv_ref[s, span, head : head + 1]).astype(BF16)
        along = back.astype(F32) * ctx_ref[s, span, lo : lo + DH].astype(F32)
        delta = lax.dot_general(
            ones, along, (((1,), (1,)), ((), ())), precision=lax.Precision.HIGHEST, preferred_element_type=F32
        )[:1]
        scores = dot_nt(keys, queries)
        allowed = segc_ref[...] == segr_ref[t]
        exact = jnp.where(allowed, jnp.exp2(scores * (SCALE * LOG2E)), 0.0)
        value_acc[...] += dot_nn(exact.astype(BF16), back)
        prob_grad = dot_nt(values, back)
        score_grad = (exact * (prob_grad - delta)).astype(BF16)
        key_acc[...] += dot_nn(score_grad, queries)
        query_grad = dot_tn(score_grad, keys) * SCALE
        grad_ref[span, lo : lo + DH] = query_grad.astype(BF16)
        return query_total + jnp.sum(query_grad, axis=0, keepdims=True)

    query_total = lax.fori_loop(0, rows // tile, one_tile, jnp.zeros((1, DH), F32))
    grad_ref[:, cols + lo : cols + lo + DH] = (key_acc[...] * SCALE).astype(BF16)
    grad_ref[:, 2 * cols + lo : 2 * cols + lo + DH] = value_acc[...].astype(BF16)
    bias_ref[s, 0:1, lo : lo + DH] = query_total
    bias_ref[s, 1:2, lo : lo + DH] = jnp.sum(value_acc[...], axis=0, keepdims=True)


def attend_back_kernel(
    r_ref, w_ref, qkv_ref, ctx_ref, inv_ref, segc_ref, segr_ref, grad_ref, bias_ref, back_ref, key_acc, value_acc, *, cols, tile
):
    back_ref[...] = dot_nn(r_ref[...], w_ref[0, :, 3 * cols : 4 * cols]).astype(BF16)
    for head in range(cols // DH):
        attend_back_head(
            qkv_ref, ctx_ref, inv_ref, back_ref, segc_ref, segr_ref, grad_ref.at[0], bias_ref, key_acc, value_acc, 0, head, cols, tile
        )


def attend_back(residual_half, weights, qkv, context, inverse, segments, cols, tile):
    rows, width = residual_half.shape
    slots, _, lanes = weights.shape
    heads = cols // DH
    whole = lambda shape: pl.BlockSpec(shape, lambda s: (0,) * len(shape))
    each = lambda shape: pl.BlockSpec((1,) + shape, lambda s: (s, 0, 0))
    return pl.pallas_call(
        functools.partial(attend_back_kernel, cols=cols, tile=tile),
        grid=(slots,),
        in_specs=[
            whole((rows, width)),
            each((width, lanes)),
            each((rows, 3 * cols)),
            each((rows, cols)),
            each((rows, heads)),
            whole((rows, 1)),
            whole((rows // tile, 1, tile)),
        ],
        out_specs=[each((rows, 3 * cols)), each((2, cols))],
        out_shape=[
            jax.ShapeDtypeStruct((slots, rows, 3 * cols), BF16),
            jax.ShapeDtypeStruct((slots, 2, cols), F32),
        ],
        scratch_shapes=[
            pltpu.VMEM((rows, cols), BF16),
            pltpu.VMEM((rows, DH), F32),
            pltpu.VMEM((rows, DH), F32),
        ],
        cost_estimate=pl.CostEstimate(
            flops=slots * (2 * rows * width * cols + 10 * rows * rows * 256 * heads),
            bytes_accessed=slots * width * lanes * 2 + rows * width * 10,
            transcendentals=slots * heads * rows * rows,
        ),
        name="attend_back",
    )(residual_half, weights, qkv, context, inverse, segments[:, None], segments.reshape(-1, 1, tile))


def plain_layer(shards, vectors, to_slot, from_slot, block_input, cotangent, gains, shifts, segments, owned, cols, units, parts):
    width, rows = block_input.shape[2], segments.shape[0]
    slots, slot = lax.axis_size("slot"), lax.axis_index("slot")
    main_units, in_lanes = shards[1].shape[1], 3 * cols
    rest = units - main_units
    spare = shards[0].shape[1] - in_lanes - cols - 2 * rest
    small_all, up_main, down_main = gather_weights(shards)
    vec_all = lax.all_gather(vectors, "slot", axis=0)
    grad_rows = jnp.where(owned[:, None], to_slot(cotangent), 0)
    upstream = grad_rows.astype(F32)
    x_float = to_slot(block_input).astype(F32)
    first_out, first_scaled, first_factor = norm_forward(x_float, gains[0], shifts[0])
    first_norm = first_out.astype(BF16)
    bias = vec_all[:, :1, :in_lanes].astype(F32) + vec_all[:, 1:2, :in_lanes].astype(F32)
    qkv, context, inverse, attention_part = attend(first_norm, small_all, bias, segments, cols, rows // 2)
    residual = x_float + part_sum(attention_part, parts) + shifts[2]
    second_out, second_scaled, second_factor = norm_forward(residual, gains[1], shifts[1])
    second_norm = second_out.astype(BF16)
    small_blocks = list(small_all)
    unit_all = vec_all[:, 2, :units].astype(F32)
    at = in_lanes + cols
    ups = list(up_main) + [b[:, at : at + rest] for b in small_blocks]
    downs = list(down_main) + [b[:, at + rest : at + 2 * rest] for b in small_blocks]
    unit_rows = list(unit_all[:, :main_units]) + list(unit_all[:, main_units:])
    pre_acts = [dot_nn(second_norm, w) + b for w, b in zip(ups, unit_rows)]
    hiddens = [gelu(p).astype(BF16) for p in pre_acts]
    output = (residual + part_sum(sum_products(hiddens, downs), parts) + shifts[3]).astype(BF16)
    down_sums = [dot_tn(grad_rows, h).astype(BF16) for h in hiddens]
    pre_grads = [gelu_back(p, dot_nn(grad_rows, w)) for p, w in zip(pre_acts, downs)]
    pre_halves = [p.astype(BF16) for p in pre_grads]
    unit_sums = [jnp.sum(p, axis=0) for p in pre_grads]
    up_sums = [dot_tn(second_norm, p).astype(BF16) for p in pre_halves]
    second_grad = part_sum(sum_products(pre_halves, ups), parts)
    residual_grad = upstream + norm_backward(second_grad, second_scaled, second_factor, gains[1])
    residual_half = residual_grad.astype(BF16)
    triple, bias_sum = attend_back(residual_half, small_all, qkv, context, inverse, segments, cols, rows // 2)
    first_part = sum_products(list(triple), [b[:, :in_lanes] for b in small_blocks])
    first_grad = part_sum(first_part, parts)
    input_grad = residual_grad + norm_backward(first_grad, first_scaled, first_factor, gains[0])
    blank = jnp.zeros((width, spare), BF16)
    small_sums = [
        jnp.concatenate(
            [
                dot_tn(first_norm, triple[s]).astype(BF16),
                dot_tn(residual_half, context[s]).astype(BF16),
                up_sums[slots + s],
                down_sums[slots + s],
                blank,
            ],
            axis=1,
        )
        for s in range(slots)
    ]
    down_grad, up_grad, small_grad = scatter_grads(
        [jnp.stack(down_sums[:slots]), jnp.stack(up_sums[:slots]), jnp.stack(small_sums)]
    )
    rows_sum = jnp.stack(
        [
            jnp.sum(first_grad * first_scaled, axis=0),
            jnp.sum(second_grad * second_scaled, axis=0),
            jnp.sum(first_grad, axis=0),
            jnp.sum(second_grad, axis=0),
            jnp.sum(residual_grad, axis=0),
            jnp.sum(upstream, axis=0),
        ]
    )
    unit_sum = jnp.stack([jnp.concatenate([unit_sums[s], unit_sums[slots + s]]) for s in range(slots)])
    rows_total, bias_total, unit_total = lax.psum((rows_sum, bias_sum, unit_sum), ("slot",) + FSDP)
    bias_grad = lax.dynamic_index_in_dim(bias_total, slot, 0, keepdims=False)
    unit_grad = lax.dynamic_index_in_dim(unit_total, slot, 0, keepdims=False)
    return (
        from_slot(output, owned), from_slot(input_grad.astype(BF16), owned), rows_total, bias_grad, unit_grad,
        down_grad, up_grad, small_grad,
    )


def on_device(
    block_input,
    segment_ids,
    norm_gains,
    row_biases,
    in_projection,
    query_value_bias,
    out_projection,
    up_weight,
    unit_bias,
    down_weight,
    cotangent,
):
    local, rows_each, width = block_input.shape
    rows_mb = segment_ids.shape[1]
    cols = in_projection.shape[2]
    units = up_weight.shape[1]
    shard_rows = up_weight.shape[0]
    slots, parts = lax.axis_size("slot"), lax.axis_size("part")
    slot, part = lax.axis_index("slot"), lax.axis_index("part")
    fsdp_index = lax.axis_index("fy") * lax.axis_size("fx") + lax.axis_index("fx")
    batch, image = slot % local, slot // local
    late = image == 1

    half_rows = rows_mb // IMG_MB
    padding = rows_mb - IMG_MB * IMG
    edge = round_up(max(half_rows - IMG, padding - (half_rows - IMG)), 16)
    tail = round_up(padding, 16)
    rows = round_up(half_rows + edge + tail, 128)
    filler = rows - half_rows - edge - tail
    paired = lax.axis_size("fy") == 2 and lax.axis_size("fx") == 2 and slots == 4 and parts == 2
    paired = paired and shard_rows % 32 == 0 and filler == 0

    def edges(main):
        near = jnp.where(late, main[:edge], main[half_rows - edge :])
        far = main[half_rows - tail :]
        return jnp.concatenate([near, far])

    def to_slot(value):
        mine = lax.dynamic_index_in_dim(value, batch, 0, keepdims=False)
        send = lax.dynamic_index_in_dim(value, 1 - batch, 0, keepdims=False)
        other = slot_swap(send, 1, slots)
        pair = jnp.where(batch == 0, jnp.stack([mine, other]), jnp.stack([other, mine]))
        main = part_gather(pair, parts).swapaxes(0, 1).reshape(half_rows, width)
        beyond = slot_swap(edges(main), local, slots)
        return jnp.concatenate([main, beyond, jnp.zeros((filler, width), value.dtype)])

    def from_slot(value, owned):
        main = value[:half_rows]
        beyond = slot_swap(value[half_rows : half_rows + edge + tail], local, slots)
        keep = owned[:half_rows, None]
        near, far = beyond[:edge], beyond[edge:]
        blank = lambda count: jnp.zeros((count, width), value.dtype)
        early_fill = jnp.concatenate([blank(half_rows - edge), near])
        late_fill = jnp.concatenate([near, blank(half_rows - edge - tail), far])
        main = jnp.where(keep, main, jnp.where(late, late_fill, early_fill))
        main = main.reshape(local, parts, rows_each, width)
        mine = lax.dynamic_index_in_dim(main, part, 1, keepdims=False)
        stay = lax.dynamic_index_in_dim(mine, batch, 0, keepdims=False)
        other = slot_swap(lax.dynamic_index_in_dim(mine, 1 - batch, 0, keepdims=False), 1, slots)
        return jnp.where(batch == 0, jnp.stack([stay, other]), jnp.stack([other, stay]))

    ids = lax.dynamic_index_in_dim(segment_ids, batch, 0, keepdims=False)
    fill_ids = jnp.full((filler,), -2, jnp.int32)
    early_ids = jnp.concatenate([ids[: half_rows + edge], ids[rows_mb - tail :], fill_ids])
    late_ids = jnp.concatenate(
        [ids[half_rows:], ids[half_rows - edge : half_rows], jnp.full((tail,), -2, jnp.int32), fill_ids]
    )
    segments = jnp.where(late, late_ids, early_ids)
    image_id = (fsdp_index * local + batch) * IMG_MB + image
    owned = (segments == image_id) | (jnp.logical_not(late) & (segments == -1))

    main_units = units // 128 * 128
    rest = units - main_units
    in_lanes = 3 * cols
    small = in_lanes + cols + 2 * rest
    lanes = round_up(small, 128)
    down_t = down_weight.T
    small_shard = jnp.concatenate(
        [
            in_projection.transpose(1, 0, 2).reshape(shard_rows, in_lanes),
            out_projection.T,
            up_weight[:, main_units:],
            down_t[:, main_units:],
            jnp.zeros((shard_rows, lanes - small), BF16),
        ],
        axis=1,
    )
    shards = [small_shard, up_weight[:, :main_units], down_t[:, :main_units]]
    triple_bias = jnp.concatenate([query_value_bias[0], jnp.zeros((cols,), F32), query_value_bias[1]])
    high = triple_bias.astype(BF16)
    low = (triple_bias - high.astype(F32)).astype(BF16)
    wide = round_up(max(in_lanes, units), 128)
    vectors = [jnp.pad(v, (0, wide - v.shape[0])) for v in (high, low, unit_bias)]
    vectors = jnp.concatenate([jnp.stack(vectors), jnp.zeros((13, wide), BF16)])
    gains, shifts = norm_gains, row_biases
    if paired:
        (
            small_all, up_main, down_main, gd, x_half, cot, _, first_norm, qkv, context, inverse, residual, second_norm,
            hidden, slope, hidden_rest, slope_rest, rest_up, rest_down,
        ) = forward_stage(
            *shards, vectors, block_input, cotangent, gains, shifts, segments, owned, cols, rest, rows, edge, tail
        )
        gu, down_grad, rest_sums, residual_half, residual_grad, y_rows, sums, unit_sums, unit_rest_sums = middle_stage(
            down_main, up_main, gd, hidden, slope, hidden_rest, slope_rest, rest_up, rest_down, cot, second_norm, residual,
            gains, shifts, cols, rest, lanes - small,
        )
        up_grad, small_grad, input_grad, output, rows_total, vec_total = backward_stage(
            small_all, gu, rest_sums, residual_half, first_norm, qkv, context, inverse, segments, x_half, residual_grad,
            y_rows, gains, owned, sums, unit_sums, unit_rest_sums, cols, rest, edge, tail, rows_each,
        )
        rows_total = rows_total[:6]
        bias_grad = vec_total[:2, :cols]
        unit_grad = jnp.concatenate([vec_total[2, :main_units], vec_total[3, :rest]])
    else:
        output, input_grad, rows_total, bias_grad, unit_grad, down_grad, up_grad, small_grad = plain_layer(
            shards, vectors, to_slot, from_slot, block_input, cotangent, gains, shifts, segments, owned, cols, units, parts
        )
    in_grad = small_grad[:, :in_lanes].reshape(shard_rows, 3, cols).transpose(1, 0, 2)
    out_grad = small_grad[:, in_lanes : in_lanes + cols].T
    at = in_lanes + cols
    up_grad = jnp.concatenate([up_grad, small_grad[:, at : at + rest]], axis=1)
    down_grad = jnp.concatenate([down_grad, small_grad[:, at + rest : at + 2 * rest]], axis=1).T
    return (
        output,
        input_grad.astype(F32),
        rows_total[:2],
        rows_total[2:],
        in_grad,
        bias_grad,
        out_grad,
        up_grad,
        unit_grad,
        down_grad,
    )


def solution(mesh):
    fsdp, tensor = mesh.shape["fsdp"], mesh.shape["tensor"]

    def layer(*arrays):
        local = arrays[0].shape[0] // fsdp
        slots = local * IMG_MB
        assert local == 2 and slots == 4 and tensor % slots == 0 and fsdp % 2 == 0
        grid = Mesh(
            mesh.devices.reshape(fsdp // 2, 2, slots, tensor // slots), ("fy", "fx", "slot", "part")
        )
        tens = ("slot", "part")
        return jax.shard_map(
            on_device,
            mesh=grid,
            in_specs=(
                P(FSDP, tens, None),
                P(FSDP, None),
                P(),
                P(),
                P(None, FSDP, tens),
                P(None, tens),
                P(tens, FSDP),
                P(FSDP, tens),
                P(tens),
                P(tens, FSDP),
                P(FSDP, tens, None),
            ),
            out_specs=(
                P(FSDP, tens, None),
                P(FSDP, tens, None),
                P(),
                P(),
                P(None, FSDP, tens),
                P(None, tens),
                P(tens, FSDP),
                P(FSDP, tens),
                P(tens),
                P(tens, FSDP),
            ),
            check_vma=False,
        )(*arrays)

    return layer
```

```python
import functools
import math

import jax
import jax.numpy as jnp
from jax import lax
from jax.experimental import pallas as pl
from jax.experimental.pallas import tpu as pltpu
from jax.sharding import Mesh
from jax.sharding import PartitionSpec as P

DH = 72
IMG = 729
IMG_MB = 2
EPS = 1e-06
GELU_C = 0.7978845608028654
F32 = jnp.float32
BF16 = jnp.bfloat16
FSDP = ("fy", "fx")
SCALE = DH ** (-0.5)
LOG2E = math.log2(math.e)


def norm_forward(values, norm_gain, norm_shift):
    center = values - jnp.mean(values, axis=-1, keepdims=True)
    factor = lax.rsqrt(jnp.mean(center * center, axis=-1, keepdims=True) + EPS)
    scaled = center * factor
    return (scaled * norm_gain + norm_shift, scaled, factor)


def norm_backward(upstream, scaled, factor, norm_gain):
    inside = upstream * norm_gain
    return factor * (
        inside
        - jnp.mean(inside, axis=-1, keepdims=True)
        - scaled * jnp.mean(inside * scaled, axis=-1, keepdims=True)
    )


def gelu(pre_act):
    return (
        0.5
        * pre_act
        * (1.0 + jnp.tanh(GELU_C * (pre_act + 0.044715 * pre_act * pre_act * pre_act)))
    )


def gelu_both(pre_act):
    square = pre_act * pre_act
    curve = jnp.tanh(GELU_C * pre_act * (1.0 + 0.044715 * square))
    rise = 0.5 * (1.0 + curve)
    slope = rise + 0.5 * pre_act * (1.0 - curve * curve) * GELU_C * (1.0 + 3.0 * 0.044715 * square)
    return pre_act * rise, slope


def gelu_back(pre_act, upstream):
    return jax.vjp(gelu, pre_act)[1](upstream)[0]


def dot_nn(left, right):
    return lax.dot_general(left, right, (((1,), (0,)), ((), ())), preferred_element_type=F32)


def dot_nt(left, right):
    return lax.dot_general(left, right, (((1,), (1,)), ((), ())), preferred_element_type=F32)


def dot_tn(left, right):
    return lax.dot_general(left, right, (((0,), (0,)), ((), ())), preferred_element_type=F32)


def sum_products(lefts, rights):
    total = dot_nt(lefts[0], rights[0])
    for left, right in zip(lefts[1:], rights[1:]):
        total = total + dot_nt(left, right)
    return total


def round_up(value, unit):
    return -(-value // unit) * unit


def swap(value, axis):
    return lax.ppermute(value, axis, [(0, 1), (1, 0)])


def slot_swap(value, stride, slots):
    return lax.ppermute(value, "slot", [(s, s ^ stride) for s in range(slots)])


def part_sum(value, parts):
    value = value.astype(BF16)
    if parts == 2:
        return value.astype(F32) + swap(value, "part").astype(F32)
    return lax.psum(value.astype(F32), "part")


def part_gather(value, parts):
    if parts == 2:
        other = swap(value, "part")
        first = lax.axis_index("part") == 0
        return jnp.stack([jnp.where(first, value, other), jnp.where(first, other, value)])
    return lax.all_gather(value, "part", axis=0)


def add_half(left, right):
    return (left.astype(F32) + right.astype(F32)).astype(BF16)


MESH = pl.DeviceIdType.MESH


class Place:
    def __init__(self):
        self.y, self.x = lax.axis_index("fy"), lax.axis_index("fx")
        self.z = lax.axis_index("slot")
        self.f = 2 * self.y + self.x
        self.across_x, self.across_y = {"fx": 1 - self.x}, {"fy": 1 - self.y}
        self.c = lax.axis_index("part")
        self.above = {"slot": jnp.minimum(self.z + 1, 3)}
        self.below = {"slot": jnp.maximum(self.z - 1, 0)}
        self.batch, self.image = self.z % 2, self.z // 2
        self.mate = {"part": 1 - self.c}
        self.pair = {"slot": self.z + 1 - 2 * self.batch}
        self.cross = {"slot": self.z + 2 - 4 * self.image}

    def slot_after(self, d):
        return {"slot": (self.z + d) % 4}

    def barrier(self):
        sem = pltpu.get_barrier_semaphore()
        others = [self.across_x, self.across_y, self.mate] + [self.slot_after(d) for d in (1, 2, 3)]
        for device in others:
            pl.semaphore_signal(sem, inc=1, device_id=device, device_id_type=MESH)
        pl.semaphore_wait(sem, len(others))

    def far_first(self, i):
        low = self.z < 2
        near = jnp.where(low, self.z, 3 - self.z)
        at = jnp.where(i == 0, 3, jnp.where(i == 1, 2, jnp.where(i == 2, 1 - near, near)))
        return jnp.where(low, at, 3 - at)


def send(src, dst, send_sem, recv_sem, device):
    return pltpu.make_async_remote_copy(
        src_ref=src, dst_ref=dst, send_sem=send_sem, recv_sem=recv_sem, device_id=device, device_id_type=MESH
    )


class Gather:
    SEMS = 11

    def __init__(self, place, shards, w, sems, local_sem, rows):
        self.p, self.shards, self.w, self.rows = place, shards, w, rows
        (self.zr, self.zu, self.zd, self.xr, self.xs, self.yr, self.ys, self.ar, self.asn, self.br, self.bs) = sems
        self.local_sem = local_sem

    def block(self, k, slot, owner, half=None):
        at, count = owner * self.rows, self.rows
        if half is not None:
            count = count // 2
            at = at + half * count
        return self.w[k].at[slot, pl.ds(pl.multiple_of(at, 16), count), :]

    def mine(self, k, slot, shard):
        return self.shards[k] if shard else self.block(k, slot, self.p.f)

    def up(self, k, slot, shard=False):
        dst = self.block(k, slot, self.p.f)
        return send(self.mine(k, slot, shard), dst, self.zu.at[k, slot], self.zr.at[k, slot], self.p.above)

    def down(self, k, slot, shard=False):
        dst = self.block(k, slot, self.p.f)
        return send(self.mine(k, slot, shard), dst, self.zd.at[k, slot], self.zr.at[k, slot], self.p.below)

    def to_x(self, k, slot, shard=False):
        dst = self.block(k, slot, self.p.f)
        return send(self.mine(k, slot, shard), dst, self.xs.at[k, slot], self.xr.at[k, slot], self.p.across_x)

    def to_y(self, k, slot, shard=False):
        dst = self.block(k, slot, self.p.f)
        return send(self.mine(k, slot, shard), dst, self.ys.at[k, slot], self.yr.at[k, slot], self.p.across_y)

    def from_x(self, k, slot):
        ref = self.block(k, slot, self.p.f ^ 1)
        return send(ref, ref, self.xs.at[k, slot], self.xr.at[k, slot], self.p.across_x)

    def from_y(self, k, slot):
        ref = self.block(k, slot, self.p.f ^ 2)
        return send(ref, ref, self.ys.at[k, slot], self.yr.at[k, slot], self.p.across_y)

    def corner_y(self, k, slot):
        ref = self.block(k, slot, self.p.f ^ 1, 0)
        return send(ref, ref, self.asn.at[k, slot], self.ar.at[k, slot], self.p.across_y)

    def corner_x(self, k, slot):
        ref = self.block(k, slot, self.p.f ^ 2, 1)
        return send(ref, ref, self.bs.at[k, slot], self.br.at[k, slot], self.p.across_x)

    def wait_corner(self, k, slot):
        ref = self.block(k, slot, self.p.f ^ 3, 0)
        send(ref, ref, self.asn.at[k, slot], self.ar.at[k, slot], self.p.across_y).wait_recv()
        ref = self.block(k, slot, self.p.f ^ 3, 1)
        send(ref, ref, self.bs.at[k, slot], self.br.at[k, slot], self.p.across_x).wait_recv()

    def local(self, k):
        return pltpu.make_async_copy(self.shards[k], self.block(k, self.p.z, self.p.f), self.local_sem.at[k])

    def start_z(self, k):
        @pl.when(self.p.z < 3)
        def _():
            self.up(k, self.p.z, True).start()

        @pl.when(self.p.z > 0)
        def _():
            self.down(k, self.p.z, True).start()

    def start_xy(self, k):
        self.to_x(k, self.p.z, True).start()
        self.to_y(k, self.p.z, True).start()
        self.local(k).start()

    def pass_on(self, k, d):
        z = self.p.z

        @pl.when(z >= d)
        def _():
            self.up(k, z - d).wait_recv()

            @pl.when(z < 3)
            def _():
                self.up(k, z - d).start()

            self.to_x(k, z - d).start()
            self.to_y(k, z - d).start()

        @pl.when(z + d <= 3)
        def _():
            self.down(k, z + d).wait_recv()

            @pl.when(z > 0)
            def _():
                self.down(k, z + d).start()

            self.to_x(k, z + d).start()
            self.to_y(k, z + d).start()

    def corner(self, k, d):
        def one(slot):
            self.from_x(k, slot).wait_recv()
            self.corner_y(k, slot).start()
            self.from_y(k, slot).wait_recv()
            self.corner_x(k, slot).start()

        z = self.p.z
        if d == 0:
            one(z)
        else:
            pl.when(z >= d)(lambda: one(z - d))
            pl.when(z + d <= 3)(lambda: one(z + d))

    def arrive(self, k):
        self.local(k).wait()
        for slot in range(4):
            self.wait_corner(k, slot)

    def drain(self, k):
        z = self.p.z
        for slot in range(4):
            self.to_x(k, slot).wait_send()
            self.to_y(k, slot).wait_send()
            self.corner_y(k, slot).wait_send()
            self.corner_x(k, slot).wait_send()

            @pl.when((z < 3) & (slot <= z))
            def _(slot=slot):
                self.up(k, slot).wait_send()

            @pl.when((z > 0) & (slot >= z))
            def _(slot=slot):
                self.down(k, slot).wait_send()


def gather_weights(shards):
    slots = lax.axis_size("slot")
    whole = [lax.all_gather(s, ("slot",) + FSDP, axis=0) for s in shards]
    return [w.reshape(slots, -1, w.shape[-1]) for w in whole]


class Rows:
    SEMS = 11

    def __init__(self, place, index, src, dst, sems, rows_each, edge, tail):
        self.p, self.src, self.dst, self.each = place, src, dst, rows_each
        self.half = 4 * rows_each
        self.edge, self.tail = edge, tail
        self.sems = [sem.at[index] for sem in sems]

    def at(self, row, count):
        return self.dst.at[pl.ds(pl.multiple_of(row, 16), count), :]

    def block(self, near, core):
        batch = self.p.batch if near else 1 - self.p.batch
        return self.at((2 * batch + core) * self.each, self.each)

    def own(self):
        return pltpu.make_async_copy(self.src.at[self.p.batch], self.block(True, self.p.c), self.sems[0])

    def to_mate(self):
        return send(self.src.at[self.p.batch], self.block(True, self.p.c), self.sems[1], self.sems[2], self.p.mate)

    def to_pair(self):
        return send(self.src.at[1 - self.p.batch], self.block(True, self.p.c), self.sems[3], self.sems[4], self.p.pair)

    def pass_on(self):
        ref = self.block(False, self.p.c)
        return send(ref, ref, self.sems[5], self.sems[6], self.p.mate)

    def edge_out(self):
        src = self.at(jnp.where(self.p.image == 0, self.half - self.edge, 0), self.edge)
        return send(src, self.at(self.half, self.edge), self.sems[7], self.sems[8], self.p.cross)

    def tail_out(self):
        src = self.at(self.half - self.tail, self.tail)
        dst = self.at(self.half + self.edge, self.tail)
        return send(src, dst, self.sems[7], self.sems[8], self.p.cross)

    def edge_mate(self):
        ref = self.at(self.half, self.edge)
        return send(ref, ref, self.sems[9], self.sems[10], self.p.mate)

    def tail_mate(self):
        ref = self.at(self.half + self.edge, self.tail)
        return send(ref, ref, self.sems[9], self.sems[10], self.p.mate)

    def start(self):
        self.to_pair().start()
        self.to_mate().start()
        self.own().start()

    def forward(self):
        ref = self.block(False, self.p.c)
        send(ref, ref, self.sems[3], self.sems[4], self.p.pair).wait_recv()
        self.pass_on().start()

    def main_ready(self):
        self.own().wait()
        ref = self.block(True, 1 - self.p.c)
        send(ref, ref, self.sems[1], self.sems[2], self.p.mate).wait_recv()
        ref = self.block(False, 1 - self.p.c)
        send(ref, ref, self.sems[5], self.sems[6], self.p.mate).wait_recv()

    def edges(self):
        pl.when(self.p.c == 0)(lambda: self.edge_out().start())
        pl.when(self.p.c == 1)(lambda: self.tail_out().start())

    def edges_forward(self):
        @pl.when(self.p.c == 0)
        def _():
            self.edge_out().wait_recv()
            self.edge_mate().start()

        @pl.when(self.p.c == 1)
        def _():
            self.tail_out().wait_recv()
            self.tail_mate().start()

    def edges_ready(self):
        pl.when(self.p.c == 0)(lambda: self.tail_mate().wait_recv())
        pl.when(self.p.c == 1)(lambda: self.edge_mate().wait_recv())

    def drain(self):
        self.to_mate().wait_send()
        self.to_pair().wait_send()
        self.pass_on().wait_send()

        @pl.when(self.p.c == 0)
        def _():
            self.edge_out().wait_send()
            self.edge_mate().wait_send()

        @pl.when(self.p.c == 1)
        def _():
            self.tail_out().wait_send()
            self.tail_mate().wait_send()


def row_tiles(rows, step, body):
    def one(t, carry):
        body(pl.ds(pl.multiple_of(t * step, 16), step))
        return carry

    lax.fori_loop(0, rows // step, one, 0)


def forward_kernel(*refs, cols, unit_rest, edge, tail, tile):
    (small_ref, up_ref, down_ref, vec_ref, x_src, c_src, gain_ref, shift_ref, segc_ref, segr_ref) = refs[:10]
    own_ref = refs[10]
    (ws, wu, wd, gd) = refs[11:15]
    outs, refs = refs[15:29], refs[29:]
    held, refs = refs[:14], refs[14:]
    (x_ref, c_ref, first_ref, qkv_ref, ctx_ref, inv_ref, res_ref, second_ref) = held[:8]
    (hidden_ref, slope_ref, hidden_rest, slope_rest, rest_up, rest_down) = held[8:]
    (blocks, unit_blocks, grads, part, part_out, part_in, bias_rest, vec_all) = refs[:8]
    gather_sems, local_sem = refs[8 : 8 + Gather.SEMS], refs[8 + Gather.SEMS]
    tail_refs = refs[9 + Gather.SEMS :]
    row_sems = tail_refs[: Rows.SEMS]
    (vec_s, vec_r, load_sem, part_s, part_r, unit_sem, grad_sem, out_sem) = tail_refs[Rows.SEMS :]

    def leave(n):
        return pltpu.make_async_copy(held[n], outs[n], out_sem.at[n])

    main, rest = up_ref.shape[1], unit_rest
    rows, width = x_ref.shape
    place = Place()
    place.barrier()
    shards = (small_ref, up_ref, down_ref)
    g = Gather(place, shards, (ws, wu, wd), gather_sems, local_sem, small_ref.shape[0])
    each = x_src.shape[1]
    x_rows = Rows(place, 0, x_src, x_ref, row_sems, each, edge, tail)
    c_rows = Rows(place, 1, c_src, c_ref, row_sems, each, edge, tail)

    def vec_to(d):
        device = place.slot_after(d)
        return send(vec_ref, vec_all.at[place.z], vec_s.at[d], vec_r.at[d], device)

    def vec_from(d):
        ref = vec_all.at[(place.z + 4 - d) % 4]
        return send(ref, ref, vec_s.at[d], vec_r.at[d], place.slot_after(d))

    g.start_z(0)
    g.start_xy(0)
    for d in (1, 2, 3):
        vec_to(d).start()
    x_rows.start()
    vec_all[place.z] = vec_ref[...]
    g.pass_on(0, 1)
    g.corner(0, 0)
    x_rows.forward()
    g.pass_on(0, 2)
    x_rows.main_ready()
    x_rows.edges()
    g.corner(0, 1)
    x_rows.edges_forward()
    g.pass_on(0, 3)
    g.start_z(1)
    x_rows.edges_ready()

    def first(span):
        value = x_ref[span, :].astype(F32)
        out, _, _ = norm_forward(value, gain_ref[0:1, :], shift_ref[0:1, :])
        first_ref[span, :] = out.astype(BF16)

    row_tiles(rows, 128, first)
    leave(0).start()
    g.corner(0, 2)
    g.corner(0, 3)
    leave(2).start()
    for d in (1, 2, 3):
        vec_from(d).wait_recv()
    g.arrive(0)

    later = []
    for k in (1, 2):
        later.append(lambda k=k: g.start_xy(k))
        if k == 1:
            later.append(lambda: c_rows.start())
        for d in (1, 2, 3):
            later.append(lambda k=k, d=d: g.pass_on(k, d))
            later.append(lambda k=k, d=d: g.corner(k, d - 1))
        if k == 1:
            later.append(lambda: g.start_z(2))
            later.append(lambda: c_rows.forward())
            later.append(lambda: (c_rows.main_ready(), c_rows.edges()))
        later.append(lambda k=k: g.corner(k, 3))
        if k == 1:
            later.append(lambda: c_rows.edges_forward())

    def step(count=1):
        for _ in range(count):
            if later:
                later.pop(0)()

    step(2)

    def load(s):
        return pltpu.make_async_copy(ws.at[s], blocks.at[s % 2], load_sem.at[s % 2])

    heads = cols // DH
    rest_up[...] = jnp.zeros_like(rest_up)
    rest_down[...] = jnp.zeros_like(rest_down)
    bias_rest[...] = jnp.zeros_like(bias_rest)
    load(0).start()
    for s in range(4):
        load(s).wait()
        if s < 3:
            load(s + 1).start()
        w = blocks.at[s % 2]
        bias = vec_all[s, 0:1, : 3 * cols].astype(F32) + vec_all[s, 1:2, : 3 * cols].astype(F32)
        projected = dot_nn(first_ref[...], w[:, : 3 * cols]) + bias
        qkv_ref[s] = projected.astype(BF16)
        step()
        for head in range(heads):
            attend_head(qkv_ref, ctx_ref, inv_ref, segc_ref, segr_ref, s, head, cols, tile)
            step()
        product = dot_nt(ctx_ref[s], w[:, 3 * cols : 4 * cols])
        at = 4 * cols
        rest_up[:, s * rest : (s + 1) * rest] = w[:, at : at + rest]
        rest_down[:, s * rest : (s + 1) * rest] = w[:, at + rest : at + 2 * rest]
        bias_rest[:, s * rest : (s + 1) * rest] = vec_all[s, 2:3, main : main + rest].astype(F32)
        if s == 0:
            part[...] = product
        else:
            part[...] += product

    def halves(h):
        return pl.ds(h * (rows // 2), rows // 2)

    def exchange(h):
        src, dst = part_out.at[halves(h), :], part_in.at[halves(h), :]
        return send(src, dst, part_s.at[h], part_r.at[h], place.mate)

    for h in (0, 1):
        part_out[halves(h), :] = part[halves(h), :].astype(BF16)
        exchange(h).start()
    step()
    for n in (3, 4, 5, 12, 13):
        leave(n).start()
    for h in (0, 1):
        exchange(h).wait_recv()

    def second(span):
        value = x_ref[span, :].astype(F32) + (part_out[span, :].astype(F32) + part_in[span, :].astype(F32))
        value = value + shift_ref[2:3, :]
        res_ref[span, :] = value
        out, _, _ = norm_forward(value, gain_ref[1:2, :], shift_ref[1:2, :])
        second_ref[span, :] = out.astype(BF16)

    row_tiles(rows, 128, second)
    g.arrive(1)

    def unit_load(s):
        return pltpu.make_async_copy(wu.at[s], unit_blocks.at[s % 2], unit_sem.at[s % 2])

    unit_load(0).start()
    for s in range(4):
        unit_load(s).wait()
        if s < 3:
            unit_load(s + 1).start()
        bias = vec_all[s, 2:3, :main].astype(F32)

        def units(span, s=s, bias=bias):
            hidden, slope = gelu_both(dot_nn(second_ref[span, :], unit_blocks[s % 2]) + bias)
            hidden_ref[s, span, :] = hidden.astype(BF16)
            slope_ref[s, span, :] = slope.astype(BF16)

        row_tiles(rows, tile, units)
        step()

    def units_rest(span):
        hidden, slope = gelu_both(dot_nn(second_ref[span, :], rest_up[...]) + bias_rest[...])
        hidden_rest[span, :] = hidden.astype(BF16)
        slope_rest[span, :] = slope.astype(BF16)

    for n in (6, 7):
        leave(n).start()
    row_tiles(rows, tile, units_rest)
    step()
    for n in (8, 9, 10, 11):
        leave(n).start()
    c_rows.edges_ready()
    c_rows.drain()
    c_ref[...] = jnp.where(own_ref[...] > 0, c_ref[...], jnp.zeros_like(c_ref))

    def grad_out(s):
        return pltpu.make_async_copy(grads.at[s % 2], gd.at[s], grad_sem.at[s % 2])

    def down_grad(s, carry):
        pl.when(s >= 2)(lambda: grad_out(s - 2).wait())
        grads[s % 2] = dot_tn(c_ref[...], hidden_ref[s]).astype(BF16)
        grad_out(s).start()
        return carry

    lax.fori_loop(0, 2, down_grad, 0)
    step()
    lax.fori_loop(2, 4, down_grad, 0)
    step(len(later))
    leave(1).start()
    for s in (2, 3):
        grad_out(s).wait()
    g.arrive(2)
    for n in range(14):
        leave(n).wait()
    for k in (0, 1, 2):
        g.drain(k)
    x_rows.drain()
    for d in (1, 2, 3):
        vec_to(d).wait_send()
    for h in (0, 1):
        exchange(h).wait_send()


def forward_stage(
    small, up, down, vectors, x_src, c_src, gains, shifts, segments, owned, cols, unit_rest, rows, edge, tail
):
    width, shard_rows, main = x_src.shape[2], small.shape[0], up.shape[1]
    heads, rest_lanes = cols // DH, round_up(4 * unit_rest, 128)
    vmem = pl.BlockSpec(memory_space=pltpu.VMEM)
    far = pl.BlockSpec(memory_space=pl.ANY)
    shape = jax.ShapeDtypeStruct
    dma = pltpu.SemaphoreType.DMA
    return pl.pallas_call(
        functools.partial(forward_kernel, cols=cols, unit_rest=unit_rest, edge=edge, tail=tail, tile=rows // 2),
        in_specs=[vmem] * 11,
        out_specs=[far] * 18,
        out_shape=[
            shape((4, width, small.shape[1]), BF16),
            shape((4, width, main), BF16),
            shape((4, width, main), BF16),
            shape((4, width, main), BF16),
            shape((rows, width), BF16),
            shape((rows, width), BF16),
            shape((rows, width), BF16),
            shape((4, rows, 3 * cols), BF16),
            shape((4, rows, cols), BF16),
            shape((4, rows, heads), F32),
            shape((rows, width), F32),
            shape((rows, width), BF16),
            shape((4, rows, main), BF16),
            shape((4, rows, main), BF16),
            shape((rows, rest_lanes), BF16),
            shape((rows, rest_lanes), BF16),
            shape((width, rest_lanes), BF16),
            shape((width, rest_lanes), BF16),
        ],
        scratch_shapes=[
            pltpu.VMEM((rows, width), BF16),
            pltpu.VMEM((rows, width), BF16),
            pltpu.VMEM((rows, width), BF16),
            pltpu.VMEM((4, rows, 3 * cols), BF16),
            pltpu.VMEM((4, rows, cols), BF16),
            pltpu.VMEM((4, rows, heads), F32),
            pltpu.VMEM((rows, width), F32),
            pltpu.VMEM((rows, width), BF16),
            pltpu.VMEM((4, rows, main), BF16),
            pltpu.VMEM((4, rows, main), BF16),
            pltpu.VMEM((rows, rest_lanes), BF16),
            pltpu.VMEM((rows, rest_lanes), BF16),
            pltpu.VMEM((width, rest_lanes), BF16),
            pltpu.VMEM((width, rest_lanes), BF16),
            pltpu.VMEM((2, width, small.shape[1]), BF16),
            pltpu.VMEM((2, width, main), BF16),
            pltpu.VMEM((2, width, main), BF16),
            pltpu.VMEM((rows, width), F32),
            pltpu.VMEM((rows, width), BF16),
            pltpu.VMEM((rows, width), BF16),
            pltpu.VMEM((1, rest_lanes), F32),
            pltpu.VMEM((4,) + vectors.shape, BF16),
        ]
        + [dma((3, 4))] * Gather.SEMS
        + [dma((3,))]
        + [dma((2,))] * Rows.SEMS
        + [dma((4,)), dma((4,)), dma((2,)), dma((2,)), dma((2,)), dma((2,)), dma((2,)), dma((14,))],
        compiler_params=pltpu.CompilerParams(collective_id=1, has_side_effects=True, vmem_limit_bytes=64000000),
        name="forward",
    )(
        small, up, down, vectors, x_src, c_src, gains, shifts, segments[:, None], segments[None, :],
        owned[:, None].astype(jnp.int32),
    )


def middle_kernel(*refs, cols, unit_rest):
    (wd, wu, gd) = refs[:3]
    (hidden_far, slope_far, hidden_rest, slope_rest, rest_up, rest_down) = refs[3:9]
    (c_far, second_far, res_far, gain_ref, shift_ref) = refs[9:14]
    gu = refs[14]
    (d_out, rest_sums, half_ref, grad_ref, y_ref, sums_ref, unit_ref, unit_rest_ref) = refs[15:23]
    (blocks, grads, pre_half, part, part_out, part_in, part_in2) = refs[23:30]
    (hidden_ref, slope_ref, c_ref, second_ref, res_ref) = refs[30:35]
    d_bufs, d_own = refs[35:40], refs[40:43]
    refs = refs[43:]
    sems, loads = refs[: Reduce.SEMS], refs[Reduce.SEMS : Reduce.SEMS + 3]
    load_sem, grad_sem, part_s, part_r, in_sem, unit_sem = refs[Reduce.SEMS + 3 :]
    rows, width = c_ref.shape
    rest = unit_rest
    place = Place()
    place.barrier()
    r = Reduce(place, (gd,), (d_own,), (d_out,), (d_bufs,), sems, loads, d_out.shape[0])

    def load(w, slot, buffer):
        return pltpu.make_async_copy(w.at[slot], blocks.at[buffer], load_sem.at[buffer])

    def halves(h):
        return pl.ds(h * (rows // 2), rows // 2)

    def exchange(n, h):
        dst = (part_in, part_in2)[n]
        src, dst = part_out.at[halves(h), :], dst.at[halves(h), :]
        return send(src, dst, part_s.at[n, h], part_r.at[n, h], place.mate)

    def enter(n):
        far, near = ((c_far, c_ref), (second_far, second_ref), (res_far, res_ref))[n]
        return pltpu.make_async_copy(far, near, in_sem.at[n])

    def unit_loads(s):
        return (
            pltpu.make_async_copy(hidden_far.at[s], hidden_ref.at[s % 2], unit_sem.at[0, s % 2]),
            pltpu.make_async_copy(slope_far.at[s], slope_ref.at[s % 2], unit_sem.at[1, s % 2]),
        )

    def start_units(s):
        for copy in unit_loads(s):
            copy.start()

    enter(0).start()
    load(wd, 0, 0).start()
    start_units(0)
    r.start(0)
    enter(1).start()
    enter(2).start()
    enter(0).wait()
    part[...] = dot_nt(hidden_rest[...], rest_down[...])
    grad_rest = slope_rest[...].astype(F32) * dot_nn(c_ref[...], rest_down[...])
    unit_rest_ref[...] = jnp.sum(grad_rest, axis=0, keepdims=True)
    half_rest = grad_rest.astype(BF16)

    def down_block(s, carry):
        load(wd, s, s % 2).wait()
        pl.when(s < 3)(lambda: load(wd, s + 1, (s + 1) % 2).start())
        pl.when(s == 3)(lambda: load(wu, 0, 0).start())
        for copy in unit_loads(s):
            copy.wait()
        pl.when(s < 3)(lambda: start_units(s + 1))
        w = blocks[s % 2]
        part[...] += dot_nt(hidden_ref[s % 2], w)
        grad = slope_ref[s % 2].astype(F32) * dot_nn(c_ref[...], w)
        pre_half[s] = grad.astype(BF16)
        unit_ref[s] = jnp.broadcast_to(jnp.sum(grad, axis=0, keepdims=True), unit_ref.shape[1:])
        r.middle_one(0, s)
        return carry

    lax.fori_loop(0, 4, down_block, 0)
    for h in (0, 1):
        part_out[halves(h), :] = part[halves(h), :].astype(BF16)
        exchange(0, h).start()
    enter(1).wait()
    enter(2).wait()
    up_sum = dot_tn(second_ref[...], half_rest).astype(BF16)
    down_sum = dot_tn(c_ref[...], hidden_rest[...]).astype(BF16)
    rest_sums[...] = jnp.zeros_like(rest_sums)
    for s in range(4):
        rest_sums[s, :, :rest] = up_sum[:, s * rest : (s + 1) * rest]
        rest_sums[s, :, rest : 2 * rest] = down_sum[:, s * rest : (s + 1) * rest]
    part[...] = dot_nt(half_rest, rest_up[...])

    def grad_out(s):
        return pltpu.make_async_copy(grads.at[s % 2], gu.at[s], grad_sem.at[s % 2])

    def up_block(s, carry):
        load(wu, s, s % 2).wait()
        pl.when(s < 3)(lambda: load(wu, s + 1, (s + 1) % 2).start())
        part[...] += dot_nt(pre_half[s], blocks[s % 2])
        pl.when(s >= 2)(lambda: grad_out(s - 2).wait())
        grads[s % 2] = dot_tn(second_ref[...], pre_half[s]).astype(BF16)
        grad_out(s).start()
        pl.when(s >= 2)(lambda: r.line_one(0, s - 2))
        return carry

    lax.fori_loop(0, 4, up_block, 0)
    for h in (0, 1):
        exchange(0, h).wait_recv()

    def output(span):
        value = part_out[span, :].astype(F32) + part_in[span, :].astype(F32)
        y_ref[span, :] = (res_ref[span, :] + value + shift_ref[3:4, :]).astype(BF16)

    row_tiles(rows, 128, output)
    for h in (0, 1):
        exchange(0, h).wait_send()
        part_out[halves(h), :] = part[halves(h), :].astype(BF16)
        exchange(1, h).start()
    r.line_one(0, 2)
    r.line_one(0, 3)
    for h in (0, 1):
        exchange(1, h).wait_recv()
    sums_ref[...] = jnp.zeros_like(sums_ref)

    def back(span):
        grad = part_out[span, :].astype(F32) + part_in2[span, :].astype(F32)
        upstream = c_ref[span, :].astype(F32)
        _, scaled, factor = norm_forward(res_ref[span, :], gain_ref[1:2, :], shift_ref[1:2, :])
        value = upstream + norm_backward(grad, scaled, factor, gain_ref[1:2, :])
        grad_ref[span, :] = value
        half_ref[span, :] = value.astype(BF16)
        sums_ref[1:2, :] += jnp.sum(grad * scaled, axis=0, keepdims=True)
        sums_ref[3:4, :] += jnp.sum(grad, axis=0, keepdims=True)
        sums_ref[4:5, :] += jnp.sum(value, axis=0, keepdims=True)
        sums_ref[5:6, :] += jnp.sum(upstream, axis=0, keepdims=True)

    row_tiles(rows, 128, back)
    for s in (2, 3):
        grad_out(s).wait()
    r.drain(0)
    for h in (0, 1):
        exchange(1, h).wait_send()


def middle_stage(
    wd, wu, gd, hidden, slope, hidden_rest, slope_rest, rest_up, rest_down, cot, second, residual, gains, shifts, cols, unit_rest, spare
):
    rows, width = cot.shape
    main, shard_rows = wd.shape[2], width // 4
    vmem = pl.BlockSpec(memory_space=pltpu.VMEM)
    far = pl.BlockSpec(memory_space=pl.ANY)
    shape = jax.ShapeDtypeStruct
    dma = pltpu.SemaphoreType.DMA
    return pl.pallas_call(
        functools.partial(middle_kernel, cols=cols, unit_rest=unit_rest),
        in_specs=[far] * 5 + [vmem] * 4 + [far] * 3 + [vmem] * 2,
        out_specs=[far] + [vmem] * 8,
        out_shape=[
            shape((4, width, main), BF16),
            shape((shard_rows, main), F32),
            shape((4, width, 2 * unit_rest + spare), BF16),
            shape((rows, width), BF16),
            shape((rows, width), F32),
            shape((rows, width), BF16),
            shape((8, width), F32),
            shape((4, 8, main), F32),
            shape((1, rest_up.shape[1]), F32),
        ],
        scratch_shapes=[
            pltpu.VMEM((2, width, main), BF16),
            pltpu.VMEM((2, width, main), BF16),
            pltpu.VMEM((4, rows, main), BF16),
            pltpu.VMEM((rows, width), F32),
            pltpu.VMEM((rows, width), BF16),
            pltpu.VMEM((rows, width), BF16),
            pltpu.VMEM((rows, width), BF16),
            pltpu.VMEM((2, rows, main), BF16),
            pltpu.VMEM((2, rows, main), BF16),
            pltpu.VMEM((rows, width), BF16),
            pltpu.VMEM((rows, width), BF16),
            pltpu.VMEM((rows, width), F32),
        ]
        + reduce_buffers(shard_rows, main)
        + reduce_terms(shard_rows, main)
        + [dma((1, 4))] * Reduce.SEMS
        + [dma((1, 4))] * 3
        + [dma((2,)), dma((2,)), dma((2, 2)), dma((2, 2)), dma((3,)), dma((2, 2))],
        compiler_params=pltpu.CompilerParams(collective_id=3, has_side_effects=True, vmem_limit_bytes=64000000),
        name="middle",
    )(wd, wu, gd, hidden, slope, hidden_rest, slope_rest, rest_up, rest_down, cot, second, residual, gains, shifts)


class Reduce:
    SEMS = 16

    def __init__(self, place, g, own, out, bufs, sems, load_sems, rows):
        self.p, self.g, self.own, self.out, self.rows = place, g, own, out, rows
        self.bufs, self.sems, self.load_sems = bufs, sems, load_sems

    def grad(self, k, slot, owner, half=None):
        at, count = owner * self.rows, self.rows
        if half is not None:
            count = count // 2
            at = at + half * count
        return self.g[k].at[slot, pl.ds(pl.multiple_of(at, 16), count), :]

    def terms(self, k, slot):
        f = self.p.f
        if self.own[k] is None:
            return self.grad(k, slot, f ^ 1, 0), self.grad(k, slot, f ^ 2, 1), self.grad(k, slot, f)
        return tuple(ref.at[slot] for ref in self.own[k])

    def loads(self, k, slot):
        f = self.p.f
        src = self.grad(k, slot, f ^ 1, 0), self.grad(k, slot, f ^ 2, 1), self.grad(k, slot, f)
        pairs = zip(src, self.terms(k, slot), self.load_sems)
        return [pltpu.make_async_copy(one, dst, sem.at[k, slot]) for one, dst, sem in pairs]

    def half(self, ref, slot, half):
        count = self.rows // 2
        return ref.at[slot, half * count : (half + 1) * count, :]

    def copy(self, k, slot, src, dst, index, device):
        return send(src, dst, self.sems[2 * index].at[k, slot], self.sems[2 * index + 1].at[k, slot], device)

    def corner_y(self, k, s):
        return self.copy(k, s, self.grad(k, s, self.p.f ^ 3, 0), self.bufs[k][0].at[s], 0, self.p.across_y)

    def corner_x(self, k, s):
        return self.copy(k, s, self.grad(k, s, self.p.f ^ 3, 1), self.bufs[k][1].at[s], 1, self.p.across_x)

    def x_low(self, k, s):
        return self.copy(k, s, self.bufs[k][0].at[s], self.half(self.bufs[k][2], s, 0), 2, self.p.across_x)

    def x_high(self, k, s):
        dst = self.half(self.bufs[k][2], s, 1)
        return self.copy(k, s, self.grad(k, s, self.p.f ^ 1, 1), dst, 3, self.p.across_x)

    def y_low(self, k, s):
        dst = self.half(self.bufs[k][3], s, 0)
        return self.copy(k, s, self.grad(k, s, self.p.f ^ 2, 0), dst, 4, self.p.across_y)

    def y_high(self, k, s):
        return self.copy(k, s, self.bufs[k][1].at[s], self.half(self.bufs[k][3], s, 1), 5, self.p.across_y)

    def up(self, k, s):
        return self.copy(k, s, self.bufs[k][2].at[s], self.bufs[k][4].at[s], 6, self.p.above)

    def down(self, k, s):
        at = jnp.where(s == self.p.z - 1, 4, s)
        return self.copy(k, s, self.bufs[k][2].at[s], self.bufs[k][4].at[at], 7, self.p.below)

    def from_above(self, k, s):
        at = jnp.where(s == self.p.z, 4, s)
        return self.copy(k, s, self.bufs[k][4].at[at], self.bufs[k][4].at[at], 7, self.p.below), at

    def start_one(self, k, s):
        self.corner_y(k, s).start()
        self.corner_x(k, s).start()
        self.y_low(k, s).start()
        self.x_high(k, s).start()

    def start(self, k):
        def one(i, carry):
            self.start_one(k, self.p.far_first(i))
            return carry

        lax.fori_loop(0, 4, one, 0)
        if self.own[k] is not None:
            for slot in range(4):
                for load in self.loads(k, slot):
                    load.start()

    def tiles(self, rows, body):
        row_tiles(rows, 48 if rows % 48 == 0 else 16, body)

    def middle_one(self, k, i):
        s, count = self.p.far_first(i), self.rows // 2
        low, high = self.bufs[k][0], self.bufs[k][1]
        if self.own[k] is not None:
            for load in self.loads(k, s):
                load.wait()
        own_low, own_high, _ = self.terms(k, s)
        self.corner_y(k, s).wait_recv()

        def add_low(span):
            low[s, span, :] = add_half(low[s, span, :], own_low[span, :])

        self.tiles(count, add_low)
        self.corner_x(k, s).wait_recv()

        def add_high(span):
            high[s, span, :] = add_half(high[s, span, :], own_high[span, :])

        self.tiles(count, add_high)
        self.x_low(k, s).start()
        self.y_high(k, s).start()

    def line_one(self, k, i):
        z, acc, side, far = self.p.z, self.bufs[k][2], self.bufs[k][3], self.bufs[k][4]
        s = self.p.far_first(i)
        self.x_low(k, s).wait_recv()
        self.x_high(k, s).wait_recv()
        self.y_low(k, s).wait_recv()
        self.y_high(k, s).wait_recv()
        own = self.terms(k, s)[2]

        def add(span):
            total = own[span, :].astype(F32) + acc[s, span, :].astype(F32) + side[s, span, :].astype(F32)
            acc[s, span, :] = total.astype(BF16)

        self.tiles(self.rows, add)

        def add_far(at):
            def body(span):
                acc[s, span, :] = add_half(acc[s, span, :], far[at, span, :])

            self.tiles(self.rows, body)

        @pl.when((z > 0) & (s >= z))
        def _():
            self.up(k, s).wait_recv()
            add_far(s)

        @pl.when((z < 3) & (s <= z))
        def _():
            copy, at = self.from_above(k, s)
            copy.wait_recv()
            add_far(at)

        @pl.when(s > z)
        def _():
            self.up(k, s).start()

        @pl.when(s < z)
        def _():
            self.down(k, s).start()

        @pl.when(s == z)
        def _():
            def final(span):
                self.out[k][span, :] = acc[s, span, :].astype(F32)

            self.tiles(self.rows, final)

    def loop(self, one):
        def body(i, carry):
            one(i)
            return carry

        lax.fori_loop(0, 4, body, 0)

    def drain(self, k):
        def one(s):
            for copy in (self.corner_y, self.corner_x, self.x_low, self.x_high, self.y_low, self.y_high):
                copy(k, s).wait_send()

            @pl.when(s > self.p.z)
            def _():
                self.up(k, s).wait_send()

            @pl.when(s < self.p.z)
            def _():
                self.down(k, s).wait_send()

        self.loop(one)


def reduce_buffers(rows, lanes):
    half, whole = pltpu.VMEM((4, rows // 2, lanes), BF16), pltpu.VMEM((4, rows, lanes), BF16)
    return [half, half, whole, whole, pltpu.VMEM((5, rows, lanes), BF16)]


def reduce_terms(rows, lanes):
    half, whole = pltpu.VMEM((4, rows // 2, lanes), BF16), pltpu.VMEM((4, rows, lanes), BF16)
    return [half, half, whole]


def scatter_grads(chunks):
    count = lax.axis_size("fy") * lax.axis_size("fx")
    split = [c.reshape(c.shape[0] * count, c.shape[1] // count, c.shape[2]) for c in chunks]
    return [lax.psum_scatter(c, ("slot",) + FSDP, scatter_dimension=0).astype(F32) for c in split]


class RowsBack:
    SEMS = 7

    def __init__(self, place, index, window, inbox, owned, out, sems, rows_each, edge, tail):
        self.p, self.window, self.inbox, self.owned, self.out = place, window, inbox, owned, out
        self.each, self.half, self.edge, self.tail = rows_each, 4 * rows_each, edge, tail
        self.sems = [sem.at[index] for sem in sems]

    def edge_out(self):
        src = self.window.at[self.half : self.half + self.edge, :]
        return send(src, self.inbox.at[: self.edge, :], self.sems[0], self.sems[1], self.p.cross)

    def tail_out(self):
        src = self.window.at[self.half + self.edge :, :]
        return send(src, self.inbox.at[self.edge :, :], self.sems[2], self.sems[3], self.p.cross)

    def block(self, near):
        batch = self.p.batch if near else 1 - self.p.batch
        row = (2 * batch + self.p.c) * self.each
        return self.window.at[pl.ds(pl.multiple_of(row, 16), self.each), :]

    def stay(self):
        return pltpu.make_async_copy(self.block(True), self.out.at[self.p.batch], self.sems[4])

    def to_pair(self):
        return send(self.block(False), self.out.at[self.p.batch], self.sems[5], self.sems[6], self.p.pair)

    def edges(self):
        pl.when(self.p.c == self.p.image)(lambda: self.edge_out().start())
        pl.when((self.p.c == 1) & (self.p.image == 0))(lambda: self.tail_out().start())

    def merge(self, row, count, at):
        keep = self.owned[row : row + count, :] > 0
        value = jnp.where(keep, self.window[row : row + count, :], self.inbox[at : at + count, :])
        self.window[row : row + count, :] = value

    def finish(self):
        p = self.p

        @pl.when((p.c == 1) & (p.image == 0))
        def _():
            self.edge_out().wait_recv()
            self.merge(self.half - self.edge, self.edge, 0)

        @pl.when((p.c == 0) & (p.image == 1))
        def _():
            self.edge_out().wait_recv()
            self.merge(0, self.edge, 0)

        @pl.when((p.c == 1) & (p.image == 1))
        def _():
            self.tail_out().wait_recv()
            self.merge(self.half - self.tail, self.tail, self.edge)

        self.to_pair().start()
        self.stay().start()

    def drain(self):
        pl.when(self.p.c == self.p.image)(lambda: self.edge_out().wait_send())
        pl.when((self.p.c == 1) & (self.p.image == 0))(lambda: self.tail_out().wait_send())
        self.stay().wait()
        self.to_pair().wait_send()
        ref = self.out.at[1 - self.p.batch]
        send(ref, ref, self.sems[5], self.sems[6], self.p.pair).wait_recv()


def backward_kernel(*refs, cols, unit_rest, edge, tail, tile):
    (ws, gu, rest_ref, half_ref, first_far, qkv_far, ctx_far, inv_far, segc_ref, segr_ref) = refs[:10]
    (x_far, res_grad_ref, y_ref, gain_ref, own_ref, old_sums, unit_ref, unit_rest_ref) = refs[10:18]
    (u_out, s_out, x_out, y_out, sums_ref, vec_ref) = refs[18:24]
    refs = refs[24:]
    (blocks, gs, part, part_out, part_in, back_ref, grad_ref, key_acc, value_acc, inbox_x, inbox_y, y_window) = refs[:12]
    bias_ref, sums_in, vec_sum, vec_in, vec_far = refs[12:17]
    first_ref, qkv_ref, ctx_ref, inv_ref, x_ref = refs[17:22]
    u_bufs, s_bufs, u_own = refs[22:27], refs[27:32], refs[32:35]
    refs = refs[35:]
    sems, loads, back_sems = refs[: Reduce.SEMS], refs[Reduce.SEMS : Reduce.SEMS + 3], refs[Reduce.SEMS + 3 : Reduce.SEMS + 3 + RowsBack.SEMS]
    load_sem, part_s, part_r, y_sems, sum_s, sum_r, vec_s, vec_r, in_sem = refs[Reduce.SEMS + 3 + RowsBack.SEMS :]
    rows, width = half_ref.shape
    shard_rows = u_out.shape[0]
    heads = cols // DH
    place = Place()
    place.barrier()
    each = x_out.shape[1]
    r = Reduce(place, (gu, gs), (u_own, None), (u_out, s_out), (u_bufs, s_bufs), sems, loads, shard_rows)
    x_back = RowsBack(place, 0, part_in, inbox_x, own_ref, x_out, back_sems, each, edge, tail)
    y_back = RowsBack(place, 1, y_window, inbox_y, own_ref, y_out, back_sems, each, edge, tail)

    def load(i):
        return pltpu.make_async_copy(ws.at[place.far_first(i)], blocks.at[i % 2], load_sem.at[i % 2])

    y_load = pltpu.make_async_copy(y_ref, y_window, y_sems.at[0])
    def slot_loads(i):
        s = place.far_first(i)
        pairs = ((qkv_far, qkv_ref), (ctx_far, ctx_ref), (inv_far, inv_ref))
        return [pltpu.make_async_copy(p[0].at[s], p[1].at[s], in_sem.at[n, i]) for n, p in enumerate(pairs)]

    first_load = pltpu.make_async_copy(first_far, first_ref, y_sems.at[1])
    x_load = pltpu.make_async_copy(x_far, x_ref, y_sems.at[2])
    load(0).start()
    for copy in slot_loads(0):
        copy.start()
    y_load.start()
    r.start(0)
    first_load.start()
    for i in (1, 2, 3):
        for copy in slot_loads(i):
            copy.start()
    x_load.start()
    y_load.wait()
    y_back.edges()

    def one_slot(i, carry):
        s = place.far_first(i)
        load(i).wait()
        for copy in slot_loads(i):
            copy.wait()

        @pl.when(i < 3)
        def _():
            load(i + 1).start()

        w = blocks.at[i % 2]
        back_ref[...] = dot_nn(half_ref[...], w[:, 3 * cols : 4 * cols]).astype(BF16)
        gs[s, :, 3 * cols : 4 * cols] = dot_tn(half_ref[...], ctx_ref[s]).astype(BF16)
        gs[s, :, 4 * cols :] = rest_ref[s]
        for head in range(heads):
            attend_back_head(
                qkv_ref, ctx_ref, inv_ref, back_ref, segc_ref, segr_ref, grad_ref, bias_ref, key_acc, value_acc, s, head, cols, tile
            )
            if head == 0:
                r.middle_one(0, i)
                pl.when(i == 1)(lambda: y_back.finish())
        pl.when(i == 0)(lambda: first_load.wait())
        gs[s, :, : 3 * cols] = dot_tn(first_ref[...], grad_ref[...]).astype(BF16)
        product = dot_nt(grad_ref[...], w[:, : 3 * cols])

        @pl.when(i == 0)
        def _():
            part[...] = product

        @pl.when(i > 0)
        def _():
            part[...] += product

        r.start_one(1, s)
        pl.when(i > 0)(lambda: r.line_one(0, i - 1))
        pl.when(i > 0)(lambda: r.middle_one(1, i - 1))
        return carry

    lax.fori_loop(0, 4, one_slot, 0)

    def halves(h):
        return pl.ds(h * (rows // 2), rows // 2)

    def exchange(h):
        src, dst = part_out.at[halves(h), :], part_in.at[halves(h), :]
        return send(src, dst, part_s.at[h], part_r.at[h], place.mate)

    for h in (0, 1):
        part_out[halves(h), :] = part[halves(h), :].astype(BF16)
        exchange(h).start()
    res_load = pltpu.make_async_copy(res_grad_ref, part, load_sem.at[0])
    res_load.start()
    r.line_one(0, 3)
    pl.when((place.z == 0) | (place.z == 3))(lambda: r.line_one(1, 0))
    for h in (0, 1):
        exchange(h).wait_recv()

    res_load.wait()
    x_load.wait()
    sums_ref[...] = old_sums[...]

    def last(span):
        grad = part_out[span, :].astype(F32) + part_in[span, :].astype(F32)
        value = x_ref[span, :].astype(F32)
        _, scaled, factor = norm_forward(value, gain_ref[0:1, :], gain_ref[0:1, :])
        result = part[span, :] + norm_backward(grad, scaled, factor, gain_ref[0:1, :])
        part_in[span, :] = result.astype(BF16)
        sums_ref[0:1, :] += jnp.sum(grad * scaled, axis=0, keepdims=True)
        sums_ref[2:3, :] += jnp.sum(grad, axis=0, keepdims=True)

    row_tiles(rows, 128, last)
    x_back.edges()

    vec_sum[...] = jnp.zeros_like(vec_sum)
    main = unit_ref.shape[2]
    rest = unit_rest
    for s in range(4):
        vec_sum[s, 0:1, :cols] = bias_ref[s, 0:1, :]
        vec_sum[s, 1:2, :cols] = bias_ref[s, 1:2, :]
        vec_sum[s, 2:3, :main] = unit_ref[s, 0:1, :]
        vec_sum[s, 3:4, :rest] = unit_rest_ref[:, s * rest : (s + 1) * rest]

    def across(n, device):
        return (
            send(sums_ref, sums_in.at[n], sum_s.at[n], sum_r.at[n], device),
            send(vec_sum, vec_in.at[n], vec_s.at[n], vec_r.at[n], device),
        )

    def along(d):
        there = (place.z + d) % 4
        device = place.slot_after(d)
        return (
            send(sums_ref, sums_in.at[1 + d], sum_s.at[1 + d], sum_r.at[1 + d], device),
            send(vec_sum.at[there], vec_far.at[d - 1], vec_s.at[1 + d], vec_r.at[1 + d], device),
        )

    def add_across(n, device):
        for copy in across(n, device):
            copy.wait()
        sums_ref[...] += sums_in[n]
        vec_sum[...] += vec_in[n]

    for copy in across(0, place.across_x):
        copy.start()
    r.middle_one(1, 3)
    pl.when((place.z == 1) | (place.z == 2))(lambda: r.line_one(1, 0))
    r.line_one(1, 1)
    add_across(0, place.across_x)
    for copy in across(1, place.across_y):
        copy.start()
    x_back.finish()
    r.line_one(1, 2)
    add_across(1, place.across_y)
    for d in (1, 2, 3):
        for copy in along(d):
            copy.start()
    r.line_one(1, 3)
    for d in (1, 2, 3):
        for copy in along(d):
            copy.wait()
    sums_ref[...] += sums_in[2] + sums_in[3] + sums_in[4]
    vec_ref[...] = vec_sum[place.z] + vec_far[0] + vec_far[1] + vec_far[2]
    for k in (0, 1):
        r.drain(k)
    x_back.drain()
    y_back.drain()
    for h in (0, 1):
        exchange(h).wait_send()


def backward_stage(
    ws, gu, rest_sums, residual_half, first_norm, qkv, context, inverse, segments, x_half, residual_grad, y_rows, gains, owned,
    sums, unit_sums, unit_rest_sums, cols, unit_rest, edge, tail, rows_each,
):
    rows, width = residual_half.shape
    shard_rows, lanes, main = width // 4, ws.shape[2], gu.shape[2]
    vmem = pl.BlockSpec(memory_space=pltpu.VMEM)
    far = pl.BlockSpec(memory_space=pl.ANY)
    shape = jax.ShapeDtypeStruct
    dma = pltpu.SemaphoreType.DMA
    wide = max(main, round_up(cols, 128))
    return pl.pallas_call(
        functools.partial(backward_kernel, cols=cols, unit_rest=unit_rest, edge=edge, tail=tail, tile=rows // 2),
        in_specs=[far] * 2 + [vmem] * 2 + [far] * 4 + [vmem] * 2 + [far] * 3 + [vmem] * 5,
        out_specs=[vmem] * 6,
        out_shape=[
            shape((shard_rows, main), F32),
            shape((shard_rows, lanes), F32),
            shape((2, rows_each, width), BF16),
            shape((2, rows_each, width), BF16),
            shape((8, width), F32),
            shape((8, wide), F32),
        ],
        scratch_shapes=[
            pltpu.VMEM((2, width, lanes), BF16),
            pltpu.VMEM((4, width, lanes), BF16),
            pltpu.VMEM((rows, width), F32),
            pltpu.VMEM((rows, width), BF16),
            pltpu.VMEM((rows, width), BF16),
            pltpu.VMEM((rows, cols), BF16),
            pltpu.VMEM((rows, 3 * cols), BF16),
            pltpu.VMEM((rows, DH), F32),
            pltpu.VMEM((rows, DH), F32),
            pltpu.VMEM((edge + tail, width), BF16),
            pltpu.VMEM((edge + tail, width), BF16),
            pltpu.VMEM((rows, width), BF16),
            pltpu.VMEM((4, 2, cols), F32),
            pltpu.VMEM((5, 8, width), F32),
            pltpu.VMEM((4, 8, wide), F32),
            pltpu.VMEM((2, 4, 8, wide), F32),
            pltpu.VMEM((3, 8, wide), F32),
            pltpu.VMEM((rows, width), BF16),
            pltpu.VMEM((4, rows, 3 * cols), BF16),
            pltpu.VMEM((4, rows, cols), BF16),
            pltpu.VMEM((4, rows, cols // DH), F32),
            pltpu.VMEM((rows, width), BF16),
        ]
        + reduce_buffers(shard_rows, main)
        + reduce_buffers(shard_rows, lanes)
        + reduce_terms(shard_rows, main)
        + [dma((2, 4))] * Reduce.SEMS
        + [dma((1, 4))] * 3
        + [dma((2,))] * RowsBack.SEMS
        + [dma((2,)), dma((2,)), dma((2,)), dma((3,)), dma((5,)), dma((5,)), dma((5,)), dma((5,)), dma((3, 4))],
        compiler_params=pltpu.CompilerParams(collective_id=2, has_side_effects=True, vmem_limit_bytes=64000000),
        name="backward",
    )(
        ws, gu, rest_sums, residual_half, first_norm, qkv, context, inverse, segments[:, None], segments.reshape(2, 1, -1),
        x_half, residual_grad, y_rows, gains, owned[:, None].astype(jnp.int32), sums, unit_sums, unit_rest_sums,
    )


def attend_head(qkv_ref, ctx_ref, inv_ref, segc_ref, segr_ref, s, head, cols, tile):
    lo = head * DH
    keys = qkv_ref[s, :, cols + lo : cols + lo + DH]
    values = qkv_ref[s, :, 2 * cols + lo : 2 * cols + lo + DH]

    def one_tile(t, carry):
        span = pl.ds(pl.multiple_of(t * tile, tile), tile)
        scores = dot_nt(qkv_ref[s, span, lo : lo + DH], keys)
        allowed = segc_ref[span, :] == segr_ref[...]
        exact = jnp.where(allowed, jnp.exp2(scores * (SCALE * LOG2E)), 0.0)
        inverse = 1.0 / jnp.sum(exact, axis=1, keepdims=True)
        context = dot_nn(exact.astype(BF16), values) * inverse
        ctx_ref[s, span, lo : lo + DH] = context.astype(BF16)
        inv_ref[s, span, head : head + 1] = inverse
        return carry

    lax.fori_loop(0, qkv_ref.shape[1] // tile, one_tile, 0)


def attend_kernel(x_ref, w_ref, b_ref, segc_ref, segr_ref, qkv_ref, ctx_ref, inv_ref, part_ref, *, cols, tile):
    block = pl.program_id(0)
    projected = dot_nn(x_ref[...], w_ref[0, :, : 3 * cols]) + b_ref[0]
    qkv_ref[0] = projected.astype(BF16)
    for head in range(cols // DH):
        attend_head(qkv_ref, ctx_ref, inv_ref, segc_ref, segr_ref, 0, head, cols, tile)
    part = dot_nt(ctx_ref[0], w_ref[0, :, 3 * cols : 4 * cols])

    @pl.when(block == 0)
    def _():
        part_ref[...] = part

    @pl.when(block > 0)
    def _():
        part_ref[...] += part


def attend(first_norm, weights, bias, segments, cols, tile):
    rows, width = first_norm.shape
    slots, _, lanes = weights.shape
    heads = cols // DH
    whole = lambda shape: pl.BlockSpec(shape, lambda s: (0,) * len(shape))
    each = lambda shape: pl.BlockSpec((1,) + shape, lambda s: (s, 0, 0))
    return pl.pallas_call(
        functools.partial(attend_kernel, cols=cols, tile=tile),
        grid=(slots,),
        in_specs=[
            whole((rows, width)),
            each((width, lanes)),
            each((1, 3 * cols)),
            whole((rows, 1)),
            whole((1, rows)),
        ],
        out_specs=[each((rows, 3 * cols)), each((rows, cols)), each((rows, heads)), whole((rows, width))],
        out_shape=[
            jax.ShapeDtypeStruct((slots, rows, 3 * cols), BF16),
            jax.ShapeDtypeStruct((slots, rows, cols), BF16),
            jax.ShapeDtypeStruct((slots, rows, heads), F32),
            jax.ShapeDtypeStruct((rows, width), F32),
        ],
        cost_estimate=pl.CostEstimate(
            flops=slots * (8 * rows * width * cols + 4 * rows * rows * 256 * heads),
            bytes_accessed=slots * width * lanes * 2 + rows * width * 10,
            transcendentals=slots * heads * rows * rows,
        ),
        name="attend",
    )(first_norm, weights, bias, segments[:, None], segments[None, :])


def attend_back_head(
    qkv_ref, ctx_ref, inv_ref, back_ref, segc_ref, segr_ref, grad_ref, bias_ref, key_acc, value_acc, s, head, cols, tile
):
    lo = head * DH
    rows = back_ref.shape[0]
    ones = jnp.ones((8, DH), F32)
    keys = qkv_ref[s, :, cols + lo : cols + lo + DH]
    values = qkv_ref[s, :, 2 * cols + lo : 2 * cols + lo + DH]
    key_acc[...] = jnp.zeros_like(key_acc)
    value_acc[...] = jnp.zeros_like(value_acc)

    def one_tile(t, query_total):
        span = pl.ds(pl.multiple_of(t * tile, tile), tile)
        queries = qkv_ref[s, span, lo : lo + DH]
        back = (back_ref[span, lo : lo + DH].astype(F32) * inv_ref[s, span, head : head + 1]).astype(BF16)
        along = back.astype(F32) * ctx_ref[s, span, lo : lo + DH].astype(F32)
        delta = lax.dot_general(
            ones, along, (((1,), (1,)), ((), ())), precision=lax.Precision.HIGHEST, preferred_element_type=F32
        )[:1]
        scores = dot_nt(keys, queries)
        allowed = segc_ref[...] == segr_ref[t]
        exact = jnp.where(allowed, jnp.exp2(scores * (SCALE * LOG2E)), 0.0)
        value_acc[...] += dot_nn(exact.astype(BF16), back)
        prob_grad = dot_nt(values, back)
        score_grad = (exact * (prob_grad - delta)).astype(BF16)
        key_acc[...] += dot_nn(score_grad, queries)
        query_grad = dot_tn(score_grad, keys) * SCALE
        grad_ref[span, lo : lo + DH] = query_grad.astype(BF16)
        return query_total + jnp.sum(query_grad, axis=0, keepdims=True)

    query_total = lax.fori_loop(0, rows // tile, one_tile, jnp.zeros((1, DH), F32))
    grad_ref[:, cols + lo : cols + lo + DH] = (key_acc[...] * SCALE).astype(BF16)
    grad_ref[:, 2 * cols + lo : 2 * cols + lo + DH] = value_acc[...].astype(BF16)
    bias_ref[s, 0:1, lo : lo + DH] = query_total
    bias_ref[s, 1:2, lo : lo + DH] = jnp.sum(value_acc[...], axis=0, keepdims=True)


def attend_back_kernel(
    r_ref, w_ref, qkv_ref, ctx_ref, inv_ref, segc_ref, segr_ref, grad_ref, bias_ref, back_ref, key_acc, value_acc, *, cols, tile
):
    back_ref[...] = dot_nn(r_ref[...], w_ref[0, :, 3 * cols : 4 * cols]).astype(BF16)
    for head in range(cols // DH):
        attend_back_head(
            qkv_ref, ctx_ref, inv_ref, back_ref, segc_ref, segr_ref, grad_ref.at[0], bias_ref, key_acc, value_acc, 0, head, cols, tile
        )


def attend_back(residual_half, weights, qkv, context, inverse, segments, cols, tile):
    rows, width = residual_half.shape
    slots, _, lanes = weights.shape
    heads = cols // DH
    whole = lambda shape: pl.BlockSpec(shape, lambda s: (0,) * len(shape))
    each = lambda shape: pl.BlockSpec((1,) + shape, lambda s: (s, 0, 0))
    return pl.pallas_call(
        functools.partial(attend_back_kernel, cols=cols, tile=tile),
        grid=(slots,),
        in_specs=[
            whole((rows, width)),
            each((width, lanes)),
            each((rows, 3 * cols)),
            each((rows, cols)),
            each((rows, heads)),
            whole((rows, 1)),
            whole((rows // tile, 1, tile)),
        ],
        out_specs=[each((rows, 3 * cols)), each((2, cols))],
        out_shape=[
            jax.ShapeDtypeStruct((slots, rows, 3 * cols), BF16),
            jax.ShapeDtypeStruct((slots, 2, cols), F32),
        ],
        scratch_shapes=[
            pltpu.VMEM((rows, cols), BF16),
            pltpu.VMEM((rows, DH), F32),
            pltpu.VMEM((rows, DH), F32),
        ],
        cost_estimate=pl.CostEstimate(
            flops=slots * (2 * rows * width * cols + 10 * rows * rows * 256 * heads),
            bytes_accessed=slots * width * lanes * 2 + rows * width * 10,
            transcendentals=slots * heads * rows * rows,
        ),
        name="attend_back",
    )(residual_half, weights, qkv, context, inverse, segments[:, None], segments.reshape(-1, 1, tile))


def plain_layer(shards, vectors, to_slot, from_slot, block_input, cotangent, gains, shifts, segments, owned, cols, units, parts):
    width, rows = block_input.shape[2], segments.shape[0]
    slots, slot = lax.axis_size("slot"), lax.axis_index("slot")
    main_units, in_lanes = shards[1].shape[1], 3 * cols
    rest = units - main_units
    spare = shards[0].shape[1] - in_lanes - cols - 2 * rest
    small_all, up_main, down_main = gather_weights(shards)
    vec_all = lax.all_gather(vectors, "slot", axis=0)
    grad_rows = jnp.where(owned[:, None], to_slot(cotangent), 0)
    upstream = grad_rows.astype(F32)
    x_float = to_slot(block_input).astype(F32)
    first_out, first_scaled, first_factor = norm_forward(x_float, gains[0], shifts[0])
    first_norm = first_out.astype(BF16)
    bias = vec_all[:, :1, :in_lanes].astype(F32) + vec_all[:, 1:2, :in_lanes].astype(F32)
    qkv, context, inverse, attention_part = attend(first_norm, small_all, bias, segments, cols, rows // 2)
    residual = x_float + part_sum(attention_part, parts) + shifts[2]
    second_out, second_scaled, second_factor = norm_forward(residual, gains[1], shifts[1])
    second_norm = second_out.astype(BF16)
    small_blocks = list(small_all)
    unit_all = vec_all[:, 2, :units].astype(F32)
    at = in_lanes + cols
    ups = list(up_main) + [b[:, at : at + rest] for b in small_blocks]
    downs = list(down_main) + [b[:, at + rest : at + 2 * rest] for b in small_blocks]
    unit_rows = list(unit_all[:, :main_units]) + list(unit_all[:, main_units:])
    pre_acts = [dot_nn(second_norm, w) + b for w, b in zip(ups, unit_rows)]
    hiddens = [gelu(p).astype(BF16) for p in pre_acts]
    output = (residual + part_sum(sum_products(hiddens, downs), parts) + shifts[3]).astype(BF16)
    down_sums = [dot_tn(grad_rows, h).astype(BF16) for h in hiddens]
    pre_grads = [gelu_back(p, dot_nn(grad_rows, w)) for p, w in zip(pre_acts, downs)]
    pre_halves = [p.astype(BF16) for p in pre_grads]
    unit_sums = [jnp.sum(p, axis=0) for p in pre_grads]
    up_sums = [dot_tn(second_norm, p).astype(BF16) for p in pre_halves]
    second_grad = part_sum(sum_products(pre_halves, ups), parts)
    residual_grad = upstream + norm_backward(second_grad, second_scaled, second_factor, gains[1])
    residual_half = residual_grad.astype(BF16)
    triple, bias_sum = attend_back(residual_half, small_all, qkv, context, inverse, segments, cols, rows // 2)
    first_part = sum_products(list(triple), [b[:, :in_lanes] for b in small_blocks])
    first_grad = part_sum(first_part, parts)
    input_grad = residual_grad + norm_backward(first_grad, first_scaled, first_factor, gains[0])
    blank = jnp.zeros((width, spare), BF16)
    small_sums = [
        jnp.concatenate(
            [
                dot_tn(first_norm, triple[s]).astype(BF16),
                dot_tn(residual_half, context[s]).astype(BF16),
                up_sums[slots + s],
                down_sums[slots + s],
                blank,
            ],
            axis=1,
        )
        for s in range(slots)
    ]
    down_grad, up_grad, small_grad = scatter_grads(
        [jnp.stack(down_sums[:slots]), jnp.stack(up_sums[:slots]), jnp.stack(small_sums)]
    )
    rows_sum = jnp.stack(
        [
            jnp.sum(first_grad * first_scaled, axis=0),
            jnp.sum(second_grad * second_scaled, axis=0),
            jnp.sum(first_grad, axis=0),
            jnp.sum(second_grad, axis=0),
            jnp.sum(residual_grad, axis=0),
            jnp.sum(upstream, axis=0),
        ]
    )
    unit_sum = jnp.stack([jnp.concatenate([unit_sums[s], unit_sums[slots + s]]) for s in range(slots)])
    rows_total, bias_total, unit_total = lax.psum((rows_sum, bias_sum, unit_sum), ("slot",) + FSDP)
    bias_grad = lax.dynamic_index_in_dim(bias_total, slot, 0, keepdims=False)
    unit_grad = lax.dynamic_index_in_dim(unit_total, slot, 0, keepdims=False)
    return (
        from_slot(output, owned), from_slot(input_grad.astype(BF16), owned), rows_total, bias_grad, unit_grad,
        down_grad, up_grad, small_grad,
    )


def on_device(
    block_input,
    segment_ids,
    norm_gains,
    row_biases,
    in_projection,
    query_value_bias,
    out_projection,
    up_weight,
    unit_bias,
    down_weight,
    cotangent,
):
    local, rows_each, width = block_input.shape
    rows_mb = segment_ids.shape[1]
    cols = in_projection.shape[2]
    units = up_weight.shape[1]
    shard_rows = up_weight.shape[0]
    slots, parts = lax.axis_size("slot"), lax.axis_size("part")
    slot, part = lax.axis_index("slot"), lax.axis_index("part")
    fsdp_index = lax.axis_index("fy") * lax.axis_size("fx") + lax.axis_index("fx")
    batch, image = slot % local, slot // local
    late = image == 1

    half_rows = rows_mb // IMG_MB
    padding = rows_mb - IMG_MB * IMG
    edge = round_up(max(half_rows - IMG, padding - (half_rows - IMG)), 16)
    tail = round_up(padding, 16)
    rows = round_up(half_rows + edge + tail, 128)
    filler = rows - half_rows - edge - tail
    paired = lax.axis_size("fy") == 2 and lax.axis_size("fx") == 2 and slots == 4 and parts == 2
    paired = paired and shard_rows % 32 == 0 and filler == 0

    def edges(main):
        near = jnp.where(late, main[:edge], main[half_rows - edge :])
        far = main[half_rows - tail :]
        return jnp.concatenate([near, far])

    def to_slot(value):
        mine = lax.dynamic_index_in_dim(value, batch, 0, keepdims=False)
        send = lax.dynamic_index_in_dim(value, 1 - batch, 0, keepdims=False)
        other = slot_swap(send, 1, slots)
        pair = jnp.where(batch == 0, jnp.stack([mine, other]), jnp.stack([other, mine]))
        main = part_gather(pair, parts).swapaxes(0, 1).reshape(half_rows, width)
        beyond = slot_swap(edges(main), local, slots)
        return jnp.concatenate([main, beyond, jnp.zeros((filler, width), value.dtype)])

    def from_slot(value, owned):
        main = value[:half_rows]
        beyond = slot_swap(value[half_rows : half_rows + edge + tail], local, slots)
        keep = owned[:half_rows, None]
        near, far = beyond[:edge], beyond[edge:]
        blank = lambda count: jnp.zeros((count, width), value.dtype)
        early_fill = jnp.concatenate([blank(half_rows - edge), near])
        late_fill = jnp.concatenate([near, blank(half_rows - edge - tail), far])
        main = jnp.where(keep, main, jnp.where(late, late_fill, early_fill))
        main = main.reshape(local, parts, rows_each, width)
        mine = lax.dynamic_index_in_dim(main, part, 1, keepdims=False)
        stay = lax.dynamic_index_in_dim(mine, batch, 0, keepdims=False)
        other = slot_swap(lax.dynamic_index_in_dim(mine, 1 - batch, 0, keepdims=False), 1, slots)
        return jnp.where(batch == 0, jnp.stack([stay, other]), jnp.stack([other, stay]))

    ids = lax.dynamic_index_in_dim(segment_ids, batch, 0, keepdims=False)
    fill_ids = jnp.full((filler,), -2, jnp.int32)
    early_ids = jnp.concatenate([ids[: half_rows + edge], ids[rows_mb - tail :], fill_ids])
    late_ids = jnp.concatenate(
        [ids[half_rows:], ids[half_rows - edge : half_rows], jnp.full((tail,), -2, jnp.int32), fill_ids]
    )
    segments = jnp.where(late, late_ids, early_ids)
    image_id = (fsdp_index * local + batch) * IMG_MB + image
    owned = (segments == image_id) | (jnp.logical_not(late) & (segments == -1))

    main_units = units // 128 * 128
    rest = units - main_units
    in_lanes = 3 * cols
    small = in_lanes + cols + 2 * rest
    lanes = round_up(small, 128)
    down_t = down_weight.T
    small_shard = jnp.concatenate(
        [
            in_projection.transpose(1, 0, 2).reshape(shard_rows, in_lanes),
            out_projection.T,
            up_weight[:, main_units:],
            down_t[:, main_units:],
            jnp.zeros((shard_rows, lanes - small), BF16),
        ],
        axis=1,
    )
    shards = [small_shard, up_weight[:, :main_units], down_t[:, :main_units]]
    triple_bias = jnp.concatenate([query_value_bias[0], jnp.zeros((cols,), F32), query_value_bias[1]])
    high = triple_bias.astype(BF16)
    low = (triple_bias - high.astype(F32)).astype(BF16)
    wide = round_up(max(in_lanes, units), 128)
    vectors = [jnp.pad(v, (0, wide - v.shape[0])) for v in (high, low, unit_bias)]
    vectors = jnp.concatenate([jnp.stack(vectors), jnp.zeros((13, wide), BF16)])
    gains, shifts = norm_gains, row_biases
    if paired:
        (
            small_all, up_main, down_main, gd, x_half, cot, first_norm, qkv, context, inverse, residual, second_norm,
            hidden, slope, hidden_rest, slope_rest, rest_up, rest_down,
        ) = forward_stage(
            *shards, vectors, block_input, cotangent, gains, shifts, segments, owned, cols, rest, rows, edge, tail
        )
        gu, down_grad, rest_sums, residual_half, residual_grad, y_rows, sums, unit_sums, unit_rest_sums = middle_stage(
            down_main, up_main, gd, hidden, slope, hidden_rest, slope_rest, rest_up, rest_down, cot, second_norm, residual,
            gains, shifts, cols, rest, lanes - small,
        )
        up_grad, small_grad, input_grad, output, rows_total, vec_total = backward_stage(
            small_all, gu, rest_sums, residual_half, first_norm, qkv, context, inverse, segments, x_half, residual_grad,
            y_rows, gains, owned, sums, unit_sums, unit_rest_sums, cols, rest, edge, tail, rows_each,
        )
        rows_total = rows_total[:6]
        bias_grad = vec_total[:2, :cols]
        unit_grad = jnp.concatenate([vec_total[2, :main_units], vec_total[3, :rest]])
    else:
        output, input_grad, rows_total, bias_grad, unit_grad, down_grad, up_grad, small_grad = plain_layer(
            shards, vectors, to_slot, from_slot, block_input, cotangent, gains, shifts, segments, owned, cols, units, parts
        )
    in_grad = small_grad[:, :in_lanes].reshape(shard_rows, 3, cols).transpose(1, 0, 2)
    out_grad = small_grad[:, in_lanes : in_lanes + cols].T
    at = in_lanes + cols
    up_grad = jnp.concatenate([up_grad, small_grad[:, at : at + rest]], axis=1)
    down_grad = jnp.concatenate([down_grad, small_grad[:, at + rest : at + 2 * rest]], axis=1).T
    return (
        output,
        input_grad.astype(F32),
        rows_total[:2],
        rows_total[2:],
        in_grad,
        bias_grad,
        out_grad,
        up_grad,
        unit_grad,
        down_grad,
    )


def solution(mesh):
    fsdp, tensor = mesh.shape["fsdp"], mesh.shape["tensor"]

    def layer(*arrays):
        local = arrays[0].shape[0] // fsdp
        slots = local * IMG_MB
        assert local == 2 and slots == 4 and tensor % slots == 0 and fsdp % 2 == 0
        grid = Mesh(
            mesh.devices.reshape(fsdp // 2, 2, slots, tensor // slots), ("fy", "fx", "slot", "part")
        )
        tens = ("slot", "part")
        return jax.shard_map(
            on_device,
            mesh=grid,
            in_specs=(
                P(FSDP, tens, None),
                P(FSDP, None),
                P(),
                P(),
                P(None, FSDP, tens),
                P(None, tens),
                P(tens, FSDP),
                P(FSDP, tens),
                P(tens),
                P(tens, FSDP),
                P(FSDP, tens, None),
            ),
            out_specs=(
                P(FSDP, tens, None),
                P(FSDP, tens, None),
                P(),
                P(),
                P(None, FSDP, tens),
                P(None, tens),
                P(tens, FSDP),
                P(FSDP, tens),
                P(tens),
                P(tens, FSDP),
            ),
            check_vma=False,
        )(*arrays)

    return layer
```

```python
import functools
import math

import jax
import jax.numpy as jnp
from jax import lax
from jax.experimental import pallas as pl
from jax.experimental.pallas import tpu as pltpu
from jax.sharding import Mesh
from jax.sharding import PartitionSpec as P

DH = 72
IMG = 729
IMG_MB = 2
EPS = 1e-06
GELU_C = 0.7978845608028654
F32 = jnp.float32
BF16 = jnp.bfloat16
FSDP = ("fy", "fx")
SCALE = DH ** (-0.5)
LOG2E = math.log2(math.e)


def norm_forward(values, norm_gain, norm_shift):
    center = values - jnp.mean(values, axis=-1, keepdims=True)
    factor = lax.rsqrt(jnp.mean(center * center, axis=-1, keepdims=True) + EPS)
    scaled = center * factor
    return (scaled * norm_gain + norm_shift, scaled, factor)


def norm_backward(upstream, scaled, factor, norm_gain):
    inside = upstream * norm_gain
    return factor * (
        inside
        - jnp.mean(inside, axis=-1, keepdims=True)
        - scaled * jnp.mean(inside * scaled, axis=-1, keepdims=True)
    )


def gelu(pre_act):
    return (
        0.5
        * pre_act
        * (1.0 + jnp.tanh(GELU_C * (pre_act + 0.044715 * pre_act * pre_act * pre_act)))
    )


def gelu_both(pre_act):
    square = pre_act * pre_act
    curve = jnp.tanh(GELU_C * pre_act * (1.0 + 0.044715 * square))
    rise = 0.5 * (1.0 + curve)
    slope = rise + 0.5 * pre_act * (1.0 - curve * curve) * GELU_C * (1.0 + 3.0 * 0.044715 * square)
    return pre_act * rise, slope


def gelu_back(pre_act, upstream):
    return jax.vjp(gelu, pre_act)[1](upstream)[0]


def dot_nn(left, right):
    return lax.dot_general(left, right, (((1,), (0,)), ((), ())), preferred_element_type=F32)


def dot_nt(left, right):
    return lax.dot_general(left, right, (((1,), (1,)), ((), ())), preferred_element_type=F32)


def dot_tn(left, right):
    return lax.dot_general(left, right, (((0,), (0,)), ((), ())), preferred_element_type=F32)


def sum_products(lefts, rights):
    total = dot_nt(lefts[0], rights[0])
    for left, right in zip(lefts[1:], rights[1:]):
        total = total + dot_nt(left, right)
    return total


def round_up(value, unit):
    return -(-value // unit) * unit


def swap(value, axis):
    return lax.ppermute(value, axis, [(0, 1), (1, 0)])


def slot_swap(value, stride, slots):
    return lax.ppermute(value, "slot", [(s, s ^ stride) for s in range(slots)])


def part_sum(value, parts):
    value = value.astype(BF16)
    if parts == 2:
        return value.astype(F32) + swap(value, "part").astype(F32)
    return lax.psum(value.astype(F32), "part")


def part_gather(value, parts):
    if parts == 2:
        other = swap(value, "part")
        first = lax.axis_index("part") == 0
        return jnp.stack([jnp.where(first, value, other), jnp.where(first, other, value)])
    return lax.all_gather(value, "part", axis=0)


def add_half(left, right):
    return (left.astype(F32) + right.astype(F32)).astype(BF16)


MESH = pl.DeviceIdType.MESH


class Place:
    def __init__(self):
        self.y, self.x = lax.axis_index("fy"), lax.axis_index("fx")
        self.z = lax.axis_index("slot")
        self.f = 2 * self.y + self.x
        self.across_x, self.across_y = {"fx": 1 - self.x}, {"fy": 1 - self.y}
        self.c = lax.axis_index("part")
        self.above = {"slot": jnp.minimum(self.z + 1, 3)}
        self.below = {"slot": jnp.maximum(self.z - 1, 0)}
        self.batch, self.image = self.z % 2, self.z // 2
        self.mate = {"part": 1 - self.c}
        self.pair = {"slot": self.z + 1 - 2 * self.batch}
        self.cross = {"slot": self.z + 2 - 4 * self.image}

    def owned(self, segments):
        mine = segments == (self.f * 2 + self.batch) * IMG_MB + self.image
        return mine | ((segments == -1) & (self.image == 0))

    def slot_after(self, d):
        return {"slot": (self.z + d) % 4}

    def barrier(self):
        sem = pltpu.get_barrier_semaphore()
        others = [self.across_x, self.across_y, self.mate] + [self.slot_after(d) for d in (1, 2, 3)]
        for device in others:
            pl.semaphore_signal(sem, inc=1, device_id=device, device_id_type=MESH)
        pl.semaphore_wait(sem, len(others))

    def far_first(self, i):
        low = self.z < 2
        near = jnp.where(low, self.z, 3 - self.z)
        at = jnp.where(i == 0, 3, jnp.where(i == 1, 2, jnp.where(i == 2, 1 - near, near)))
        return jnp.where(low, at, 3 - at)


def send(src, dst, send_sem, recv_sem, device):
    return pltpu.make_async_remote_copy(
        src_ref=src, dst_ref=dst, send_sem=send_sem, recv_sem=recv_sem, device_id=device, device_id_type=MESH
    )


class Gather:
    SEMS = 11

    def __init__(self, place, shards, w, sems, local_sem, rows):
        self.p, self.shards, self.w, self.rows = place, shards, w, rows
        (self.zr, self.zu, self.zd, self.xr, self.xs, self.yr, self.ys, self.ar, self.asn, self.br, self.bs) = sems
        self.local_sem = local_sem

    def block(self, k, slot, owner, half=None):
        at, count = owner * self.rows, self.rows
        if half is not None:
            count = count // 2
            at = at + half * count
        return self.w[k].at[slot, pl.ds(pl.multiple_of(at, 16), count), :]

    def mine(self, k, slot, shard):
        return self.shards[k] if shard else self.block(k, slot, self.p.f)

    def up(self, k, slot, shard=False):
        dst = self.block(k, slot, self.p.f)
        return send(self.mine(k, slot, shard), dst, self.zu.at[k, slot], self.zr.at[k, slot], self.p.above)

    def down(self, k, slot, shard=False):
        dst = self.block(k, slot, self.p.f)
        return send(self.mine(k, slot, shard), dst, self.zd.at[k, slot], self.zr.at[k, slot], self.p.below)

    def to_x(self, k, slot, shard=False):
        dst = self.block(k, slot, self.p.f)
        return send(self.mine(k, slot, shard), dst, self.xs.at[k, slot], self.xr.at[k, slot], self.p.across_x)

    def to_y(self, k, slot, shard=False):
        dst = self.block(k, slot, self.p.f)
        return send(self.mine(k, slot, shard), dst, self.ys.at[k, slot], self.yr.at[k, slot], self.p.across_y)

    def from_x(self, k, slot):
        ref = self.block(k, slot, self.p.f ^ 1)
        return send(ref, ref, self.xs.at[k, slot], self.xr.at[k, slot], self.p.across_x)

    def from_y(self, k, slot):
        ref = self.block(k, slot, self.p.f ^ 2)
        return send(ref, ref, self.ys.at[k, slot], self.yr.at[k, slot], self.p.across_y)

    def corner_y(self, k, slot):
        ref = self.block(k, slot, self.p.f ^ 1, 0)
        return send(ref, ref, self.asn.at[k, slot], self.ar.at[k, slot], self.p.across_y)

    def corner_x(self, k, slot):
        ref = self.block(k, slot, self.p.f ^ 2, 1)
        return send(ref, ref, self.bs.at[k, slot], self.br.at[k, slot], self.p.across_x)

    def wait_corner(self, k, slot):
        ref = self.block(k, slot, self.p.f ^ 3, 0)
        send(ref, ref, self.asn.at[k, slot], self.ar.at[k, slot], self.p.across_y).wait_recv()
        ref = self.block(k, slot, self.p.f ^ 3, 1)
        send(ref, ref, self.bs.at[k, slot], self.br.at[k, slot], self.p.across_x).wait_recv()

    def local(self, k):
        return pltpu.make_async_copy(self.shards[k], self.block(k, self.p.z, self.p.f), self.local_sem.at[k])

    def start_z(self, k):
        @pl.when(self.p.z < 3)
        def _():
            self.up(k, self.p.z, True).start()

        @pl.when(self.p.z > 0)
        def _():
            self.down(k, self.p.z, True).start()

    def start_xy(self, k):
        self.to_x(k, self.p.z, True).start()
        self.to_y(k, self.p.z, True).start()
        self.local(k).start()

    def pass_on(self, k, d):
        z = self.p.z

        @pl.when(z >= d)
        def _():
            self.up(k, z - d).wait_recv()

            @pl.when(z < 3)
            def _():
                self.up(k, z - d).start()

            self.to_x(k, z - d).start()
            self.to_y(k, z - d).start()

        @pl.when(z + d <= 3)
        def _():
            self.down(k, z + d).wait_recv()

            @pl.when(z > 0)
            def _():
                self.down(k, z + d).start()

            self.to_x(k, z + d).start()
            self.to_y(k, z + d).start()

    def corner(self, k, d):
        def one(slot):
            self.from_x(k, slot).wait_recv()
            self.corner_y(k, slot).start()
            self.from_y(k, slot).wait_recv()
            self.corner_x(k, slot).start()

        z = self.p.z
        if d == 0:
            one(z)
        else:
            pl.when(z >= d)(lambda: one(z - d))
            pl.when(z + d <= 3)(lambda: one(z + d))

    def arrive(self, k):
        self.local(k).wait()
        for slot in range(4):
            self.wait_corner(k, slot)

    def drain(self, k):
        z = self.p.z
        for slot in range(4):
            self.to_x(k, slot).wait_send()
            self.to_y(k, slot).wait_send()
            self.corner_y(k, slot).wait_send()
            self.corner_x(k, slot).wait_send()

            @pl.when((z < 3) & (slot <= z))
            def _(slot=slot):
                self.up(k, slot).wait_send()

            @pl.when((z > 0) & (slot >= z))
            def _(slot=slot):
                self.down(k, slot).wait_send()


def gather_weights(shards):
    slots = lax.axis_size("slot")
    whole = [lax.all_gather(s, ("slot",) + FSDP, axis=0) for s in shards]
    return [w.reshape(slots, -1, w.shape[-1]) for w in whole]


class Rows:
    SEMS = 11

    def __init__(self, place, index, src, dst, sems, rows_each, edge, tail):
        self.p, self.src, self.dst, self.each = place, src, dst, rows_each
        self.half = 4 * rows_each
        self.edge, self.tail = edge, tail
        self.sems = [sem.at[index] for sem in sems]

    def at(self, row, count):
        return self.dst.at[pl.ds(pl.multiple_of(row, 16), count), :]

    def block(self, near, core):
        batch = self.p.batch if near else 1 - self.p.batch
        return self.at((2 * batch + core) * self.each, self.each)

    def own(self):
        return pltpu.make_async_copy(self.src.at[self.p.batch], self.block(True, self.p.c), self.sems[0])

    def to_mate(self):
        return send(self.src.at[self.p.batch], self.block(True, self.p.c), self.sems[1], self.sems[2], self.p.mate)

    def to_pair(self):
        return send(self.src.at[1 - self.p.batch], self.block(True, self.p.c), self.sems[3], self.sems[4], self.p.pair)

    def pass_on(self):
        ref = self.block(False, self.p.c)
        return send(ref, ref, self.sems[5], self.sems[6], self.p.mate)

    def edge_out(self):
        src = self.at(jnp.where(self.p.image == 0, self.half - self.edge, 0), self.edge)
        return send(src, self.at(self.half, self.edge), self.sems[7], self.sems[8], self.p.cross)

    def tail_out(self):
        src = self.at(self.half - self.tail, self.tail)
        dst = self.at(self.half + self.edge, self.tail)
        return send(src, dst, self.sems[7], self.sems[8], self.p.cross)

    def edge_mate(self):
        ref = self.at(self.half, self.edge)
        return send(ref, ref, self.sems[9], self.sems[10], self.p.mate)

    def tail_mate(self):
        ref = self.at(self.half + self.edge, self.tail)
        return send(ref, ref, self.sems[9], self.sems[10], self.p.mate)

    def start(self):
        self.to_pair().start()
        self.to_mate().start()
        self.own().start()

    def forward(self):
        ref = self.block(False, self.p.c)
        send(ref, ref, self.sems[3], self.sems[4], self.p.pair).wait_recv()
        self.pass_on().start()

    def main_ready(self):
        self.own().wait()
        ref = self.block(True, 1 - self.p.c)
        send(ref, ref, self.sems[1], self.sems[2], self.p.mate).wait_recv()
        ref = self.block(False, 1 - self.p.c)
        send(ref, ref, self.sems[5], self.sems[6], self.p.mate).wait_recv()

    def edges(self):
        pl.when(self.p.c == 0)(lambda: self.edge_out().start())
        pl.when(self.p.c == 1)(lambda: self.tail_out().start())

    def edges_forward(self):
        @pl.when(self.p.c == 0)
        def _():
            self.edge_out().wait_recv()
            self.edge_mate().start()

        @pl.when(self.p.c == 1)
        def _():
            self.tail_out().wait_recv()
            self.tail_mate().start()

    def edges_ready(self):
        pl.when(self.p.c == 0)(lambda: self.tail_mate().wait_recv())
        pl.when(self.p.c == 1)(lambda: self.edge_mate().wait_recv())

    def drain(self):
        self.to_mate().wait_send()
        self.to_pair().wait_send()
        self.pass_on().wait_send()

        @pl.when(self.p.c == 0)
        def _():
            self.edge_out().wait_send()
            self.edge_mate().wait_send()

        @pl.when(self.p.c == 1)
        def _():
            self.tail_out().wait_send()
            self.tail_mate().wait_send()


def row_tiles(rows, step, body):
    def one(t, carry):
        body(pl.ds(pl.multiple_of(t * step, 16), step))
        return carry

    lax.fori_loop(0, rows // step, one, 0)


def forward_kernel(*refs, cols, unit_rest, edge, tail, tile):
    (in_ref, out_ref, up_whole, down_whole, qv_ref, unit_ref, x_src, c_src, gain_ref, shift_ref, segc_ref) = refs[:11]
    segr_ref, refs = refs[11], refs[1:]
    (ws, wu, wd, gd) = refs[11:15]
    outs, refs = refs[15:29], refs[29:]
    held, refs = refs[:14], refs[14:]
    (x_ref, c_ref, first_ref, qkv_ref, ctx_ref, inv_ref, res_ref, second_ref) = held[:8]
    (hidden_ref, slope_ref, hidden_rest, slope_rest, rest_up, rest_down) = held[8:]
    (blocks, unit_blocks, grads, part, part_out, part_in, bias_rest, vec_all) = refs[:8]
    (small_ref, up_ref, down_ref, vec_ref) = refs[8:12]
    gather_sems, local_sem = refs[12 : 12 + Gather.SEMS], refs[12 + Gather.SEMS]
    tail_refs = refs[13 + Gather.SEMS :]
    row_sems = tail_refs[: Rows.SEMS]
    (vec_s, vec_r, load_sem, part_s, part_r, unit_sem, grad_sem, out_sem) = tail_refs[Rows.SEMS :]

    def leave(n):
        return pltpu.make_async_copy(held[n], outs[n], out_sem.at[n])

    main, rest = up_ref.shape[1], unit_rest
    rows, width = x_ref.shape
    place = Place()
    for n in range(3):
        small_ref[:, n * cols : (n + 1) * cols] = in_ref[n]
    at = 3 * cols
    small_ref[:, at : at + cols] = out_ref[...].T
    at = at + cols
    small_ref[:, at : at + rest] = up_whole[:, main:]
    small_ref[:, at + rest : at + 2 * rest] = down_whole[main:, :].T
    at = at + 2 * rest
    if at < small_ref.shape[1]:
        small_ref[:, at:] = jnp.zeros((small_ref.shape[0], small_ref.shape[1] - at), BF16)
    vec_ref[...] = jnp.zeros_like(vec_ref)
    for n in (0, 1):
        high = qv_ref[n : n + 1, :].astype(BF16)
        lo = 2 * n * cols
        vec_ref[0:1, lo : lo + cols] = high
        vec_ref[1:2, lo : lo + cols] = (qv_ref[n : n + 1, :] - high.astype(F32)).astype(BF16)
    vec_ref[2:3, : main + rest] = unit_ref[...]
    place.barrier()
    shards = (small_ref, up_ref, down_ref)
    g = Gather(place, shards, (ws, wu, wd), gather_sems, local_sem, small_ref.shape[0])
    each = x_src.shape[1]
    x_rows = Rows(place, 0, x_src, x_ref, row_sems, each, edge, tail)
    c_rows = Rows(place, 1, c_src, c_ref, row_sems, each, edge, tail)

    def vec_to(d):
        device = place.slot_after(d)
        return send(vec_ref, vec_all.at[place.z], vec_s.at[d], vec_r.at[d], device)

    def vec_from(d):
        ref = vec_all.at[(place.z + 4 - d) % 4]
        return send(ref, ref, vec_s.at[d], vec_r.at[d], place.slot_after(d))

    g.start_z(0)
    g.start_xy(0)
    for d in (1, 2, 3):
        vec_to(d).start()
    x_rows.start()
    vec_all[place.z] = vec_ref[...]
    up_ref[...] = up_whole[:, :main]
    down_ref[...] = down_whole[:main, :].T
    g.pass_on(0, 1)
    g.corner(0, 0)
    x_rows.forward()
    g.pass_on(0, 2)
    x_rows.main_ready()
    x_rows.edges()
    g.corner(0, 1)
    x_rows.edges_forward()
    g.pass_on(0, 3)
    g.start_z(1)
    x_rows.edges_ready()

    def first(span):
        value = x_ref[span, :].astype(F32)
        out, _, _ = norm_forward(value, gain_ref[0:1, :], shift_ref[0:1, :])
        first_ref[span, :] = out.astype(BF16)

    row_tiles(rows, 128, first)
    leave(0).start()
    g.corner(0, 2)
    g.corner(0, 3)
    leave(2).start()
    for d in (1, 2, 3):
        vec_from(d).wait_recv()
    g.arrive(0)

    later = []
    for k in (1, 2):
        later.append(lambda k=k: g.start_xy(k))
        if k == 1:
            later.append(lambda: c_rows.start())
        for d in (1, 2, 3):
            later.append(lambda k=k, d=d: g.pass_on(k, d))
            later.append(lambda k=k, d=d: g.corner(k, d - 1))
        if k == 1:
            later.append(lambda: g.start_z(2))
            later.append(lambda: c_rows.forward())
            later.append(lambda: (c_rows.main_ready(), c_rows.edges()))
        later.append(lambda k=k: g.corner(k, 3))
        if k == 1:
            later.append(lambda: c_rows.edges_forward())

    def step(count=1):
        for _ in range(count):
            if later:
                later.pop(0)()

    step(2)

    def load(s):
        return pltpu.make_async_copy(ws.at[s], blocks.at[s % 2], load_sem.at[s % 2])

    heads = cols // DH
    rest_up[...] = jnp.zeros_like(rest_up)
    rest_down[...] = jnp.zeros_like(rest_down)
    bias_rest[...] = jnp.zeros_like(bias_rest)
    part[...] = jnp.zeros_like(part)
    load(0).start()
    points = 1 + heads
    inside = [later.pop(0) for _ in range(4 * points)]

    def at_point(s, n):
        for one in range(4):
            pl.when(s == one)(lambda one=one: inside[one * points + n]() and None)

    def one_slot(s, carry):
        load(s).wait()
        pl.when(s < 3)(lambda: load(s + 1).start())
        w = blocks.at[s % 2]
        bias = vec_all[s, 0:1, : 3 * cols].astype(F32) + vec_all[s, 1:2, : 3 * cols].astype(F32)
        projected = dot_nn(first_ref[...], w[:, : 3 * cols]) + bias
        qkv_ref[s] = projected.astype(BF16)
        at_point(s, 0)
        for head in range(heads):
            attend_head(qkv_ref, ctx_ref, inv_ref, segc_ref, segr_ref, s, head, cols, tile)
            at_point(s, 1 + head)
        part[...] += dot_nt(ctx_ref[s], w[:, 3 * cols : 4 * cols])
        at = 4 * cols
        for one in range(4):

            @pl.when(s == one)
            def _(one=one):
                rest_up[:, one * rest : (one + 1) * rest] = w[:, at : at + rest]
                rest_down[:, one * rest : (one + 1) * rest] = w[:, at + rest : at + 2 * rest]
                bias_rest[:, one * rest : (one + 1) * rest] = vec_all[one, 2:3, main : main + rest].astype(F32)

        return carry

    lax.fori_loop(0, 4, one_slot, 0)

    def halves(h):
        return pl.ds(h * (rows // 2), rows // 2)

    def exchange(h):
        src, dst = part_out.at[halves(h), :], part_in.at[halves(h), :]
        return send(src, dst, part_s.at[h], part_r.at[h], place.mate)

    for h in (0, 1):
        part_out[halves(h), :] = part[halves(h), :].astype(BF16)
        exchange(h).start()
    step()
    for n in (3, 4, 5, 12, 13):
        leave(n).start()
    for h in (0, 1):
        exchange(h).wait_recv()

    def second(span):
        value = x_ref[span, :].astype(F32) + (part_out[span, :].astype(F32) + part_in[span, :].astype(F32))
        value = value + shift_ref[2:3, :]
        res_ref[span, :] = value
        out, _, _ = norm_forward(value, gain_ref[1:2, :], shift_ref[1:2, :])
        second_ref[span, :] = out.astype(BF16)

    row_tiles(rows, 128, second)
    g.arrive(1)

    def unit_load(s):
        return pltpu.make_async_copy(wu.at[s], unit_blocks.at[s % 2], unit_sem.at[s % 2])

    unit_load(0).start()
    passing = [later.pop(0) for _ in range(4)]

    def one_block(s, carry):
        unit_load(s).wait()
        pl.when(s < 3)(lambda: unit_load(s + 1).start())
        bias = vec_all[s, 2:3, :main].astype(F32)

        def units(span):
            hidden, slope = gelu_both(dot_nn(second_ref[span, :], unit_blocks[s % 2]) + bias)
            hidden_ref[s, span, :] = hidden.astype(BF16)
            slope_ref[s, span, :] = slope.astype(BF16)

        row_tiles(rows, tile, units)
        for one in range(4):
            pl.when(s == one)(lambda one=one: passing[one]() and None)
        return carry

    lax.fori_loop(0, 4, one_block, 0)

    def units_rest(span):
        hidden, slope = gelu_both(dot_nn(second_ref[span, :], rest_up[...]) + bias_rest[...])
        hidden_rest[span, :] = hidden.astype(BF16)
        slope_rest[span, :] = slope.astype(BF16)

    for n in (6, 7):
        leave(n).start()
    row_tiles(rows, tile, units_rest)
    step()
    for n in (8, 9, 10, 11):
        leave(n).start()
    c_rows.edges_ready()
    c_rows.drain()
    c_ref[...] = jnp.where(place.owned(segc_ref[...]), c_ref[...], jnp.zeros_like(c_ref))

    def grad_out(s):
        return pltpu.make_async_copy(grads.at[s % 2], gd.at[s], grad_sem.at[s % 2])

    def down_grad(s, carry):
        pl.when(s >= 2)(lambda: grad_out(s - 2).wait())
        grads[s % 2] = dot_tn(c_ref[...], hidden_ref[s]).astype(BF16)
        grad_out(s).start()
        return carry

    lax.fori_loop(0, 2, down_grad, 0)
    step()
    lax.fori_loop(2, 4, down_grad, 0)
    step(len(later))
    leave(1).start()
    for s in (2, 3):
        grad_out(s).wait()
    g.arrive(2)
    for n in range(14):
        leave(n).wait()
    for k in (0, 1, 2):
        g.drain(k)
    x_rows.drain()
    for d in (1, 2, 3):
        vec_to(d).wait_send()
    for h in (0, 1):
        exchange(h).wait_send()


def forward_stage(
    weights, biases, x_src, c_src, gains, shifts, segc, segr, cols, units, lanes, edge, tail
):
    rows, width, shard_rows, main = segc.shape[0], x_src.shape[2], weights[2].shape[0], units // 128 * 128
    unit_rest = units - main
    heads, rest_lanes = cols // DH, round_up(4 * unit_rest, 128)
    vectors = (16, round_up(max(3 * cols, units), 128))
    vmem = pl.BlockSpec(memory_space=pltpu.VMEM)
    far = pl.BlockSpec(memory_space=pl.ANY)
    shape = jax.ShapeDtypeStruct
    dma = pltpu.SemaphoreType.DMA
    return pl.pallas_call(
        functools.partial(forward_kernel, cols=cols, unit_rest=unit_rest, edge=edge, tail=tail, tile=rows // 2),
        in_specs=[vmem] * 12,
        out_specs=[far] * 18,
        out_shape=[
            shape((4, width, lanes), BF16),
            shape((4, width, main), BF16),
            shape((4, width, main), BF16),
            shape((4, width, main), BF16),
            shape((rows, width), BF16),
            shape((rows, width), BF16),
            shape((rows, width), BF16),
            shape((4, rows, 3 * cols), BF16),
            shape((4, rows, cols), BF16),
            shape((4, rows, heads), F32),
            shape((rows, width), F32),
            shape((rows, width), BF16),
            shape((4, rows, main), BF16),
            shape((4, rows, main), BF16),
            shape((rows, rest_lanes), BF16),
            shape((rows, rest_lanes), BF16),
            shape((width, rest_lanes), BF16),
            shape((width, rest_lanes), BF16),
        ],
        scratch_shapes=[
            pltpu.VMEM((rows, width), BF16),
            pltpu.VMEM((rows, width), BF16),
            pltpu.VMEM((rows, width), BF16),
            pltpu.VMEM((4, rows, 3 * cols), BF16),
            pltpu.VMEM((4, rows, cols), BF16),
            pltpu.VMEM((4, rows, heads), F32),
            pltpu.VMEM((rows, width), F32),
            pltpu.VMEM((rows, width), BF16),
            pltpu.VMEM((4, rows, main), BF16),
            pltpu.VMEM((4, rows, main), BF16),
            pltpu.VMEM((rows, rest_lanes), BF16),
            pltpu.VMEM((rows, rest_lanes), BF16),
            pltpu.VMEM((width, rest_lanes), BF16),
            pltpu.VMEM((width, rest_lanes), BF16),
            pltpu.VMEM((2, width, lanes), BF16),
            pltpu.VMEM((2, width, main), BF16),
            pltpu.VMEM((2, width, main), BF16),
            pltpu.VMEM((rows, width), F32),
            pltpu.VMEM((rows, width), BF16),
            pltpu.VMEM((rows, width), BF16),
            pltpu.VMEM((1, rest_lanes), F32),
            pltpu.VMEM((4,) + vectors, BF16),
            pltpu.VMEM((shard_rows, lanes), BF16),
            pltpu.VMEM((shard_rows, main), BF16),
            pltpu.VMEM((shard_rows, main), BF16),
            pltpu.VMEM(vectors, BF16),
        ]
        + [dma((3, 4))] * Gather.SEMS
        + [dma((3,))]
        + [dma((2,))] * Rows.SEMS
        + [dma((4,)), dma((4,)), dma((2,)), dma((2,)), dma((2,)), dma((2,)), dma((2,)), dma((14,))],
        compiler_params=pltpu.CompilerParams(collective_id=1, has_side_effects=True, vmem_limit_bytes=64000000),
        name="forward",
    )(*weights, *biases, x_src, c_src, gains, shifts, segc, segr)


def middle_kernel(*refs, cols, unit_rest):
    (wd, wu, gd) = refs[:3]
    (hidden_far, slope_far, hidden_rest, slope_rest, rest_up, rest_down) = refs[3:9]
    (c_far, second_far, res_far, gain_ref, shift_ref) = refs[9:14]
    gu = refs[14]
    (d_out, rest_sums, half_ref, grad_ref, y_ref, sums_ref, unit_ref, unit_rest_ref) = refs[15:23]
    (blocks, grads, pre_half, part, part_out, part_in, part_in2) = refs[23:30]
    (hidden_ref, slope_ref, c_ref, second_ref, res_ref) = refs[30:35]
    d_bufs, d_own = refs[35:40], refs[40:43]
    refs = refs[43:]
    sems, loads = refs[: Reduce.SEMS], refs[Reduce.SEMS : Reduce.SEMS + 3]
    load_sem, grad_sem, part_s, part_r, in_sem, unit_sem = refs[Reduce.SEMS + 3 :]
    rows, width = c_ref.shape
    rest = unit_rest
    place = Place()
    place.barrier()

    def down_final(total):
        d_out[...] = total[...].astype(F32).T

    r = Reduce(place, (gd,), (d_own,), (down_final,), (d_bufs,), sems, loads, d_out.shape[1])

    def load(w, slot, buffer):
        return pltpu.make_async_copy(w.at[slot], blocks.at[buffer], load_sem.at[buffer])

    def halves(h):
        return pl.ds(h * (rows // 2), rows // 2)

    def exchange(n, h):
        dst = (part_in, part_in2)[n]
        src, dst = part_out.at[halves(h), :], dst.at[halves(h), :]
        return send(src, dst, part_s.at[n, h], part_r.at[n, h], place.mate)

    def enter(n):
        far, near = ((c_far, c_ref), (second_far, second_ref), (res_far, res_ref))[n]
        return pltpu.make_async_copy(far, near, in_sem.at[n])

    def unit_loads(s):
        return (
            pltpu.make_async_copy(hidden_far.at[s], hidden_ref.at[s % 2], unit_sem.at[0, s % 2]),
            pltpu.make_async_copy(slope_far.at[s], slope_ref.at[s % 2], unit_sem.at[1, s % 2]),
        )

    def start_units(s):
        for copy in unit_loads(s):
            copy.start()

    enter(0).start()
    load(wd, 0, 0).start()
    start_units(0)
    r.start(0)
    enter(1).start()
    enter(2).start()
    enter(0).wait()
    part[...] = dot_nt(hidden_rest[...], rest_down[...])
    grad_rest = slope_rest[...].astype(F32) * dot_nn(c_ref[...], rest_down[...])
    unit_rest_ref[...] = jnp.sum(grad_rest, axis=0, keepdims=True)
    half_rest = grad_rest.astype(BF16)

    def down_block(s, carry):
        load(wd, s, s % 2).wait()
        pl.when(s < 3)(lambda: load(wd, s + 1, (s + 1) % 2).start())
        pl.when(s == 3)(lambda: load(wu, 0, 0).start())
        for copy in unit_loads(s):
            copy.wait()
        pl.when(s < 3)(lambda: start_units(s + 1))
        w = blocks[s % 2]
        part[...] += dot_nt(hidden_ref[s % 2], w)
        grad = slope_ref[s % 2].astype(F32) * dot_nn(c_ref[...], w)
        pre_half[s] = grad.astype(BF16)
        unit_ref[s] = jnp.broadcast_to(jnp.sum(grad, axis=0, keepdims=True), unit_ref.shape[1:])
        r.middle_one(0, s)
        return carry

    lax.fori_loop(0, 4, down_block, 0)
    for h in (0, 1):
        part_out[halves(h), :] = part[halves(h), :].astype(BF16)
        exchange(0, h).start()
    enter(1).wait()
    enter(2).wait()
    up_sum = dot_tn(second_ref[...], half_rest).astype(BF16)
    down_sum = dot_tn(c_ref[...], hidden_rest[...]).astype(BF16)
    rest_sums[...] = jnp.zeros_like(rest_sums)
    for s in range(4):
        rest_sums[s, :, :rest] = up_sum[:, s * rest : (s + 1) * rest]
        rest_sums[s, :, rest : 2 * rest] = down_sum[:, s * rest : (s + 1) * rest]
    part[...] = dot_nt(half_rest, rest_up[...])

    def grad_out(s):
        return pltpu.make_async_copy(grads.at[s % 2], gu.at[s], grad_sem.at[s % 2])

    def up_block(s, carry):
        load(wu, s, s % 2).wait()
        pl.when(s < 3)(lambda: load(wu, s + 1, (s + 1) % 2).start())
        part[...] += dot_nt(pre_half[s], blocks[s % 2])
        pl.when(s >= 2)(lambda: grad_out(s - 2).wait())
        grads[s % 2] = dot_tn(second_ref[...], pre_half[s]).astype(BF16)
        grad_out(s).start()
        pl.when(s >= 2)(lambda: r.line_one(0, s - 2))
        return carry

    lax.fori_loop(0, 4, up_block, 0)
    for h in (0, 1):
        exchange(0, h).wait_recv()

    def output(span):
        value = part_out[span, :].astype(F32) + part_in[span, :].astype(F32)
        y_ref[span, :] = (res_ref[span, :] + value + shift_ref[3:4, :]).astype(BF16)

    row_tiles(rows, 128, output)
    for h in (0, 1):
        exchange(0, h).wait_send()
        part_out[halves(h), :] = part[halves(h), :].astype(BF16)
        exchange(1, h).start()
    r.line_one(0, 2)
    r.line_one(0, 3)
    for h in (0, 1):
        exchange(1, h).wait_recv()
    sums_ref[...] = jnp.zeros_like(sums_ref)

    def back(span):
        grad = part_out[span, :].astype(F32) + part_in2[span, :].astype(F32)
        upstream = c_ref[span, :].astype(F32)
        _, scaled, factor = norm_forward(res_ref[span, :], gain_ref[1:2, :], shift_ref[1:2, :])
        value = upstream + norm_backward(grad, scaled, factor, gain_ref[1:2, :])
        grad_ref[span, :] = value
        half_ref[span, :] = value.astype(BF16)
        sums_ref[1:2, :] += jnp.sum(grad * scaled, axis=0, keepdims=True)
        sums_ref[3:4, :] += jnp.sum(grad, axis=0, keepdims=True)
        sums_ref[4:5, :] += jnp.sum(value, axis=0, keepdims=True)
        sums_ref[5:6, :] += jnp.sum(upstream, axis=0, keepdims=True)

    row_tiles(rows, 128, back)
    for s in (2, 3):
        grad_out(s).wait()
    r.drain(0)
    for h in (0, 1):
        exchange(1, h).wait_send()


def middle_stage(
    wd, wu, gd, hidden, slope, hidden_rest, slope_rest, rest_up, rest_down, cot, second, residual, gains, shifts, cols, unit_rest, spare
):
    rows, width = cot.shape
    main, shard_rows = wd.shape[2], width // 4
    vmem = pl.BlockSpec(memory_space=pltpu.VMEM)
    far = pl.BlockSpec(memory_space=pl.ANY)
    shape = jax.ShapeDtypeStruct
    dma = pltpu.SemaphoreType.DMA
    return pl.pallas_call(
        functools.partial(middle_kernel, cols=cols, unit_rest=unit_rest),
        in_specs=[far] * 5 + [vmem] * 4 + [far] * 3 + [vmem] * 2,
        out_specs=[far] + [vmem] * 8,
        out_shape=[
            shape((4, width, main), BF16),
            shape((main, shard_rows), F32),
            shape((4, width, 2 * unit_rest + spare), BF16),
            shape((rows, width), BF16),
            shape((rows, width), F32),
            shape((rows, width), BF16),
            shape((8, width), F32),
            shape((4, 8, main), F32),
            shape((1, rest_up.shape[1]), F32),
        ],
        scratch_shapes=[
            pltpu.VMEM((2, width, main), BF16),
            pltpu.VMEM((2, width, main), BF16),
            pltpu.VMEM((4, rows, main), BF16),
            pltpu.VMEM((rows, width), F32),
            pltpu.VMEM((rows, width), BF16),
            pltpu.VMEM((rows, width), BF16),
            pltpu.VMEM((rows, width), BF16),
            pltpu.VMEM((2, rows, main), BF16),
            pltpu.VMEM((2, rows, main), BF16),
            pltpu.VMEM((rows, width), BF16),
            pltpu.VMEM((rows, width), BF16),
            pltpu.VMEM((rows, width), F32),
        ]
        + reduce_buffers(shard_rows, main)
        + reduce_terms(shard_rows, main)
        + [dma((1, 4))] * Reduce.SEMS
        + [dma((1, 4))] * 3
        + [dma((2,)), dma((2,)), dma((2, 2)), dma((2, 2)), dma((3,)), dma((2, 2))],
        compiler_params=pltpu.CompilerParams(collective_id=3, has_side_effects=True, vmem_limit_bytes=64000000),
        name="middle",
    )(wd, wu, gd, hidden, slope, hidden_rest, slope_rest, rest_up, rest_down, cot, second, residual, gains, shifts)


class Reduce:
    SEMS = 16

    def __init__(self, place, g, own, out, bufs, sems, load_sems, rows):
        self.p, self.g, self.own, self.out, self.rows = place, g, own, out, rows
        self.bufs, self.sems, self.load_sems = bufs, sems, load_sems

    def grad(self, k, slot, owner, half=None):
        at, count = owner * self.rows, self.rows
        if half is not None:
            count = count // 2
            at = at + half * count
        return self.g[k].at[slot, pl.ds(pl.multiple_of(at, 16), count), :]

    def terms(self, k, slot):
        f = self.p.f
        if self.own[k] is None:
            return self.grad(k, slot, f ^ 1, 0), self.grad(k, slot, f ^ 2, 1), self.grad(k, slot, f)
        return tuple(ref.at[slot] for ref in self.own[k])

    def loads(self, k, slot):
        f = self.p.f
        src = self.grad(k, slot, f ^ 1, 0), self.grad(k, slot, f ^ 2, 1), self.grad(k, slot, f)
        pairs = zip(src, self.terms(k, slot), self.load_sems)
        return [pltpu.make_async_copy(one, dst, sem.at[k, slot]) for one, dst, sem in pairs]

    def half(self, ref, slot, half):
        count = self.rows // 2
        return ref.at[slot, half * count : (half + 1) * count, :]

    def copy(self, k, slot, src, dst, index, device):
        return send(src, dst, self.sems[2 * index].at[k, slot], self.sems[2 * index + 1].at[k, slot], device)

    def corner_y(self, k, s):
        return self.copy(k, s, self.grad(k, s, self.p.f ^ 3, 0), self.bufs[k][0].at[s], 0, self.p.across_y)

    def corner_x(self, k, s):
        return self.copy(k, s, self.grad(k, s, self.p.f ^ 3, 1), self.bufs[k][1].at[s], 1, self.p.across_x)

    def x_low(self, k, s):
        return self.copy(k, s, self.bufs[k][0].at[s], self.half(self.bufs[k][2], s, 0), 2, self.p.across_x)

    def x_high(self, k, s):
        dst = self.half(self.bufs[k][2], s, 1)
        return self.copy(k, s, self.grad(k, s, self.p.f ^ 1, 1), dst, 3, self.p.across_x)

    def y_low(self, k, s):
        dst = self.half(self.bufs[k][3], s, 0)
        return self.copy(k, s, self.grad(k, s, self.p.f ^ 2, 0), dst, 4, self.p.across_y)

    def y_high(self, k, s):
        return self.copy(k, s, self.bufs[k][1].at[s], self.half(self.bufs[k][3], s, 1), 5, self.p.across_y)

    def up(self, k, s):
        return self.copy(k, s, self.bufs[k][2].at[s], self.bufs[k][4].at[s], 6, self.p.above)

    def down(self, k, s):
        at = jnp.where(s == self.p.z - 1, 4, s)
        return self.copy(k, s, self.bufs[k][2].at[s], self.bufs[k][4].at[at], 7, self.p.below)

    def from_above(self, k, s):
        at = jnp.where(s == self.p.z, 4, s)
        return self.copy(k, s, self.bufs[k][4].at[at], self.bufs[k][4].at[at], 7, self.p.below), at

    def start_one(self, k, s):
        self.corner_y(k, s).start()
        self.corner_x(k, s).start()
        self.y_low(k, s).start()
        self.x_high(k, s).start()

    def start(self, k):
        def one(i, carry):
            self.start_one(k, self.p.far_first(i))
            return carry

        lax.fori_loop(0, 4, one, 0)
        if self.own[k] is not None:
            for slot in range(4):
                for load in self.loads(k, slot):
                    load.start()

    def tiles(self, rows, body):
        row_tiles(rows, 48 if rows % 48 == 0 else 16, body)

    def middle_one(self, k, i):
        s, count = self.p.far_first(i), self.rows // 2
        low, high = self.bufs[k][0], self.bufs[k][1]
        if self.own[k] is not None:
            for load in self.loads(k, s):
                load.wait()
        own_low, own_high, _ = self.terms(k, s)
        self.corner_y(k, s).wait_recv()

        def add_low(span):
            low[s, span, :] = add_half(low[s, span, :], own_low[span, :])

        self.tiles(count, add_low)
        self.corner_x(k, s).wait_recv()

        def add_high(span):
            high[s, span, :] = add_half(high[s, span, :], own_high[span, :])

        self.tiles(count, add_high)
        self.x_low(k, s).start()
        self.y_high(k, s).start()

    def line_one(self, k, i):
        z, acc, side, far = self.p.z, self.bufs[k][2], self.bufs[k][3], self.bufs[k][4]
        s = self.p.far_first(i)
        self.x_low(k, s).wait_recv()
        self.x_high(k, s).wait_recv()
        self.y_low(k, s).wait_recv()
        self.y_high(k, s).wait_recv()
        own = self.terms(k, s)[2]

        def add(span):
            total = own[span, :].astype(F32) + acc[s, span, :].astype(F32) + side[s, span, :].astype(F32)
            acc[s, span, :] = total.astype(BF16)

        self.tiles(self.rows, add)

        def add_far(at):
            def body(span):
                acc[s, span, :] = add_half(acc[s, span, :], far[at, span, :])

            self.tiles(self.rows, body)

        @pl.when((z > 0) & (s >= z))
        def _():
            self.up(k, s).wait_recv()
            add_far(s)

        @pl.when((z < 3) & (s <= z))
        def _():
            copy, at = self.from_above(k, s)
            copy.wait_recv()
            add_far(at)

        @pl.when(s > z)
        def _():
            self.up(k, s).start()

        @pl.when(s < z)
        def _():
            self.down(k, s).start()

        @pl.when(s == z)
        def _():
            self.out[k](acc.at[s])

    def loop(self, one):
        def body(i, carry):
            one(i)
            return carry

        lax.fori_loop(0, 4, body, 0)

    def drain(self, k):
        def one(s):
            for copy in (self.corner_y, self.corner_x, self.x_low, self.x_high, self.y_low, self.y_high):
                copy(k, s).wait_send()

            @pl.when(s > self.p.z)
            def _():
                self.up(k, s).wait_send()

            @pl.when(s < self.p.z)
            def _():
                self.down(k, s).wait_send()

        self.loop(one)


def reduce_buffers(rows, lanes):
    half, whole = pltpu.VMEM((4, rows // 2, lanes), BF16), pltpu.VMEM((4, rows, lanes), BF16)
    return [half, half, whole, whole, pltpu.VMEM((5, rows, lanes), BF16)]


def reduce_terms(rows, lanes):
    half, whole = pltpu.VMEM((4, rows // 2, lanes), BF16), pltpu.VMEM((4, rows, lanes), BF16)
    return [half, half, whole]


def scatter_grads(chunks):
    count = lax.axis_size("fy") * lax.axis_size("fx")
    split = [c.reshape(c.shape[0] * count, c.shape[1] // count, c.shape[2]) for c in chunks]
    return [lax.psum_scatter(c, ("slot",) + FSDP, scatter_dimension=0).astype(F32) for c in split]


class RowsBack:
    SEMS = 7

    def __init__(self, place, index, window, inbox, owned, out, sems, rows_each, edge, tail):
        self.p, self.window, self.inbox, self.owned, self.out = place, window, inbox, owned, out
        self.each, self.half, self.edge, self.tail = rows_each, 4 * rows_each, edge, tail
        self.sems = [sem.at[index] for sem in sems]

    def edge_out(self):
        src = self.window.at[self.half : self.half + self.edge, :]
        return send(src, self.inbox.at[: self.edge, :], self.sems[0], self.sems[1], self.p.cross)

    def tail_out(self):
        src = self.window.at[self.half + self.edge :, :]
        return send(src, self.inbox.at[self.edge :, :], self.sems[2], self.sems[3], self.p.cross)

    def block(self, near):
        batch = self.p.batch if near else 1 - self.p.batch
        row = (2 * batch + self.p.c) * self.each
        return self.window.at[pl.ds(pl.multiple_of(row, 16), self.each), :]

    def stay(self):
        return pltpu.make_async_copy(self.block(True), self.out.at[self.p.batch], self.sems[4])

    def to_pair(self):
        return send(self.block(False), self.out.at[self.p.batch], self.sems[5], self.sems[6], self.p.pair)

    def edges(self):
        pl.when(self.p.c == self.p.image)(lambda: self.edge_out().start())
        pl.when((self.p.c == 1) & (self.p.image == 0))(lambda: self.tail_out().start())

    def merge(self, row, count, at):
        keep = self.p.owned(self.owned[row : row + count, :])
        value = jnp.where(keep, self.window[row : row + count, :], self.inbox[at : at + count, :])
        self.window[row : row + count, :] = value

    def finish(self):
        p = self.p

        @pl.when((p.c == 1) & (p.image == 0))
        def _():
            self.edge_out().wait_recv()
            self.merge(self.half - self.edge, self.edge, 0)

        @pl.when((p.c == 0) & (p.image == 1))
        def _():
            self.edge_out().wait_recv()
            self.merge(0, self.edge, 0)

        @pl.when((p.c == 1) & (p.image == 1))
        def _():
            self.tail_out().wait_recv()
            self.merge(self.half - self.tail, self.tail, self.edge)

        self.to_pair().start()
        self.stay().start()

    def drain(self):
        pl.when(self.p.c == self.p.image)(lambda: self.edge_out().wait_send())
        pl.when((self.p.c == 1) & (self.p.image == 0))(lambda: self.tail_out().wait_send())
        self.stay().wait()
        self.to_pair().wait_send()
        ref = self.out.at[1 - self.p.batch]
        send(ref, ref, self.sems[5], self.sems[6], self.p.pair).wait_recv()


def backward_kernel(*refs, cols, unit_rest, edge, tail, tile):
    (ws, gu, rest_ref, half_ref, first_far, qkv_far, ctx_far, inv_far, segc_ref, segr_whole) = refs[:10]
    (x_far, res_grad_ref, y_ref, gain_ref, d_in, old_sums, unit_ref, unit_rest_ref) = refs[10:18]
    (in_out, out_out, up_out, down_out, x_final, y_out, gain_out, shift_out, qv_out, unit_out) = refs[18:28]
    refs = refs[28:]
    (segr_ref, x_out, sums_ref), refs = refs[:3], refs[3:]
    (blocks, gs, part, part_out, part_in, back_ref, grad_ref, key_acc, value_acc, inbox_x, inbox_y) = refs[:11]
    y_window = part_out
    bias_ref, sums_in, vec_sum, vec_in, vec_far = refs[11:16]
    first_ref, qkv_ref, ctx_ref, inv_ref, x_ref = refs[16:21]
    u_bufs, s_bufs, u_own = refs[21:26], refs[26:31], refs[31:34]
    refs = refs[34:]
    sems, loads, back_sems = refs[: Reduce.SEMS], refs[Reduce.SEMS : Reduce.SEMS + 3], refs[Reduce.SEMS + 3 : Reduce.SEMS + 3 + RowsBack.SEMS]
    load_sem, part_s, part_r, y_sems, sum_s, sum_r, vec_s, vec_r, in_sem = refs[Reduce.SEMS + 3 + RowsBack.SEMS :]
    rows, width = half_ref.shape
    shard_rows, main, rest = up_out.shape[0], gu.shape[2], unit_rest
    heads = cols // DH
    place = Place()
    place.barrier()
    each = x_out.shape[1]

    def up_final(total):
        up_out[:, :main] = total[...].astype(F32)

    def small_final(total):
        for n in range(3):
            in_out[n] = total[:, n * cols : (n + 1) * cols].astype(F32)
        at = 3 * cols
        out_out[...] = total[:, at : at + cols].astype(F32).T
        at = at + cols
        up_out[:, main:] = total[:, at : at + rest].astype(F32)
        down_out[main:, :] = total[:, at + rest : at + 2 * rest].astype(F32).T

    r = Reduce(place, (gu, gs), (u_own, None), (up_final, small_final), (u_bufs, s_bufs), sems, loads, shard_rows)
    x_back = RowsBack(place, 0, part_in, inbox_x, segc_ref, x_out, back_sems, each, edge, tail)
    y_back = RowsBack(place, 1, y_window, inbox_y, segc_ref, y_out, back_sems, each, edge, tail)

    def load(i):
        return pltpu.make_async_copy(ws.at[place.far_first(i)], blocks.at[i % 2], load_sem.at[i % 2])

    y_load = pltpu.make_async_copy(y_ref, y_window, y_sems.at[0])
    def slot_loads(i):
        s = place.far_first(i)
        pairs = ((qkv_far, qkv_ref), (ctx_far, ctx_ref), (inv_far, inv_ref))
        return [pltpu.make_async_copy(p[0].at[s], p[1].at[s], in_sem.at[n, i]) for n, p in enumerate(pairs)]

    first_load = pltpu.make_async_copy(first_far, first_ref, y_sems.at[1])
    x_load = pltpu.make_async_copy(x_far, x_ref, y_sems.at[2])
    load(0).start()
    for copy in slot_loads(0):
        copy.start()
    y_load.start()
    r.start(0)
    for t in range(rows // tile):
        segr_ref[t] = segr_whole[:, t * tile : (t + 1) * tile]
    down_out[:main, :] = d_in[...]
    first_load.start()
    for i in (1, 2, 3):
        for copy in slot_loads(i):
            copy.start()
    x_load.start()
    y_load.wait()
    y_back.edges()

    def one_slot(i, carry):
        s = place.far_first(i)
        load(i).wait()
        for copy in slot_loads(i):
            copy.wait()

        @pl.when(i < 3)
        def _():
            load(i + 1).start()

        w = blocks.at[i % 2]
        back_ref[...] = dot_nn(half_ref[...], w[:, 3 * cols : 4 * cols]).astype(BF16)
        gs[s, :, 3 * cols : 4 * cols] = dot_tn(half_ref[...], ctx_ref[s]).astype(BF16)
        gs[s, :, 4 * cols :] = rest_ref[s]
        for head in range(heads):
            attend_back_head(
                qkv_ref, ctx_ref, inv_ref, back_ref, segc_ref, segr_ref, grad_ref, bias_ref, key_acc, value_acc, s, head, cols, tile
            )
            if head == 0:
                r.middle_one(0, i)
                pl.when(i == 1)(lambda: y_back.finish())
        pl.when(i == 0)(lambda: first_load.wait())
        gs[s, :, : 3 * cols] = dot_tn(first_ref[...], grad_ref[...]).astype(BF16)
        product = dot_nt(grad_ref[...], w[:, : 3 * cols])

        @pl.when(i == 0)
        def _():
            part[...] = product

        @pl.when(i > 0)
        def _():
            part[...] += product

        r.start_one(1, s)
        pl.when(i > 0)(lambda: r.line_one(0, i - 1))
        pl.when(i > 0)(lambda: r.middle_one(1, i - 1))
        return carry

    lax.fori_loop(0, 4, one_slot, 0)

    def halves(h):
        return pl.ds(h * (rows // 2), rows // 2)

    def exchange(h):
        src, dst = part_out.at[halves(h), :], part_in.at[halves(h), :]
        return send(src, dst, part_s.at[h], part_r.at[h], place.mate)

    y_back.drain()
    for h in (0, 1):
        part_out[halves(h), :] = part[halves(h), :].astype(BF16)
        exchange(h).start()
    res_load = pltpu.make_async_copy(res_grad_ref, part, load_sem.at[0])
    res_load.start()
    r.line_one(0, 3)
    pl.when((place.z == 0) | (place.z == 3))(lambda: r.line_one(1, 0))
    for h in (0, 1):
        exchange(h).wait_recv()

    res_load.wait()
    x_load.wait()
    sums_ref[...] = old_sums[...]

    def last(span):
        grad = part_out[span, :].astype(F32) + part_in[span, :].astype(F32)
        value = x_ref[span, :].astype(F32)
        _, scaled, factor = norm_forward(value, gain_ref[0:1, :], gain_ref[0:1, :])
        result = part[span, :] + norm_backward(grad, scaled, factor, gain_ref[0:1, :])
        part_in[span, :] = result.astype(BF16)
        sums_ref[0:1, :] += jnp.sum(grad * scaled, axis=0, keepdims=True)
        sums_ref[2:3, :] += jnp.sum(grad, axis=0, keepdims=True)

    row_tiles(rows, 128, last)
    x_back.edges()

    vec_sum[...] = jnp.zeros_like(vec_sum)
    for s in range(4):
        vec_sum[s, 0:1, :cols] = bias_ref[s, 0:1, :]
        vec_sum[s, 1:2, :cols] = bias_ref[s, 1:2, :]
        vec_sum[s, 2:3, :main] = unit_ref[s, 0:1, :]
        vec_sum[s, 3:4, :rest] = unit_rest_ref[:, s * rest : (s + 1) * rest]

    def across(n, device):
        return (
            send(sums_ref, sums_in.at[n], sum_s.at[n], sum_r.at[n], device),
            send(vec_sum, vec_in.at[n], vec_s.at[n], vec_r.at[n], device),
        )

    def along(d):
        there = (place.z + d) % 4
        device = place.slot_after(d)
        return (
            send(sums_ref, sums_in.at[1 + d], sum_s.at[1 + d], sum_r.at[1 + d], device),
            send(vec_sum.at[there], vec_far.at[d - 1], vec_s.at[1 + d], vec_r.at[1 + d], device),
        )

    def add_across(n, device):
        for copy in across(n, device):
            copy.wait()
        sums_ref[...] += sums_in[n]
        vec_sum[...] += vec_in[n]

    for copy in across(0, place.across_x):
        copy.start()
    r.middle_one(1, 3)
    pl.when((place.z == 1) | (place.z == 2))(lambda: r.line_one(1, 0))
    r.line_one(1, 1)
    add_across(0, place.across_x)
    for copy in across(1, place.across_y):
        copy.start()
    x_back.finish()
    r.line_one(1, 2)
    add_across(1, place.across_y)
    for d in (1, 2, 3):
        for copy in along(d):
            copy.start()
    r.line_one(1, 3)
    for d in (1, 2, 3):
        for copy in along(d):
            copy.wait()
    sums_ref[...] += sums_in[2] + sums_in[3] + sums_in[4]
    gain_out[...] = sums_ref[0:2, :]
    shift_out[...] = sums_ref[2:6, :]
    total = vec_sum[place.z] + vec_far[0] + vec_far[1] + vec_far[2]
    qv_out[...] = total[0:2, :cols]
    unit_out[:, :main] = total[2:3, :main]
    unit_out[:, main:] = total[3:4, :rest]
    for k in (0, 1):
        r.drain(k)
    x_back.drain()
    x_final[...] = x_out[...].astype(F32)
    for h in (0, 1):
        exchange(h).wait_send()


def backward_stage(
    ws, gu, rest_sums, residual_half, first_norm, qkv, context, inverse, segc, segr, x_half, residual_grad, y_rows, gains, down_sum,
    sums, unit_sums, unit_rest_sums, cols, unit_rest, edge, tail, rows_each,
):
    rows, width = residual_half.shape
    shard_rows, lanes, main = width // 4, ws.shape[2], gu.shape[2]
    vmem = pl.BlockSpec(memory_space=pltpu.VMEM)
    far = pl.BlockSpec(memory_space=pl.ANY)
    shape = jax.ShapeDtypeStruct
    dma = pltpu.SemaphoreType.DMA
    wide = max(main, round_up(cols, 128))
    return pl.pallas_call(
        functools.partial(backward_kernel, cols=cols, unit_rest=unit_rest, edge=edge, tail=tail, tile=rows // 2),
        in_specs=[far] * 2 + [vmem] * 2 + [far] * 4 + [vmem] * 2 + [far] * 3 + [vmem] * 5,
        out_specs=[vmem] * 10,
        out_shape=[
            shape((3, shard_rows, cols), F32),
            shape((cols, shard_rows), F32),
            shape((shard_rows, main + unit_rest), F32),
            shape((main + unit_rest, shard_rows), F32),
            shape((2, rows_each, width), F32),
            shape((2, rows_each, width), BF16),
            shape((2, width), F32),
            shape((4, width), F32),
            shape((2, cols), F32),
            shape((1, main + unit_rest), F32),
        ],
        scratch_shapes=[
            pltpu.VMEM((2, 1, rows // 2), jnp.int32),
            pltpu.VMEM((2, rows_each, width), BF16),
            pltpu.VMEM((8, width), F32),
            pltpu.VMEM((2, width, lanes), BF16),
            pltpu.VMEM((4, width, lanes), BF16),
            pltpu.VMEM((rows, width), F32),
            pltpu.VMEM((rows, width), BF16),
            pltpu.VMEM((rows, width), BF16),
            pltpu.VMEM((rows, cols), BF16),
            pltpu.VMEM((rows, 3 * cols), BF16),
            pltpu.VMEM((rows, DH), F32),
            pltpu.VMEM((rows, DH), F32),
            pltpu.VMEM((edge + tail, width), BF16),
            pltpu.VMEM((edge + tail, width), BF16),
            pltpu.VMEM((4, 2, cols), F32),
            pltpu.VMEM((5, 8, width), F32),
            pltpu.VMEM((4, 8, wide), F32),
            pltpu.VMEM((2, 4, 8, wide), F32),
            pltpu.VMEM((3, 8, wide), F32),
            pltpu.VMEM((rows, width), BF16),
            pltpu.VMEM((4, rows, 3 * cols), BF16),
            pltpu.VMEM((4, rows, cols), BF16),
            pltpu.VMEM((4, rows, cols // DH), F32),
            pltpu.VMEM((rows, width), BF16),
        ]
        + reduce_buffers(shard_rows, main)
        + reduce_buffers(shard_rows, lanes)
        + reduce_terms(shard_rows, main)
        + [dma((2, 4))] * Reduce.SEMS
        + [dma((1, 4))] * 3
        + [dma((2,))] * RowsBack.SEMS
        + [dma((2,)), dma((2,)), dma((2,)), dma((3,)), dma((5,)), dma((5,)), dma((5,)), dma((5,)), dma((3, 4))],
        compiler_params=pltpu.CompilerParams(collective_id=2, has_side_effects=True, vmem_limit_bytes=64000000),
        name="backward",
    )(
        ws, gu, rest_sums, residual_half, first_norm, qkv, context, inverse, segc, segr,
        x_half, residual_grad, y_rows, gains, down_sum, sums, unit_sums, unit_rest_sums,
    )


def attend_head(qkv_ref, ctx_ref, inv_ref, segc_ref, segr_ref, s, head, cols, tile):
    lo = head * DH
    keys = qkv_ref[s, :, cols + lo : cols + lo + DH]
    values = qkv_ref[s, :, 2 * cols + lo : 2 * cols + lo + DH]

    def one_tile(t, carry):
        span = pl.ds(pl.multiple_of(t * tile, tile), tile)
        scores = dot_nt(qkv_ref[s, span, lo : lo + DH], keys)
        allowed = segc_ref[span, :] == segr_ref[...]
        exact = jnp.where(allowed, jnp.exp2(scores * (SCALE * LOG2E)), 0.0)
        inverse = 1.0 / jnp.sum(exact, axis=1, keepdims=True)
        context = dot_nn(exact.astype(BF16), values) * inverse
        ctx_ref[s, span, lo : lo + DH] = context.astype(BF16)
        inv_ref[s, span, head : head + 1] = inverse
        return carry

    lax.fori_loop(0, qkv_ref.shape[1] // tile, one_tile, 0)


def attend_kernel(x_ref, w_ref, b_ref, segc_ref, segr_ref, qkv_ref, ctx_ref, inv_ref, part_ref, *, cols, tile):
    block = pl.program_id(0)
    projected = dot_nn(x_ref[...], w_ref[0, :, : 3 * cols]) + b_ref[0]
    qkv_ref[0] = projected.astype(BF16)
    for head in range(cols // DH):
        attend_head(qkv_ref, ctx_ref, inv_ref, segc_ref, segr_ref, 0, head, cols, tile)
    part = dot_nt(ctx_ref[0], w_ref[0, :, 3 * cols : 4 * cols])

    @pl.when(block == 0)
    def _():
        part_ref[...] = part

    @pl.when(block > 0)
    def _():
        part_ref[...] += part


def attend(first_norm, weights, bias, segments, cols, tile):
    rows, width = first_norm.shape
    slots, _, lanes = weights.shape
    heads = cols // DH
    whole = lambda shape: pl.BlockSpec(shape, lambda s: (0,) * len(shape))
    each = lambda shape: pl.BlockSpec((1,) + shape, lambda s: (s, 0, 0))
    return pl.pallas_call(
        functools.partial(attend_kernel, cols=cols, tile=tile),
        grid=(slots,),
        in_specs=[
            whole((rows, width)),
            each((width, lanes)),
            each((1, 3 * cols)),
            whole((rows, 1)),
            whole((1, rows)),
        ],
        out_specs=[each((rows, 3 * cols)), each((rows, cols)), each((rows, heads)), whole((rows, width))],
        out_shape=[
            jax.ShapeDtypeStruct((slots, rows, 3 * cols), BF16),
            jax.ShapeDtypeStruct((slots, rows, cols), BF16),
            jax.ShapeDtypeStruct((slots, rows, heads), F32),
            jax.ShapeDtypeStruct((rows, width), F32),
        ],
        cost_estimate=pl.CostEstimate(
            flops=slots * (8 * rows * width * cols + 4 * rows * rows * 256 * heads),
            bytes_accessed=slots * width * lanes * 2 + rows * width * 10,
            transcendentals=slots * heads * rows * rows,
        ),
        name="attend",
    )(first_norm, weights, bias, segments[:, None], segments[None, :])


def attend_back_head(
    qkv_ref, ctx_ref, inv_ref, back_ref, segc_ref, segr_ref, grad_ref, bias_ref, key_acc, value_acc, s, head, cols, tile
):
    lo = head * DH
    rows = back_ref.shape[0]
    ones = jnp.ones((8, DH), F32)
    keys = qkv_ref[s, :, cols + lo : cols + lo + DH]
    values = qkv_ref[s, :, 2 * cols + lo : 2 * cols + lo + DH]
    key_acc[...] = jnp.zeros_like(key_acc)
    value_acc[...] = jnp.zeros_like(value_acc)

    def one_tile(t, query_total):
        span = pl.ds(pl.multiple_of(t * tile, tile), tile)
        queries = qkv_ref[s, span, lo : lo + DH]
        back = (back_ref[span, lo : lo + DH].astype(F32) * inv_ref[s, span, head : head + 1]).astype(BF16)
        along = back.astype(F32) * ctx_ref[s, span, lo : lo + DH].astype(F32)
        delta = lax.dot_general(
            ones, along, (((1,), (1,)), ((), ())), precision=lax.Precision.HIGHEST, preferred_element_type=F32
        )[:1]
        scores = dot_nt(keys, queries)
        allowed = segc_ref[...] == segr_ref[t]
        exact = jnp.where(allowed, jnp.exp2(scores * (SCALE * LOG2E)), 0.0)
        value_acc[...] += dot_nn(exact.astype(BF16), back)
        prob_grad = dot_nt(values, back)
        score_grad = (exact * (prob_grad - delta)).astype(BF16)
        key_acc[...] += dot_nn(score_grad, queries)
        query_grad = dot_tn(score_grad, keys) * SCALE
        grad_ref[span, lo : lo + DH] = query_grad.astype(BF16)
        return query_total + jnp.sum(query_grad, axis=0, keepdims=True)

    query_total = lax.fori_loop(0, rows // tile, one_tile, jnp.zeros((1, DH), F32))
    grad_ref[:, cols + lo : cols + lo + DH] = (key_acc[...] * SCALE).astype(BF16)
    grad_ref[:, 2 * cols + lo : 2 * cols + lo + DH] = value_acc[...].astype(BF16)
    bias_ref[s, 0:1, lo : lo + DH] = query_total
    bias_ref[s, 1:2, lo : lo + DH] = jnp.sum(value_acc[...], axis=0, keepdims=True)


def attend_back_kernel(
    r_ref, w_ref, qkv_ref, ctx_ref, inv_ref, segc_ref, segr_ref, grad_ref, bias_ref, back_ref, key_acc, value_acc, *, cols, tile
):
    back_ref[...] = dot_nn(r_ref[...], w_ref[0, :, 3 * cols : 4 * cols]).astype(BF16)
    for head in range(cols // DH):
        attend_back_head(
            qkv_ref, ctx_ref, inv_ref, back_ref, segc_ref, segr_ref, grad_ref.at[0], bias_ref, key_acc, value_acc, 0, head, cols, tile
        )


def attend_back(residual_half, weights, qkv, context, inverse, segments, cols, tile):
    rows, width = residual_half.shape
    slots, _, lanes = weights.shape
    heads = cols // DH
    whole = lambda shape: pl.BlockSpec(shape, lambda s: (0,) * len(shape))
    each = lambda shape: pl.BlockSpec((1,) + shape, lambda s: (s, 0, 0))
    return pl.pallas_call(
        functools.partial(attend_back_kernel, cols=cols, tile=tile),
        grid=(slots,),
        in_specs=[
            whole((rows, width)),
            each((width, lanes)),
            each((rows, 3 * cols)),
            each((rows, cols)),
            each((rows, heads)),
            whole((rows, 1)),
            whole((rows // tile, 1, tile)),
        ],
        out_specs=[each((rows, 3 * cols)), each((2, cols))],
        out_shape=[
            jax.ShapeDtypeStruct((slots, rows, 3 * cols), BF16),
            jax.ShapeDtypeStruct((slots, 2, cols), F32),
        ],
        scratch_shapes=[
            pltpu.VMEM((rows, cols), BF16),
            pltpu.VMEM((rows, DH), F32),
            pltpu.VMEM((rows, DH), F32),
        ],
        cost_estimate=pl.CostEstimate(
            flops=slots * (2 * rows * width * cols + 10 * rows * rows * 256 * heads),
            bytes_accessed=slots * width * lanes * 2 + rows * width * 10,
            transcendentals=slots * heads * rows * rows,
        ),
        name="attend_back",
    )(residual_half, weights, qkv, context, inverse, segments[:, None], segments.reshape(-1, 1, tile))


def plain_layer(shards, vectors, to_slot, from_slot, block_input, cotangent, gains, shifts, segments, owned, cols, units, parts):
    width, rows = block_input.shape[2], segments.shape[0]
    slots, slot = lax.axis_size("slot"), lax.axis_index("slot")
    main_units, in_lanes = shards[1].shape[1], 3 * cols
    rest = units - main_units
    spare = shards[0].shape[1] - in_lanes - cols - 2 * rest
    small_all, up_main, down_main = gather_weights(shards)
    vec_all = lax.all_gather(vectors, "slot", axis=0)
    grad_rows = jnp.where(owned[:, None], to_slot(cotangent), 0)
    upstream = grad_rows.astype(F32)
    x_float = to_slot(block_input).astype(F32)
    first_out, first_scaled, first_factor = norm_forward(x_float, gains[0], shifts[0])
    first_norm = first_out.astype(BF16)
    bias = vec_all[:, :1, :in_lanes].astype(F32) + vec_all[:, 1:2, :in_lanes].astype(F32)
    qkv, context, inverse, attention_part = attend(first_norm, small_all, bias, segments, cols, rows // 2)
    residual = x_float + part_sum(attention_part, parts) + shifts[2]
    second_out, second_scaled, second_factor = norm_forward(residual, gains[1], shifts[1])
    second_norm = second_out.astype(BF16)
    small_blocks = list(small_all)
    unit_all = vec_all[:, 2, :units].astype(F32)
    at = in_lanes + cols
    ups = list(up_main) + [b[:, at : at + rest] for b in small_blocks]
    downs = list(down_main) + [b[:, at + rest : at + 2 * rest] for b in small_blocks]
    unit_rows = list(unit_all[:, :main_units]) + list(unit_all[:, main_units:])
    pre_acts = [dot_nn(second_norm, w) + b for w, b in zip(ups, unit_rows)]
    hiddens = [gelu(p).astype(BF16) for p in pre_acts]
    output = (residual + part_sum(sum_products(hiddens, downs), parts) + shifts[3]).astype(BF16)
    down_sums = [dot_tn(grad_rows, h).astype(BF16) for h in hiddens]
    pre_grads = [gelu_back(p, dot_nn(grad_rows, w)) for p, w in zip(pre_acts, downs)]
    pre_halves = [p.astype(BF16) for p in pre_grads]
    unit_sums = [jnp.sum(p, axis=0) for p in pre_grads]
    up_sums = [dot_tn(second_norm, p).astype(BF16) for p in pre_halves]
    second_grad = part_sum(sum_products(pre_halves, ups), parts)
    residual_grad = upstream + norm_backward(second_grad, second_scaled, second_factor, gains[1])
    residual_half = residual_grad.astype(BF16)
    triple, bias_sum = attend_back(residual_half, small_all, qkv, context, inverse, segments, cols, rows // 2)
    first_part = sum_products(list(triple), [b[:, :in_lanes] for b in small_blocks])
    first_grad = part_sum(first_part, parts)
    input_grad = residual_grad + norm_backward(first_grad, first_scaled, first_factor, gains[0])
    blank = jnp.zeros((width, spare), BF16)
    small_sums = [
        jnp.concatenate(
            [
                dot_tn(first_norm, triple[s]).astype(BF16),
                dot_tn(residual_half, context[s]).astype(BF16),
                up_sums[slots + s],
                down_sums[slots + s],
                blank,
            ],
            axis=1,
        )
        for s in range(slots)
    ]
    down_grad, up_grad, small_grad = scatter_grads(
        [jnp.stack(down_sums[:slots]), jnp.stack(up_sums[:slots]), jnp.stack(small_sums)]
    )
    rows_sum = jnp.stack(
        [
            jnp.sum(first_grad * first_scaled, axis=0),
            jnp.sum(second_grad * second_scaled, axis=0),
            jnp.sum(first_grad, axis=0),
            jnp.sum(second_grad, axis=0),
            jnp.sum(residual_grad, axis=0),
            jnp.sum(upstream, axis=0),
        ]
    )
    unit_sum = jnp.stack([jnp.concatenate([unit_sums[s], unit_sums[slots + s]]) for s in range(slots)])
    rows_total, bias_total, unit_total = lax.psum((rows_sum, bias_sum, unit_sum), ("slot",) + FSDP)
    bias_grad = lax.dynamic_index_in_dim(bias_total, slot, 0, keepdims=False)
    unit_grad = lax.dynamic_index_in_dim(unit_total, slot, 0, keepdims=False)
    return (
        from_slot(output, owned), from_slot(input_grad.astype(BF16), owned), rows_total, bias_grad, unit_grad,
        down_grad, up_grad, small_grad,
    )


def on_device(
    block_input,
    segment_ids,
    norm_gains,
    row_biases,
    in_projection,
    query_value_bias,
    out_projection,
    up_weight,
    unit_bias,
    down_weight,
    cotangent,
):
    local, rows_each, width = block_input.shape
    rows_mb = segment_ids.shape[1]
    cols = in_projection.shape[2]
    units = up_weight.shape[1]
    shard_rows = up_weight.shape[0]
    slots, parts = lax.axis_size("slot"), lax.axis_size("part")
    slot, part = lax.axis_index("slot"), lax.axis_index("part")
    fsdp_index = lax.axis_index("fy") * lax.axis_size("fx") + lax.axis_index("fx")
    batch, image = slot % local, slot // local
    late = image == 1

    half_rows = rows_mb // IMG_MB
    padding = rows_mb - IMG_MB * IMG
    edge = round_up(max(half_rows - IMG, padding - (half_rows - IMG)), 16)
    tail = round_up(padding, 16)
    rows = round_up(half_rows + edge + tail, 128)
    filler = rows - half_rows - edge - tail
    paired = lax.axis_size("fy") == 2 and lax.axis_size("fx") == 2 and slots == 4 and parts == 2
    paired = paired and shard_rows % 32 == 0 and filler == 0

    def edges(main):
        near = jnp.where(late, main[:edge], main[half_rows - edge :])
        far = main[half_rows - tail :]
        return jnp.concatenate([near, far])

    def to_slot(value):
        mine = lax.dynamic_index_in_dim(value, batch, 0, keepdims=False)
        send = lax.dynamic_index_in_dim(value, 1 - batch, 0, keepdims=False)
        other = slot_swap(send, 1, slots)
        pair = jnp.where(batch == 0, jnp.stack([mine, other]), jnp.stack([other, mine]))
        main = part_gather(pair, parts).swapaxes(0, 1).reshape(half_rows, width)
        beyond = slot_swap(edges(main), local, slots)
        return jnp.concatenate([main, beyond, jnp.zeros((filler, width), value.dtype)])

    def from_slot(value, owned):
        main = value[:half_rows]
        beyond = slot_swap(value[half_rows : half_rows + edge + tail], local, slots)
        keep = owned[:half_rows, None]
        near, far = beyond[:edge], beyond[edge:]
        blank = lambda count: jnp.zeros((count, width), value.dtype)
        early_fill = jnp.concatenate([blank(half_rows - edge), near])
        late_fill = jnp.concatenate([near, blank(half_rows - edge - tail), far])
        main = jnp.where(keep, main, jnp.where(late, late_fill, early_fill))
        main = main.reshape(local, parts, rows_each, width)
        mine = lax.dynamic_index_in_dim(main, part, 1, keepdims=False)
        stay = lax.dynamic_index_in_dim(mine, batch, 0, keepdims=False)
        other = slot_swap(lax.dynamic_index_in_dim(mine, 1 - batch, 0, keepdims=False), 1, slots)
        return jnp.where(batch == 0, jnp.stack([stay, other]), jnp.stack([other, stay]))

    ids = jnp.where(batch == 0, segment_ids[:1], segment_ids[1:])
    filler_ids = lambda count: jnp.full((1, count), -2, jnp.int32)
    early_ids = jnp.concatenate([ids[:, : half_rows + edge], ids[:, rows_mb - tail :], filler_ids(filler)], axis=1)
    late_ids = jnp.concatenate(
        [ids[:, half_rows:], ids[:, half_rows - edge : half_rows], filler_ids(tail + filler)], axis=1
    )
    segr = jnp.where(late, late_ids, early_ids)
    segc = segr.reshape(rows, 1)

    main_units = units // 128 * 128
    rest = units - main_units
    in_lanes = 3 * cols
    small = in_lanes + cols + 2 * rest
    lanes = round_up(small, 128)
    gains, shifts = norm_gains, row_biases
    if paired:
        (
            small_all, up_main, down_main, gd, x_half, cot, first_norm, qkv, context, inverse, residual, second_norm,
            hidden, slope, hidden_rest, slope_rest, rest_up, rest_down,
        ) = forward_stage(
            (in_projection, out_projection, up_weight, down_weight), (query_value_bias, unit_bias.reshape(1, units)),
            block_input, cotangent, gains, shifts, segc, segr, cols, units, lanes, edge, tail,
        )
        gu, down_sum, rest_sums, residual_half, residual_grad, y_rows, sums, unit_sums, unit_rest_sums = middle_stage(
            down_main, up_main, gd, hidden, slope, hidden_rest, slope_rest, rest_up, rest_down, cot, second_norm, residual,
            gains, shifts, cols, rest, lanes - small,
        )
        in_grad, out_grad, up_grad, down_grad, input_grad, output, gain_grad, shift_grad, bias_grad, unit_grad = backward_stage(
            small_all, gu, rest_sums, residual_half, first_norm, qkv, context, inverse, segc, segr, x_half, residual_grad,
            y_rows, gains, down_sum, sums, unit_sums, unit_rest_sums, cols, rest, edge, tail, rows_each,
        )
        unit_grad = unit_grad.reshape(units)
    else:
        segments = segc[:, 0]
        image_id = (fsdp_index * local + batch) * IMG_MB + image
        owned = (segments == image_id) | (jnp.logical_not(late) & (segments == -1))
        down_t = down_weight.T
        small_shard = jnp.concatenate(
            [
                in_projection.transpose(1, 0, 2).reshape(shard_rows, in_lanes),
                out_projection.T,
                up_weight[:, main_units:],
                down_t[:, main_units:],
                jnp.zeros((shard_rows, lanes - small), BF16),
            ],
            axis=1,
        )
        shards = [small_shard, up_weight[:, :main_units], down_t[:, :main_units]]
        triple_bias = jnp.concatenate([query_value_bias[0], jnp.zeros((cols,), F32), query_value_bias[1]])
        high = triple_bias.astype(BF16)
        low = (triple_bias - high.astype(F32)).astype(BF16)
        wide = round_up(max(in_lanes, units), 128)
        vectors = [jnp.pad(v, (0, wide - v.shape[0])) for v in (high, low, unit_bias)]
        vectors = jnp.concatenate([jnp.stack(vectors), jnp.zeros((13, wide), BF16)])
        output, input_grad, rows_total, bias_grad, unit_grad, down_grad, up_grad, small_grad = plain_layer(
            shards, vectors, to_slot, from_slot, block_input, cotangent, gains, shifts, segments, owned, cols, units, parts
        )
        in_grad = small_grad[:, :in_lanes].reshape(shard_rows, 3, cols).transpose(1, 0, 2)
        out_grad = small_grad[:, in_lanes : in_lanes + cols].T
        at = in_lanes + cols
        up_grad = jnp.concatenate([up_grad, small_grad[:, at : at + rest]], axis=1)
        down_grad = jnp.concatenate([down_grad, small_grad[:, at + rest : at + 2 * rest]], axis=1).T
        gain_grad, shift_grad = rows_total[:2], rows_total[2:]
    return (
        output,
        input_grad.astype(F32),
        gain_grad,
        shift_grad,
        in_grad,
        bias_grad,
        out_grad,
        up_grad,
        unit_grad,
        down_grad,
    )


def solution(mesh):
    fsdp, tensor = mesh.shape["fsdp"], mesh.shape["tensor"]

    def layer(*arrays):
        local = arrays[0].shape[0] // fsdp
        slots = local * IMG_MB
        assert local == 2 and slots == 4 and tensor % slots == 0 and fsdp % 2 == 0
        grid = Mesh(
            mesh.devices.reshape(fsdp // 2, 2, slots, tensor // slots), ("fy", "fx", "slot", "part")
        )
        tens = ("slot", "part")
        return jax.shard_map(
            on_device,
            mesh=grid,
            in_specs=(
                P(FSDP, tens, None),
                P(FSDP, None),
                P(),
                P(),
                P(None, FSDP, tens),
                P(None, tens),
                P(tens, FSDP),
                P(FSDP, tens),
                P(tens),
                P(tens, FSDP),
                P(FSDP, tens, None),
            ),
            out_specs=(
                P(FSDP, tens, None),
                P(FSDP, tens, None),
                P(),
                P(),
                P(None, FSDP, tens),
                P(None, tens),
                P(tens, FSDP),
                P(FSDP, tens),
                P(tens),
                P(tens, FSDP),
            ),
            check_vma=False,
        )(*arrays)

    return layer
```

```python
import functools
import math

import jax
import jax.numpy as jnp
from jax import lax
from jax.experimental import pallas as pl
from jax.experimental.pallas import tpu as pltpu
from jax.sharding import Mesh
from jax.sharding import PartitionSpec as P

DH = 72
IMG = 729
IMG_MB = 2
EPS = 1e-06
GELU_C = 0.7978845608028654
F32 = jnp.float32
BF16 = jnp.bfloat16
FSDP = ("fy", "fx")
SCALE = DH ** (-0.5)
LOG2E = math.log2(math.e)


def norm_forward(values, norm_gain, norm_shift):
    center = values - jnp.mean(values, axis=-1, keepdims=True)
    factor = lax.rsqrt(jnp.mean(center * center, axis=-1, keepdims=True) + EPS)
    scaled = center * factor
    return (scaled * norm_gain + norm_shift, scaled, factor)


def norm_backward(upstream, scaled, factor, norm_gain):
    inside = upstream * norm_gain
    return factor * (
        inside
        - jnp.mean(inside, axis=-1, keepdims=True)
        - scaled * jnp.mean(inside * scaled, axis=-1, keepdims=True)
    )


def gelu(pre_act):
    return (
        0.5
        * pre_act
        * (1.0 + jnp.tanh(GELU_C * (pre_act + 0.044715 * pre_act * pre_act * pre_act)))
    )


def gelu_both(pre_act):
    square = pre_act * pre_act
    curve = jnp.tanh(GELU_C * pre_act * (1.0 + 0.044715 * square))
    rise = 0.5 * (1.0 + curve)
    slope = rise + 0.5 * pre_act * (1.0 - curve * curve) * GELU_C * (1.0 + 3.0 * 0.044715 * square)
    return pre_act * rise, slope


def gelu_back(pre_act, upstream):
    return jax.vjp(gelu, pre_act)[1](upstream)[0]


def dot_nn(left, right):
    return lax.dot_general(left, right, (((1,), (0,)), ((), ())), preferred_element_type=F32)


def dot_nt(left, right):
    return lax.dot_general(left, right, (((1,), (1,)), ((), ())), preferred_element_type=F32)


def dot_tn(left, right):
    return lax.dot_general(left, right, (((0,), (0,)), ((), ())), preferred_element_type=F32)


def sum_products(lefts, rights):
    total = dot_nt(lefts[0], rights[0])
    for left, right in zip(lefts[1:], rights[1:]):
        total = total + dot_nt(left, right)
    return total


def round_up(value, unit):
    return -(-value // unit) * unit


def swap(value, axis):
    return lax.ppermute(value, axis, [(0, 1), (1, 0)])


def slot_swap(value, stride, slots):
    return lax.ppermute(value, "slot", [(s, s ^ stride) for s in range(slots)])


def part_sum(value, parts):
    value = value.astype(BF16)
    if parts == 2:
        return value.astype(F32) + swap(value, "part").astype(F32)
    return lax.psum(value.astype(F32), "part")


def part_gather(value, parts):
    if parts == 2:
        other = swap(value, "part")
        first = lax.axis_index("part") == 0
        return jnp.stack([jnp.where(first, value, other), jnp.where(first, other, value)])
    return lax.all_gather(value, "part", axis=0)


def add_half(left, right):
    return (left.astype(F32) + right.astype(F32)).astype(BF16)


MESH = pl.DeviceIdType.MESH


class Place:
    def __init__(self):
        self.y, self.x = lax.axis_index("fy"), lax.axis_index("fx")
        self.z = lax.axis_index("slot")
        self.f = 2 * self.y + self.x
        self.across_x, self.across_y = {"fx": 1 - self.x}, {"fy": 1 - self.y}
        self.c = lax.axis_index("part")
        self.above = {"slot": jnp.minimum(self.z + 1, 3)}
        self.below = {"slot": jnp.maximum(self.z - 1, 0)}
        self.batch, self.image = self.z % 2, self.z // 2
        self.mate = {"part": 1 - self.c}
        self.pair = {"slot": self.z + 1 - 2 * self.batch}
        self.cross = {"slot": self.z + 2 - 4 * self.image}

    def owned(self, segments):
        mine = segments == (self.f * 2 + self.batch) * IMG_MB + self.image
        return mine | ((segments == -1) & (self.image == 0))

    def behind(self):
        return jnp.where((self.z == 1) | (self.z == 2), 1, 0)

    def slot_after(self, d):
        return {"slot": (self.z + d) % 4}

    def barrier(self):
        sem = pltpu.get_barrier_semaphore()
        others = [self.across_x, self.across_y, self.mate] + [self.slot_after(d) for d in (1, 2, 3)]
        for device in others:
            pl.semaphore_signal(sem, inc=1, device_id=device, device_id_type=MESH)
        pl.semaphore_wait(sem, len(others))

    def far_first(self, i):
        low = self.z < 2
        near = jnp.where(low, self.z, 3 - self.z)
        at = jnp.where(i == 0, 3, jnp.where(i == 1, 2, jnp.where(i == 2, 1 - near, near)))
        return jnp.where(low, at, 3 - at)


def send(src, dst, send_sem, recv_sem, device):
    return pltpu.make_async_remote_copy(
        src_ref=src, dst_ref=dst, send_sem=send_sem, recv_sem=recv_sem, device_id=device, device_id_type=MESH
    )


class Gather:
    SEMS = 11

    def __init__(self, place, shards, w, sems, local_sem, rows):
        self.p, self.shards, self.w, self.rows = place, shards, w, rows
        (self.zr, self.zu, self.zd, self.xr, self.xs, self.yr, self.ys, self.ar, self.asn, self.br, self.bs) = sems
        self.local_sem = local_sem

    def block(self, k, slot, owner, half=None):
        at, count = owner * self.rows, self.rows
        if half is not None:
            count = count // 2
            at = at + half * count
        return self.w[k].at[slot, pl.ds(pl.multiple_of(at, 16), count), :]

    def mine(self, k, slot, shard):
        return self.shards[k] if shard else self.block(k, slot, self.p.f)

    def up(self, k, slot, shard=False):
        dst = self.block(k, slot, self.p.f)
        return send(self.mine(k, slot, shard), dst, self.zu.at[k, slot], self.zr.at[k, slot], self.p.above)

    def down(self, k, slot, shard=False):
        dst = self.block(k, slot, self.p.f)
        return send(self.mine(k, slot, shard), dst, self.zd.at[k, slot], self.zr.at[k, slot], self.p.below)

    def to_x(self, k, slot, shard=False):
        dst = self.block(k, slot, self.p.f)
        return send(self.mine(k, slot, shard), dst, self.xs.at[k, slot], self.xr.at[k, slot], self.p.across_x)

    def to_y(self, k, slot, shard=False):
        dst = self.block(k, slot, self.p.f)
        return send(self.mine(k, slot, shard), dst, self.ys.at[k, slot], self.yr.at[k, slot], self.p.across_y)

    def from_x(self, k, slot):
        ref = self.block(k, slot, self.p.f ^ 1)
        return send(ref, ref, self.xs.at[k, slot], self.xr.at[k, slot], self.p.across_x)

    def from_y(self, k, slot):
        ref = self.block(k, slot, self.p.f ^ 2)
        return send(ref, ref, self.ys.at[k, slot], self.yr.at[k, slot], self.p.across_y)

    def corner_y(self, k, slot):
        ref = self.block(k, slot, self.p.f ^ 1, 0)
        return send(ref, ref, self.asn.at[k, slot], self.ar.at[k, slot], self.p.across_y)

    def corner_x(self, k, slot):
        ref = self.block(k, slot, self.p.f ^ 2, 1)
        return send(ref, ref, self.bs.at[k, slot], self.br.at[k, slot], self.p.across_x)

    def wait_corner(self, k, slot):
        ref = self.block(k, slot, self.p.f ^ 3, 0)
        send(ref, ref, self.asn.at[k, slot], self.ar.at[k, slot], self.p.across_y).wait_recv()
        ref = self.block(k, slot, self.p.f ^ 3, 1)
        send(ref, ref, self.bs.at[k, slot], self.br.at[k, slot], self.p.across_x).wait_recv()

    def local(self, k):
        return pltpu.make_async_copy(self.shards[k], self.block(k, self.p.z, self.p.f), self.local_sem.at[k])

    def start_z(self, k):
        @pl.when(self.p.z < 3)
        def _():
            self.up(k, self.p.z, True).start()

        @pl.when(self.p.z > 0)
        def _():
            self.down(k, self.p.z, True).start()

    def start_xy(self, k):
        self.to_x(k, self.p.z, True).start()
        self.to_y(k, self.p.z, True).start()
        self.local(k).start()

    def pass_on(self, k, d):
        z = self.p.z

        @pl.when(z >= d)
        def _():
            self.up(k, z - d).wait_recv()

            @pl.when(z < 3)
            def _():
                self.up(k, z - d).start()

            self.to_x(k, z - d).start()
            self.to_y(k, z - d).start()

        @pl.when(z + d <= 3)
        def _():
            self.down(k, z + d).wait_recv()

            @pl.when(z > 0)
            def _():
                self.down(k, z + d).start()

            self.to_x(k, z + d).start()
            self.to_y(k, z + d).start()

    def corner(self, k, d):
        def one(slot):
            self.from_x(k, slot).wait_recv()
            self.corner_y(k, slot).start()
            self.from_y(k, slot).wait_recv()
            self.corner_x(k, slot).start()

        z = self.p.z
        if d == 0:
            one(z)
        else:
            pl.when(z >= d)(lambda: one(z - d))
            pl.when(z + d <= 3)(lambda: one(z + d))

    def arrive(self, k):
        self.local(k).wait()
        for slot in range(4):
            self.wait_corner(k, slot)

    def drain(self, k):
        z = self.p.z
        for slot in range(4):
            self.to_x(k, slot).wait_send()
            self.to_y(k, slot).wait_send()
            self.corner_y(k, slot).wait_send()
            self.corner_x(k, slot).wait_send()

            @pl.when((z < 3) & (slot <= z))
            def _(slot=slot):
                self.up(k, slot).wait_send()

            @pl.when((z > 0) & (slot >= z))
            def _(slot=slot):
                self.down(k, slot).wait_send()


def gather_weights(shards):
    slots = lax.axis_size("slot")
    whole = [lax.all_gather(s, ("slot",) + FSDP, axis=0) for s in shards]
    return [w.reshape(slots, -1, w.shape[-1]) for w in whole]


class Rows:
    SEMS = 11

    def __init__(self, place, index, src, dst, sems, rows_each, edge, tail):
        self.p, self.src, self.dst, self.each = place, src, dst, rows_each
        self.half = 4 * rows_each
        self.edge, self.tail = edge, tail
        self.sems = [sem.at[index] for sem in sems]

    def at(self, row, count):
        return self.dst.at[pl.ds(pl.multiple_of(row, 16), count), :]

    def block(self, near, core):
        batch = self.p.batch if near else 1 - self.p.batch
        return self.at((2 * batch + core) * self.each, self.each)

    def own(self):
        return pltpu.make_async_copy(self.src.at[self.p.batch], self.block(True, self.p.c), self.sems[0])

    def to_mate(self):
        return send(self.src.at[self.p.batch], self.block(True, self.p.c), self.sems[1], self.sems[2], self.p.mate)

    def to_pair(self):
        return send(self.src.at[1 - self.p.batch], self.block(True, self.p.c), self.sems[3], self.sems[4], self.p.pair)

    def pass_on(self):
        ref = self.block(False, self.p.c)
        return send(ref, ref, self.sems[5], self.sems[6], self.p.mate)

    def edge_out(self):
        src = self.at(jnp.where(self.p.image == 0, self.half - self.edge, 0), self.edge)
        return send(src, self.at(self.half, self.edge), self.sems[7], self.sems[8], self.p.cross)

    def tail_out(self):
        src = self.at(self.half - self.tail, self.tail)
        dst = self.at(self.half + self.edge, self.tail)
        return send(src, dst, self.sems[7], self.sems[8], self.p.cross)

    def edge_mate(self):
        ref = self.at(self.half, self.edge)
        return send(ref, ref, self.sems[9], self.sems[10], self.p.mate)

    def tail_mate(self):
        ref = self.at(self.half + self.edge, self.tail)
        return send(ref, ref, self.sems[9], self.sems[10], self.p.mate)

    def start(self):
        self.to_pair().start()
        self.to_mate().start()
        self.own().start()

    def forward(self):
        ref = self.block(False, self.p.c)
        send(ref, ref, self.sems[3], self.sems[4], self.p.pair).wait_recv()
        self.pass_on().start()

    def main_ready(self):
        self.own().wait()
        ref = self.block(True, 1 - self.p.c)
        send(ref, ref, self.sems[1], self.sems[2], self.p.mate).wait_recv()
        ref = self.block(False, 1 - self.p.c)
        send(ref, ref, self.sems[5], self.sems[6], self.p.mate).wait_recv()

    def edges(self):
        pl.when(self.p.c == 0)(lambda: self.edge_out().start())
        pl.when(self.p.c == 1)(lambda: self.tail_out().start())

    def edges_forward(self):
        @pl.when(self.p.c == 0)
        def _():
            self.edge_out().wait_recv()
            self.edge_mate().start()

        @pl.when(self.p.c == 1)
        def _():
            self.tail_out().wait_recv()
            self.tail_mate().start()

    def edges_ready(self):
        pl.when(self.p.c == 0)(lambda: self.tail_mate().wait_recv())
        pl.when(self.p.c == 1)(lambda: self.edge_mate().wait_recv())

    def drain(self):
        self.to_mate().wait_send()
        self.to_pair().wait_send()
        self.pass_on().wait_send()

        @pl.when(self.p.c == 0)
        def _():
            self.edge_out().wait_send()
            self.edge_mate().wait_send()

        @pl.when(self.p.c == 1)
        def _():
            self.tail_out().wait_send()
            self.tail_mate().wait_send()


def row_tiles(rows, step, body):
    def one(t, carry):
        body(pl.ds(pl.multiple_of(t * step, 16), step))
        return carry

    lax.fori_loop(0, rows // step, one, 0)


def forward_kernel(*refs, cols, unit_rest, edge, tail, tile):
    (in_ref, out_ref, up_whole, down_whole, qv_ref, unit_ref, x_src, c_src, gain_ref, shift_ref, segc_ref) = refs[:11]
    segr_ref, refs = refs[11], refs[1:]
    (ws, wu, wd, gd) = refs[11:15]
    outs, refs = refs[15:29], refs[29:]
    held, refs = refs[:14], refs[14:]
    (x_ref, c_ref, first_ref, qkv_ref, ctx_ref, inv_ref, res_ref, second_ref) = held[:8]
    (hidden_ref, slope_ref, hidden_rest, slope_rest, rest_up, rest_down) = held[8:]
    (blocks, unit_blocks, grads, part, part_out, part_in, bias_rest, vec_all) = refs[:8]
    (small_ref, up_ref, down_ref, vec_ref) = refs[8:12]
    gather_sems, local_sem = refs[12 : 12 + Gather.SEMS], refs[12 + Gather.SEMS]
    tail_refs = refs[13 + Gather.SEMS :]
    row_sems = tail_refs[: Rows.SEMS]
    (vec_s, vec_r, load_sem, part_s, part_r, unit_sem, grad_sem, out_sem) = tail_refs[Rows.SEMS :]

    def leave(n):
        return pltpu.make_async_copy(held[n], outs[n], out_sem.at[n])

    main, rest = up_ref.shape[1], unit_rest
    rows, width = x_ref.shape
    place = Place()
    for n in range(3):
        small_ref[:, n * cols : (n + 1) * cols] = in_ref[n].T
    at = 3 * cols
    small_ref[:, at : at + cols] = out_ref[...].T
    at = at + cols
    small_ref[:, at : at + rest] = up_whole[:, main:]
    small_ref[:, at + rest : at + 2 * rest] = down_whole[:, main:]
    at = at + 2 * rest
    if at < small_ref.shape[1]:
        small_ref[:, at:] = jnp.zeros((small_ref.shape[0], small_ref.shape[1] - at), BF16)
    vec_ref[...] = jnp.zeros_like(vec_ref)
    for n in (0, 1):
        high = qv_ref[n : n + 1, :].astype(BF16)
        lo = 2 * n * cols
        vec_ref[0:1, lo : lo + cols] = high
        vec_ref[1:2, lo : lo + cols] = (qv_ref[n : n + 1, :] - high.astype(F32)).astype(BF16)
    vec_ref[2:3, : main + rest] = unit_ref[...]
    place.barrier()
    shards = (small_ref, up_ref, down_ref)
    g = Gather(place, shards, (ws, wu, wd), gather_sems, local_sem, small_ref.shape[0])
    each = x_src.shape[1]
    x_rows = Rows(place, 0, x_src, x_ref, row_sems, each, edge, tail)
    c_rows = Rows(place, 1, c_src, c_ref, row_sems, each, edge, tail)

    def vec_to(d):
        device = place.slot_after(d)
        return send(vec_ref, vec_all.at[place.z], vec_s.at[d], vec_r.at[d], device)

    def vec_from(d):
        ref = vec_all.at[(place.z + 4 - d) % 4]
        return send(ref, ref, vec_s.at[d], vec_r.at[d], place.slot_after(d))

    g.start_z(0)
    g.start_xy(0)
    for d in (1, 2, 3):
        vec_to(d).start()
    x_rows.start()
    vec_all[place.z] = vec_ref[...]
    up_ref[...] = up_whole[:, :main]
    down_ref[...] = down_whole[:, :main]
    g.pass_on(0, 1)
    g.corner(0, 0)
    x_rows.forward()
    g.pass_on(0, 2)
    x_rows.main_ready()
    x_rows.edges()
    g.corner(0, 1)
    x_rows.edges_forward()
    g.pass_on(0, 3)
    g.start_z(1)
    x_rows.edges_ready()

    def first(span):
        value = x_ref[span, :].astype(F32)
        out, _, _ = norm_forward(value, gain_ref[0:1, :], shift_ref[0:1, :])
        first_ref[span, :] = out.astype(BF16)

    row_tiles(rows, 128, first)
    leave(0).start()
    g.corner(0, 2)
    g.corner(0, 3)
    leave(2).start()
    for d in (1, 2, 3):
        vec_from(d).wait_recv()
    g.arrive(0)

    later = []
    for k in (1, 2):
        later.append(lambda k=k: g.start_xy(k))
        if k == 1:
            later.append(lambda: c_rows.start())
        for d in (1, 2, 3):
            later.append(lambda k=k, d=d: g.pass_on(k, d))
            later.append(lambda k=k, d=d: g.corner(k, d - 1))
        if k == 1:
            later.append(lambda: g.start_z(2))
            later.append(lambda: c_rows.forward())
            later.append(lambda: (c_rows.main_ready(), c_rows.edges()))
        later.append(lambda k=k: g.corner(k, 3))
        if k == 1:
            later.append(lambda: c_rows.edges_forward())

    def step(count=1):
        for _ in range(count):
            if later:
                later.pop(0)()

    step(2)

    def load(s):
        return pltpu.make_async_copy(ws.at[s], blocks.at[s % 2], load_sem.at[s % 2])

    heads = cols // DH
    rest_up[...] = jnp.zeros_like(rest_up)
    rest_down[...] = jnp.zeros_like(rest_down)
    bias_rest[...] = jnp.zeros_like(bias_rest)
    part[...] = jnp.zeros_like(part)
    load(0).start()
    points = 1 + heads
    inside = [later.pop(0) for _ in range(4 * points)]

    def at_point(s, n):
        for one in range(4):
            pl.when(s == one)(lambda one=one: inside[one * points + n]() and None)

    def one_slot(s, carry):
        load(s).wait()
        pl.when(s < 3)(lambda: load(s + 1).start())
        w = blocks.at[s % 2]
        bias = vec_all[s, 0:1, : 3 * cols].astype(F32) + vec_all[s, 1:2, : 3 * cols].astype(F32)
        projected = dot_nn(first_ref[...], w[:, : 3 * cols]) + bias
        qkv_ref[s] = projected.astype(BF16)
        at_point(s, 0)
        for head in range(heads):
            attend_head(qkv_ref, ctx_ref, inv_ref, segc_ref, segr_ref, s, head, cols, tile)
            at_point(s, 1 + head)
        part[...] += dot_nt(ctx_ref[s], w[:, 3 * cols : 4 * cols])
        at = 4 * cols
        for one in range(4):

            @pl.when(s == one)
            def _(one=one):
                rest_up[:, one * rest : (one + 1) * rest] = w[:, at : at + rest]
                rest_down[:, one * rest : (one + 1) * rest] = w[:, at + rest : at + 2 * rest]
                bias_rest[:, one * rest : (one + 1) * rest] = vec_all[one, 2:3, main : main + rest].astype(F32)

        return carry

    lax.fori_loop(0, 4, one_slot, 0)

    def halves(h):
        return pl.ds(h * (rows // 2), rows // 2)

    def exchange(h):
        src, dst = part_out.at[halves(h), :], part_in.at[halves(h), :]
        return send(src, dst, part_s.at[h], part_r.at[h], place.mate)

    for h in (0, 1):
        part_out[halves(h), :] = part[halves(h), :].astype(BF16)
        exchange(h).start()
    step()
    for n in (3, 4, 5, 12, 13):
        leave(n).start()
    for h in (0, 1):
        exchange(h).wait_recv()

    def second(span):
        value = x_ref[span, :].astype(F32) + (part_out[span, :].astype(F32) + part_in[span, :].astype(F32))
        value = value + shift_ref[2:3, :]
        res_ref[span, :] = value
        out, _, _ = norm_forward(value, gain_ref[1:2, :], shift_ref[1:2, :])
        second_ref[span, :] = out.astype(BF16)

    row_tiles(rows, 128, second)
    g.arrive(1)

    def unit_load(s):
        return pltpu.make_async_copy(wu.at[s], unit_blocks.at[s % 2], unit_sem.at[s % 2])

    unit_load(0).start()
    passing = [later.pop(0) for _ in range(4)]

    def one_block(s, carry):
        unit_load(s).wait()
        pl.when(s < 3)(lambda: unit_load(s + 1).start())
        bias = vec_all[s, 2:3, :main].astype(F32)

        def units(span):
            hidden, slope = gelu_both(dot_nn(second_ref[span, :], unit_blocks[s % 2]) + bias)
            hidden_ref[s, span, :] = hidden.astype(BF16)
            slope_ref[s, span, :] = slope.astype(BF16)

        row_tiles(rows, tile, units)
        for one in range(4):
            pl.when(s == one)(lambda one=one: passing[one]() and None)
        return carry

    lax.fori_loop(0, 4, one_block, 0)

    def units_rest(span):
        hidden, slope = gelu_both(dot_nn(second_ref[span, :], rest_up[...]) + bias_rest[...])
        hidden_rest[span, :] = hidden.astype(BF16)
        slope_rest[span, :] = slope.astype(BF16)

    for n in (6, 7):
        leave(n).start()
    row_tiles(rows, tile, units_rest)
    step()
    for n in (8, 9, 10, 11):
        leave(n).start()
    c_rows.edges_ready()
    c_rows.drain()
    c_ref[...] = jnp.where(place.owned(segc_ref[...]), c_ref[...], jnp.zeros_like(c_ref))

    def grad_out(s):
        return pltpu.make_async_copy(grads.at[s % 2], gd.at[s], grad_sem.at[s % 2])

    def down_grad(s, carry):
        pl.when(s >= 2)(lambda: grad_out(s - 2).wait())
        grads[s % 2] = dot_tn(c_ref[...], hidden_ref[s]).astype(BF16)
        grad_out(s).start()
        return carry

    lax.fori_loop(0, 2, down_grad, 0)
    step()
    lax.fori_loop(2, 4, down_grad, 0)
    step(len(later))
    leave(1).start()
    for s in (2, 3):
        grad_out(s).wait()
    g.arrive(2)
    for n in range(14):
        leave(n).wait()
    for k in (0, 1, 2):
        g.drain(k)
    x_rows.drain()
    for d in (1, 2, 3):
        vec_to(d).wait_send()
    for h in (0, 1):
        exchange(h).wait_send()


def forward_stage(
    weights, biases, x_src, c_src, gains, shifts, segc, segr, cols, units, lanes, edge, tail
):
    rows, width, shard_rows, main = segc.shape[0], x_src.shape[2], weights[2].shape[0], units // 128 * 128
    unit_rest = units - main
    heads, rest_lanes = cols // DH, round_up(4 * unit_rest, 128)
    vectors = (16, round_up(max(3 * cols, units), 128))
    vmem = pl.BlockSpec(memory_space=pltpu.VMEM)
    far = pl.BlockSpec(memory_space=pl.ANY)
    shape = jax.ShapeDtypeStruct
    dma = pltpu.SemaphoreType.DMA
    return pl.pallas_call(
        functools.partial(forward_kernel, cols=cols, unit_rest=unit_rest, edge=edge, tail=tail, tile=rows // 2),
        in_specs=[vmem] * 12,
        out_specs=[far] * 18,
        out_shape=[
            shape((4, width, lanes), BF16),
            shape((4, width, main), BF16),
            shape((4, width, main), BF16),
            shape((4, width, main), BF16),
            shape((rows, width), BF16),
            shape((rows, width), BF16),
            shape((rows, width), BF16),
            shape((4, rows, 3 * cols), BF16),
            shape((4, rows, cols), BF16),
            shape((4, rows, heads), F32),
            shape((rows, width), F32),
            shape((rows, width), BF16),
            shape((4, rows, main), BF16),
            shape((4, rows, main), BF16),
            shape((rows, rest_lanes), BF16),
            shape((rows, rest_lanes), BF16),
            shape((width, rest_lanes), BF16),
            shape((width, rest_lanes), BF16),
        ],
        scratch_shapes=[
            pltpu.VMEM((rows, width), BF16),
            pltpu.VMEM((rows, width), BF16),
            pltpu.VMEM((rows, width), BF16),
            pltpu.VMEM((4, rows, 3 * cols), BF16),
            pltpu.VMEM((4, rows, cols), BF16),
            pltpu.VMEM((4, rows, heads), F32),
            pltpu.VMEM((rows, width), F32),
            pltpu.VMEM((rows, width), BF16),
            pltpu.VMEM((4, rows, main), BF16),
            pltpu.VMEM((4, rows, main), BF16),
            pltpu.VMEM((rows, rest_lanes), BF16),
            pltpu.VMEM((rows, rest_lanes), BF16),
            pltpu.VMEM((width, rest_lanes), BF16),
            pltpu.VMEM((width, rest_lanes), BF16),
            pltpu.VMEM((2, width, lanes), BF16),
            pltpu.VMEM((2, width, main), BF16),
            pltpu.VMEM((2, width, main), BF16),
            pltpu.VMEM((rows, width), F32),
            pltpu.VMEM((rows, width), BF16),
            pltpu.VMEM((rows, width), BF16),
            pltpu.VMEM((1, rest_lanes), F32),
            pltpu.VMEM((4,) + vectors, BF16),
            pltpu.VMEM((shard_rows, lanes), BF16),
            pltpu.VMEM((shard_rows, main), BF16),
            pltpu.VMEM((shard_rows, main), BF16),
            pltpu.VMEM(vectors, BF16),
        ]
        + [dma((3, 4))] * Gather.SEMS
        + [dma((3,))]
        + [dma((2,))] * Rows.SEMS
        + [dma((4,)), dma((4,)), dma((2,)), dma((2,)), dma((2,)), dma((2,)), dma((2,)), dma((14,))],
        compiler_params=pltpu.CompilerParams(collective_id=1, has_side_effects=True, vmem_limit_bytes=64000000),
        name="forward",
    )(*weights, *biases, x_src, c_src, gains, shifts, segc, segr)


def middle_kernel(*refs, cols, unit_rest):
    (wd, wu, gd) = refs[:3]
    (hidden_far, slope_far, hidden_rest, slope_rest, rest_up, rest_down) = refs[3:9]
    (c_far, second_far, res_far, gain_ref, shift_ref) = refs[9:14]
    gu = refs[14]
    (d_out, rest_sums, half_ref, grad_ref, y_ref, sums_ref, unit_ref, unit_rest_ref) = refs[15:23]
    (blocks, grads, pre_half, part, part_out, part_in, part_in2) = refs[23:30]
    (hidden_ref, slope_ref, c_ref, second_ref, res_ref) = refs[30:35]
    d_bufs, d_own = refs[35:40], refs[40:43]
    refs = refs[43:]
    sems, loads = refs[: Reduce.SEMS], refs[Reduce.SEMS : Reduce.SEMS + 3]
    load_sem, grad_sem, part_s, part_r, in_sem, unit_sem = refs[Reduce.SEMS + 3 :]
    rows, width = c_ref.shape
    rest = unit_rest
    place = Place()
    place.barrier()

    def down_final(total):
        d_out[...] = total[...].astype(F32)

    r = Reduce(place, (gd,), (d_own,), (down_final,), (d_bufs,), sems, loads, d_out.shape[0])

    def load(w, slot, buffer):
        return pltpu.make_async_copy(w.at[slot], blocks.at[buffer], load_sem.at[buffer])

    def halves(h):
        return pl.ds(h * (rows // 2), rows // 2)

    def exchange(n, h):
        dst = (part_in, part_in2)[n]
        src, dst = part_out.at[halves(h), :], dst.at[halves(h), :]
        return send(src, dst, part_s.at[n, h], part_r.at[n, h], place.mate)

    def enter(n):
        far, near = ((c_far, c_ref), (second_far, second_ref), (res_far, res_ref))[n]
        return pltpu.make_async_copy(far, near, in_sem.at[n])

    def unit_loads(s):
        return (
            pltpu.make_async_copy(hidden_far.at[s], hidden_ref.at[s % 2], unit_sem.at[0, s % 2]),
            pltpu.make_async_copy(slope_far.at[s], slope_ref.at[s % 2], unit_sem.at[1, s % 2]),
        )

    def start_units(s):
        for copy in unit_loads(s):
            copy.start()

    enter(0).start()
    load(wd, 0, 0).start()
    start_units(0)
    r.start(0)
    enter(1).start()
    enter(2).start()
    enter(0).wait()
    part[...] = dot_nt(hidden_rest[...], rest_down[...])
    grad_rest = slope_rest[...].astype(F32) * dot_nn(c_ref[...], rest_down[...])
    unit_rest_ref[...] = jnp.sum(grad_rest, axis=0, keepdims=True)
    half_rest = grad_rest.astype(BF16)

    def down_block(s, carry):
        load(wd, s, s % 2).wait()
        pl.when(s < 3)(lambda: load(wd, s + 1, (s + 1) % 2).start())
        pl.when(s == 3)(lambda: load(wu, 0, 0).start())
        for copy in unit_loads(s):
            copy.wait()
        pl.when(s < 3)(lambda: start_units(s + 1))
        w = blocks[s % 2]
        part[...] += dot_nt(hidden_ref[s % 2], w)
        grad = slope_ref[s % 2].astype(F32) * dot_nn(c_ref[...], w)
        pre_half[s] = grad.astype(BF16)
        unit_ref[s] = jnp.broadcast_to(jnp.sum(grad, axis=0, keepdims=True), unit_ref.shape[1:])
        r.middle_one(0, s)
        return carry

    lax.fori_loop(0, 4, down_block, 0)
    for h in (0, 1):
        part_out[halves(h), :] = part[halves(h), :].astype(BF16)
        exchange(0, h).start()
    part[...] = dot_nt(half_rest, rest_up[...])

    def up_block(s, carry):
        load(wu, s, s % 2).wait()
        pl.when(s < 3)(lambda: load(wu, s + 1, (s + 1) % 2).start())
        part[...] += dot_nt(pre_half[s], blocks[s % 2])
        return carry

    lax.fori_loop(0, 4, up_block, 0)
    enter(1).wait()
    enter(2).wait()
    for h in (0, 1):
        exchange(0, h).wait_recv()

    def output(span):
        value = part_out[span, :].astype(F32) + part_in[span, :].astype(F32)
        y_ref[span, :] = (res_ref[span, :] + value + shift_ref[3:4, :]).astype(BF16)

    row_tiles(rows, 128, output)
    for h in (0, 1):
        exchange(0, h).wait_send()
        part_out[halves(h), :] = part[halves(h), :].astype(BF16)
        exchange(1, h).start()

    def grad_out(s):
        return pltpu.make_async_copy(grads.at[s % 2], gu.at[s], grad_sem.at[s % 2])

    def up_grad(s, carry):
        pl.when(s >= 2)(lambda: grad_out(s - 2).wait())
        grads[s % 2] = dot_tn(second_ref[...], pre_half[s]).astype(BF16)
        grad_out(s).start()
        n = s - place.behind()
        pl.when((n >= 0) & (n < 3))(lambda: r.line_one(0, n))
        return carry

    lax.fori_loop(0, 4, up_grad, 0)
    up_sum = dot_tn(second_ref[...], half_rest).astype(BF16)
    down_sum = dot_tn(c_ref[...], hidden_rest[...]).astype(BF16)
    rest_sums[...] = jnp.zeros_like(rest_sums)
    for s in range(4):
        rest_sums[s, :, :rest] = up_sum[:, s * rest : (s + 1) * rest]
        rest_sums[s, :, rest : 2 * rest] = down_sum[:, s * rest : (s + 1) * rest]
    for h in (0, 1):
        exchange(1, h).wait_recv()
    sums_ref[...] = jnp.zeros_like(sums_ref)

    def back(span):
        grad = part_out[span, :].astype(F32) + part_in2[span, :].astype(F32)
        upstream = c_ref[span, :].astype(F32)
        _, scaled, factor = norm_forward(res_ref[span, :], gain_ref[1:2, :], shift_ref[1:2, :])
        value = upstream + norm_backward(grad, scaled, factor, gain_ref[1:2, :])
        grad_ref[span, :] = value
        half_ref[span, :] = value.astype(BF16)
        sums_ref[1:2, :] += jnp.sum(grad * scaled, axis=0, keepdims=True)
        sums_ref[3:4, :] += jnp.sum(grad, axis=0, keepdims=True)
        sums_ref[4:5, :] += jnp.sum(value, axis=0, keepdims=True)
        sums_ref[5:6, :] += jnp.sum(upstream, axis=0, keepdims=True)

    row_tiles(rows, 128, back)
    r.line_one(0, 3)
    for s in (2, 3):
        grad_out(s).wait()
    r.drain(0)
    for h in (0, 1):
        exchange(1, h).wait_send()


def middle_stage(
    wd, wu, gd, hidden, slope, hidden_rest, slope_rest, rest_up, rest_down, cot, second, residual, gains, shifts, cols, unit_rest, spare
):
    rows, width = cot.shape
    main, shard_rows = wd.shape[2], width // 4
    vmem = pl.BlockSpec(memory_space=pltpu.VMEM)
    far = pl.BlockSpec(memory_space=pl.ANY)
    shape = jax.ShapeDtypeStruct
    dma = pltpu.SemaphoreType.DMA
    return pl.pallas_call(
        functools.partial(middle_kernel, cols=cols, unit_rest=unit_rest),
        in_specs=[far] * 5 + [vmem] * 4 + [far] * 3 + [vmem] * 2,
        out_specs=[far] + [vmem] * 8,
        out_shape=[
            shape((4, width, main), BF16),
            shape((shard_rows, main), F32),
            shape((4, width, 2 * unit_rest + spare), BF16),
            shape((rows, width), BF16),
            shape((rows, width), F32),
            shape((rows, width), BF16),
            shape((8, width), F32),
            shape((4, 8, main), F32),
            shape((1, rest_up.shape[1]), F32),
        ],
        scratch_shapes=[
            pltpu.VMEM((2, width, main), BF16),
            pltpu.VMEM((2, width, main), BF16),
            pltpu.VMEM((4, rows, main), BF16),
            pltpu.VMEM((rows, width), F32),
            pltpu.VMEM((rows, width), BF16),
            pltpu.VMEM((rows, width), BF16),
            pltpu.VMEM((rows, width), BF16),
            pltpu.VMEM((2, rows, main), BF16),
            pltpu.VMEM((2, rows, main), BF16),
            pltpu.VMEM((rows, width), BF16),
            pltpu.VMEM((rows, width), BF16),
            pltpu.VMEM((rows, width), F32),
        ]
        + reduce_buffers(shard_rows, main)
        + reduce_terms(shard_rows, main)
        + [dma((1, 4))] * Reduce.SEMS
        + [dma((1, 4))] * 3
        + [dma((2,)), dma((2,)), dma((2, 2)), dma((2, 2)), dma((3,)), dma((2, 2))],
        compiler_params=pltpu.CompilerParams(collective_id=3, has_side_effects=True, vmem_limit_bytes=64000000),
        name="middle",
    )(wd, wu, gd, hidden, slope, hidden_rest, slope_rest, rest_up, rest_down, cot, second, residual, gains, shifts)


class Reduce:
    SEMS = 16

    def __init__(self, place, g, own, out, bufs, sems, load_sems, rows):
        self.p, self.g, self.own, self.out, self.rows = place, g, own, out, rows
        self.bufs, self.sems, self.load_sems = bufs, sems, load_sems

    def grad(self, k, slot, owner, half=None):
        at, count = owner * self.rows, self.rows
        if half is not None:
            count = count // 2
            at = at + half * count
        return self.g[k].at[slot, pl.ds(pl.multiple_of(at, 16), count), :]

    def terms(self, k, slot):
        f = self.p.f
        if self.own[k] is None:
            return self.grad(k, slot, f ^ 1, 0), self.grad(k, slot, f ^ 2, 1), self.grad(k, slot, f)
        return tuple(ref.at[slot] for ref in self.own[k])

    def loads(self, k, slot):
        f = self.p.f
        src = self.grad(k, slot, f ^ 1, 0), self.grad(k, slot, f ^ 2, 1), self.grad(k, slot, f)
        pairs = zip(src, self.terms(k, slot), self.load_sems)
        return [pltpu.make_async_copy(one, dst, sem.at[k, slot]) for one, dst, sem in pairs]

    def half(self, ref, slot, half):
        count = self.rows // 2
        return ref.at[slot, half * count : (half + 1) * count, :]

    def copy(self, k, slot, src, dst, index, device):
        return send(src, dst, self.sems[2 * index].at[k, slot], self.sems[2 * index + 1].at[k, slot], device)

    def corner_y(self, k, s):
        return self.copy(k, s, self.grad(k, s, self.p.f ^ 3, 0), self.bufs[k][0].at[s], 0, self.p.across_y)

    def corner_x(self, k, s):
        return self.copy(k, s, self.grad(k, s, self.p.f ^ 3, 1), self.bufs[k][1].at[s], 1, self.p.across_x)

    def x_low(self, k, s):
        return self.copy(k, s, self.bufs[k][0].at[s], self.half(self.bufs[k][2], s, 0), 2, self.p.across_x)

    def x_high(self, k, s):
        dst = self.half(self.bufs[k][2], s, 1)
        return self.copy(k, s, self.grad(k, s, self.p.f ^ 1, 1), dst, 3, self.p.across_x)

    def y_low(self, k, s):
        dst = self.half(self.bufs[k][3], s, 0)
        return self.copy(k, s, self.grad(k, s, self.p.f ^ 2, 0), dst, 4, self.p.across_y)

    def y_high(self, k, s):
        return self.copy(k, s, self.bufs[k][1].at[s], self.half(self.bufs[k][3], s, 1), 5, self.p.across_y)

    def up(self, k, s):
        return self.copy(k, s, self.bufs[k][2].at[s], self.bufs[k][4].at[s], 6, self.p.above)

    def down(self, k, s):
        at = jnp.where(s == self.p.z - 1, 4, s)
        return self.copy(k, s, self.bufs[k][2].at[s], self.bufs[k][4].at[at], 7, self.p.below)

    def from_above(self, k, s):
        at = jnp.where(s == self.p.z, 4, s)
        return self.copy(k, s, self.bufs[k][4].at[at], self.bufs[k][4].at[at], 7, self.p.below), at

    def start_one(self, k, s):
        self.corner_y(k, s).start()
        self.corner_x(k, s).start()
        self.y_low(k, s).start()
        self.x_high(k, s).start()

    def start(self, k):
        def one(i, carry):
            self.start_one(k, self.p.far_first(i))
            return carry

        lax.fori_loop(0, 4, one, 0)
        if self.own[k] is not None:
            for slot in range(4):
                for load in self.loads(k, slot):
                    load.start()

    def tiles(self, rows, body):
        row_tiles(rows, 48 if rows % 48 == 0 else 16, body)

    def middle_one(self, k, i):
        s, count = self.p.far_first(i), self.rows // 2
        low, high = self.bufs[k][0], self.bufs[k][1]
        if self.own[k] is not None:
            for load in self.loads(k, s):
                load.wait()
        own_low, own_high, _ = self.terms(k, s)
        self.corner_y(k, s).wait_recv()

        def add_low(span):
            low[s, span, :] = add_half(low[s, span, :], own_low[span, :])

        self.tiles(count, add_low)
        self.corner_x(k, s).wait_recv()

        def add_high(span):
            high[s, span, :] = add_half(high[s, span, :], own_high[span, :])

        self.tiles(count, add_high)
        self.x_low(k, s).start()
        self.y_high(k, s).start()

    def line_one(self, k, i):
        z, acc, side, far = self.p.z, self.bufs[k][2], self.bufs[k][3], self.bufs[k][4]
        s = self.p.far_first(i)
        self.x_low(k, s).wait_recv()
        self.x_high(k, s).wait_recv()
        self.y_low(k, s).wait_recv()
        self.y_high(k, s).wait_recv()
        own = self.terms(k, s)[2]

        def add(span):
            total = own[span, :].astype(F32) + acc[s, span, :].astype(F32) + side[s, span, :].astype(F32)
            acc[s, span, :] = total.astype(BF16)

        self.tiles(self.rows, add)

        def add_far(at):
            def body(span):
                acc[s, span, :] = add_half(acc[s, span, :], far[at, span, :])

            self.tiles(self.rows, body)

        @pl.when((z > 0) & (s >= z))
        def _():
            self.up(k, s).wait_recv()
            add_far(s)

        @pl.when((z < 3) & (s <= z))
        def _():
            copy, at = self.from_above(k, s)
            copy.wait_recv()
            add_far(at)

        @pl.when(s > z)
        def _():
            self.up(k, s).start()

        @pl.when(s < z)
        def _():
            self.down(k, s).start()

        @pl.when(s == z)
        def _():
            self.out[k](acc.at[s])

    def loop(self, one):
        def body(i, carry):
            one(i)
            return carry

        lax.fori_loop(0, 4, body, 0)

    def drain(self, k):
        def one(s):
            for copy in (self.corner_y, self.corner_x, self.x_low, self.x_high, self.y_low, self.y_high):
                copy(k, s).wait_send()

            @pl.when(s > self.p.z)
            def _():
                self.up(k, s).wait_send()

            @pl.when(s < self.p.z)
            def _():
                self.down(k, s).wait_send()

        self.loop(one)


def reduce_buffers(rows, lanes):
    half, whole = pltpu.VMEM((4, rows // 2, lanes), BF16), pltpu.VMEM((4, rows, lanes), BF16)
    return [half, half, whole, whole, pltpu.VMEM((5, rows, lanes), BF16)]


def reduce_terms(rows, lanes):
    half, whole = pltpu.VMEM((4, rows // 2, lanes), BF16), pltpu.VMEM((4, rows, lanes), BF16)
    return [half, half, whole]


def scatter_grads(chunks):
    count = lax.axis_size("fy") * lax.axis_size("fx")
    split = [c.reshape(c.shape[0] * count, c.shape[1] // count, c.shape[2]) for c in chunks]
    return [lax.psum_scatter(c, ("slot",) + FSDP, scatter_dimension=0).astype(F32) for c in split]


class RowsBack:
    SEMS = 7

    def __init__(self, place, index, window, inbox, owned, out, sems, rows_each, edge, tail):
        self.p, self.window, self.inbox, self.owned, self.out = place, window, inbox, owned, out
        self.each, self.half, self.edge, self.tail = rows_each, 4 * rows_each, edge, tail
        self.sems = [sem.at[index] for sem in sems]

    def edge_out(self):
        src = self.window.at[self.half : self.half + self.edge, :]
        return send(src, self.inbox.at[: self.edge, :], self.sems[0], self.sems[1], self.p.cross)

    def tail_out(self):
        src = self.window.at[self.half + self.edge :, :]
        return send(src, self.inbox.at[self.edge :, :], self.sems[2], self.sems[3], self.p.cross)

    def block(self, near):
        batch = self.p.batch if near else 1 - self.p.batch
        row = (2 * batch + self.p.c) * self.each
        return self.window.at[pl.ds(pl.multiple_of(row, 16), self.each), :]

    def stay(self):
        return pltpu.make_async_copy(self.block(True), self.out.at[self.p.batch], self.sems[4])

    def to_pair(self):
        return send(self.block(False), self.out.at[self.p.batch], self.sems[5], self.sems[6], self.p.pair)

    def edges(self):
        pl.when(self.p.c == self.p.image)(lambda: self.edge_out().start())
        pl.when((self.p.c == 1) & (self.p.image == 0))(lambda: self.tail_out().start())

    def merge(self, row, count, at):
        keep = self.p.owned(self.owned[row : row + count, :])
        value = jnp.where(keep, self.window[row : row + count, :], self.inbox[at : at + count, :])
        self.window[row : row + count, :] = value

    def finish(self):
        p = self.p

        @pl.when((p.c == 1) & (p.image == 0))
        def _():
            self.edge_out().wait_recv()
            self.merge(self.half - self.edge, self.edge, 0)

        @pl.when((p.c == 0) & (p.image == 1))
        def _():
            self.edge_out().wait_recv()
            self.merge(0, self.edge, 0)

        @pl.when((p.c == 1) & (p.image == 1))
        def _():
            self.tail_out().wait_recv()
            self.merge(self.half - self.tail, self.tail, self.edge)

        self.to_pair().start()
        self.stay().start()

    def drain(self):
        pl.when(self.p.c == self.p.image)(lambda: self.edge_out().wait_send())
        pl.when((self.p.c == 1) & (self.p.image == 0))(lambda: self.tail_out().wait_send())
        self.stay().wait()
        self.to_pair().wait_send()
        ref = self.out.at[1 - self.p.batch]
        send(ref, ref, self.sems[5], self.sems[6], self.p.pair).wait_recv()


def backward_kernel(*refs, cols, unit_rest, edge, tail, tile):
    (ws, gu, rest_ref, half_ref, first_far, qkv_far, ctx_far, inv_far, segc_ref, segr_whole) = refs[:10]
    (x_far, res_grad_ref, y_ref, gain_ref, d_in, old_sums, unit_ref, unit_rest_ref) = refs[10:18]
    (in_out, out_out, up_out, down_out, x_final, y_out, gain_out, shift_out, qv_out, unit_out) = refs[18:28]
    refs = refs[28:]
    (segr_ref, x_out, sums_ref), refs = refs[:3], refs[3:]
    (blocks, gs, part, part_out, part_in, back_ref, grad_ref, key_acc, value_acc, inbox_x, inbox_y) = refs[:11]
    y_window = part_out
    bias_ref, sums_in, vec_sum, vec_in, vec_far = refs[11:16]
    first_ref, qkv_ref, ctx_ref, inv_ref, x_ref = refs[16:21]
    u_bufs, s_bufs, u_own = refs[21:26], refs[26:31], refs[31:34]
    refs = refs[34:]
    sems, loads, back_sems = refs[: Reduce.SEMS], refs[Reduce.SEMS : Reduce.SEMS + 3], refs[Reduce.SEMS + 3 : Reduce.SEMS + 3 + RowsBack.SEMS]
    load_sem, part_s, part_r, y_sems, sum_s, sum_r, vec_s, vec_r, in_sem = refs[Reduce.SEMS + 3 + RowsBack.SEMS :]
    rows, width = half_ref.shape
    shard_rows, main, rest = up_out.shape[0], gu.shape[2], unit_rest
    heads = cols // DH
    place = Place()
    place.barrier()
    each = x_out.shape[1]

    def up_final(total):
        up_out[:, :main] = total[...].astype(F32)

    def small_final(total):
        for n in range(3):
            in_out[n] = total[:, n * cols : (n + 1) * cols].astype(F32).T
        at = 3 * cols
        out_out[...] = total[:, at : at + cols].astype(F32).T
        at = at + cols
        up_out[:, main:] = total[:, at : at + rest].astype(F32)
        down_out[:, main:] = total[:, at + rest : at + 2 * rest].astype(F32)

    r = Reduce(place, (gu, gs), (u_own, None), (up_final, small_final), (u_bufs, s_bufs), sems, loads, shard_rows)
    x_back = RowsBack(place, 0, part_in, inbox_x, segc_ref, x_out, back_sems, each, edge, tail)
    y_back = RowsBack(place, 1, y_window, inbox_y, segc_ref, y_out, back_sems, each, edge, tail)

    def load(i):
        return pltpu.make_async_copy(ws.at[place.far_first(i)], blocks.at[i % 2], load_sem.at[i % 2])

    y_load = pltpu.make_async_copy(y_ref, y_window, y_sems.at[0])
    def slot_loads(i):
        s = place.far_first(i)
        pairs = ((qkv_far, qkv_ref), (ctx_far, ctx_ref), (inv_far, inv_ref))
        return [pltpu.make_async_copy(p[0].at[s], p[1].at[s], in_sem.at[n, i]) for n, p in enumerate(pairs)]

    first_load = pltpu.make_async_copy(first_far, first_ref, y_sems.at[1])
    x_load = pltpu.make_async_copy(x_far, x_ref, y_sems.at[2])
    load(0).start()
    for copy in slot_loads(0):
        copy.start()
    y_load.start()
    r.start(0)
    for t in range(rows // tile):
        segr_ref[t] = segr_whole[:, t * tile : (t + 1) * tile]
    down_out[:, :main] = d_in[...]
    first_load.start()
    for i in (1, 2, 3):
        for copy in slot_loads(i):
            copy.start()
    x_load.start()
    y_load.wait()
    y_back.edges()

    def one_slot(i, carry):
        s = place.far_first(i)
        load(i).wait()
        for copy in slot_loads(i):
            copy.wait()

        @pl.when(i < 3)
        def _():
            load(i + 1).start()

        w = blocks.at[i % 2]
        back_ref[...] = dot_nn(half_ref[...], w[:, 3 * cols : 4 * cols]).astype(BF16)
        gs[s, :, 3 * cols : 4 * cols] = dot_tn(half_ref[...], ctx_ref[s]).astype(BF16)
        gs[s, :, 4 * cols :] = rest_ref[s]
        for head in range(heads):
            attend_back_head(
                qkv_ref, ctx_ref, inv_ref, back_ref, segc_ref, segr_ref, grad_ref, bias_ref, key_acc, value_acc, s, head, cols, tile
            )
            if head == 0:
                r.middle_one(0, i)
                pl.when(i == 1)(lambda: y_back.finish())
        pl.when(i == 0)(lambda: first_load.wait())
        gs[s, :, : 3 * cols] = dot_tn(first_ref[...], grad_ref[...]).astype(BF16)
        product = dot_nt(grad_ref[...], w[:, : 3 * cols])

        @pl.when(i == 0)
        def _():
            part[...] = product

        @pl.when(i > 0)
        def _():
            part[...] += product

        r.start_one(1, s)
        pl.when(i > place.behind())(lambda: r.line_one(0, i - 1 - place.behind()))
        pl.when(i > 0)(lambda: r.middle_one(1, i - 1))
        return carry

    lax.fori_loop(0, 4, one_slot, 0)

    def halves(h):
        return pl.ds(h * (rows // 2), rows // 2)

    def exchange(h):
        src, dst = part_out.at[halves(h), :], part_in.at[halves(h), :]
        return send(src, dst, part_s.at[h], part_r.at[h], place.mate)

    y_back.drain()
    for h in (0, 1):
        part_out[halves(h), :] = part[halves(h), :].astype(BF16)
        exchange(h).start()
    res_load = pltpu.make_async_copy(res_grad_ref, part, load_sem.at[0])
    res_load.start()
    pl.when(place.behind() == 1)(lambda: r.line_one(0, 2))
    r.line_one(0, 3)
    pl.when((place.z == 0) | (place.z == 3))(lambda: r.line_one(1, 0))
    for h in (0, 1):
        exchange(h).wait_recv()

    res_load.wait()
    x_load.wait()
    sums_ref[...] = old_sums[...]

    def last(span):
        grad = part_out[span, :].astype(F32) + part_in[span, :].astype(F32)
        value = x_ref[span, :].astype(F32)
        _, scaled, factor = norm_forward(value, gain_ref[0:1, :], gain_ref[0:1, :])
        result = part[span, :] + norm_backward(grad, scaled, factor, gain_ref[0:1, :])
        part_in[span, :] = result.astype(BF16)
        sums_ref[0:1, :] += jnp.sum(grad * scaled, axis=0, keepdims=True)
        sums_ref[2:3, :] += jnp.sum(grad, axis=0, keepdims=True)

    row_tiles(rows, 128, last)
    x_back.edges()

    vec_sum[...] = jnp.zeros_like(vec_sum)
    for s in range(4):
        vec_sum[s, 0:1, :cols] = bias_ref[s, 0:1, :]
        vec_sum[s, 1:2, :cols] = bias_ref[s, 1:2, :]
        vec_sum[s, 2:3, :main] = unit_ref[s, 0:1, :]
        vec_sum[s, 3:4, :rest] = unit_rest_ref[:, s * rest : (s + 1) * rest]

    def across(n, device):
        return (
            send(sums_ref, sums_in.at[n], sum_s.at[n], sum_r.at[n], device),
            send(vec_sum, vec_in.at[n], vec_s.at[n], vec_r.at[n], device),
        )

    def along(d):
        there = (place.z + d) % 4
        device = place.slot_after(d)
        return (
            send(sums_ref, sums_in.at[1 + d], sum_s.at[1 + d], sum_r.at[1 + d], device),
            send(vec_sum.at[there], vec_far.at[d - 1], vec_s.at[1 + d], vec_r.at[1 + d], device),
        )

    def add_across(n, device):
        for copy in across(n, device):
            copy.wait()
        sums_ref[...] += sums_in[n]
        vec_sum[...] += vec_in[n]

    for copy in across(0, place.across_x):
        copy.start()
    r.middle_one(1, 3)
    pl.when((place.z == 1) | (place.z == 2))(lambda: r.line_one(1, 0))
    r.line_one(1, 1)
    add_across(0, place.across_x)
    for copy in across(1, place.across_y):
        copy.start()
    x_back.finish()
    r.line_one(1, 2)
    add_across(1, place.across_y)
    for d in (1, 2, 3):
        for copy in along(d):
            copy.start()
    r.line_one(1, 3)
    for d in (1, 2, 3):
        for copy in along(d):
            copy.wait()
    sums_ref[...] += sums_in[2] + sums_in[3] + sums_in[4]
    gain_out[...] = sums_ref[0:2, :]
    shift_out[...] = sums_ref[2:6, :]
    total = vec_sum[place.z] + vec_far[0] + vec_far[1] + vec_far[2]
    qv_out[...] = total[0:2, :cols]
    unit_out[:, :main] = total[2:3, :main]
    unit_out[:, main:] = total[3:4, :rest]
    for k in (0, 1):
        r.drain(k)
    x_back.drain()
    x_final[...] = x_out[...].astype(F32)
    for h in (0, 1):
        exchange(h).wait_send()


def backward_stage(
    ws, gu, rest_sums, residual_half, first_norm, qkv, context, inverse, segc, segr, x_half, residual_grad, y_rows, gains, down_sum,
    sums, unit_sums, unit_rest_sums, cols, unit_rest, edge, tail, rows_each,
):
    rows, width = residual_half.shape
    shard_rows, lanes, main = width // 4, ws.shape[2], gu.shape[2]
    vmem = pl.BlockSpec(memory_space=pltpu.VMEM)
    far = pl.BlockSpec(memory_space=pl.ANY)
    shape = jax.ShapeDtypeStruct
    dma = pltpu.SemaphoreType.DMA
    wide = max(main, round_up(cols, 128))
    return pl.pallas_call(
        functools.partial(backward_kernel, cols=cols, unit_rest=unit_rest, edge=edge, tail=tail, tile=rows // 2),
        in_specs=[far] * 2 + [vmem] * 2 + [far] * 4 + [vmem] * 2 + [far] * 3 + [vmem] * 5,
        out_specs=[vmem] * 10,
        out_shape=[
            shape((3, cols, shard_rows), F32),
            shape((cols, shard_rows), F32),
            shape((shard_rows, main + unit_rest), F32),
            shape((shard_rows, main + unit_rest), F32),
            shape((2, rows_each, width), F32),
            shape((2, rows_each, width), BF16),
            shape((2, width), F32),
            shape((4, width), F32),
            shape((2, cols), F32),
            shape((1, main + unit_rest), F32),
        ],
        scratch_shapes=[
            pltpu.VMEM((2, 1, rows // 2), jnp.int32),
            pltpu.VMEM((2, rows_each, width), BF16),
            pltpu.VMEM((8, width), F32),
            pltpu.VMEM((2, width, lanes), BF16),
            pltpu.VMEM((4, width, lanes), BF16),
            pltpu.VMEM((rows, width), F32),
            pltpu.VMEM((rows, width), BF16),
            pltpu.VMEM((rows, width), BF16),
            pltpu.VMEM((rows, cols), BF16),
            pltpu.VMEM((rows, 3 * cols), BF16),
            pltpu.VMEM((rows, DH), F32),
            pltpu.VMEM((rows, DH), F32),
            pltpu.VMEM((edge + tail, width), BF16),
            pltpu.VMEM((edge + tail, width), BF16),
            pltpu.VMEM((4, 2, cols), F32),
            pltpu.VMEM((5, 8, width), F32),
            pltpu.VMEM((4, 8, wide), F32),
            pltpu.VMEM((2, 4, 8, wide), F32),
            pltpu.VMEM((3, 8, wide), F32),
            pltpu.VMEM((rows, width), BF16),
            pltpu.VMEM((4, rows, 3 * cols), BF16),
            pltpu.VMEM((4, rows, cols), BF16),
            pltpu.VMEM((4, rows, cols // DH), F32),
            pltpu.VMEM((rows, width), BF16),
        ]
        + reduce_buffers(shard_rows, main)
        + reduce_buffers(shard_rows, lanes)
        + reduce_terms(shard_rows, main)
        + [dma((2, 4))] * Reduce.SEMS
        + [dma((1, 4))] * 3
        + [dma((2,))] * RowsBack.SEMS
        + [dma((2,)), dma((2,)), dma((2,)), dma((3,)), dma((5,)), dma((5,)), dma((5,)), dma((5,)), dma((3, 4))],
        compiler_params=pltpu.CompilerParams(collective_id=2, has_side_effects=True, vmem_limit_bytes=64000000),
        name="backward",
    )(
        ws, gu, rest_sums, residual_half, first_norm, qkv, context, inverse, segc, segr,
        x_half, residual_grad, y_rows, gains, down_sum, sums, unit_sums, unit_rest_sums,
    )


def attend_head(qkv_ref, ctx_ref, inv_ref, segc_ref, segr_ref, s, head, cols, tile):
    lo = head * DH
    keys = qkv_ref[s, :, cols + lo : cols + lo + DH]
    values = qkv_ref[s, :, 2 * cols + lo : 2 * cols + lo + DH]

    def one_tile(t, carry):
        span = pl.ds(pl.multiple_of(t * tile, tile), tile)
        scores = dot_nt(qkv_ref[s, span, lo : lo + DH], keys)
        allowed = segc_ref[span, :] == segr_ref[...]
        exact = jnp.where(allowed, jnp.exp2(scores * (SCALE * LOG2E)), 0.0)
        inverse = 1.0 / jnp.sum(exact, axis=1, keepdims=True)
        context = dot_nn(exact.astype(BF16), values) * inverse
        ctx_ref[s, span, lo : lo + DH] = context.astype(BF16)
        inv_ref[s, span, head : head + 1] = inverse
        return carry

    lax.fori_loop(0, qkv_ref.shape[1] // tile, one_tile, 0)


def attend_kernel(x_ref, w_ref, b_ref, segc_ref, segr_ref, qkv_ref, ctx_ref, inv_ref, part_ref, *, cols, tile):
    block = pl.program_id(0)
    projected = dot_nn(x_ref[...], w_ref[0, :, : 3 * cols]) + b_ref[0]
    qkv_ref[0] = projected.astype(BF16)
    for head in range(cols // DH):
        attend_head(qkv_ref, ctx_ref, inv_ref, segc_ref, segr_ref, 0, head, cols, tile)
    part = dot_nt(ctx_ref[0], w_ref[0, :, 3 * cols : 4 * cols])

    @pl.when(block == 0)
    def _():
        part_ref[...] = part

    @pl.when(block > 0)
    def _():
        part_ref[...] += part


def attend(first_norm, weights, bias, segments, cols, tile):
    rows, width = first_norm.shape
    slots, _, lanes = weights.shape
    heads = cols // DH
    whole = lambda shape: pl.BlockSpec(shape, lambda s: (0,) * len(shape))
    each = lambda shape: pl.BlockSpec((1,) + shape, lambda s: (s, 0, 0))
    return pl.pallas_call(
        functools.partial(attend_kernel, cols=cols, tile=tile),
        grid=(slots,),
        in_specs=[
            whole((rows, width)),
            each((width, lanes)),
            each((1, 3 * cols)),
            whole((rows, 1)),
            whole((1, rows)),
        ],
        out_specs=[each((rows, 3 * cols)), each((rows, cols)), each((rows, heads)), whole((rows, width))],
        out_shape=[
            jax.ShapeDtypeStruct((slots, rows, 3 * cols), BF16),
            jax.ShapeDtypeStruct((slots, rows, cols), BF16),
            jax.ShapeDtypeStruct((slots, rows, heads), F32),
            jax.ShapeDtypeStruct((rows, width), F32),
        ],
        cost_estimate=pl.CostEstimate(
            flops=slots * (8 * rows * width * cols + 4 * rows * rows * 256 * heads),
            bytes_accessed=slots * width * lanes * 2 + rows * width * 10,
            transcendentals=slots * heads * rows * rows,
        ),
        name="attend",
    )(first_norm, weights, bias, segments[:, None], segments[None, :])


def attend_back_head(
    qkv_ref, ctx_ref, inv_ref, back_ref, segc_ref, segr_ref, grad_ref, bias_ref, key_acc, value_acc, s, head, cols, tile
):
    lo = head * DH
    rows = back_ref.shape[0]
    ones = jnp.ones((8, DH), F32)
    keys = qkv_ref[s, :, cols + lo : cols + lo + DH]
    values = qkv_ref[s, :, 2 * cols + lo : 2 * cols + lo + DH]
    key_acc[...] = jnp.zeros_like(key_acc)
    value_acc[...] = jnp.zeros_like(value_acc)

    def one_tile(t, query_total):
        span = pl.ds(pl.multiple_of(t * tile, tile), tile)
        queries = qkv_ref[s, span, lo : lo + DH]
        back = (back_ref[span, lo : lo + DH].astype(F32) * inv_ref[s, span, head : head + 1]).astype(BF16)
        along = back.astype(F32) * ctx_ref[s, span, lo : lo + DH].astype(F32)
        delta = lax.dot_general(
            ones, along, (((1,), (1,)), ((), ())), precision=lax.Precision.HIGHEST, preferred_element_type=F32
        )[:1]
        scores = dot_nt(keys, queries)
        allowed = segc_ref[...] == segr_ref[t]
        exact = jnp.where(allowed, jnp.exp2(scores * (SCALE * LOG2E)), 0.0)
        value_acc[...] += dot_nn(exact.astype(BF16), back)
        prob_grad = dot_nt(values, back)
        score_grad = (exact * (prob_grad - delta)).astype(BF16)
        key_acc[...] += dot_nn(score_grad, queries)
        query_grad = dot_tn(score_grad, keys) * SCALE
        grad_ref[span, lo : lo + DH] = query_grad.astype(BF16)
        return query_total + jnp.sum(query_grad, axis=0, keepdims=True)

    query_total = lax.fori_loop(0, rows // tile, one_tile, jnp.zeros((1, DH), F32))
    grad_ref[:, cols + lo : cols + lo + DH] = (key_acc[...] * SCALE).astype(BF16)
    grad_ref[:, 2 * cols + lo : 2 * cols + lo + DH] = value_acc[...].astype(BF16)
    bias_ref[s, 0:1, lo : lo + DH] = query_total
    bias_ref[s, 1:2, lo : lo + DH] = jnp.sum(value_acc[...], axis=0, keepdims=True)


def attend_back_kernel(
    r_ref, w_ref, qkv_ref, ctx_ref, inv_ref, segc_ref, segr_ref, grad_ref, bias_ref, back_ref, key_acc, value_acc, *, cols, tile
):
    back_ref[...] = dot_nn(r_ref[...], w_ref[0, :, 3 * cols : 4 * cols]).astype(BF16)
    for head in range(cols // DH):
        attend_back_head(
            qkv_ref, ctx_ref, inv_ref, back_ref, segc_ref, segr_ref, grad_ref.at[0], bias_ref, key_acc, value_acc, 0, head, cols, tile
        )


def attend_back(residual_half, weights, qkv, context, inverse, segments, cols, tile):
    rows, width = residual_half.shape
    slots, _, lanes = weights.shape
    heads = cols // DH
    whole = lambda shape: pl.BlockSpec(shape, lambda s: (0,) * len(shape))
    each = lambda shape: pl.BlockSpec((1,) + shape, lambda s: (s, 0, 0))
    return pl.pallas_call(
        functools.partial(attend_back_kernel, cols=cols, tile=tile),
        grid=(slots,),
        in_specs=[
            whole((rows, width)),
            each((width, lanes)),
            each((rows, 3 * cols)),
            each((rows, cols)),
            each((rows, heads)),
            whole((rows, 1)),
            whole((rows // tile, 1, tile)),
        ],
        out_specs=[each((rows, 3 * cols)), each((2, cols))],
        out_shape=[
            jax.ShapeDtypeStruct((slots, rows, 3 * cols), BF16),
            jax.ShapeDtypeStruct((slots, 2, cols), F32),
        ],
        scratch_shapes=[
            pltpu.VMEM((rows, cols), BF16),
            pltpu.VMEM((rows, DH), F32),
            pltpu.VMEM((rows, DH), F32),
        ],
        cost_estimate=pl.CostEstimate(
            flops=slots * (2 * rows * width * cols + 10 * rows * rows * 256 * heads),
            bytes_accessed=slots * width * lanes * 2 + rows * width * 10,
            transcendentals=slots * heads * rows * rows,
        ),
        name="attend_back",
    )(residual_half, weights, qkv, context, inverse, segments[:, None], segments.reshape(-1, 1, tile))


def plain_layer(shards, vectors, to_slot, from_slot, block_input, cotangent, gains, shifts, segments, owned, cols, units, parts):
    width, rows = block_input.shape[2], segments.shape[0]
    slots, slot = lax.axis_size("slot"), lax.axis_index("slot")
    main_units, in_lanes = shards[1].shape[1], 3 * cols
    rest = units - main_units
    spare = shards[0].shape[1] - in_lanes - cols - 2 * rest
    small_all, up_main, down_main = gather_weights(shards)
    vec_all = lax.all_gather(vectors, "slot", axis=0)
    grad_rows = jnp.where(owned[:, None], to_slot(cotangent), 0)
    upstream = grad_rows.astype(F32)
    x_float = to_slot(block_input).astype(F32)
    first_out, first_scaled, first_factor = norm_forward(x_float, gains[0], shifts[0])
    first_norm = first_out.astype(BF16)
    bias = vec_all[:, :1, :in_lanes].astype(F32) + vec_all[:, 1:2, :in_lanes].astype(F32)
    qkv, context, inverse, attention_part = attend(first_norm, small_all, bias, segments, cols, rows // 2)
    residual = x_float + part_sum(attention_part, parts) + shifts[2]
    second_out, second_scaled, second_factor = norm_forward(residual, gains[1], shifts[1])
    second_norm = second_out.astype(BF16)
    small_blocks = list(small_all)
    unit_all = vec_all[:, 2, :units].astype(F32)
    at = in_lanes + cols
    ups = list(up_main) + [b[:, at : at + rest] for b in small_blocks]
    downs = list(down_main) + [b[:, at + rest : at + 2 * rest] for b in small_blocks]
    unit_rows = list(unit_all[:, :main_units]) + list(unit_all[:, main_units:])
    pre_acts = [dot_nn(second_norm, w) + b for w, b in zip(ups, unit_rows)]
    hiddens = [gelu(p).astype(BF16) for p in pre_acts]
    output = (residual + part_sum(sum_products(hiddens, downs), parts) + shifts[3]).astype(BF16)
    down_sums = [dot_tn(grad_rows, h).astype(BF16) for h in hiddens]
    pre_grads = [gelu_back(p, dot_nn(grad_rows, w)) for p, w in zip(pre_acts, downs)]
    pre_halves = [p.astype(BF16) for p in pre_grads]
    unit_sums = [jnp.sum(p, axis=0) for p in pre_grads]
    up_sums = [dot_tn(second_norm, p).astype(BF16) for p in pre_halves]
    second_grad = part_sum(sum_products(pre_halves, ups), parts)
    residual_grad = upstream + norm_backward(second_grad, second_scaled, second_factor, gains[1])
    residual_half = residual_grad.astype(BF16)
    triple, bias_sum = attend_back(residual_half, small_all, qkv, context, inverse, segments, cols, rows // 2)
    first_part = sum_products(list(triple), [b[:, :in_lanes] for b in small_blocks])
    first_grad = part_sum(first_part, parts)
    input_grad = residual_grad + norm_backward(first_grad, first_scaled, first_factor, gains[0])
    blank = jnp.zeros((width, spare), BF16)
    small_sums = [
        jnp.concatenate(
            [
                dot_tn(first_norm, triple[s]).astype(BF16),
                dot_tn(residual_half, context[s]).astype(BF16),
                up_sums[slots + s],
                down_sums[slots + s],
                blank,
            ],
            axis=1,
        )
        for s in range(slots)
    ]
    down_grad, up_grad, small_grad = scatter_grads(
        [jnp.stack(down_sums[:slots]), jnp.stack(up_sums[:slots]), jnp.stack(small_sums)]
    )
    rows_sum = jnp.stack(
        [
            jnp.sum(first_grad * first_scaled, axis=0),
            jnp.sum(second_grad * second_scaled, axis=0),
            jnp.sum(first_grad, axis=0),
            jnp.sum(second_grad, axis=0),
            jnp.sum(residual_grad, axis=0),
            jnp.sum(upstream, axis=0),
        ]
    )
    unit_sum = jnp.stack([jnp.concatenate([unit_sums[s], unit_sums[slots + s]]) for s in range(slots)])
    rows_total, bias_total, unit_total = lax.psum((rows_sum, bias_sum, unit_sum), ("slot",) + FSDP)
    bias_grad = lax.dynamic_index_in_dim(bias_total, slot, 0, keepdims=False)
    unit_grad = lax.dynamic_index_in_dim(unit_total, slot, 0, keepdims=False)
    return (
        from_slot(output, owned), from_slot(input_grad.astype(BF16), owned), rows_total, bias_grad, unit_grad,
        down_grad, up_grad, small_grad,
    )


def on_device(
    block_input,
    segment_ids,
    norm_gains,
    row_biases,
    in_projection,
    query_value_bias,
    out_projection,
    up_weight,
    unit_bias,
    down_weight,
    cotangent,
):
    local, rows_each, width = block_input.shape
    rows_mb = segment_ids.shape[1]
    cols = in_projection.shape[2]
    units = up_weight.shape[1]
    shard_rows = up_weight.shape[0]
    slots, parts = lax.axis_size("slot"), lax.axis_size("part")
    slot, part = lax.axis_index("slot"), lax.axis_index("part")
    fsdp_index = lax.axis_index("fy") * lax.axis_size("fx") + lax.axis_index("fx")
    batch, image = slot % local, slot // local
    late = image == 1

    half_rows = rows_mb // IMG_MB
    padding = rows_mb - IMG_MB * IMG
    edge = round_up(max(half_rows - IMG, padding - (half_rows - IMG)), 16)
    tail = round_up(padding, 16)
    rows = round_up(half_rows + edge + tail, 128)
    filler = rows - half_rows - edge - tail
    paired = lax.axis_size("fy") == 2 and lax.axis_size("fx") == 2 and slots == 4 and parts == 2
    paired = paired and shard_rows % 32 == 0 and filler == 0

    def edges(main):
        near = jnp.where(late, main[:edge], main[half_rows - edge :])
        far = main[half_rows - tail :]
        return jnp.concatenate([near, far])

    def to_slot(value):
        mine = lax.dynamic_index_in_dim(value, batch, 0, keepdims=False)
        send = lax.dynamic_index_in_dim(value, 1 - batch, 0, keepdims=False)
        other = slot_swap(send, 1, slots)
        pair = jnp.where(batch == 0, jnp.stack([mine, other]), jnp.stack([other, mine]))
        main = part_gather(pair, parts).swapaxes(0, 1).reshape(half_rows, width)
        beyond = slot_swap(edges(main), local, slots)
        return jnp.concatenate([main, beyond, jnp.zeros((filler, width), value.dtype)])

    def from_slot(value, owned):
        main = value[:half_rows]
        beyond = slot_swap(value[half_rows : half_rows + edge + tail], local, slots)
        keep = owned[:half_rows, None]
        near, far = beyond[:edge], beyond[edge:]
        blank = lambda count: jnp.zeros((count, width), value.dtype)
        early_fill = jnp.concatenate([blank(half_rows - edge), near])
        late_fill = jnp.concatenate([near, blank(half_rows - edge - tail), far])
        main = jnp.where(keep, main, jnp.where(late, late_fill, early_fill))
        main = main.reshape(local, parts, rows_each, width)
        mine = lax.dynamic_index_in_dim(main, part, 1, keepdims=False)
        stay = lax.dynamic_index_in_dim(mine, batch, 0, keepdims=False)
        other = slot_swap(lax.dynamic_index_in_dim(mine, 1 - batch, 0, keepdims=False), 1, slots)
        return jnp.where(batch == 0, jnp.stack([stay, other]), jnp.stack([other, stay]))

    ids = jnp.where(batch == 0, segment_ids[:1], segment_ids[1:])
    filler_ids = lambda count: jnp.full((1, count), -2, jnp.int32)
    early_ids = jnp.concatenate([ids[:, : half_rows + edge], ids[:, rows_mb - tail :], filler_ids(filler)], axis=1)
    late_ids = jnp.concatenate(
        [ids[:, half_rows:], ids[:, half_rows - edge : half_rows], filler_ids(tail + filler)], axis=1
    )
    segr = jnp.where(late, late_ids, early_ids)
    segc = segr.reshape(rows, 1)

    main_units = units // 128 * 128
    rest = units - main_units
    in_lanes = 3 * cols
    small = in_lanes + cols + 2 * rest
    lanes = round_up(small, 128)
    gains, shifts = norm_gains, row_biases
    if paired:
        (
            small_all, up_main, down_main, gd, x_half, cot, first_norm, qkv, context, inverse, residual, second_norm,
            hidden, slope, hidden_rest, slope_rest, rest_up, rest_down,
        ) = forward_stage(
            (in_projection.swapaxes(1, 2), out_projection, up_weight, down_weight.T), (query_value_bias, unit_bias.reshape(1, units)),
            block_input, cotangent, gains, shifts, segc, segr, cols, units, lanes, edge, tail,
        )
        gu, down_sum, rest_sums, residual_half, residual_grad, y_rows, sums, unit_sums, unit_rest_sums = middle_stage(
            down_main, up_main, gd, hidden, slope, hidden_rest, slope_rest, rest_up, rest_down, cot, second_norm, residual,
            gains, shifts, cols, rest, lanes - small,
        )
        in_grad, out_grad, up_grad, down_grad, input_grad, output, gain_grad, shift_grad, bias_grad, unit_grad = backward_stage(
            small_all, gu, rest_sums, residual_half, first_norm, qkv, context, inverse, segc, segr, x_half, residual_grad,
            y_rows, gains, down_sum, sums, unit_sums, unit_rest_sums, cols, rest, edge, tail, rows_each,
        )
        unit_grad = unit_grad.reshape(units)
        in_grad, down_grad = in_grad.swapaxes(1, 2), down_grad.T
    else:
        segments = segc[:, 0]
        image_id = (fsdp_index * local + batch) * IMG_MB + image
        owned = (segments == image_id) | (jnp.logical_not(late) & (segments == -1))
        down_t = down_weight.T
        small_shard = jnp.concatenate(
            [
                in_projection.transpose(1, 0, 2).reshape(shard_rows, in_lanes),
                out_projection.T,
                up_weight[:, main_units:],
                down_t[:, main_units:],
                jnp.zeros((shard_rows, lanes - small), BF16),
            ],
            axis=1,
        )
        shards = [small_shard, up_weight[:, :main_units], down_t[:, :main_units]]
        triple_bias = jnp.concatenate([query_value_bias[0], jnp.zeros((cols,), F32), query_value_bias[1]])
        high = triple_bias.astype(BF16)
        low = (triple_bias - high.astype(F32)).astype(BF16)
        wide = round_up(max(in_lanes, units), 128)
        vectors = [jnp.pad(v, (0, wide - v.shape[0])) for v in (high, low, unit_bias)]
        vectors = jnp.concatenate([jnp.stack(vectors), jnp.zeros((13, wide), BF16)])
        output, input_grad, rows_total, bias_grad, unit_grad, down_grad, up_grad, small_grad = plain_layer(
            shards, vectors, to_slot, from_slot, block_input, cotangent, gains, shifts, segments, owned, cols, units, parts
        )
        in_grad = small_grad[:, :in_lanes].reshape(shard_rows, 3, cols).transpose(1, 0, 2)
        out_grad = small_grad[:, in_lanes : in_lanes + cols].T
        at = in_lanes + cols
        up_grad = jnp.concatenate([up_grad, small_grad[:, at : at + rest]], axis=1)
        down_grad = jnp.concatenate([down_grad, small_grad[:, at + rest : at + 2 * rest]], axis=1).T
        gain_grad, shift_grad = rows_total[:2], rows_total[2:]
    return (
        output,
        input_grad.astype(F32),
        gain_grad,
        shift_grad,
        in_grad,
        bias_grad,
        out_grad,
        up_grad,
        unit_grad,
        down_grad,
    )


def solution(mesh):
    fsdp, tensor = mesh.shape["fsdp"], mesh.shape["tensor"]

    def layer(*arrays):
        local = arrays[0].shape[0] // fsdp
        slots = local * IMG_MB
        assert local == 2 and slots == 4 and tensor % slots == 0 and fsdp % 2 == 0
        grid = Mesh(
            mesh.devices.reshape(fsdp // 2, 2, slots, tensor // slots), ("fy", "fx", "slot", "part")
        )
        tens = ("slot", "part")
        return jax.shard_map(
            on_device,
            mesh=grid,
            in_specs=(
                P(FSDP, tens, None),
                P(FSDP, None),
                P(),
                P(),
                P(None, FSDP, tens),
                P(None, tens),
                P(tens, FSDP),
                P(FSDP, tens),
                P(tens),
                P(tens, FSDP),
                P(FSDP, tens, None),
            ),
            out_specs=(
                P(FSDP, tens, None),
                P(FSDP, tens, None),
                P(),
                P(),
                P(None, FSDP, tens),
                P(None, tens),
                P(tens, FSDP),
                P(FSDP, tens),
                P(tens),
                P(tens, FSDP),
            ),
            check_vma=False,
        )(*arrays)

    return layer
```

```python
import functools
import math

import jax
import jax.numpy as jnp
from jax import lax
from jax.experimental import pallas as pl
from jax.experimental.pallas import tpu as pltpu
from jax.sharding import Mesh
from jax.sharding import PartitionSpec as P

DH = 72
IMG = 729
IMG_MB = 2
EPS = 1e-06
GELU_C = 0.7978845608028654
F32 = jnp.float32
BF16 = jnp.bfloat16
FSDP = ("fy", "fx")
SCALE = DH ** (-0.5)
LOG2E = math.log2(math.e)


def norm_forward(values, norm_gain, norm_shift):
    center = values - jnp.mean(values, axis=-1, keepdims=True)
    factor = lax.rsqrt(jnp.mean(center * center, axis=-1, keepdims=True) + EPS)
    scaled = center * factor
    return (scaled * norm_gain + norm_shift, scaled, factor)


def norm_backward(upstream, scaled, factor, norm_gain):
    inside = upstream * norm_gain
    return factor * (
        inside
        - jnp.mean(inside, axis=-1, keepdims=True)
        - scaled * jnp.mean(inside * scaled, axis=-1, keepdims=True)
    )


def gelu(pre_act):
    return (
        0.5
        * pre_act
        * (1.0 + jnp.tanh(GELU_C * (pre_act + 0.044715 * pre_act * pre_act * pre_act)))
    )


def gelu_both(pre_act):
    square = pre_act * pre_act
    curve = jnp.tanh(GELU_C * pre_act * (1.0 + 0.044715 * square))
    rise = 0.5 * (1.0 + curve)
    slope = rise + 0.5 * pre_act * (1.0 - curve * curve) * GELU_C * (1.0 + 3.0 * 0.044715 * square)
    return pre_act * rise, slope


def gelu_back(pre_act, upstream):
    return jax.vjp(gelu, pre_act)[1](upstream)[0]


def dot_nn(left, right):
    return lax.dot_general(left, right, (((1,), (0,)), ((), ())), preferred_element_type=F32)


def dot_nt(left, right):
    return lax.dot_general(left, right, (((1,), (1,)), ((), ())), preferred_element_type=F32)


def dot_tn(left, right):
    return lax.dot_general(left, right, (((0,), (0,)), ((), ())), preferred_element_type=F32)


def sum_products(lefts, rights):
    total = dot_nt(lefts[0], rights[0])
    for left, right in zip(lefts[1:], rights[1:]):
        total = total + dot_nt(left, right)
    return total


def round_up(value, unit):
    return -(-value // unit) * unit


def swap(value, axis):
    return lax.ppermute(value, axis, [(0, 1), (1, 0)])


def slot_swap(value, stride, slots):
    return lax.ppermute(value, "slot", [(s, s ^ stride) for s in range(slots)])


def part_sum(value, parts):
    value = value.astype(BF16)
    if parts == 2:
        return value.astype(F32) + swap(value, "part").astype(F32)
    return lax.psum(value.astype(F32), "part")


def part_gather(value, parts):
    if parts == 2:
        other = swap(value, "part")
        first = lax.axis_index("part") == 0
        return jnp.stack([jnp.where(first, value, other), jnp.where(first, other, value)])
    return lax.all_gather(value, "part", axis=0)


def add_half(left, right):
    return (left.astype(F32) + right.astype(F32)).astype(BF16)


MESH = pl.DeviceIdType.MESH


class Place:
    def __init__(self):
        self.y, self.x = lax.axis_index("fy"), lax.axis_index("fx")
        self.z = lax.axis_index("slot")
        self.f = 2 * self.y + self.x
        self.across_x, self.across_y = {"fx": 1 - self.x}, {"fy": 1 - self.y}
        self.c = lax.axis_index("part")
        self.above = {"slot": jnp.minimum(self.z + 1, 3)}
        self.below = {"slot": jnp.maximum(self.z - 1, 0)}
        self.batch, self.image = self.z % 2, self.z // 2
        self.mate = {"part": 1 - self.c}
        self.pair = {"slot": self.z + 1 - 2 * self.batch}
        self.cross = {"slot": self.z + 2 - 4 * self.image}

    def owned(self, segments):
        mine = segments == (self.f * 2 + self.batch) * IMG_MB + self.image
        return mine | ((segments == -1) & (self.image == 0))

    def behind(self):
        return jnp.where((self.z == 1) | (self.z == 2), 1, 0)

    def slot_after(self, d):
        return {"slot": (self.z + d) % 4}

    def barrier(self):
        sem = pltpu.get_barrier_semaphore()
        others = [self.across_x, self.across_y, self.mate] + [self.slot_after(d) for d in (1, 2, 3)]
        for device in others:
            pl.semaphore_signal(sem, inc=1, device_id=device, device_id_type=MESH)
        pl.semaphore_wait(sem, len(others))

    def far_first(self, i):
        low = self.z < 2
        near = jnp.where(low, self.z, 3 - self.z)
        at = jnp.where(i == 0, 3, jnp.where(i == 1, 2, jnp.where(i == 2, 1 - near, near)))
        return jnp.where(low, at, 3 - at)


def send(src, dst, send_sem, recv_sem, device):
    return pltpu.make_async_remote_copy(
        src_ref=src, dst_ref=dst, send_sem=send_sem, recv_sem=recv_sem, device_id=device, device_id_type=MESH
    )


class Gather:
    SEMS = 11

    def __init__(self, place, shards, w, sems, local_sem, rows):
        self.p, self.shards, self.w, self.rows = place, shards, w, rows
        (self.zr, self.zu, self.zd, self.xr, self.xs, self.yr, self.ys, self.ar, self.asn, self.br, self.bs) = sems
        self.local_sem = local_sem

    def block(self, k, slot, owner, half=None):
        at, count = owner * self.rows, self.rows
        if half is not None:
            count = count // 2
            at = at + half * count
        return self.w[k].at[slot, pl.ds(pl.multiple_of(at, 16), count), :]

    def mine(self, k, slot, shard):
        return self.shards[k] if shard else self.block(k, slot, self.p.f)

    def up(self, k, slot, shard=False):
        dst = self.block(k, slot, self.p.f)
        return send(self.mine(k, slot, shard), dst, self.zu.at[k, slot], self.zr.at[k, slot], self.p.above)

    def down(self, k, slot, shard=False):
        dst = self.block(k, slot, self.p.f)
        return send(self.mine(k, slot, shard), dst, self.zd.at[k, slot], self.zr.at[k, slot], self.p.below)

    def to_x(self, k, slot, shard=False):
        dst = self.block(k, slot, self.p.f)
        return send(self.mine(k, slot, shard), dst, self.xs.at[k, slot], self.xr.at[k, slot], self.p.across_x)

    def to_y(self, k, slot, shard=False):
        dst = self.block(k, slot, self.p.f)
        return send(self.mine(k, slot, shard), dst, self.ys.at[k, slot], self.yr.at[k, slot], self.p.across_y)

    def from_x(self, k, slot):
        ref = self.block(k, slot, self.p.f ^ 1)
        return send(ref, ref, self.xs.at[k, slot], self.xr.at[k, slot], self.p.across_x)

    def from_y(self, k, slot):
        ref = self.block(k, slot, self.p.f ^ 2)
        return send(ref, ref, self.ys.at[k, slot], self.yr.at[k, slot], self.p.across_y)

    def corner_y(self, k, slot):
        ref = self.block(k, slot, self.p.f ^ 1, 0)
        return send(ref, ref, self.asn.at[k, slot], self.ar.at[k, slot], self.p.across_y)

    def corner_x(self, k, slot):
        ref = self.block(k, slot, self.p.f ^ 2, 1)
        return send(ref, ref, self.bs.at[k, slot], self.br.at[k, slot], self.p.across_x)

    def wait_corner(self, k, slot):
        ref = self.block(k, slot, self.p.f ^ 3, 0)
        send(ref, ref, self.asn.at[k, slot], self.ar.at[k, slot], self.p.across_y).wait_recv()
        ref = self.block(k, slot, self.p.f ^ 3, 1)
        send(ref, ref, self.bs.at[k, slot], self.br.at[k, slot], self.p.across_x).wait_recv()

    def local(self, k):
        return pltpu.make_async_copy(self.shards[k], self.block(k, self.p.z, self.p.f), self.local_sem.at[k])

    def start_z(self, k):
        @pl.when(self.p.z < 3)
        def _():
            self.up(k, self.p.z, True).start()

        @pl.when(self.p.z > 0)
        def _():
            self.down(k, self.p.z, True).start()

    def start_xy(self, k):
        self.to_x(k, self.p.z, True).start()
        self.to_y(k, self.p.z, True).start()
        self.local(k).start()

    def pass_on(self, k, d):
        z = self.p.z

        @pl.when(z >= d)
        def _():
            self.up(k, z - d).wait_recv()

            @pl.when(z < 3)
            def _():
                self.up(k, z - d).start()

            self.to_x(k, z - d).start()
            self.to_y(k, z - d).start()

        @pl.when(z + d <= 3)
        def _():
            self.down(k, z + d).wait_recv()

            @pl.when(z > 0)
            def _():
                self.down(k, z + d).start()

            self.to_x(k, z + d).start()
            self.to_y(k, z + d).start()

    def corner(self, k, d):
        def one(slot):
            self.from_x(k, slot).wait_recv()
            self.corner_y(k, slot).start()
            self.from_y(k, slot).wait_recv()
            self.corner_x(k, slot).start()

        z = self.p.z
        if d == 0:
            one(z)
        else:
            pl.when(z >= d)(lambda: one(z - d))
            pl.when(z + d <= 3)(lambda: one(z + d))

    def arrive(self, k):
        self.local(k).wait()
        for slot in range(4):
            self.wait_corner(k, slot)

    def drain(self, k):
        z = self.p.z
        for slot in range(4):
            self.to_x(k, slot).wait_send()
            self.to_y(k, slot).wait_send()
            self.corner_y(k, slot).wait_send()
            self.corner_x(k, slot).wait_send()

            @pl.when((z < 3) & (slot <= z))
            def _(slot=slot):
                self.up(k, slot).wait_send()

            @pl.when((z > 0) & (slot >= z))
            def _(slot=slot):
                self.down(k, slot).wait_send()


def gather_weights(shards):
    slots = lax.axis_size("slot")
    whole = [lax.all_gather(s, ("slot",) + FSDP, axis=0) for s in shards]
    return [w.reshape(slots, -1, w.shape[-1]) for w in whole]


class Rows:
    SEMS = 11

    def __init__(self, place, index, src, dst, sems, rows_each, edge, tail):
        self.p, self.src, self.dst, self.each = place, src, dst, rows_each
        self.half = 4 * rows_each
        self.edge, self.tail = edge, tail
        self.sems = [sem.at[index] for sem in sems]

    def at(self, row, count):
        return self.dst.at[pl.ds(pl.multiple_of(row, 16), count), :]

    def block(self, near, core):
        batch = self.p.batch if near else 1 - self.p.batch
        return self.at((2 * batch + core) * self.each, self.each)

    def own(self):
        return pltpu.make_async_copy(self.src.at[self.p.batch], self.block(True, self.p.c), self.sems[0])

    def to_mate(self):
        return send(self.src.at[self.p.batch], self.block(True, self.p.c), self.sems[1], self.sems[2], self.p.mate)

    def to_pair(self):
        return send(self.src.at[1 - self.p.batch], self.block(True, self.p.c), self.sems[3], self.sems[4], self.p.pair)

    def pass_on(self):
        ref = self.block(False, self.p.c)
        return send(ref, ref, self.sems[5], self.sems[6], self.p.mate)

    def edge_out(self):
        src = self.at(jnp.where(self.p.image == 0, self.half - self.edge, 0), self.edge)
        return send(src, self.at(self.half, self.edge), self.sems[7], self.sems[8], self.p.cross)

    def tail_out(self):
        src = self.at(self.half - self.tail, self.tail)
        dst = self.at(self.half + self.edge, self.tail)
        return send(src, dst, self.sems[7], self.sems[8], self.p.cross)

    def edge_mate(self):
        ref = self.at(self.half, self.edge)
        return send(ref, ref, self.sems[9], self.sems[10], self.p.mate)

    def tail_mate(self):
        ref = self.at(self.half + self.edge, self.tail)
        return send(ref, ref, self.sems[9], self.sems[10], self.p.mate)

    def start(self):
        self.to_pair().start()
        self.to_mate().start()
        self.own().start()

    def forward(self):
        ref = self.block(False, self.p.c)
        send(ref, ref, self.sems[3], self.sems[4], self.p.pair).wait_recv()
        self.pass_on().start()

    def main_ready(self):
        self.own().wait()
        ref = self.block(True, 1 - self.p.c)
        send(ref, ref, self.sems[1], self.sems[2], self.p.mate).wait_recv()
        ref = self.block(False, 1 - self.p.c)
        send(ref, ref, self.sems[5], self.sems[6], self.p.mate).wait_recv()

    def edges(self):
        pl.when(self.p.c == 0)(lambda: self.edge_out().start())
        pl.when(self.p.c == 1)(lambda: self.tail_out().start())

    def edges_forward(self):
        @pl.when(self.p.c == 0)
        def _():
            self.edge_out().wait_recv()
            self.edge_mate().start()

        @pl.when(self.p.c == 1)
        def _():
            self.tail_out().wait_recv()
            self.tail_mate().start()

    def edges_ready(self):
        pl.when(self.p.c == 0)(lambda: self.tail_mate().wait_recv())
        pl.when(self.p.c == 1)(lambda: self.edge_mate().wait_recv())

    def drain(self):
        self.to_mate().wait_send()
        self.to_pair().wait_send()
        self.pass_on().wait_send()

        @pl.when(self.p.c == 0)
        def _():
            self.edge_out().wait_send()
            self.edge_mate().wait_send()

        @pl.when(self.p.c == 1)
        def _():
            self.tail_out().wait_send()
            self.tail_mate().wait_send()


def row_tiles(rows, step, body):
    def one(t, carry):
        body(pl.ds(pl.multiple_of(t * step, 16), step))
        return carry

    lax.fori_loop(0, rows // step, one, 0)


def forward_kernel(*refs, cols, unit_rest, edge, tail, tile):
    (in_ref, out_ref, up_whole, down_whole, qv_ref, unit_ref, x_src, c_src, gain_ref, shift_ref, segc_ref) = refs[:11]
    segr_ref, refs = refs[11], refs[1:]
    (ws, wu, wd, gd) = refs[11:15]
    outs, refs = refs[15:29], refs[29:]
    held, refs = refs[:14], refs[14:]
    (x_ref, c_ref, first_ref, qkv_ref, ctx_ref, inv_ref, res_ref, second_ref) = held[:8]
    (hidden_ref, slope_ref, hidden_rest, slope_rest, rest_up, rest_down) = held[8:]
    (blocks, unit_blocks, grads, part, part_out, part_in, bias_rest, vec_all) = refs[:8]
    (small_ref, up_ref, down_ref, vec_ref) = refs[8:12]
    gather_sems, local_sem = refs[12 : 12 + Gather.SEMS], refs[12 + Gather.SEMS]
    tail_refs = refs[13 + Gather.SEMS :]
    row_sems = tail_refs[: Rows.SEMS]
    (vec_s, vec_r, load_sem, part_s, part_r, unit_sem, grad_sem, out_sem) = tail_refs[Rows.SEMS :]

    def leave(n):
        return pltpu.make_async_copy(held[n], outs[n], out_sem.at[n])

    main, rest = up_ref.shape[1], unit_rest
    rows, width = x_ref.shape
    place = Place()
    for n in range(3):
        small_ref[:, n * cols : (n + 1) * cols] = in_ref[n].T
    at = 3 * cols
    small_ref[:, at : at + cols] = out_ref[...].T
    at = at + cols
    small_ref[:, at : at + rest] = up_whole[:, main:]
    small_ref[:, at + rest : at + 2 * rest] = down_whole[:, main:]
    at = at + 2 * rest
    if at < small_ref.shape[1]:
        small_ref[:, at:] = jnp.zeros((small_ref.shape[0], small_ref.shape[1] - at), BF16)
    vec_ref[...] = jnp.zeros_like(vec_ref)
    for n in (0, 1):
        high = qv_ref[n : n + 1, :].astype(BF16)
        lo = 2 * n * cols
        vec_ref[0:1, lo : lo + cols] = high
        vec_ref[1:2, lo : lo + cols] = (qv_ref[n : n + 1, :] - high.astype(F32)).astype(BF16)
    vec_ref[2:3, : main + rest] = unit_ref[...]
    place.barrier()
    shards = (small_ref, up_ref, down_ref)
    g = Gather(place, shards, (ws, wu, wd), gather_sems, local_sem, small_ref.shape[0])
    each = x_src.shape[1]
    x_rows = Rows(place, 0, x_src, x_ref, row_sems, each, edge, tail)
    c_rows = Rows(place, 1, c_src, c_ref, row_sems, each, edge, tail)

    def vec_to(d):
        device = place.slot_after(d)
        return send(vec_ref, vec_all.at[place.z], vec_s.at[d], vec_r.at[d], device)

    def vec_from(d):
        ref = vec_all.at[(place.z + 4 - d) % 4]
        return send(ref, ref, vec_s.at[d], vec_r.at[d], place.slot_after(d))

    g.start_z(0)
    g.start_xy(0)
    for d in (1, 2, 3):
        vec_to(d).start()
    x_rows.start()
    vec_all[place.z] = vec_ref[...]
    up_ref[...] = up_whole[:, :main]
    down_ref[...] = down_whole[:, :main]
    g.pass_on(0, 1)
    g.corner(0, 0)
    x_rows.forward()
    g.pass_on(0, 2)
    x_rows.main_ready()
    x_rows.edges()
    g.corner(0, 1)
    x_rows.edges_forward()
    g.pass_on(0, 3)
    g.start_z(1)
    x_rows.edges_ready()

    def first(span):
        value = x_ref[span, :].astype(F32)
        out, _, _ = norm_forward(value, gain_ref[0:1, :], shift_ref[0:1, :])
        first_ref[span, :] = out.astype(BF16)

    row_tiles(rows, 128, first)
    leave(0).start()
    g.corner(0, 2)
    g.corner(0, 3)
    leave(2).start()
    for d in (1, 2, 3):
        vec_from(d).wait_recv()
    g.arrive(0)

    later = []
    for k in (1, 2):
        later.append(lambda k=k: g.start_xy(k))
        if k == 1:
            later.append(lambda: c_rows.start())
        for d in (1, 2, 3):
            later.append(lambda k=k, d=d: g.pass_on(k, d))
            later.append(lambda k=k, d=d: g.corner(k, d - 1))
        if k == 1:
            later.append(lambda: g.start_z(2))
            later.append(lambda: c_rows.forward())
            later.append(lambda: (c_rows.main_ready(), c_rows.edges()))
        later.append(lambda k=k: g.corner(k, 3))
        if k == 1:
            later.append(lambda: c_rows.edges_forward())

    def step(count=1):
        for _ in range(count):
            if later:
                later.pop(0)()

    step(2)

    def load(s):
        return pltpu.make_async_copy(ws.at[s], blocks.at[s % 2], load_sem.at[s % 2])

    heads = cols // DH
    rest_up[...] = jnp.zeros_like(rest_up)
    rest_down[...] = jnp.zeros_like(rest_down)
    bias_rest[...] = jnp.zeros_like(bias_rest)
    part[...] = jnp.zeros_like(part)
    load(0).start()
    points = 1 + heads
    inside = [later.pop(0) for _ in range(4 * points)]

    def at_point(s, n):
        for one in range(4):
            pl.when(s == one)(lambda one=one: inside[one * points + n]() and None)

    def one_slot(s, carry):
        load(s).wait()
        pl.when(s < 3)(lambda: load(s + 1).start())
        w = blocks.at[s % 2]
        bias = vec_all[s, 0:1, : 3 * cols].astype(F32) + vec_all[s, 1:2, : 3 * cols].astype(F32)
        projected = dot_nn(first_ref[...], w[:, : 3 * cols]) + bias
        qkv_ref[s] = projected.astype(BF16)
        at_point(s, 0)
        for head in range(heads):
            attend_head(qkv_ref, ctx_ref, inv_ref, segc_ref, segr_ref, s, head, cols, tile)
            at_point(s, 1 + head)
        part[...] += dot_nt(ctx_ref[s], w[:, 3 * cols : 4 * cols])
        at = 4 * cols
        for one in range(4):

            @pl.when(s == one)
            def _(one=one):
                rest_up[:, one * rest : (one + 1) * rest] = w[:, at : at + rest]
                rest_down[:, one * rest : (one + 1) * rest] = w[:, at + rest : at + 2 * rest]
                bias_rest[:, one * rest : (one + 1) * rest] = vec_all[one, 2:3, main : main + rest].astype(F32)

        return carry

    lax.fori_loop(0, 4, one_slot, 0)

    def halves(h):
        return pl.ds(h * (rows // 2), rows // 2)

    def exchange(h):
        src, dst = part_out.at[halves(h), :], part_in.at[halves(h), :]
        return send(src, dst, part_s.at[h], part_r.at[h], place.mate)

    for h in (0, 1):
        part_out[halves(h), :] = part[halves(h), :].astype(BF16)
        exchange(h).start()
    step()
    for n in (3, 4, 5, 12, 13):
        leave(n).start()
    for h in (0, 1):
        exchange(h).wait_recv()

    def second(span):
        value = x_ref[span, :].astype(F32) + (part_out[span, :].astype(F32) + part_in[span, :].astype(F32))
        value = value + shift_ref[2:3, :]
        res_ref[span, :] = value
        out, _, _ = norm_forward(value, gain_ref[1:2, :], shift_ref[1:2, :])
        second_ref[span, :] = out.astype(BF16)

    row_tiles(rows, 128, second)
    g.arrive(1)

    def unit_load(s):
        return pltpu.make_async_copy(wu.at[s], unit_blocks.at[s % 2], unit_sem.at[s % 2])

    unit_load(0).start()
    passing = [later.pop(0) for _ in range(4)]

    def one_block(s, carry):
        unit_load(s).wait()
        pl.when(s < 3)(lambda: unit_load(s + 1).start())
        bias = vec_all[s, 2:3, :main].astype(F32)

        def units(span):
            hidden, slope = gelu_both(dot_nn(second_ref[span, :], unit_blocks[s % 2]) + bias)
            hidden_ref[s, span, :] = hidden.astype(BF16)
            slope_ref[s, span, :] = slope.astype(BF16)

        row_tiles(rows, tile, units)
        for one in range(4):
            pl.when(s == one)(lambda one=one: passing[one]() and None)
        return carry

    lax.fori_loop(0, 4, one_block, 0)

    def units_rest(span):
        hidden, slope = gelu_both(dot_nn(second_ref[span, :], rest_up[...]) + bias_rest[...])
        hidden_rest[span, :] = hidden.astype(BF16)
        slope_rest[span, :] = slope.astype(BF16)

    for n in (6, 7):
        leave(n).start()
    row_tiles(rows, tile, units_rest)
    step()
    for n in (8, 9, 10, 11):
        leave(n).start()
    c_rows.edges_ready()
    c_rows.drain()
    c_ref[...] = jnp.where(place.owned(segc_ref[...]), c_ref[...], jnp.zeros_like(c_ref))

    def grad_out(s):
        return pltpu.make_async_copy(grads.at[s % 2], gd.at[s], grad_sem.at[s % 2])

    def down_grad(s, carry):
        pl.when(s >= 2)(lambda: grad_out(s - 2).wait())
        grads[s % 2] = dot_tn(c_ref[...], hidden_ref[s]).astype(BF16)
        grad_out(s).start()
        return carry

    lax.fori_loop(0, 2, down_grad, 0)
    step()
    lax.fori_loop(2, 4, down_grad, 0)
    step(len(later))
    leave(1).start()
    for s in (2, 3):
        grad_out(s).wait()
    g.arrive(2)
    for n in range(14):
        leave(n).wait()
    for k in (0, 1, 2):
        g.drain(k)
    x_rows.drain()
    for d in (1, 2, 3):
        vec_to(d).wait_send()
    for h in (0, 1):
        exchange(h).wait_send()


def forward_stage(
    weights, biases, x_src, c_src, gains, shifts, segc, segr, cols, units, lanes, edge, tail
):
    rows, width, shard_rows, main = segc.shape[0], x_src.shape[2], weights[2].shape[0], units // 128 * 128
    unit_rest = units - main
    heads, rest_lanes = cols // DH, round_up(4 * unit_rest, 128)
    vectors = (16, round_up(max(3 * cols, units), 128))
    vmem = pl.BlockSpec(memory_space=pltpu.VMEM)
    far = pl.BlockSpec(memory_space=pl.ANY)
    shape = jax.ShapeDtypeStruct
    dma = pltpu.SemaphoreType.DMA
    return pl.pallas_call(
        functools.partial(forward_kernel, cols=cols, unit_rest=unit_rest, edge=edge, tail=tail, tile=rows // 2),
        in_specs=[vmem] * 12,
        out_specs=[far] * 18,
        out_shape=[
            shape((4, width, lanes), BF16),
            shape((4, width, main), BF16),
            shape((4, width, main), BF16),
            shape((4, width, main), BF16),
            shape((rows, width), BF16),
            shape((rows, width), BF16),
            shape((rows, width), BF16),
            shape((4, rows, 3 * cols), BF16),
            shape((4, rows, cols), BF16),
            shape((4, rows, heads), F32),
            shape((rows, width), F32),
            shape((rows, width), BF16),
            shape((4, rows, main), BF16),
            shape((4, rows, main), BF16),
            shape((rows, rest_lanes), BF16),
            shape((rows, rest_lanes), BF16),
            shape((width, rest_lanes), BF16),
            shape((width, rest_lanes), BF16),
        ],
        scratch_shapes=[
            pltpu.VMEM((rows, width), BF16),
            pltpu.VMEM((rows, width), BF16),
            pltpu.VMEM((rows, width), BF16),
            pltpu.VMEM((4, rows, 3 * cols), BF16),
            pltpu.VMEM((4, rows, cols), BF16),
            pltpu.VMEM((4, rows, heads), F32),
            pltpu.VMEM((rows, width), F32),
            pltpu.VMEM((rows, width), BF16),
            pltpu.VMEM((4, rows, main), BF16),
            pltpu.VMEM((4, rows, main), BF16),
            pltpu.VMEM((rows, rest_lanes), BF16),
            pltpu.VMEM((rows, rest_lanes), BF16),
            pltpu.VMEM((width, rest_lanes), BF16),
            pltpu.VMEM((width, rest_lanes), BF16),
            pltpu.VMEM((2, width, lanes), BF16),
            pltpu.VMEM((2, width, main), BF16),
            pltpu.VMEM((2, width, main), BF16),
            pltpu.VMEM((rows, width), F32),
            pltpu.VMEM((rows, width), BF16),
            pltpu.VMEM((rows, width), BF16),
            pltpu.VMEM((1, rest_lanes), F32),
            pltpu.VMEM((4,) + vectors, BF16),
            pltpu.VMEM((shard_rows, lanes), BF16),
            pltpu.VMEM((shard_rows, main), BF16),
            pltpu.VMEM((shard_rows, main), BF16),
            pltpu.VMEM(vectors, BF16),
        ]
        + [dma((3, 4))] * Gather.SEMS
        + [dma((3,))]
        + [dma((2,))] * Rows.SEMS
        + [dma((4,)), dma((4,)), dma((2,)), dma((2,)), dma((2,)), dma((2,)), dma((2,)), dma((14,))],
        compiler_params=pltpu.CompilerParams(collective_id=1, has_side_effects=True, vmem_limit_bytes=64000000),
        name="forward",
    )(*weights, *biases, x_src, c_src, gains, shifts, segc, segr)


def middle_kernel(*refs, cols, unit_rest):
    (wd, wu, gd) = refs[:3]
    (hidden_far, slope_far, hidden_rest, slope_rest, rest_up, rest_down) = refs[3:9]
    (c_far, second_far, res_far, gain_ref, shift_ref) = refs[9:14]
    gu = refs[14]
    (d_out, rest_sums, half_ref, grad_ref, y_ref, sums_ref, unit_ref, unit_rest_ref) = refs[15:23]
    (blocks, grads, pre_half, part, part_out, part_in, part_in2) = refs[23:30]
    (hidden_ref, slope_ref, c_ref, second_ref, res_ref) = refs[30:35]
    d_bufs, d_own = refs[35:40], refs[40:43]
    refs = refs[43:]
    sems, loads = refs[: Reduce.SEMS], refs[Reduce.SEMS : Reduce.SEMS + 3]
    load_sem, grad_sem, part_s, part_r, in_sem, unit_sem = refs[Reduce.SEMS + 3 :]
    rows, width = c_ref.shape
    rest = unit_rest
    place = Place()
    place.barrier()

    def down_final(total):
        d_out[...] = total[...].astype(F32)

    r = Reduce(place, (gd,), (d_own,), (down_final,), (d_bufs,), sems, loads, d_out.shape[0])

    def load(w, slot, buffer):
        return pltpu.make_async_copy(w.at[slot], blocks.at[buffer], load_sem.at[buffer])

    def halves(h):
        return pl.ds(h * (rows // 2), rows // 2)

    def exchange(n, h):
        dst = (part_in, part_in2)[n]
        src, dst = part_out.at[halves(h), :], dst.at[halves(h), :]
        return send(src, dst, part_s.at[n, h], part_r.at[n, h], place.mate)

    def enter(n):
        far, near = ((c_far, c_ref), (second_far, second_ref), (res_far, res_ref))[n]
        return pltpu.make_async_copy(far, near, in_sem.at[n])

    def unit_loads(s):
        return (
            pltpu.make_async_copy(hidden_far.at[s], hidden_ref.at[s % 2], unit_sem.at[0, s % 2]),
            pltpu.make_async_copy(slope_far.at[s], slope_ref.at[s % 2], unit_sem.at[1, s % 2]),
        )

    def start_units(s):
        for copy in unit_loads(s):
            copy.start()

    enter(0).start()
    load(wd, 0, 0).start()
    start_units(0)
    r.start(0)
    enter(1).start()
    enter(2).start()
    enter(0).wait()
    part[...] = dot_nt(hidden_rest[...], rest_down[...])
    grad_rest = slope_rest[...].astype(F32) * dot_nn(c_ref[...], rest_down[...])
    unit_rest_ref[...] = jnp.sum(grad_rest, axis=0, keepdims=True)
    half_rest = grad_rest.astype(BF16)

    def down_block(s, carry):
        load(wd, s, s % 2).wait()
        pl.when(s < 3)(lambda: load(wd, s + 1, (s + 1) % 2).start())
        pl.when(s == 3)(lambda: load(wu, 0, 0).start())
        for copy in unit_loads(s):
            copy.wait()
        pl.when(s < 3)(lambda: start_units(s + 1))
        w = blocks[s % 2]
        part[...] += dot_nt(hidden_ref[s % 2], w)
        grad = slope_ref[s % 2].astype(F32) * dot_nn(c_ref[...], w)
        pre_half[s] = grad.astype(BF16)
        unit_ref[s] = jnp.broadcast_to(jnp.sum(grad, axis=0, keepdims=True), unit_ref.shape[1:])
        r.middle_one(0, s)
        return carry

    lax.fori_loop(0, 4, down_block, 0)
    for h in (0, 1):
        part_out[halves(h), :] = part[halves(h), :].astype(BF16)
        exchange(0, h).start()
    part[...] = dot_nt(half_rest, rest_up[...])

    def up_block(s, carry):
        load(wu, s, s % 2).wait()
        pl.when(s < 3)(lambda: load(wu, s + 1, (s + 1) % 2).start())
        part[...] += dot_nt(pre_half[s], blocks[s % 2])
        return carry

    lax.fori_loop(0, 4, up_block, 0)
    enter(1).wait()
    enter(2).wait()
    for h in (0, 1):
        exchange(0, h).wait_recv()

    def output(span):
        value = part_out[span, :].astype(F32) + part_in[span, :].astype(F32)
        y_ref[span, :] = (res_ref[span, :] + value + shift_ref[3:4, :]).astype(BF16)

    row_tiles(rows, 128, output)
    for h in (0, 1):
        exchange(0, h).wait_send()
        part_out[halves(h), :] = part[halves(h), :].astype(BF16)
        exchange(1, h).start()

    def grad_out(s):
        return pltpu.make_async_copy(grads.at[s % 2], gu.at[s], grad_sem.at[s % 2])

    def up_grad(s, carry):
        pl.when(s >= 2)(lambda: grad_out(s - 2).wait())
        grads[s % 2] = dot_tn(second_ref[...], pre_half[s]).astype(BF16)
        grad_out(s).start()
        n = s - place.behind()
        pl.when((n >= 0) & (n < 3))(lambda: r.line_one(0, n))
        return carry

    lax.fori_loop(0, 4, up_grad, 0)
    up_sum = dot_tn(second_ref[...], half_rest).astype(BF16)
    down_sum = dot_tn(c_ref[...], hidden_rest[...]).astype(BF16)
    rest_sums[...] = jnp.zeros_like(rest_sums)
    for s in range(4):
        rest_sums[s, :, :rest] = up_sum[:, s * rest : (s + 1) * rest]
        rest_sums[s, :, rest : 2 * rest] = down_sum[:, s * rest : (s + 1) * rest]
    for h in (0, 1):
        exchange(1, h).wait_recv()
    sums_ref[...] = jnp.zeros_like(sums_ref)

    def back(span):
        grad = part_out[span, :].astype(F32) + part_in2[span, :].astype(F32)
        upstream = c_ref[span, :].astype(F32)
        _, scaled, factor = norm_forward(res_ref[span, :], gain_ref[1:2, :], shift_ref[1:2, :])
        value = upstream + norm_backward(grad, scaled, factor, gain_ref[1:2, :])
        grad_ref[span, :] = value
        half_ref[span, :] = value.astype(BF16)
        sums_ref[1:2, :] += jnp.sum(grad * scaled, axis=0, keepdims=True)
        sums_ref[3:4, :] += jnp.sum(grad, axis=0, keepdims=True)
        sums_ref[4:5, :] += jnp.sum(value, axis=0, keepdims=True)
        sums_ref[5:6, :] += jnp.sum(upstream, axis=0, keepdims=True)

    row_tiles(rows, 128, back)
    r.line_one(0, 3)
    for s in (2, 3):
        grad_out(s).wait()
    r.drain(0)
    for h in (0, 1):
        exchange(1, h).wait_send()


def middle_stage(
    wd, wu, gd, hidden, slope, hidden_rest, slope_rest, rest_up, rest_down, cot, second, residual, gains, shifts, cols, unit_rest, spare
):
    rows, width = cot.shape
    main, shard_rows = wd.shape[2], width // 4
    vmem = pl.BlockSpec(memory_space=pltpu.VMEM)
    far = pl.BlockSpec(memory_space=pl.ANY)
    shape = jax.ShapeDtypeStruct
    dma = pltpu.SemaphoreType.DMA
    return pl.pallas_call(
        functools.partial(middle_kernel, cols=cols, unit_rest=unit_rest),
        in_specs=[far] * 5 + [vmem] * 4 + [far] * 3 + [vmem] * 2,
        out_specs=[far] + [vmem] * 8,
        out_shape=[
            shape((4, width, main), BF16),
            shape((shard_rows, main), F32),
            shape((4, width, 2 * unit_rest + spare), BF16),
            shape((rows, width), BF16),
            shape((rows, width), F32),
            shape((rows, width), BF16),
            shape((8, width), F32),
            shape((4, 8, main), F32),
            shape((1, rest_up.shape[1]), F32),
        ],
        scratch_shapes=[
            pltpu.VMEM((2, width, main), BF16),
            pltpu.VMEM((2, width, main), BF16),
            pltpu.VMEM((4, rows, main), BF16),
            pltpu.VMEM((rows, width), F32),
            pltpu.VMEM((rows, width), BF16),
            pltpu.VMEM((rows, width), BF16),
            pltpu.VMEM((rows, width), BF16),
            pltpu.VMEM((2, rows, main), BF16),
            pltpu.VMEM((2, rows, main), BF16),
            pltpu.VMEM((rows, width), BF16),
            pltpu.VMEM((rows, width), BF16),
            pltpu.VMEM((rows, width), F32),
        ]
        + reduce_buffers(shard_rows, main)
        + reduce_terms(shard_rows, main)
        + [dma((1, 4))] * Reduce.SEMS
        + [dma((1, 4))] * 3
        + [dma((2,)), dma((2,)), dma((2, 2)), dma((2, 2)), dma((3,)), dma((2, 2))],
        compiler_params=pltpu.CompilerParams(collective_id=3, has_side_effects=True, vmem_limit_bytes=64000000),
        name="middle",
    )(wd, wu, gd, hidden, slope, hidden_rest, slope_rest, rest_up, rest_down, cot, second, residual, gains, shifts)


class Reduce:
    SEMS = 16

    def __init__(self, place, g, own, out, bufs, sems, load_sems, rows):
        self.p, self.g, self.own, self.out, self.rows = place, g, own, out, rows
        self.bufs, self.sems, self.load_sems = bufs, sems, load_sems

    def grad(self, k, slot, owner, half=None):
        at, count = owner * self.rows, self.rows
        if half is not None:
            count = count // 2
            at = at + half * count
        return self.g[k].at[slot, pl.ds(pl.multiple_of(at, 16), count), :]

    def terms(self, k, slot):
        f = self.p.f
        if self.own[k] is None:
            return self.grad(k, slot, f ^ 1, 0), self.grad(k, slot, f ^ 2, 1), self.grad(k, slot, f)
        return tuple(ref.at[slot] for ref in self.own[k])

    def loads(self, k, slot):
        f = self.p.f
        src = self.grad(k, slot, f ^ 1, 0), self.grad(k, slot, f ^ 2, 1), self.grad(k, slot, f)
        pairs = zip(src, self.terms(k, slot), self.load_sems)
        return [pltpu.make_async_copy(one, dst, sem.at[k, slot]) for one, dst, sem in pairs]

    def half(self, ref, slot, half):
        count = self.rows // 2
        return ref.at[slot, half * count : (half + 1) * count, :]

    def copy(self, k, slot, src, dst, index, device):
        return send(src, dst, self.sems[2 * index].at[k, slot], self.sems[2 * index + 1].at[k, slot], device)

    def corner_y(self, k, s):
        return self.copy(k, s, self.grad(k, s, self.p.f ^ 3, 0), self.bufs[k][0].at[s], 0, self.p.across_y)

    def corner_x(self, k, s):
        return self.copy(k, s, self.grad(k, s, self.p.f ^ 3, 1), self.bufs[k][1].at[s], 1, self.p.across_x)

    def x_low(self, k, s):
        return self.copy(k, s, self.bufs[k][0].at[s], self.half(self.bufs[k][2], s, 0), 2, self.p.across_x)

    def x_high(self, k, s):
        dst = self.half(self.bufs[k][2], s, 1)
        return self.copy(k, s, self.grad(k, s, self.p.f ^ 1, 1), dst, 3, self.p.across_x)

    def y_low(self, k, s):
        dst = self.half(self.bufs[k][3], s, 0)
        return self.copy(k, s, self.grad(k, s, self.p.f ^ 2, 0), dst, 4, self.p.across_y)

    def y_high(self, k, s):
        return self.copy(k, s, self.bufs[k][1].at[s], self.half(self.bufs[k][3], s, 1), 5, self.p.across_y)

    def up(self, k, s):
        return self.copy(k, s, self.bufs[k][2].at[s], self.bufs[k][4].at[s], 6, self.p.above)

    def down(self, k, s):
        at = jnp.where(s == self.p.z - 1, 4, s)
        return self.copy(k, s, self.bufs[k][2].at[s], self.bufs[k][4].at[at], 7, self.p.below)

    def from_above(self, k, s):
        at = jnp.where(s == self.p.z, 4, s)
        return self.copy(k, s, self.bufs[k][4].at[at], self.bufs[k][4].at[at], 7, self.p.below), at

    def start_one(self, k, s):
        self.corner_y(k, s).start()
        self.corner_x(k, s).start()
        self.y_low(k, s).start()
        self.x_high(k, s).start()

    def start(self, k):
        def one(i, carry):
            self.start_one(k, self.p.far_first(i))
            return carry

        lax.fori_loop(0, 4, one, 0)
        if self.own[k] is not None:
            for slot in range(4):
                for load in self.loads(k, slot):
                    load.start()

    def tiles(self, rows, body):
        row_tiles(rows, 48 if rows % 48 == 0 else 16, body)

    def middle_one(self, k, i):
        s, count = self.p.far_first(i), self.rows // 2
        low, high = self.bufs[k][0], self.bufs[k][1]
        if self.own[k] is not None:
            for load in self.loads(k, s):
                load.wait()
        own_low, own_high, _ = self.terms(k, s)
        self.corner_y(k, s).wait_recv()

        def add_low(span):
            low[s, span, :] = add_half(low[s, span, :], own_low[span, :])

        self.tiles(count, add_low)
        self.corner_x(k, s).wait_recv()

        def add_high(span):
            high[s, span, :] = add_half(high[s, span, :], own_high[span, :])

        self.tiles(count, add_high)
        self.x_low(k, s).start()
        self.y_high(k, s).start()

    def line_one(self, k, i):
        z, acc, side, far = self.p.z, self.bufs[k][2], self.bufs[k][3], self.bufs[k][4]
        s = self.p.far_first(i)
        self.x_low(k, s).wait_recv()
        self.x_high(k, s).wait_recv()
        self.y_low(k, s).wait_recv()
        self.y_high(k, s).wait_recv()
        own = self.terms(k, s)[2]

        def add(span):
            total = own[span, :].astype(F32) + acc[s, span, :].astype(F32) + side[s, span, :].astype(F32)
            acc[s, span, :] = total.astype(BF16)

        self.tiles(self.rows, add)

        def add_far(at):
            def body(span):
                acc[s, span, :] = add_half(acc[s, span, :], far[at, span, :])

            self.tiles(self.rows, body)

        @pl.when((z > 0) & (s >= z))
        def _():
            self.up(k, s).wait_recv()
            add_far(s)

        @pl.when((z < 3) & (s <= z))
        def _():
            copy, at = self.from_above(k, s)
            copy.wait_recv()
            add_far(at)

        @pl.when(s > z)
        def _():
            self.up(k, s).start()

        @pl.when(s < z)
        def _():
            self.down(k, s).start()

        @pl.when(s == z)
        def _():
            self.out[k](acc.at[s])

    def loop(self, one):
        def body(i, carry):
            one(i)
            return carry

        lax.fori_loop(0, 4, body, 0)

    def drain(self, k):
        def one(s):
            for copy in (self.corner_y, self.corner_x, self.x_low, self.x_high, self.y_low, self.y_high):
                copy(k, s).wait_send()

            @pl.when(s > self.p.z)
            def _():
                self.up(k, s).wait_send()

            @pl.when(s < self.p.z)
            def _():
                self.down(k, s).wait_send()

        self.loop(one)


def reduce_buffers(rows, lanes):
    half, whole = pltpu.VMEM((4, rows // 2, lanes), BF16), pltpu.VMEM((4, rows, lanes), BF16)
    return [half, half, whole, whole, pltpu.VMEM((5, rows, lanes), BF16)]


def reduce_terms(rows, lanes):
    half, whole = pltpu.VMEM((4, rows // 2, lanes), BF16), pltpu.VMEM((4, rows, lanes), BF16)
    return [half, half, whole]


def scatter_grads(chunks):
    count = lax.axis_size("fy") * lax.axis_size("fx")
    split = [c.reshape(c.shape[0] * count, c.shape[1] // count, c.shape[2]) for c in chunks]
    return [lax.psum_scatter(c, ("slot",) + FSDP, scatter_dimension=0).astype(F32) for c in split]


class RowsBack:
    SEMS = 7

    def __init__(self, place, index, window, inbox, owned, out, sems, rows_each, edge, tail):
        self.p, self.window, self.inbox, self.owned, self.out = place, window, inbox, owned, out
        self.each, self.half, self.edge, self.tail = rows_each, 4 * rows_each, edge, tail
        self.sems = [sem.at[index] for sem in sems]

    def edge_out(self):
        src = self.window.at[self.half : self.half + self.edge, :]
        return send(src, self.inbox.at[: self.edge, :], self.sems[0], self.sems[1], self.p.cross)

    def tail_out(self):
        src = self.window.at[self.half + self.edge :, :]
        return send(src, self.inbox.at[self.edge :, :], self.sems[2], self.sems[3], self.p.cross)

    def block(self, near):
        batch = self.p.batch if near else 1 - self.p.batch
        row = (2 * batch + self.p.c) * self.each
        return self.window.at[pl.ds(pl.multiple_of(row, 16), self.each), :]

    def stay(self):
        return pltpu.make_async_copy(self.block(True), self.out.at[self.p.batch], self.sems[4])

    def to_pair(self):
        return send(self.block(False), self.out.at[self.p.batch], self.sems[5], self.sems[6], self.p.pair)

    def edges(self):
        pl.when(self.p.c == self.p.image)(lambda: self.edge_out().start())
        pl.when((self.p.c == 1) & (self.p.image == 0))(lambda: self.tail_out().start())

    def merge(self, row, count, at):
        keep = self.p.owned(self.owned[row : row + count, :])
        value = jnp.where(keep, self.window[row : row + count, :], self.inbox[at : at + count, :])
        self.window[row : row + count, :] = value

    def finish(self):
        p = self.p

        @pl.when((p.c == 1) & (p.image == 0))
        def _():
            self.edge_out().wait_recv()
            self.merge(self.half - self.edge, self.edge, 0)

        @pl.when((p.c == 0) & (p.image == 1))
        def _():
            self.edge_out().wait_recv()
            self.merge(0, self.edge, 0)

        @pl.when((p.c == 1) & (p.image == 1))
        def _():
            self.tail_out().wait_recv()
            self.merge(self.half - self.tail, self.tail, self.edge)

        self.to_pair().start()
        self.stay().start()

    def drain(self):
        pl.when(self.p.c == self.p.image)(lambda: self.edge_out().wait_send())
        pl.when((self.p.c == 1) & (self.p.image == 0))(lambda: self.tail_out().wait_send())
        self.stay().wait()
        self.to_pair().wait_send()
        ref = self.out.at[1 - self.p.batch]
        send(ref, ref, self.sems[5], self.sems[6], self.p.pair).wait_recv()


def backward_kernel(*refs, cols, unit_rest, edge, tail, tile):
    (ws, gu, rest_ref, half_ref, first_far, qkv_far, ctx_far, inv_far, segc_ref, segr_whole) = refs[:10]
    (x_far, res_grad_ref, y_ref, gain_ref, d_in, old_sums, unit_ref, unit_rest_ref) = refs[10:18]
    (in_out, out_out, up_out, down_out, x_final, y_out, gain_out, shift_out, qv_out, unit_out) = refs[18:28]
    refs = refs[28:]
    (segr_ref, x_out, sums_ref), refs = refs[:3], refs[3:]
    (blocks, gs, part, part_out, part_in, back_ref, grad_ref, key_acc, value_acc, inbox_x, inbox_y) = refs[:11]
    y_window = part_out
    bias_ref, sums_in, vec_sum, vec_in, vec_far = refs[11:16]
    first_ref, qkv_ref, ctx_ref, inv_ref, x_ref = refs[16:21]
    u_bufs, s_bufs, u_own = refs[21:26], refs[26:31], refs[31:34]
    refs = refs[34:]
    sems, loads, back_sems = refs[: Reduce.SEMS], refs[Reduce.SEMS : Reduce.SEMS + 3], refs[Reduce.SEMS + 3 : Reduce.SEMS + 3 + RowsBack.SEMS]
    load_sem, part_s, part_r, y_sems, sum_s, sum_r, vec_s, vec_r, in_sem = refs[Reduce.SEMS + 3 + RowsBack.SEMS :]
    rows, width = half_ref.shape
    shard_rows, main, rest = up_out.shape[0], gu.shape[2], unit_rest
    heads = cols // DH
    place = Place()
    place.barrier()
    each = x_out.shape[1]

    def up_final(total):
        up_out[:, :main] = total[...].astype(F32)

    def small_final(total):
        for n in range(3):
            in_out[n] = total[:, n * cols : (n + 1) * cols].astype(F32).T
        at = 3 * cols
        out_out[...] = total[:, at : at + cols].astype(F32).T
        at = at + cols
        up_out[:, main:] = total[:, at : at + rest].astype(F32)
        down_out[:, main:] = total[:, at + rest : at + 2 * rest].astype(F32)

    r = Reduce(place, (gu, gs), (u_own, None), (up_final, small_final), (u_bufs, s_bufs), sems, loads, shard_rows)
    x_back = RowsBack(place, 0, part_in, inbox_x, segc_ref, x_out, back_sems, each, edge, tail)
    y_back = RowsBack(place, 1, y_window, inbox_y, segc_ref, y_out, back_sems, each, edge, tail)

    def load(i):
        return pltpu.make_async_copy(ws.at[place.far_first(i)], blocks.at[i % 2], load_sem.at[i % 2])

    y_load = pltpu.make_async_copy(y_ref, y_window, y_sems.at[0])
    def slot_loads(i):
        s = place.far_first(i)
        pairs = ((qkv_far, qkv_ref), (ctx_far, ctx_ref), (inv_far, inv_ref))
        return [pltpu.make_async_copy(p[0].at[s], p[1].at[s], in_sem.at[n, i]) for n, p in enumerate(pairs)]

    first_load = pltpu.make_async_copy(first_far, first_ref, y_sems.at[1])
    x_load = pltpu.make_async_copy(x_far, x_ref, y_sems.at[2])
    load(0).start()
    for copy in slot_loads(0):
        copy.start()
    y_load.start()
    r.start(0)
    for t in range(rows // tile):
        segr_ref[t] = segr_whole[:, t * tile : (t + 1) * tile]
    down_out[:, :main] = d_in[...]
    first_load.start()
    for i in (1, 2, 3):
        for copy in slot_loads(i):
            copy.start()
    x_load.start()
    y_load.wait()
    y_back.edges()

    def one_slot(i, carry):
        s = place.far_first(i)
        load(i).wait()
        for copy in slot_loads(i):
            copy.wait()

        @pl.when(i < 3)
        def _():
            load(i + 1).start()

        w = blocks.at[i % 2]
        back_ref[...] = dot_nn(half_ref[...], w[:, 3 * cols : 4 * cols]).astype(BF16)
        gs[s, :, 3 * cols : 4 * cols] = dot_tn(half_ref[...], ctx_ref[s]).astype(BF16)
        gs[s, :, 4 * cols :] = rest_ref[s]
        for head in range(heads):
            attend_back_head(
                qkv_ref, ctx_ref, inv_ref, back_ref, segc_ref, segr_ref, grad_ref, bias_ref, key_acc, value_acc, s, head, cols, tile
            )
            if head == 0:
                r.middle_one(0, i)
                pl.when(i == 1)(lambda: y_back.finish())
        pl.when(i == 0)(lambda: first_load.wait())
        gs[s, :, : 3 * cols] = dot_tn(first_ref[...], grad_ref[...]).astype(BF16)
        product = dot_nt(grad_ref[...], w[:, : 3 * cols])

        @pl.when(i == 0)
        def _():
            part[...] = product

        @pl.when(i > 0)
        def _():
            part[...] += product

        r.start_one(1, s)
        pl.when(i > place.behind())(lambda: r.line_one(0, i - 1 - place.behind()))
        pl.when(i > 0)(lambda: r.middle_one(1, i - 1))
        pl.when(i > 1 + place.behind())(lambda: r.line_one(1, i - 2 - place.behind()))
        return carry

    lax.fori_loop(0, 4, one_slot, 0)

    def halves(h):
        return pl.ds(h * (rows // 2), rows // 2)

    def exchange(h):
        src, dst = part_out.at[halves(h), :], part_in.at[halves(h), :]
        return send(src, dst, part_s.at[h], part_r.at[h], place.mate)

    y_back.drain()
    for h in (0, 1):
        part_out[halves(h), :] = part[halves(h), :].astype(BF16)
        exchange(h).start()
    res_load = pltpu.make_async_copy(res_grad_ref, part, load_sem.at[0])
    res_load.start()
    pl.when(place.behind() == 1)(lambda: r.line_one(0, 2))
    r.line_one(0, 3)
    pl.when(place.behind() == 1)(lambda: r.line_one(1, 1))
    r.middle_one(1, 3)
    for h in (0, 1):
        exchange(h).wait_recv()

    res_load.wait()
    x_load.wait()
    sums_ref[...] = old_sums[...]

    def last(span):
        grad = part_out[span, :].astype(F32) + part_in[span, :].astype(F32)
        value = x_ref[span, :].astype(F32)
        _, scaled, factor = norm_forward(value, gain_ref[0:1, :], gain_ref[0:1, :])
        result = part[span, :] + norm_backward(grad, scaled, factor, gain_ref[0:1, :])
        part_in[span, :] = result.astype(BF16)
        sums_ref[0:1, :] += jnp.sum(grad * scaled, axis=0, keepdims=True)
        sums_ref[2:3, :] += jnp.sum(grad, axis=0, keepdims=True)

    row_tiles(rows, 128, last)
    x_back.edges()

    vec_sum[...] = jnp.zeros_like(vec_sum)
    for s in range(4):
        vec_sum[s, 0:1, :cols] = bias_ref[s, 0:1, :]
        vec_sum[s, 1:2, :cols] = bias_ref[s, 1:2, :]
        vec_sum[s, 2:3, :main] = unit_ref[s, 0:1, :]
        vec_sum[s, 3:4, :rest] = unit_rest_ref[:, s * rest : (s + 1) * rest]

    def across(n, device):
        return (
            send(sums_ref, sums_in.at[n], sum_s.at[n], sum_r.at[n], device),
            send(vec_sum, vec_in.at[n], vec_s.at[n], vec_r.at[n], device),
        )

    def along(d):
        there = (place.z + d) % 4
        device = place.slot_after(d)
        return (
            send(sums_ref, sums_in.at[1 + d], sum_s.at[1 + d], sum_r.at[1 + d], device),
            send(vec_sum.at[there], vec_far.at[d - 1], vec_s.at[1 + d], vec_r.at[1 + d], device),
        )

    def add_across(n, device):
        for copy in across(n, device):
            copy.wait()
        sums_ref[...] += sums_in[n]
        vec_sum[...] += vec_in[n]

    for copy in across(0, place.across_x):
        copy.start()
    r.line_one(1, 2)
    add_across(0, place.across_x)
    for copy in across(1, place.across_y):
        copy.start()
    x_back.finish()
    add_across(1, place.across_y)
    for d in (1, 2, 3):
        for copy in along(d):
            copy.start()
    r.line_one(1, 3)
    for d in (1, 2, 3):
        for copy in along(d):
            copy.wait()
    sums_ref[...] += sums_in[2] + sums_in[3] + sums_in[4]
    gain_out[...] = sums_ref[0:2, :]
    shift_out[...] = sums_ref[2:6, :]
    total = vec_sum[place.z] + vec_far[0] + vec_far[1] + vec_far[2]
    qv_out[...] = total[0:2, :cols]
    unit_out[:, :main] = total[2:3, :main]
    unit_out[:, main:] = total[3:4, :rest]
    for k in (0, 1):
        r.drain(k)
    x_back.drain()
    x_final[...] = x_out[...].astype(F32)
    for h in (0, 1):
        exchange(h).wait_send()


def backward_stage(
    ws, gu, rest_sums, residual_half, first_norm, qkv, context, inverse, segc, segr, x_half, residual_grad, y_rows, gains, down_sum,
    sums, unit_sums, unit_rest_sums, cols, unit_rest, edge, tail, rows_each,
):
    rows, width = residual_half.shape
    shard_rows, lanes, main = width // 4, ws.shape[2], gu.shape[2]
    vmem = pl.BlockSpec(memory_space=pltpu.VMEM)
    far = pl.BlockSpec(memory_space=pl.ANY)
    shape = jax.ShapeDtypeStruct
    dma = pltpu.SemaphoreType.DMA
    wide = max(main, round_up(cols, 128))
    return pl.pallas_call(
        functools.partial(backward_kernel, cols=cols, unit_rest=unit_rest, edge=edge, tail=tail, tile=rows // 2),
        in_specs=[far] * 2 + [vmem] * 2 + [far] * 4 + [vmem] * 2 + [far] * 3 + [vmem] * 5,
        out_specs=[vmem] * 10,
        out_shape=[
            shape((3, cols, shard_rows), F32),
            shape((cols, shard_rows), F32),
            shape((shard_rows, main + unit_rest), F32),
            shape((shard_rows, main + unit_rest), F32),
            shape((2, rows_each, width), F32),
            shape((2, rows_each, width), BF16),
            shape((2, width), F32),
            shape((4, width), F32),
            shape((2, cols), F32),
            shape((1, main + unit_rest), F32),
        ],
        scratch_shapes=[
            pltpu.VMEM((2, 1, rows // 2), jnp.int32),
            pltpu.VMEM((2, rows_each, width), BF16),
            pltpu.VMEM((8, width), F32),
            pltpu.VMEM((2, width, lanes), BF16),
            pltpu.VMEM((4, width, lanes), BF16),
            pltpu.VMEM((rows, width), F32),
            pltpu.VMEM((rows, width), BF16),
            pltpu.VMEM((rows, width), BF16),
            pltpu.VMEM((rows, cols), BF16),
            pltpu.VMEM((rows, 3 * cols), BF16),
            pltpu.VMEM((rows, DH), F32),
            pltpu.VMEM((rows, DH), F32),
            pltpu.VMEM((edge + tail, width), BF16),
            pltpu.VMEM((edge + tail, width), BF16),
            pltpu.VMEM((4, 2, cols), F32),
            pltpu.VMEM((5, 8, width), F32),
            pltpu.VMEM((4, 8, wide), F32),
            pltpu.VMEM((2, 4, 8, wide), F32),
            pltpu.VMEM((3, 8, wide), F32),
            pltpu.VMEM((rows, width), BF16),
            pltpu.VMEM((4, rows, 3 * cols), BF16),
            pltpu.VMEM((4, rows, cols), BF16),
            pltpu.VMEM((4, rows, cols // DH), F32),
            pltpu.VMEM((rows, width), BF16),
        ]
        + reduce_buffers(shard_rows, main)
        + reduce_buffers(shard_rows, lanes)
        + reduce_terms(shard_rows, main)
        + [dma((2, 4))] * Reduce.SEMS
        + [dma((1, 4))] * 3
        + [dma((2,))] * RowsBack.SEMS
        + [dma((2,)), dma((2,)), dma((2,)), dma((3,)), dma((5,)), dma((5,)), dma((5,)), dma((5,)), dma((3, 4))],
        compiler_params=pltpu.CompilerParams(collective_id=2, has_side_effects=True, vmem_limit_bytes=64000000),
        name="backward",
    )(
        ws, gu, rest_sums, residual_half, first_norm, qkv, context, inverse, segc, segr,
        x_half, residual_grad, y_rows, gains, down_sum, sums, unit_sums, unit_rest_sums,
    )


def attend_head(qkv_ref, ctx_ref, inv_ref, segc_ref, segr_ref, s, head, cols, tile):
    lo = head * DH
    keys = qkv_ref[s, :, cols + lo : cols + lo + DH]
    values = qkv_ref[s, :, 2 * cols + lo : 2 * cols + lo + DH]

    def one_tile(t, carry):
        span = pl.ds(pl.multiple_of(t * tile, tile), tile)
        scores = dot_nt(qkv_ref[s, span, lo : lo + DH], keys)
        allowed = segc_ref[span, :] == segr_ref[...]
        exact = jnp.where(allowed, jnp.exp2(scores * (SCALE * LOG2E)), 0.0)
        inverse = 1.0 / jnp.sum(exact, axis=1, keepdims=True)
        context = dot_nn(exact.astype(BF16), values) * inverse
        ctx_ref[s, span, lo : lo + DH] = context.astype(BF16)
        inv_ref[s, span, head : head + 1] = inverse
        return carry

    lax.fori_loop(0, qkv_ref.shape[1] // tile, one_tile, 0)


def attend_kernel(x_ref, w_ref, b_ref, segc_ref, segr_ref, qkv_ref, ctx_ref, inv_ref, part_ref, *, cols, tile):
    block = pl.program_id(0)
    projected = dot_nn(x_ref[...], w_ref[0, :, : 3 * cols]) + b_ref[0]
    qkv_ref[0] = projected.astype(BF16)
    for head in range(cols // DH):
        attend_head(qkv_ref, ctx_ref, inv_ref, segc_ref, segr_ref, 0, head, cols, tile)
    part = dot_nt(ctx_ref[0], w_ref[0, :, 3 * cols : 4 * cols])

    @pl.when(block == 0)
    def _():
        part_ref[...] = part

    @pl.when(block > 0)
    def _():
        part_ref[...] += part


def attend(first_norm, weights, bias, segments, cols, tile):
    rows, width = first_norm.shape
    slots, _, lanes = weights.shape
    heads = cols // DH
    whole = lambda shape: pl.BlockSpec(shape, lambda s: (0,) * len(shape))
    each = lambda shape: pl.BlockSpec((1,) + shape, lambda s: (s, 0, 0))
    return pl.pallas_call(
        functools.partial(attend_kernel, cols=cols, tile=tile),
        grid=(slots,),
        in_specs=[
            whole((rows, width)),
            each((width, lanes)),
            each((1, 3 * cols)),
            whole((rows, 1)),
            whole((1, rows)),
        ],
        out_specs=[each((rows, 3 * cols)), each((rows, cols)), each((rows, heads)), whole((rows, width))],
        out_shape=[
            jax.ShapeDtypeStruct((slots, rows, 3 * cols), BF16),
            jax.ShapeDtypeStruct((slots, rows, cols), BF16),
            jax.ShapeDtypeStruct((slots, rows, heads), F32),
            jax.ShapeDtypeStruct((rows, width), F32),
        ],
        cost_estimate=pl.CostEstimate(
            flops=slots * (8 * rows * width * cols + 4 * rows * rows * 256 * heads),
            bytes_accessed=slots * width * lanes * 2 + rows * width * 10,
            transcendentals=slots * heads * rows * rows,
        ),
        name="attend",
    )(first_norm, weights, bias, segments[:, None], segments[None, :])


def attend_back_head(
    qkv_ref, ctx_ref, inv_ref, back_ref, segc_ref, segr_ref, grad_ref, bias_ref, key_acc, value_acc, s, head, cols, tile
):
    lo = head * DH
    rows = back_ref.shape[0]
    ones = jnp.ones((8, DH), F32)
    keys = qkv_ref[s, :, cols + lo : cols + lo + DH]
    values = qkv_ref[s, :, 2 * cols + lo : 2 * cols + lo + DH]
    key_acc[...] = jnp.zeros_like(key_acc)
    value_acc[...] = jnp.zeros_like(value_acc)

    def one_tile(t, query_total):
        span = pl.ds(pl.multiple_of(t * tile, tile), tile)
        queries = qkv_ref[s, span, lo : lo + DH]
        back = (back_ref[span, lo : lo + DH].astype(F32) * inv_ref[s, span, head : head + 1]).astype(BF16)
        along = back.astype(F32) * ctx_ref[s, span, lo : lo + DH].astype(F32)
        delta = lax.dot_general(
            ones, along, (((1,), (1,)), ((), ())), precision=lax.Precision.HIGHEST, preferred_element_type=F32
        )[:1]
        scores = dot_nt(keys, queries)
        allowed = segc_ref[...] == segr_ref[t]
        exact = jnp.where(allowed, jnp.exp2(scores * (SCALE * LOG2E)), 0.0)
        value_acc[...] += dot_nn(exact.astype(BF16), back)
        prob_grad = dot_nt(values, back)
        score_grad = (exact * (prob_grad - delta)).astype(BF16)
        key_acc[...] += dot_nn(score_grad, queries)
        query_grad = dot_tn(score_grad, keys) * SCALE
        grad_ref[span, lo : lo + DH] = query_grad.astype(BF16)
        return query_total + jnp.sum(query_grad, axis=0, keepdims=True)

    query_total = lax.fori_loop(0, rows // tile, one_tile, jnp.zeros((1, DH), F32))
    grad_ref[:, cols + lo : cols + lo + DH] = (key_acc[...] * SCALE).astype(BF16)
    grad_ref[:, 2 * cols + lo : 2 * cols + lo + DH] = value_acc[...].astype(BF16)
    bias_ref[s, 0:1, lo : lo + DH] = query_total
    bias_ref[s, 1:2, lo : lo + DH] = jnp.sum(value_acc[...], axis=0, keepdims=True)


def attend_back_kernel(
    r_ref, w_ref, qkv_ref, ctx_ref, inv_ref, segc_ref, segr_ref, grad_ref, bias_ref, back_ref, key_acc, value_acc, *, cols, tile
):
    back_ref[...] = dot_nn(r_ref[...], w_ref[0, :, 3 * cols : 4 * cols]).astype(BF16)
    for head in range(cols // DH):
        attend_back_head(
            qkv_ref, ctx_ref, inv_ref, back_ref, segc_ref, segr_ref, grad_ref.at[0], bias_ref, key_acc, value_acc, 0, head, cols, tile
        )


def attend_back(residual_half, weights, qkv, context, inverse, segments, cols, tile):
    rows, width = residual_half.shape
    slots, _, lanes = weights.shape
    heads = cols // DH
    whole = lambda shape: pl.BlockSpec(shape, lambda s: (0,) * len(shape))
    each = lambda shape: pl.BlockSpec((1,) + shape, lambda s: (s, 0, 0))
    return pl.pallas_call(
        functools.partial(attend_back_kernel, cols=cols, tile=tile),
        grid=(slots,),
        in_specs=[
            whole((rows, width)),
            each((width, lanes)),
            each((rows, 3 * cols)),
            each((rows, cols)),
            each((rows, heads)),
            whole((rows, 1)),
            whole((rows // tile, 1, tile)),
        ],
        out_specs=[each((rows, 3 * cols)), each((2, cols))],
        out_shape=[
            jax.ShapeDtypeStruct((slots, rows, 3 * cols), BF16),
            jax.ShapeDtypeStruct((slots, 2, cols), F32),
        ],
        scratch_shapes=[
            pltpu.VMEM((rows, cols), BF16),
            pltpu.VMEM((rows, DH), F32),
            pltpu.VMEM((rows, DH), F32),
        ],
        cost_estimate=pl.CostEstimate(
            flops=slots * (2 * rows * width * cols + 10 * rows * rows * 256 * heads),
            bytes_accessed=slots * width * lanes * 2 + rows * width * 10,
            transcendentals=slots * heads * rows * rows,
        ),
        name="attend_back",
    )(residual_half, weights, qkv, context, inverse, segments[:, None], segments.reshape(-1, 1, tile))


def plain_layer(shards, vectors, to_slot, from_slot, block_input, cotangent, gains, shifts, segments, owned, cols, units, parts):
    width, rows = block_input.shape[2], segments.shape[0]
    slots, slot = lax.axis_size("slot"), lax.axis_index("slot")
    main_units, in_lanes = shards[1].shape[1], 3 * cols
    rest = units - main_units
    spare = shards[0].shape[1] - in_lanes - cols - 2 * rest
    small_all, up_main, down_main = gather_weights(shards)
    vec_all = lax.all_gather(vectors, "slot", axis=0)
    grad_rows = jnp.where(owned[:, None], to_slot(cotangent), 0)
    upstream = grad_rows.astype(F32)
    x_float = to_slot(block_input).astype(F32)
    first_out, first_scaled, first_factor = norm_forward(x_float, gains[0], shifts[0])
    first_norm = first_out.astype(BF16)
    bias = vec_all[:, :1, :in_lanes].astype(F32) + vec_all[:, 1:2, :in_lanes].astype(F32)
    qkv, context, inverse, attention_part = attend(first_norm, small_all, bias, segments, cols, rows // 2)
    residual = x_float + part_sum(attention_part, parts) + shifts[2]
    second_out, second_scaled, second_factor = norm_forward(residual, gains[1], shifts[1])
    second_norm = second_out.astype(BF16)
    small_blocks = list(small_all)
    unit_all = vec_all[:, 2, :units].astype(F32)
    at = in_lanes + cols
    ups = list(up_main) + [b[:, at : at + rest] for b in small_blocks]
    downs = list(down_main) + [b[:, at + rest : at + 2 * rest] for b in small_blocks]
    unit_rows = list(unit_all[:, :main_units]) + list(unit_all[:, main_units:])
    pre_acts = [dot_nn(second_norm, w) + b for w, b in zip(ups, unit_rows)]
    hiddens = [gelu(p).astype(BF16) for p in pre_acts]
    output = (residual + part_sum(sum_products(hiddens, downs), parts) + shifts[3]).astype(BF16)
    down_sums = [dot_tn(grad_rows, h).astype(BF16) for h in hiddens]
    pre_grads = [gelu_back(p, dot_nn(grad_rows, w)) for p, w in zip(pre_acts, downs)]
    pre_halves = [p.astype(BF16) for p in pre_grads]
    unit_sums = [jnp.sum(p, axis=0) for p in pre_grads]
    up_sums = [dot_tn(second_norm, p).astype(BF16) for p in pre_halves]
    second_grad = part_sum(sum_products(pre_halves, ups), parts)
    residual_grad = upstream + norm_backward(second_grad, second_scaled, second_factor, gains[1])
    residual_half = residual_grad.astype(BF16)
    triple, bias_sum = attend_back(residual_half, small_all, qkv, context, inverse, segments, cols, rows // 2)
    first_part = sum_products(list(triple), [b[:, :in_lanes] for b in small_blocks])
    first_grad = part_sum(first_part, parts)
    input_grad = residual_grad + norm_backward(first_grad, first_scaled, first_factor, gains[0])
    blank = jnp.zeros((width, spare), BF16)
    small_sums = [
        jnp.concatenate(
            [
                dot_tn(first_norm, triple[s]).astype(BF16),
                dot_tn(residual_half, context[s]).astype(BF16),
                up_sums[slots + s],
                down_sums[slots + s],
                blank,
            ],
            axis=1,
        )
        for s in range(slots)
    ]
    down_grad, up_grad, small_grad = scatter_grads(
        [jnp.stack(down_sums[:slots]), jnp.stack(up_sums[:slots]), jnp.stack(small_sums)]
    )
    rows_sum = jnp.stack(
        [
            jnp.sum(first_grad * first_scaled, axis=0),
            jnp.sum(second_grad * second_scaled, axis=0),
            jnp.sum(first_grad, axis=0),
            jnp.sum(second_grad, axis=0),
            jnp.sum(residual_grad, axis=0),
            jnp.sum(upstream, axis=0),
        ]
    )
    unit_sum = jnp.stack([jnp.concatenate([unit_sums[s], unit_sums[slots + s]]) for s in range(slots)])
    rows_total, bias_total, unit_total = lax.psum((rows_sum, bias_sum, unit_sum), ("slot",) + FSDP)
    bias_grad = lax.dynamic_index_in_dim(bias_total, slot, 0, keepdims=False)
    unit_grad = lax.dynamic_index_in_dim(unit_total, slot, 0, keepdims=False)
    return (
        from_slot(output, owned), from_slot(input_grad.astype(BF16), owned), rows_total, bias_grad, unit_grad,
        down_grad, up_grad, small_grad,
    )


def on_device(
    block_input,
    segment_ids,
    norm_gains,
    row_biases,
    in_projection,
    query_value_bias,
    out_projection,
    up_weight,
    unit_bias,
    down_weight,
    cotangent,
):
    local, rows_each, width = block_input.shape
    rows_mb = segment_ids.shape[1]
    cols = in_projection.shape[2]
    units = up_weight.shape[1]
    shard_rows = up_weight.shape[0]
    slots, parts = lax.axis_size("slot"), lax.axis_size("part")
    slot, part = lax.axis_index("slot"), lax.axis_index("part")
    fsdp_index = lax.axis_index("fy") * lax.axis_size("fx") + lax.axis_index("fx")
    batch, image = slot % local, slot // local
    late = image == 1

    half_rows = rows_mb // IMG_MB
    padding = rows_mb - IMG_MB * IMG
    edge = round_up(max(half_rows - IMG, padding - (half_rows - IMG)), 16)
    tail = round_up(padding, 16)
    rows = round_up(half_rows + edge + tail, 128)
    filler = rows - half_rows - edge - tail
    paired = lax.axis_size("fy") == 2 and lax.axis_size("fx") == 2 and slots == 4 and parts == 2
    paired = paired and shard_rows % 32 == 0 and filler == 0

    def edges(main):
        near = jnp.where(late, main[:edge], main[half_rows - edge :])
        far = main[half_rows - tail :]
        return jnp.concatenate([near, far])

    def to_slot(value):
        mine = lax.dynamic_index_in_dim(value, batch, 0, keepdims=False)
        send = lax.dynamic_index_in_dim(value, 1 - batch, 0, keepdims=False)
        other = slot_swap(send, 1, slots)
        pair = jnp.where(batch == 0, jnp.stack([mine, other]), jnp.stack([other, mine]))
        main = part_gather(pair, parts).swapaxes(0, 1).reshape(half_rows, width)
        beyond = slot_swap(edges(main), local, slots)
        return jnp.concatenate([main, beyond, jnp.zeros((filler, width), value.dtype)])

    def from_slot(value, owned):
        main = value[:half_rows]
        beyond = slot_swap(value[half_rows : half_rows + edge + tail], local, slots)
        keep = owned[:half_rows, None]
        near, far = beyond[:edge], beyond[edge:]
        blank = lambda count: jnp.zeros((count, width), value.dtype)
        early_fill = jnp.concatenate([blank(half_rows - edge), near])
        late_fill = jnp.concatenate([near, blank(half_rows - edge - tail), far])
        main = jnp.where(keep, main, jnp.where(late, late_fill, early_fill))
        main = main.reshape(local, parts, rows_each, width)
        mine = lax.dynamic_index_in_dim(main, part, 1, keepdims=False)
        stay = lax.dynamic_index_in_dim(mine, batch, 0, keepdims=False)
        other = slot_swap(lax.dynamic_index_in_dim(mine, 1 - batch, 0, keepdims=False), 1, slots)
        return jnp.where(batch == 0, jnp.stack([stay, other]), jnp.stack([other, stay]))

    ids = jnp.where(batch == 0, segment_ids[:1], segment_ids[1:])
    filler_ids = lambda count: jnp.full((1, count), -2, jnp.int32)
    early_ids = jnp.concatenate([ids[:, : half_rows + edge], ids[:, rows_mb - tail :], filler_ids(filler)], axis=1)
    late_ids = jnp.concatenate(
        [ids[:, half_rows:], ids[:, half_rows - edge : half_rows], filler_ids(tail + filler)], axis=1
    )
    segr = jnp.where(late, late_ids, early_ids)
    segc = segr.reshape(rows, 1)

    main_units = units // 128 * 128
    rest = units - main_units
    in_lanes = 3 * cols
    small = in_lanes + cols + 2 * rest
    lanes = round_up(small, 128)
    gains, shifts = norm_gains, row_biases
    if paired:
        (
            small_all, up_main, down_main, gd, x_half, cot, first_norm, qkv, context, inverse, residual, second_norm,
            hidden, slope, hidden_rest, slope_rest, rest_up, rest_down,
        ) = forward_stage(
            (in_projection.swapaxes(1, 2), out_projection, up_weight, down_weight.T), (query_value_bias, unit_bias.reshape(1, units)),
            block_input, cotangent, gains, shifts, segc, segr, cols, units, lanes, edge, tail,
        )
        gu, down_sum, rest_sums, residual_half, residual_grad, y_rows, sums, unit_sums, unit_rest_sums = middle_stage(
            down_main, up_main, gd, hidden, slope, hidden_rest, slope_rest, rest_up, rest_down, cot, second_norm, residual,
            gains, shifts, cols, rest, lanes - small,
        )
        in_grad, out_grad, up_grad, down_grad, input_grad, output, gain_grad, shift_grad, bias_grad, unit_grad = backward_stage(
            small_all, gu, rest_sums, residual_half, first_norm, qkv, context, inverse, segc, segr, x_half, residual_grad,
            y_rows, gains, down_sum, sums, unit_sums, unit_rest_sums, cols, rest, edge, tail, rows_each,
        )
        unit_grad = unit_grad.reshape(units)
        in_grad, down_grad = in_grad.swapaxes(1, 2), down_grad.T
    else:
        segments = segc[:, 0]
        image_id = (fsdp_index * local + batch) * IMG_MB + image
        owned = (segments == image_id) | (jnp.logical_not(late) & (segments == -1))
        down_t = down_weight.T
        small_shard = jnp.concatenate(
            [
                in_projection.transpose(1, 0, 2).reshape(shard_rows, in_lanes),
                out_projection.T,
                up_weight[:, main_units:],
                down_t[:, main_units:],
                jnp.zeros((shard_rows, lanes - small), BF16),
            ],
            axis=1,
        )
        shards = [small_shard, up_weight[:, :main_units], down_t[:, :main_units]]
        triple_bias = jnp.concatenate([query_value_bias[0], jnp.zeros((cols,), F32), query_value_bias[1]])
        high = triple_bias.astype(BF16)
        low = (triple_bias - high.astype(F32)).astype(BF16)
        wide = round_up(max(in_lanes, units), 128)
        vectors = [jnp.pad(v, (0, wide - v.shape[0])) for v in (high, low, unit_bias)]
        vectors = jnp.concatenate([jnp.stack(vectors), jnp.zeros((13, wide), BF16)])
        output, input_grad, rows_total, bias_grad, unit_grad, down_grad, up_grad, small_grad = plain_layer(
            shards, vectors, to_slot, from_slot, block_input, cotangent, gains, shifts, segments, owned, cols, units, parts
        )
        in_grad = small_grad[:, :in_lanes].reshape(shard_rows, 3, cols).transpose(1, 0, 2)
        out_grad = small_grad[:, in_lanes : in_lanes + cols].T
        at = in_lanes + cols
        up_grad = jnp.concatenate([up_grad, small_grad[:, at : at + rest]], axis=1)
        down_grad = jnp.concatenate([down_grad, small_grad[:, at + rest : at + 2 * rest]], axis=1).T
        gain_grad, shift_grad = rows_total[:2], rows_total[2:]
    return (
        output,
        input_grad.astype(F32),
        gain_grad,
        shift_grad,
        in_grad,
        bias_grad,
        out_grad,
        up_grad,
        unit_grad,
        down_grad,
    )


def solution(mesh):
    fsdp, tensor = mesh.shape["fsdp"], mesh.shape["tensor"]

    def layer(*arrays):
        local = arrays[0].shape[0] // fsdp
        slots = local * IMG_MB
        assert local == 2 and slots == 4 and tensor % slots == 0 and fsdp % 2 == 0
        grid = Mesh(
            mesh.devices.reshape(fsdp // 2, 2, slots, tensor // slots), ("fy", "fx", "slot", "part")
        )
        tens = ("slot", "part")
        return jax.shard_map(
            on_device,
            mesh=grid,
            in_specs=(
                P(FSDP, tens, None),
                P(FSDP, None),
                P(),
                P(),
                P(None, FSDP, tens),
                P(None, tens),
                P(tens, FSDP),
                P(FSDP, tens),
                P(tens),
                P(tens, FSDP),
                P(FSDP, tens, None),
            ),
            out_specs=(
                P(FSDP, tens, None),
                P(FSDP, tens, None),
                P(),
                P(),
                P(None, FSDP, tens),
                P(None, tens),
                P(tens, FSDP),
                P(FSDP, tens),
                P(tens),
                P(tens, FSDP),
            ),
            check_vma=False,
        )(*arrays)

    return layer
```

```python
import functools
import math

import jax
import jax.numpy as jnp
from jax import lax
from jax.experimental import pallas as pl
from jax.experimental.pallas import tpu as pltpu
from jax.sharding import Mesh
from jax.sharding import PartitionSpec as P

DH = 72
IMG = 729
IMG_MB = 2
EPS = 1e-06
GELU_C = 0.7978845608028654
F32 = jnp.float32
BF16 = jnp.bfloat16
FSDP = ("fy", "fx")
SCALE = DH ** (-0.5)
LOG2E = math.log2(math.e)


def norm_forward(values, norm_gain, norm_shift):
    center = values - jnp.mean(values, axis=-1, keepdims=True)
    factor = lax.rsqrt(jnp.mean(center * center, axis=-1, keepdims=True) + EPS)
    scaled = center * factor
    return (scaled * norm_gain + norm_shift, scaled, factor)


def norm_backward(upstream, scaled, factor, norm_gain):
    inside = upstream * norm_gain
    return factor * (
        inside
        - jnp.mean(inside, axis=-1, keepdims=True)
        - scaled * jnp.mean(inside * scaled, axis=-1, keepdims=True)
    )


def gelu(pre_act):
    return (
        0.5
        * pre_act
        * (1.0 + jnp.tanh(GELU_C * (pre_act + 0.044715 * pre_act * pre_act * pre_act)))
    )


def gelu_both(pre_act):
    square = pre_act * pre_act
    curve = jnp.tanh(GELU_C * pre_act * (1.0 + 0.044715 * square))
    rise = 0.5 * (1.0 + curve)
    slope = rise + 0.5 * pre_act * (1.0 - curve * curve) * GELU_C * (1.0 + 3.0 * 0.044715 * square)
    return pre_act * rise, slope


def gelu_back(pre_act, upstream):
    return jax.vjp(gelu, pre_act)[1](upstream)[0]


def dot_nn(left, right):
    return lax.dot_general(left, right, (((1,), (0,)), ((), ())), preferred_element_type=F32)


def dot_nt(left, right):
    return lax.dot_general(left, right, (((1,), (1,)), ((), ())), preferred_element_type=F32)


def dot_tn(left, right):
    return lax.dot_general(left, right, (((0,), (0,)), ((), ())), preferred_element_type=F32)


def sum_products(lefts, rights):
    total = dot_nt(lefts[0], rights[0])
    for left, right in zip(lefts[1:], rights[1:]):
        total = total + dot_nt(left, right)
    return total


def round_up(value, unit):
    return -(-value // unit) * unit


def swap(value, axis):
    return lax.ppermute(value, axis, [(0, 1), (1, 0)])


def slot_swap(value, stride, slots):
    return lax.ppermute(value, "slot", [(s, s ^ stride) for s in range(slots)])


def part_sum(value, parts):
    value = value.astype(BF16)
    if parts == 2:
        return value.astype(F32) + swap(value, "part").astype(F32)
    return lax.psum(value.astype(F32), "part")


def part_gather(value, parts):
    if parts == 2:
        other = swap(value, "part")
        first = lax.axis_index("part") == 0
        return jnp.stack([jnp.where(first, value, other), jnp.where(first, other, value)])
    return lax.all_gather(value, "part", axis=0)


def add_half(left, right):
    return (left.astype(F32) + right.astype(F32)).astype(BF16)


MESH = pl.DeviceIdType.MESH


class Place:
    def __init__(self):
        self.y, self.x = lax.axis_index("fy"), lax.axis_index("fx")
        self.z = lax.axis_index("slot")
        self.f = 2 * self.y + self.x
        self.across_x, self.across_y = {"fx": 1 - self.x}, {"fy": 1 - self.y}
        self.c = lax.axis_index("part")
        self.above = {"slot": jnp.minimum(self.z + 1, 3)}
        self.below = {"slot": jnp.maximum(self.z - 1, 0)}
        self.batch, self.image = self.z % 2, self.z // 2
        self.mate = {"part": 1 - self.c}
        self.pair = {"slot": self.z + 1 - 2 * self.batch}
        self.cross = {"slot": self.z + 2 - 4 * self.image}

    def owned(self, segments):
        mine = segments == (self.f * 2 + self.batch) * IMG_MB + self.image
        return mine | ((segments == -1) & (self.image == 0))

    def behind(self):
        return jnp.where((self.z == 1) | (self.z == 2), 1, 0)

    def slot_after(self, d):
        return {"slot": (self.z + d) % 4}

    def barrier(self):
        sem = pltpu.get_barrier_semaphore()
        others = [self.across_x, self.across_y, self.mate] + [self.slot_after(d) for d in (1, 2, 3)]
        for device in others:
            pl.semaphore_signal(sem, inc=1, device_id=device, device_id_type=MESH)
        pl.semaphore_wait(sem, len(others))

    def far_first(self, i):
        low = self.z < 2
        near = jnp.where(low, self.z, 3 - self.z)
        at = jnp.where(i == 0, 3, jnp.where(i == 1, 2, jnp.where(i == 2, 1 - near, near)))
        return jnp.where(low, at, 3 - at)


def send(src, dst, send_sem, recv_sem, device):
    return pltpu.make_async_remote_copy(
        src_ref=src, dst_ref=dst, send_sem=send_sem, recv_sem=recv_sem, device_id=device, device_id_type=MESH
    )


class Gather:
    SEMS = 11

    def __init__(self, place, shards, w, sems, local_sem, rows):
        self.p, self.shards, self.w, self.rows = place, shards, w, rows
        (self.zr, self.zu, self.zd, self.xr, self.xs, self.yr, self.ys, self.ar, self.asn, self.br, self.bs) = sems
        self.local_sem = local_sem

    def block(self, k, slot, owner, half=None):
        at, count = owner * self.rows, self.rows
        if half is not None:
            count = count // 2
            at = at + half * count
        return self.w[k].at[slot, pl.ds(pl.multiple_of(at, 16), count), :]

    def mine(self, k, slot, shard):
        return self.shards[k] if shard else self.block(k, slot, self.p.f)

    def up(self, k, slot, shard=False):
        dst = self.block(k, slot, self.p.f)
        return send(self.mine(k, slot, shard), dst, self.zu.at[k, slot], self.zr.at[k, slot], self.p.above)

    def down(self, k, slot, shard=False):
        dst = self.block(k, slot, self.p.f)
        return send(self.mine(k, slot, shard), dst, self.zd.at[k, slot], self.zr.at[k, slot], self.p.below)

    def to_x(self, k, slot, shard=False):
        dst = self.block(k, slot, self.p.f)
        return send(self.mine(k, slot, shard), dst, self.xs.at[k, slot], self.xr.at[k, slot], self.p.across_x)

    def to_y(self, k, slot, shard=False):
        dst = self.block(k, slot, self.p.f)
        return send(self.mine(k, slot, shard), dst, self.ys.at[k, slot], self.yr.at[k, slot], self.p.across_y)

    def from_x(self, k, slot):
        ref = self.block(k, slot, self.p.f ^ 1)
        return send(ref, ref, self.xs.at[k, slot], self.xr.at[k, slot], self.p.across_x)

    def from_y(self, k, slot):
        ref = self.block(k, slot, self.p.f ^ 2)
        return send(ref, ref, self.ys.at[k, slot], self.yr.at[k, slot], self.p.across_y)

    def corner_y(self, k, slot):
        ref = self.block(k, slot, self.p.f ^ 1, 0)
        return send(ref, ref, self.asn.at[k, slot], self.ar.at[k, slot], self.p.across_y)

    def corner_x(self, k, slot):
        ref = self.block(k, slot, self.p.f ^ 2, 1)
        return send(ref, ref, self.bs.at[k, slot], self.br.at[k, slot], self.p.across_x)

    def wait_corner(self, k, slot):
        ref = self.block(k, slot, self.p.f ^ 3, 0)
        send(ref, ref, self.asn.at[k, slot], self.ar.at[k, slot], self.p.across_y).wait_recv()
        ref = self.block(k, slot, self.p.f ^ 3, 1)
        send(ref, ref, self.bs.at[k, slot], self.br.at[k, slot], self.p.across_x).wait_recv()

    def local(self, k):
        return pltpu.make_async_copy(self.shards[k], self.block(k, self.p.z, self.p.f), self.local_sem.at[k])

    def start_z(self, k):
        @pl.when(self.p.z < 3)
        def _():
            self.up(k, self.p.z, True).start()

        @pl.when(self.p.z > 0)
        def _():
            self.down(k, self.p.z, True).start()

    def start_xy(self, k):
        self.to_x(k, self.p.z, True).start()
        self.to_y(k, self.p.z, True).start()
        self.local(k).start()

    def pass_on(self, k, d):
        z = self.p.z

        @pl.when(z >= d)
        def _():
            self.up(k, z - d).wait_recv()

            @pl.when(z < 3)
            def _():
                self.up(k, z - d).start()

            self.to_x(k, z - d).start()
            self.to_y(k, z - d).start()

        @pl.when(z + d <= 3)
        def _():
            self.down(k, z + d).wait_recv()

            @pl.when(z > 0)
            def _():
                self.down(k, z + d).start()

            self.to_x(k, z + d).start()
            self.to_y(k, z + d).start()

    def corner(self, k, d):
        def one(slot):
            self.from_x(k, slot).wait_recv()
            self.corner_y(k, slot).start()
            self.from_y(k, slot).wait_recv()
            self.corner_x(k, slot).start()

        z = self.p.z
        if d == 0:
            one(z)
        else:
            pl.when(z >= d)(lambda: one(z - d))
            pl.when(z + d <= 3)(lambda: one(z + d))

    def arrive(self, k):
        self.local(k).wait()
        for slot in range(4):
            self.wait_corner(k, slot)

    def drain(self, k):
        z = self.p.z
        for slot in range(4):
            self.to_x(k, slot).wait_send()
            self.to_y(k, slot).wait_send()
            self.corner_y(k, slot).wait_send()
            self.corner_x(k, slot).wait_send()

            @pl.when((z < 3) & (slot <= z))
            def _(slot=slot):
                self.up(k, slot).wait_send()

            @pl.when((z > 0) & (slot >= z))
            def _(slot=slot):
                self.down(k, slot).wait_send()


def gather_weights(shards):
    slots = lax.axis_size("slot")
    whole = [lax.all_gather(s, ("slot",) + FSDP, axis=0) for s in shards]
    return [w.reshape(slots, -1, w.shape[-1]) for w in whole]


class Rows:
    SEMS = 11

    def __init__(self, place, index, src, dst, sems, rows_each, edge, tail):
        self.p, self.src, self.dst, self.each = place, src, dst, rows_each
        self.half = 4 * rows_each
        self.edge, self.tail = edge, tail
        self.sems = [sem.at[index] for sem in sems]

    def at(self, row, count):
        return self.dst.at[pl.ds(pl.multiple_of(row, 16), count), :]

    def block(self, near, core):
        batch = self.p.batch if near else 1 - self.p.batch
        return self.at((2 * batch + core) * self.each, self.each)

    def own(self):
        return pltpu.make_async_copy(self.src.at[self.p.batch], self.block(True, self.p.c), self.sems[0])

    def to_mate(self):
        return send(self.src.at[self.p.batch], self.block(True, self.p.c), self.sems[1], self.sems[2], self.p.mate)

    def to_pair(self):
        return send(self.src.at[1 - self.p.batch], self.block(True, self.p.c), self.sems[3], self.sems[4], self.p.pair)

    def pass_on(self):
        ref = self.block(False, self.p.c)
        return send(ref, ref, self.sems[5], self.sems[6], self.p.mate)

    def edge_out(self):
        src = self.at(jnp.where(self.p.image == 0, self.half - self.edge, 0), self.edge)
        return send(src, self.at(self.half, self.edge), self.sems[7], self.sems[8], self.p.cross)

    def tail_out(self):
        src = self.at(self.half - self.tail, self.tail)
        dst = self.at(self.half + self.edge, self.tail)
        return send(src, dst, self.sems[7], self.sems[8], self.p.cross)

    def edge_mate(self):
        ref = self.at(self.half, self.edge)
        return send(ref, ref, self.sems[9], self.sems[10], self.p.mate)

    def tail_mate(self):
        ref = self.at(self.half + self.edge, self.tail)
        return send(ref, ref, self.sems[9], self.sems[10], self.p.mate)

    def start(self):
        self.to_pair().start()
        self.to_mate().start()
        self.own().start()

    def forward(self):
        ref = self.block(False, self.p.c)
        send(ref, ref, self.sems[3], self.sems[4], self.p.pair).wait_recv()
        self.pass_on().start()

    def main_ready(self):
        self.own().wait()
        ref = self.block(True, 1 - self.p.c)
        send(ref, ref, self.sems[1], self.sems[2], self.p.mate).wait_recv()
        ref = self.block(False, 1 - self.p.c)
        send(ref, ref, self.sems[5], self.sems[6], self.p.mate).wait_recv()

    def edges(self):
        pl.when(self.p.c == 0)(lambda: self.edge_out().start())
        pl.when(self.p.c == 1)(lambda: self.tail_out().start())

    def edges_forward(self):
        @pl.when(self.p.c == 0)
        def _():
            self.edge_out().wait_recv()
            self.edge_mate().start()

        @pl.when(self.p.c == 1)
        def _():
            self.tail_out().wait_recv()
            self.tail_mate().start()

    def edges_ready(self):
        pl.when(self.p.c == 0)(lambda: self.tail_mate().wait_recv())
        pl.when(self.p.c == 1)(lambda: self.edge_mate().wait_recv())

    def drain(self):
        self.to_mate().wait_send()
        self.to_pair().wait_send()
        self.pass_on().wait_send()

        @pl.when(self.p.c == 0)
        def _():
            self.edge_out().wait_send()
            self.edge_mate().wait_send()

        @pl.when(self.p.c == 1)
        def _():
            self.tail_out().wait_send()
            self.tail_mate().wait_send()


def row_tiles(rows, step, body):
    def one(t, carry):
        body(pl.ds(pl.multiple_of(t * step, 16), step))
        return carry

    lax.fori_loop(0, rows // step, one, 0)


def forward_kernel(*refs, cols, unit_rest, edge, tail, tile):
    (in_ref, out_ref, up_whole, down_whole, qv_ref, unit_ref, x_src, c_src, gain_ref, shift_ref, segc_ref) = refs[:11]
    segr_ref, refs = refs[11], refs[1:]
    (ws, wu, wd, gd) = refs[11:15]
    outs, refs = refs[15:29], refs[29:]
    held, refs = refs[:14], refs[14:]
    (x_ref, c_ref, first_ref, qkv_ref, ctx_ref, inv_ref, res_ref, second_ref) = held[:8]
    (hidden_ref, slope_ref, hidden_rest, slope_rest, rest_up, rest_down) = held[8:]
    (blocks, unit_blocks, grads, part, part_out, part_in, bias_rest, vec_all) = refs[:8]
    (small_ref, up_ref, down_ref, vec_ref) = refs[8:12]
    gather_sems, local_sem = refs[12 : 12 + Gather.SEMS], refs[12 + Gather.SEMS]
    tail_refs = refs[13 + Gather.SEMS :]
    row_sems = tail_refs[: Rows.SEMS]
    (vec_s, vec_r, load_sem, part_s, part_r, unit_sem, grad_sem, out_sem) = tail_refs[Rows.SEMS :]

    def leave(n):
        return pltpu.make_async_copy(held[n], outs[n], out_sem.at[n])

    main, rest = up_ref.shape[1], unit_rest
    rows, width = x_ref.shape
    place = Place()
    for n in range(3):
        small_ref[:, n * cols : (n + 1) * cols] = in_ref[n].T
    at = 3 * cols
    small_ref[:, at : at + cols] = out_ref[...].T
    at = at + cols
    small_ref[:, at : at + rest] = up_whole[:, main:]
    small_ref[:, at + rest : at + 2 * rest] = down_whole[:, main:]
    at = at + 2 * rest
    if at < small_ref.shape[1]:
        small_ref[:, at:] = jnp.zeros((small_ref.shape[0], small_ref.shape[1] - at), BF16)
    vec_ref[...] = jnp.zeros_like(vec_ref)
    for n in (0, 1):
        high = qv_ref[n : n + 1, :].astype(BF16)
        lo = 2 * n * cols
        vec_ref[0:1, lo : lo + cols] = high
        vec_ref[1:2, lo : lo + cols] = (qv_ref[n : n + 1, :] - high.astype(F32)).astype(BF16)
    vec_ref[2:3, : main + rest] = unit_ref[...].reshape(1, main + rest)
    place.barrier()
    shards = (small_ref, up_ref, down_ref)
    g = Gather(place, shards, (ws, wu, wd), gather_sems, local_sem, small_ref.shape[0])
    each = x_src.shape[1]
    x_rows = Rows(place, 0, x_src, x_ref, row_sems, each, edge, tail)
    c_rows = Rows(place, 1, c_src, c_ref, row_sems, each, edge, tail)

    def vec_to(d):
        device = place.slot_after(d)
        return send(vec_ref, vec_all.at[place.z], vec_s.at[d], vec_r.at[d], device)

    def vec_from(d):
        ref = vec_all.at[(place.z + 4 - d) % 4]
        return send(ref, ref, vec_s.at[d], vec_r.at[d], place.slot_after(d))

    g.start_z(0)
    g.start_xy(0)
    for d in (1, 2, 3):
        vec_to(d).start()
    x_rows.start()
    vec_all[place.z] = vec_ref[...]
    up_ref[...] = up_whole[:, :main]
    down_ref[...] = down_whole[:, :main]
    g.pass_on(0, 1)
    g.corner(0, 0)
    x_rows.forward()
    g.pass_on(0, 2)
    x_rows.main_ready()
    x_rows.edges()
    g.corner(0, 1)
    x_rows.edges_forward()
    g.pass_on(0, 3)
    g.start_z(1)
    x_rows.edges_ready()

    def first(span):
        value = x_ref[span, :].astype(F32)
        out, _, _ = norm_forward(value, gain_ref[0:1, :], shift_ref[0:1, :])
        first_ref[span, :] = out.astype(BF16)

    row_tiles(rows, 128, first)
    leave(0).start()
    g.corner(0, 2)
    g.corner(0, 3)
    leave(2).start()
    for d in (1, 2, 3):
        vec_from(d).wait_recv()
    g.arrive(0)

    later = []
    for k in (1, 2):
        later.append(lambda k=k: g.start_xy(k))
        if k == 1:
            later.append(lambda: c_rows.start())
        for d in (1, 2, 3):
            later.append(lambda k=k, d=d: g.pass_on(k, d))
            later.append(lambda k=k, d=d: g.corner(k, d - 1))
        if k == 1:
            later.append(lambda: g.start_z(2))
            later.append(lambda: c_rows.forward())
            later.append(lambda: (c_rows.main_ready(), c_rows.edges()))
        later.append(lambda k=k: g.corner(k, 3))
        if k == 1:
            later.append(lambda: c_rows.edges_forward())

    def step(count=1):
        for _ in range(count):
            if later:
                later.pop(0)()

    step(2)

    def load(s):
        return pltpu.make_async_copy(ws.at[s], blocks.at[s % 2], load_sem.at[s % 2])

    heads = cols // DH
    rest_up[...] = jnp.zeros_like(rest_up)
    rest_down[...] = jnp.zeros_like(rest_down)
    bias_rest[...] = jnp.zeros_like(bias_rest)
    part[...] = jnp.zeros_like(part)
    load(0).start()
    points = 1 + heads
    inside = [later.pop(0) for _ in range(4 * points)]

    def at_point(s, n):
        for one in range(4):
            pl.when(s == one)(lambda one=one: inside[one * points + n]() and None)

    def one_slot(s, carry):
        load(s).wait()
        pl.when(s < 3)(lambda: load(s + 1).start())
        w = blocks.at[s % 2]
        bias = vec_all[s, 0:1, : 3 * cols].astype(F32) + vec_all[s, 1:2, : 3 * cols].astype(F32)
        projected = dot_nn(first_ref[...], w[:, : 3 * cols]) + bias
        qkv_ref[s] = projected.astype(BF16)
        at_point(s, 0)
        for head in range(heads):
            attend_head(qkv_ref, ctx_ref, inv_ref, segc_ref, segr_ref, s, head, cols, tile)
            at_point(s, 1 + head)
        part[...] += dot_nt(ctx_ref[s], w[:, 3 * cols : 4 * cols])
        at = 4 * cols
        for one in range(4):

            @pl.when(s == one)
            def _(one=one):
                rest_up[:, one * rest : (one + 1) * rest] = w[:, at : at + rest]
                rest_down[:, one * rest : (one + 1) * rest] = w[:, at + rest : at + 2 * rest]
                bias_rest[:, one * rest : (one + 1) * rest] = vec_all[one, 2:3, main : main + rest].astype(F32)

        return carry

    lax.fori_loop(0, 4, one_slot, 0)

    def halves(h):
        return pl.ds(h * (rows // 2), rows // 2)

    def exchange(h):
        src, dst = part_out.at[halves(h), :], part_in.at[halves(h), :]
        return send(src, dst, part_s.at[h], part_r.at[h], place.mate)

    for h in (0, 1):
        part_out[halves(h), :] = part[halves(h), :].astype(BF16)
        exchange(h).start()
    step()
    for n in (3, 4, 5, 12, 13):
        leave(n).start()
    for h in (0, 1):
        exchange(h).wait_recv()

    def second(span):
        value = x_ref[span, :].astype(F32) + (part_out[span, :].astype(F32) + part_in[span, :].astype(F32))
        value = value + shift_ref[2:3, :]
        res_ref[span, :] = value
        out, _, _ = norm_forward(value, gain_ref[1:2, :], shift_ref[1:2, :])
        second_ref[span, :] = out.astype(BF16)

    row_tiles(rows, 128, second)
    g.arrive(1)

    def unit_load(s):
        return pltpu.make_async_copy(wu.at[s], unit_blocks.at[s % 2], unit_sem.at[s % 2])

    unit_load(0).start()
    passing = [later.pop(0) for _ in range(4)]

    def one_block(s, carry):
        unit_load(s).wait()
        pl.when(s < 3)(lambda: unit_load(s + 1).start())
        bias = vec_all[s, 2:3, :main].astype(F32)

        def units(span):
            hidden, slope = gelu_both(dot_nn(second_ref[span, :], unit_blocks[s % 2]) + bias)
            hidden_ref[s, span, :] = hidden.astype(BF16)
            slope_ref[s, span, :] = slope.astype(BF16)

        row_tiles(rows, tile, units)
        for one in range(4):
            pl.when(s == one)(lambda one=one: passing[one]() and None)
        return carry

    lax.fori_loop(0, 4, one_block, 0)

    def units_rest(span):
        hidden, slope = gelu_both(dot_nn(second_ref[span, :], rest_up[...]) + bias_rest[...])
        hidden_rest[span, :] = hidden.astype(BF16)
        slope_rest[span, :] = slope.astype(BF16)

    for n in (6, 7):
        leave(n).start()
    row_tiles(rows, tile, units_rest)
    step()
    for n in (8, 9, 10, 11):
        leave(n).start()
    c_rows.edges_ready()
    c_rows.drain()
    c_ref[...] = jnp.where(place.owned(segc_ref[...]), c_ref[...], jnp.zeros_like(c_ref))

    def grad_out(s):
        return pltpu.make_async_copy(grads.at[s % 2], gd.at[s], grad_sem.at[s % 2])

    def down_grad(s, carry):
        pl.when(s >= 2)(lambda: grad_out(s - 2).wait())
        grads[s % 2] = dot_tn(c_ref[...], hidden_ref[s]).astype(BF16)
        grad_out(s).start()
        return carry

    lax.fori_loop(0, 2, down_grad, 0)
    step()
    lax.fori_loop(2, 4, down_grad, 0)
    step(len(later))
    leave(1).start()
    for s in (2, 3):
        grad_out(s).wait()
    g.arrive(2)
    for n in range(14):
        leave(n).wait()
    for k in (0, 1, 2):
        g.drain(k)
    x_rows.drain()
    for d in (1, 2, 3):
        vec_to(d).wait_send()
    for h in (0, 1):
        exchange(h).wait_send()


def forward_stage(
    weights, biases, x_src, c_src, gains, shifts, segc, segr, cols, units, lanes, edge, tail
):
    rows, width, shard_rows, main = segc.shape[0], x_src.shape[2], weights[2].shape[0], units // 128 * 128
    unit_rest = units - main
    heads, rest_lanes = cols // DH, round_up(4 * unit_rest, 128)
    vectors = (16, round_up(max(3 * cols, units), 128))
    vmem = pl.BlockSpec(memory_space=pltpu.VMEM)
    far = pl.BlockSpec(memory_space=pl.ANY)
    shape = jax.ShapeDtypeStruct
    dma = pltpu.SemaphoreType.DMA
    return pl.pallas_call(
        functools.partial(forward_kernel, cols=cols, unit_rest=unit_rest, edge=edge, tail=tail, tile=rows // 2),
        in_specs=[vmem] * 12,
        out_specs=[far] * 18,
        out_shape=[
            shape((4, width, lanes), BF16),
            shape((4, width, main), BF16),
            shape((4, width, main), BF16),
            shape((4, width, main), BF16),
            shape((rows, width), BF16),
            shape((rows, width), BF16),
            shape((rows, width), BF16),
            shape((4, rows, 3 * cols), BF16),
            shape((4, rows, cols), BF16),
            shape((4, rows, heads), F32),
            shape((rows, width), F32),
            shape((rows, width), BF16),
            shape((4, rows, main), BF16),
            shape((4, rows, main), BF16),
            shape((rows, rest_lanes), BF16),
            shape((rows, rest_lanes), BF16),
            shape((width, rest_lanes), BF16),
            shape((width, rest_lanes), BF16),
        ],
        scratch_shapes=[
            pltpu.VMEM((rows, width), BF16),
            pltpu.VMEM((rows, width), BF16),
            pltpu.VMEM((rows, width), BF16),
            pltpu.VMEM((4, rows, 3 * cols), BF16),
            pltpu.VMEM((4, rows, cols), BF16),
            pltpu.VMEM((4, rows, heads), F32),
            pltpu.VMEM((rows, width), F32),
            pltpu.VMEM((rows, width), BF16),
            pltpu.VMEM((4, rows, main), BF16),
            pltpu.VMEM((4, rows, main), BF16),
            pltpu.VMEM((rows, rest_lanes), BF16),
            pltpu.VMEM((rows, rest_lanes), BF16),
            pltpu.VMEM((width, rest_lanes), BF16),
            pltpu.VMEM((width, rest_lanes), BF16),
            pltpu.VMEM((2, width, lanes), BF16),
            pltpu.VMEM((2, width, main), BF16),
            pltpu.VMEM((2, width, main), BF16),
            pltpu.VMEM((rows, width), F32),
            pltpu.VMEM((rows, width), BF16),
            pltpu.VMEM((rows, width), BF16),
            pltpu.VMEM((1, rest_lanes), F32),
            pltpu.VMEM((4,) + vectors, BF16),
            pltpu.VMEM((shard_rows, lanes), BF16),
            pltpu.VMEM((shard_rows, main), BF16),
            pltpu.VMEM((shard_rows, main), BF16),
            pltpu.VMEM(vectors, BF16),
        ]
        + [dma((3, 4))] * Gather.SEMS
        + [dma((3,))]
        + [dma((2,))] * Rows.SEMS
        + [dma((4,)), dma((4,)), dma((2,)), dma((2,)), dma((2,)), dma((2,)), dma((2,)), dma((14,))],
        compiler_params=pltpu.CompilerParams(collective_id=1, has_side_effects=True, vmem_limit_bytes=64000000),
        name="forward",
    )(*weights, *biases, x_src, c_src, gains, shifts, segc, segr)


def middle_kernel(*refs, cols, unit_rest):
    (wd, wu, gd) = refs[:3]
    (hidden_far, slope_far, hidden_rest, slope_rest, rest_up, rest_down) = refs[3:9]
    (c_far, second_far, res_far, gain_ref, shift_ref) = refs[9:14]
    gu = refs[14]
    (d_out, rest_sums, half_ref, grad_ref, y_ref, sums_ref, unit_ref, unit_rest_ref) = refs[15:23]
    (blocks, grads, pre_half, part, part_out, part_in, part_in2) = refs[23:30]
    (hidden_ref, slope_ref, c_ref, second_ref, res_ref) = refs[30:35]
    d_bufs, d_own = refs[35:40], refs[40:43]
    refs = refs[43:]
    sems, loads = refs[: Reduce.SEMS], refs[Reduce.SEMS : Reduce.SEMS + 3]
    load_sem, grad_sem, part_s, part_r, in_sem, unit_sem = refs[Reduce.SEMS + 3 :]
    rows, width = c_ref.shape
    rest = unit_rest
    place = Place()
    place.barrier()

    def down_final(total):
        d_out[...] = total[...].astype(F32)

    r = Reduce(place, (gd,), (d_own,), (down_final,), (d_bufs,), sems, loads, d_out.shape[0])

    def load(w, slot, buffer):
        return pltpu.make_async_copy(w.at[slot], blocks.at[buffer], load_sem.at[buffer])

    def halves(h):
        return pl.ds(h * (rows // 2), rows // 2)

    def exchange(n, h):
        dst = (part_in, part_in2)[n]
        src, dst = part_out.at[halves(h), :], dst.at[halves(h), :]
        return send(src, dst, part_s.at[n, h], part_r.at[n, h], place.mate)

    def enter(n):
        far, near = ((c_far, c_ref), (second_far, second_ref), (res_far, res_ref))[n]
        return pltpu.make_async_copy(far, near, in_sem.at[n])

    def unit_loads(s):
        return (
            pltpu.make_async_copy(hidden_far.at[s], hidden_ref.at[s % 2], unit_sem.at[0, s % 2]),
            pltpu.make_async_copy(slope_far.at[s], slope_ref.at[s % 2], unit_sem.at[1, s % 2]),
        )

    def start_units(s):
        for copy in unit_loads(s):
            copy.start()

    enter(0).start()
    load(wd, 0, 0).start()
    start_units(0)
    r.start(0)
    enter(1).start()
    enter(2).start()
    enter(0).wait()
    part[...] = dot_nt(hidden_rest[...], rest_down[...])
    grad_rest = slope_rest[...].astype(F32) * dot_nn(c_ref[...], rest_down[...])
    unit_rest_ref[...] = jnp.sum(grad_rest, axis=0, keepdims=True)
    half_rest = grad_rest.astype(BF16)

    def down_block(s, carry):
        load(wd, s, s % 2).wait()
        pl.when(s < 3)(lambda: load(wd, s + 1, (s + 1) % 2).start())
        pl.when(s == 3)(lambda: load(wu, 0, 0).start())
        for copy in unit_loads(s):
            copy.wait()
        pl.when(s < 3)(lambda: start_units(s + 1))
        w = blocks[s % 2]
        part[...] += dot_nt(hidden_ref[s % 2], w)
        grad = slope_ref[s % 2].astype(F32) * dot_nn(c_ref[...], w)
        pre_half[s] = grad.astype(BF16)
        unit_ref[s] = jnp.broadcast_to(jnp.sum(grad, axis=0, keepdims=True), unit_ref.shape[1:])
        r.middle_one(0, s)
        return carry

    lax.fori_loop(0, 4, down_block, 0)
    for h in (0, 1):
        part_out[halves(h), :] = part[halves(h), :].astype(BF16)
        exchange(0, h).start()
    part[...] = dot_nt(half_rest, rest_up[...])

    def up_block(s, carry):
        load(wu, s, s % 2).wait()
        pl.when(s < 3)(lambda: load(wu, s + 1, (s + 1) % 2).start())
        part[...] += dot_nt(pre_half[s], blocks[s % 2])
        return carry

    lax.fori_loop(0, 4, up_block, 0)
    enter(1).wait()
    enter(2).wait()
    for h in (0, 1):
        exchange(0, h).wait_recv()

    def output(span):
        value = part_out[span, :].astype(F32) + part_in[span, :].astype(F32)
        y_ref[span, :] = (res_ref[span, :] + value + shift_ref[3:4, :]).astype(BF16)

    row_tiles(rows, 128, output)
    for h in (0, 1):
        exchange(0, h).wait_send()
        part_out[halves(h), :] = part[halves(h), :].astype(BF16)
        exchange(1, h).start()

    def grad_out(s):
        return pltpu.make_async_copy(grads.at[s % 2], gu.at[s], grad_sem.at[s % 2])

    def up_grad(s, carry):
        pl.when(s >= 2)(lambda: grad_out(s - 2).wait())
        grads[s % 2] = dot_tn(second_ref[...], pre_half[s]).astype(BF16)
        grad_out(s).start()
        n = s - place.behind()
        pl.when((n >= 0) & (n < 3))(lambda: r.line_one(0, n))
        return carry

    lax.fori_loop(0, 4, up_grad, 0)
    up_sum = dot_tn(second_ref[...], half_rest).astype(BF16)
    down_sum = dot_tn(c_ref[...], hidden_rest[...]).astype(BF16)
    rest_sums[...] = jnp.zeros_like(rest_sums)
    for s in range(4):
        rest_sums[s, :, :rest] = up_sum[:, s * rest : (s + 1) * rest]
        rest_sums[s, :, rest : 2 * rest] = down_sum[:, s * rest : (s + 1) * rest]
    for h in (0, 1):
        exchange(1, h).wait_recv()
    sums_ref[...] = jnp.zeros_like(sums_ref)

    def back(span):
        grad = part_out[span, :].astype(F32) + part_in2[span, :].astype(F32)
        upstream = c_ref[span, :].astype(F32)
        _, scaled, factor = norm_forward(res_ref[span, :], gain_ref[1:2, :], shift_ref[1:2, :])
        value = upstream + norm_backward(grad, scaled, factor, gain_ref[1:2, :])
        grad_ref[span, :] = value
        half_ref[span, :] = value.astype(BF16)
        sums_ref[1:2, :] += jnp.sum(grad * scaled, axis=0, keepdims=True)
        sums_ref[3:4, :] += jnp.sum(grad, axis=0, keepdims=True)
        sums_ref[4:5, :] += jnp.sum(value, axis=0, keepdims=True)
        sums_ref[5:6, :] += jnp.sum(upstream, axis=0, keepdims=True)

    row_tiles(rows, 128, back)
    r.line_one(0, 3)
    for s in (2, 3):
        grad_out(s).wait()
    r.drain(0)
    for h in (0, 1):
        exchange(1, h).wait_send()


def middle_stage(
    wd, wu, gd, hidden, slope, hidden_rest, slope_rest, rest_up, rest_down, cot, second, residual, gains, shifts, cols, unit_rest, spare
):
    rows, width = cot.shape
    main, shard_rows = wd.shape[2], width // 4
    vmem = pl.BlockSpec(memory_space=pltpu.VMEM)
    far = pl.BlockSpec(memory_space=pl.ANY)
    shape = jax.ShapeDtypeStruct
    dma = pltpu.SemaphoreType.DMA
    return pl.pallas_call(
        functools.partial(middle_kernel, cols=cols, unit_rest=unit_rest),
        in_specs=[far] * 5 + [vmem] * 4 + [far] * 3 + [vmem] * 2,
        out_specs=[far] + [vmem] * 8,
        out_shape=[
            shape((4, width, main), BF16),
            shape((shard_rows, main), F32),
            shape((4, width, 2 * unit_rest + spare), BF16),
            shape((rows, width), BF16),
            shape((rows, width), F32),
            shape((rows, width), BF16),
            shape((8, width), F32),
            shape((4, 8, main), F32),
            shape((1, rest_up.shape[1]), F32),
        ],
        scratch_shapes=[
            pltpu.VMEM((2, width, main), BF16),
            pltpu.VMEM((2, width, main), BF16),
            pltpu.VMEM((4, rows, main), BF16),
            pltpu.VMEM((rows, width), F32),
            pltpu.VMEM((rows, width), BF16),
            pltpu.VMEM((rows, width), BF16),
            pltpu.VMEM((rows, width), BF16),
            pltpu.VMEM((2, rows, main), BF16),
            pltpu.VMEM((2, rows, main), BF16),
            pltpu.VMEM((rows, width), BF16),
            pltpu.VMEM((rows, width), BF16),
            pltpu.VMEM((rows, width), F32),
        ]
        + reduce_buffers(shard_rows, main)
        + reduce_terms(shard_rows, main)
        + [dma((1, 4))] * Reduce.SEMS
        + [dma((1, 4))] * 3
        + [dma((2,)), dma((2,)), dma((2, 2)), dma((2, 2)), dma((3,)), dma((2, 2))],
        compiler_params=pltpu.CompilerParams(collective_id=3, has_side_effects=True, vmem_limit_bytes=64000000),
        name="middle",
    )(wd, wu, gd, hidden, slope, hidden_rest, slope_rest, rest_up, rest_down, cot, second, residual, gains, shifts)


class Reduce:
    SEMS = 16

    def __init__(self, place, g, own, out, bufs, sems, load_sems, rows):
        self.p, self.g, self.own, self.out, self.rows = place, g, own, out, rows
        self.bufs, self.sems, self.load_sems = bufs, sems, load_sems

    def grad(self, k, slot, owner, half=None):
        at, count = owner * self.rows, self.rows
        if half is not None:
            count = count // 2
            at = at + half * count
        return self.g[k].at[slot, pl.ds(pl.multiple_of(at, 16), count), :]

    def terms(self, k, slot):
        f = self.p.f
        if self.own[k] is None:
            return self.grad(k, slot, f ^ 1, 0), self.grad(k, slot, f ^ 2, 1), self.grad(k, slot, f)
        return tuple(ref.at[slot] for ref in self.own[k])

    def loads(self, k, slot):
        f = self.p.f
        src = self.grad(k, slot, f ^ 1, 0), self.grad(k, slot, f ^ 2, 1), self.grad(k, slot, f)
        pairs = zip(src, self.terms(k, slot), self.load_sems)
        return [pltpu.make_async_copy(one, dst, sem.at[k, slot]) for one, dst, sem in pairs]

    def half(self, ref, slot, half):
        count = self.rows // 2
        return ref.at[slot, half * count : (half + 1) * count, :]

    def copy(self, k, slot, src, dst, index, device):
        return send(src, dst, self.sems[2 * index].at[k, slot], self.sems[2 * index + 1].at[k, slot], device)

    def corner_y(self, k, s):
        return self.copy(k, s, self.grad(k, s, self.p.f ^ 3, 0), self.bufs[k][0].at[s], 0, self.p.across_y)

    def corner_x(self, k, s):
        return self.copy(k, s, self.grad(k, s, self.p.f ^ 3, 1), self.bufs[k][1].at[s], 1, self.p.across_x)

    def x_low(self, k, s):
        return self.copy(k, s, self.bufs[k][0].at[s], self.half(self.bufs[k][2], s, 0), 2, self.p.across_x)

    def x_high(self, k, s):
        dst = self.half(self.bufs[k][2], s, 1)
        return self.copy(k, s, self.grad(k, s, self.p.f ^ 1, 1), dst, 3, self.p.across_x)

    def y_low(self, k, s):
        dst = self.half(self.bufs[k][3], s, 0)
        return self.copy(k, s, self.grad(k, s, self.p.f ^ 2, 0), dst, 4, self.p.across_y)

    def y_high(self, k, s):
        return self.copy(k, s, self.bufs[k][1].at[s], self.half(self.bufs[k][3], s, 1), 5, self.p.across_y)

    def up(self, k, s):
        return self.copy(k, s, self.bufs[k][2].at[s], self.bufs[k][4].at[s], 6, self.p.above)

    def down(self, k, s):
        at = jnp.where(s == self.p.z - 1, 4, s)
        return self.copy(k, s, self.bufs[k][2].at[s], self.bufs[k][4].at[at], 7, self.p.below)

    def from_above(self, k, s):
        at = jnp.where(s == self.p.z, 4, s)
        return self.copy(k, s, self.bufs[k][4].at[at], self.bufs[k][4].at[at], 7, self.p.below), at

    def start_one(self, k, s):
        self.corner_y(k, s).start()
        self.corner_x(k, s).start()
        self.y_low(k, s).start()
        self.x_high(k, s).start()

    def start(self, k):
        def one(i, carry):
            self.start_one(k, self.p.far_first(i))
            return carry

        lax.fori_loop(0, 4, one, 0)
        if self.own[k] is not None:
            for slot in range(4):
                for load in self.loads(k, slot):
                    load.start()

    def tiles(self, rows, body):
        row_tiles(rows, 48 if rows % 48 == 0 else 16, body)

    def middle_one(self, k, i):
        s, count = self.p.far_first(i), self.rows // 2
        low, high = self.bufs[k][0], self.bufs[k][1]
        if self.own[k] is not None:
            for load in self.loads(k, s):
                load.wait()
        own_low, own_high, _ = self.terms(k, s)
        self.corner_y(k, s).wait_recv()

        def add_low(span):
            low[s, span, :] = add_half(low[s, span, :], own_low[span, :])

        self.tiles(count, add_low)
        self.corner_x(k, s).wait_recv()

        def add_high(span):
            high[s, span, :] = add_half(high[s, span, :], own_high[span, :])

        self.tiles(count, add_high)
        self.x_low(k, s).start()
        self.y_high(k, s).start()

    def line_one(self, k, i):
        z, acc, side, far = self.p.z, self.bufs[k][2], self.bufs[k][3], self.bufs[k][4]
        s = self.p.far_first(i)
        self.x_low(k, s).wait_recv()
        self.x_high(k, s).wait_recv()
        self.y_low(k, s).wait_recv()
        self.y_high(k, s).wait_recv()
        own = self.terms(k, s)[2]

        def add(span):
            total = own[span, :].astype(F32) + acc[s, span, :].astype(F32) + side[s, span, :].astype(F32)
            acc[s, span, :] = total.astype(BF16)

        self.tiles(self.rows, add)

        def add_far(at):
            def body(span):
                acc[s, span, :] = add_half(acc[s, span, :], far[at, span, :])

            self.tiles(self.rows, body)

        @pl.when((z > 0) & (s >= z))
        def _():
            self.up(k, s).wait_recv()
            add_far(s)

        @pl.when((z < 3) & (s <= z))
        def _():
            copy, at = self.from_above(k, s)
            copy.wait_recv()
            add_far(at)

        @pl.when(s > z)
        def _():
            self.up(k, s).start()

        @pl.when(s < z)
        def _():
            self.down(k, s).start()

        @pl.when(s == z)
        def _():
            self.out[k](acc.at[s])

    def loop(self, one):
        def body(i, carry):
            one(i)
            return carry

        lax.fori_loop(0, 4, body, 0)

    def drain(self, k):
        def one(s):
            for copy in (self.corner_y, self.corner_x, self.x_low, self.x_high, self.y_low, self.y_high):
                copy(k, s).wait_send()

            @pl.when(s > self.p.z)
            def _():
                self.up(k, s).wait_send()

            @pl.when(s < self.p.z)
            def _():
                self.down(k, s).wait_send()

        self.loop(one)


def reduce_buffers(rows, lanes):
    half, whole = pltpu.VMEM((4, rows // 2, lanes), BF16), pltpu.VMEM((4, rows, lanes), BF16)
    return [half, half, whole, whole, pltpu.VMEM((5, rows, lanes), BF16)]


def reduce_terms(rows, lanes):
    half, whole = pltpu.VMEM((4, rows // 2, lanes), BF16), pltpu.VMEM((4, rows, lanes), BF16)
    return [half, half, whole]


def scatter_grads(chunks):
    count = lax.axis_size("fy") * lax.axis_size("fx")
    split = [c.reshape(c.shape[0] * count, c.shape[1] // count, c.shape[2]) for c in chunks]
    return [lax.psum_scatter(c, ("slot",) + FSDP, scatter_dimension=0).astype(F32) for c in split]


class RowsBack:
    SEMS = 7

    def __init__(self, place, index, window, inbox, owned, out, sems, rows_each, edge, tail):
        self.p, self.window, self.inbox, self.owned, self.out = place, window, inbox, owned, out
        self.each, self.half, self.edge, self.tail = rows_each, 4 * rows_each, edge, tail
        self.sems = [sem.at[index] for sem in sems]

    def edge_out(self):
        src = self.window.at[self.half : self.half + self.edge, :]
        return send(src, self.inbox.at[: self.edge, :], self.sems[0], self.sems[1], self.p.cross)

    def tail_out(self):
        src = self.window.at[self.half + self.edge :, :]
        return send(src, self.inbox.at[self.edge :, :], self.sems[2], self.sems[3], self.p.cross)

    def block(self, near):
        batch = self.p.batch if near else 1 - self.p.batch
        row = (2 * batch + self.p.c) * self.each
        return self.window.at[pl.ds(pl.multiple_of(row, 16), self.each), :]

    def stay(self):
        return pltpu.make_async_copy(self.block(True), self.out.at[self.p.batch], self.sems[4])

    def to_pair(self):
        return send(self.block(False), self.out.at[self.p.batch], self.sems[5], self.sems[6], self.p.pair)

    def edges(self):
        pl.when(self.p.c == self.p.image)(lambda: self.edge_out().start())
        pl.when((self.p.c == 1) & (self.p.image == 0))(lambda: self.tail_out().start())

    def merge(self, row, count, at):
        keep = self.p.owned(self.owned[row : row + count, :])
        value = jnp.where(keep, self.window[row : row + count, :], self.inbox[at : at + count, :])
        self.window[row : row + count, :] = value

    def finish(self):
        p = self.p

        @pl.when((p.c == 1) & (p.image == 0))
        def _():
            self.edge_out().wait_recv()
            self.merge(self.half - self.edge, self.edge, 0)

        @pl.when((p.c == 0) & (p.image == 1))
        def _():
            self.edge_out().wait_recv()
            self.merge(0, self.edge, 0)

        @pl.when((p.c == 1) & (p.image == 1))
        def _():
            self.tail_out().wait_recv()
            self.merge(self.half - self.tail, self.tail, self.edge)

        self.to_pair().start()
        self.stay().start()

    def drain(self):
        pl.when(self.p.c == self.p.image)(lambda: self.edge_out().wait_send())
        pl.when((self.p.c == 1) & (self.p.image == 0))(lambda: self.tail_out().wait_send())
        self.stay().wait()
        self.to_pair().wait_send()
        ref = self.out.at[1 - self.p.batch]
        send(ref, ref, self.sems[5], self.sems[6], self.p.pair).wait_recv()


def backward_kernel(*refs, cols, unit_rest, edge, tail, tile):
    (ws, gu, rest_ref, half_ref, first_far, qkv_far, ctx_far, inv_far, segc_ref, segr_whole) = refs[:10]
    (x_far, res_grad_ref, y_ref, gain_ref, d_in, old_sums, unit_ref, unit_rest_ref) = refs[10:18]
    (in_out, out_out, up_out, down_out, x_final, y_out, gain_out, shift_out, qv_out, unit_out) = refs[18:28]
    refs = refs[28:]
    (segr_ref, x_out, sums_ref), refs = refs[:3], refs[3:]
    (blocks, gs, part, part_out, part_in, back_ref, grad_ref, key_acc, value_acc, inbox_x, inbox_y) = refs[:11]
    y_window = part_out
    bias_ref, sums_in, vec_sum, vec_in, vec_far = refs[11:16]
    first_ref, qkv_ref, ctx_ref, inv_ref, x_ref = refs[16:21]
    u_bufs, s_bufs, u_own = refs[21:26], refs[26:31], refs[31:34]
    refs = refs[34:]
    sems, loads, back_sems = refs[: Reduce.SEMS], refs[Reduce.SEMS : Reduce.SEMS + 3], refs[Reduce.SEMS + 3 : Reduce.SEMS + 3 + RowsBack.SEMS]
    load_sem, part_s, part_r, y_sems, sum_s, sum_r, vec_s, vec_r, in_sem = refs[Reduce.SEMS + 3 + RowsBack.SEMS :]
    rows, width = half_ref.shape
    shard_rows, main, rest = up_out.shape[0], gu.shape[2], unit_rest
    heads = cols // DH
    place = Place()
    place.barrier()
    each = x_out.shape[1]

    def up_final(total):
        up_out[:, :main] = total[...].astype(F32)

    def small_final(total):
        for n in range(3):
            in_out[n] = total[:, n * cols : (n + 1) * cols].astype(F32).T
        at = 3 * cols
        out_out[...] = total[:, at : at + cols].astype(F32).T
        at = at + cols
        up_out[:, main:] = total[:, at : at + rest].astype(F32)
        down_out[:, main:] = total[:, at + rest : at + 2 * rest].astype(F32)

    r = Reduce(place, (gu, gs), (u_own, None), (up_final, small_final), (u_bufs, s_bufs), sems, loads, shard_rows)
    x_back = RowsBack(place, 0, part_in, inbox_x, segc_ref, x_out, back_sems, each, edge, tail)
    y_back = RowsBack(place, 1, y_window, inbox_y, segc_ref, y_out, back_sems, each, edge, tail)

    def load(i):
        return pltpu.make_async_copy(ws.at[place.far_first(i)], blocks.at[i % 2], load_sem.at[i % 2])

    y_load = pltpu.make_async_copy(y_ref, y_window, y_sems.at[0])
    def slot_loads(i):
        s = place.far_first(i)
        pairs = ((qkv_far, qkv_ref), (ctx_far, ctx_ref), (inv_far, inv_ref))
        return [pltpu.make_async_copy(p[0].at[s], p[1].at[s], in_sem.at[n, i]) for n, p in enumerate(pairs)]

    first_load = pltpu.make_async_copy(first_far, first_ref, y_sems.at[1])
    x_load = pltpu.make_async_copy(x_far, x_ref, y_sems.at[2])
    load(0).start()
    for copy in slot_loads(0):
        copy.start()
    y_load.start()
    r.start(0)
    for t in range(rows // tile):
        segr_ref[t] = segr_whole[:, t * tile : (t + 1) * tile]
    down_out[:, :main] = d_in[...]
    first_load.start()
    for i in (1, 2, 3):
        for copy in slot_loads(i):
            copy.start()
    x_load.start()
    y_load.wait()
    y_back.edges()

    def one_slot(i, carry):
        s = place.far_first(i)
        load(i).wait()
        for copy in slot_loads(i):
            copy.wait()

        @pl.when(i < 3)
        def _():
            load(i + 1).start()

        w = blocks.at[i % 2]
        back_ref[...] = dot_nn(half_ref[...], w[:, 3 * cols : 4 * cols]).astype(BF16)
        gs[s, :, 3 * cols : 4 * cols] = dot_tn(half_ref[...], ctx_ref[s]).astype(BF16)
        gs[s, :, 4 * cols :] = rest_ref[s]
        for head in range(heads):
            attend_back_head(
                qkv_ref, ctx_ref, inv_ref, back_ref, segc_ref, segr_ref, grad_ref, bias_ref, key_acc, value_acc, s, head, cols, tile
            )
            if head == 0:
                r.middle_one(0, i)
                pl.when(i == 1)(lambda: y_back.finish())
        pl.when(i == 0)(lambda: first_load.wait())
        gs[s, :, : 3 * cols] = dot_tn(first_ref[...], grad_ref[...]).astype(BF16)
        product = dot_nt(grad_ref[...], w[:, : 3 * cols])

        @pl.when(i == 0)
        def _():
            part[...] = product

        @pl.when(i > 0)
        def _():
            part[...] += product

        r.start_one(1, s)
        pl.when(i > place.behind())(lambda: r.line_one(0, i - 1 - place.behind()))
        pl.when(i > 0)(lambda: r.middle_one(1, i - 1))
        pl.when(i > 1 + place.behind())(lambda: r.line_one(1, i - 2 - place.behind()))
        return carry

    lax.fori_loop(0, 4, one_slot, 0)

    def halves(h):
        return pl.ds(h * (rows // 2), rows // 2)

    def exchange(h):
        src, dst = part_out.at[halves(h), :], part_in.at[halves(h), :]
        return send(src, dst, part_s.at[h], part_r.at[h], place.mate)

    y_back.drain()
    for h in (0, 1):
        part_out[halves(h), :] = part[halves(h), :].astype(BF16)
        exchange(h).start()
    res_load = pltpu.make_async_copy(res_grad_ref, part, load_sem.at[0])
    res_load.start()
    pl.when(place.behind() == 1)(lambda: r.line_one(0, 2))
    r.line_one(0, 3)
    pl.when(place.behind() == 1)(lambda: r.line_one(1, 1))
    r.middle_one(1, 3)
    for h in (0, 1):
        exchange(h).wait_recv()

    res_load.wait()
    x_load.wait()
    sums_ref[...] = old_sums[...]

    def last(span):
        grad = part_out[span, :].astype(F32) + part_in[span, :].astype(F32)
        value = x_ref[span, :].astype(F32)
        _, scaled, factor = norm_forward(value, gain_ref[0:1, :], gain_ref[0:1, :])
        result = part[span, :] + norm_backward(grad, scaled, factor, gain_ref[0:1, :])
        part_in[span, :] = result.astype(BF16)
        sums_ref[0:1, :] += jnp.sum(grad * scaled, axis=0, keepdims=True)
        sums_ref[2:3, :] += jnp.sum(grad, axis=0, keepdims=True)

    row_tiles(rows, 128, last)
    x_back.edges()

    vec_sum[...] = jnp.zeros_like(vec_sum)
    for s in range(4):
        vec_sum[s, 0:1, :cols] = bias_ref[s, 0:1, :]
        vec_sum[s, 1:2, :cols] = bias_ref[s, 1:2, :]
        vec_sum[s, 2:3, :main] = unit_ref[s, 0:1, :]
        vec_sum[s, 3:4, :rest] = unit_rest_ref[:, s * rest : (s + 1) * rest]

    def across(n, device):
        return (
            send(sums_ref, sums_in.at[n], sum_s.at[n], sum_r.at[n], device),
            send(vec_sum, vec_in.at[n], vec_s.at[n], vec_r.at[n], device),
        )

    def along(d):
        there = (place.z + d) % 4
        device = place.slot_after(d)
        return (
            send(sums_ref, sums_in.at[1 + d], sum_s.at[1 + d], sum_r.at[1 + d], device),
            send(vec_sum.at[there], vec_far.at[d - 1], vec_s.at[1 + d], vec_r.at[1 + d], device),
        )

    def add_across(n, device):
        for copy in across(n, device):
            copy.wait()
        sums_ref[...] += sums_in[n]
        vec_sum[...] += vec_in[n]

    for copy in across(0, place.across_x):
        copy.start()
    r.line_one(1, 2)
    add_across(0, place.across_x)
    for copy in across(1, place.across_y):
        copy.start()
    x_back.finish()
    add_across(1, place.across_y)
    for d in (1, 2, 3):
        for copy in along(d):
            copy.start()
    r.line_one(1, 3)
    for d in (1, 2, 3):
        for copy in along(d):
            copy.wait()
    sums_ref[...] += sums_in[2] + sums_in[3] + sums_in[4]
    gain_out[...] = sums_ref[0:2, :]
    shift_out[...] = sums_ref[2:6, :]
    total = vec_sum[place.z] + vec_far[0] + vec_far[1] + vec_far[2]
    qv_out[...] = total[0:2, :cols]
    unit_out[:main] = total[2:3, :main].reshape(main)
    unit_out[main:] = total[3:4, :rest].reshape(rest)
    for k in (0, 1):
        r.drain(k)
    x_back.drain()
    x_final[...] = x_out[...].astype(F32)
    for h in (0, 1):
        exchange(h).wait_send()


def backward_stage(
    ws, gu, rest_sums, residual_half, first_norm, qkv, context, inverse, segc, segr, x_half, residual_grad, y_rows, gains, down_sum,
    sums, unit_sums, unit_rest_sums, cols, unit_rest, edge, tail, rows_each,
):
    rows, width = residual_half.shape
    shard_rows, lanes, main = width // 4, ws.shape[2], gu.shape[2]
    vmem = pl.BlockSpec(memory_space=pltpu.VMEM)
    far = pl.BlockSpec(memory_space=pl.ANY)
    shape = jax.ShapeDtypeStruct
    dma = pltpu.SemaphoreType.DMA
    wide = max(main, round_up(cols, 128))
    return pl.pallas_call(
        functools.partial(backward_kernel, cols=cols, unit_rest=unit_rest, edge=edge, tail=tail, tile=rows // 2),
        in_specs=[far] * 2 + [vmem] * 2 + [far] * 4 + [vmem] * 2 + [far] * 3 + [vmem] * 5,
        out_specs=[vmem] * 10,
        out_shape=[
            shape((3, cols, shard_rows), F32),
            shape((cols, shard_rows), F32),
            shape((shard_rows, main + unit_rest), F32),
            shape((shard_rows, main + unit_rest), F32),
            shape((2, rows_each, width), F32),
            shape((2, rows_each, width), BF16),
            shape((2, width), F32),
            shape((4, width), F32),
            shape((2, cols), F32),
            shape((main + unit_rest,), F32),
        ],
        scratch_shapes=[
            pltpu.VMEM((2, 1, rows // 2), jnp.int32),
            pltpu.VMEM((2, rows_each, width), BF16),
            pltpu.VMEM((8, width), F32),
            pltpu.VMEM((2, width, lanes), BF16),
            pltpu.VMEM((4, width, lanes), BF16),
            pltpu.VMEM((rows, width), F32),
            pltpu.VMEM((rows, width), BF16),
            pltpu.VMEM((rows, width), BF16),
            pltpu.VMEM((rows, cols), BF16),
            pltpu.VMEM((rows, 3 * cols), BF16),
            pltpu.VMEM((rows, DH), F32),
            pltpu.VMEM((rows, DH), F32),
            pltpu.VMEM((edge + tail, width), BF16),
            pltpu.VMEM((edge + tail, width), BF16),
            pltpu.VMEM((4, 2, cols), F32),
            pltpu.VMEM((5, 8, width), F32),
            pltpu.VMEM((4, 8, wide), F32),
            pltpu.VMEM((2, 4, 8, wide), F32),
            pltpu.VMEM((3, 8, wide), F32),
            pltpu.VMEM((rows, width), BF16),
            pltpu.VMEM((4, rows, 3 * cols), BF16),
            pltpu.VMEM((4, rows, cols), BF16),
            pltpu.VMEM((4, rows, cols // DH), F32),
            pltpu.VMEM((rows, width), BF16),
        ]
        + reduce_buffers(shard_rows, main)
        + reduce_buffers(shard_rows, lanes)
        + reduce_terms(shard_rows, main)
        + [dma((2, 4))] * Reduce.SEMS
        + [dma((1, 4))] * 3
        + [dma((2,))] * RowsBack.SEMS
        + [dma((2,)), dma((2,)), dma((2,)), dma((3,)), dma((5,)), dma((5,)), dma((5,)), dma((5,)), dma((3, 4))],
        compiler_params=pltpu.CompilerParams(collective_id=2, has_side_effects=True, vmem_limit_bytes=64000000),
        name="backward",
    )(
        ws, gu, rest_sums, residual_half, first_norm, qkv, context, inverse, segc, segr,
        x_half, residual_grad, y_rows, gains, down_sum, sums, unit_sums, unit_rest_sums,
    )


def attend_head(qkv_ref, ctx_ref, inv_ref, segc_ref, segr_ref, s, head, cols, tile):
    lo = head * DH
    keys = qkv_ref[s, :, cols + lo : cols + lo + DH]
    values = qkv_ref[s, :, 2 * cols + lo : 2 * cols + lo + DH]

    def one_tile(t, carry):
        span = pl.ds(pl.multiple_of(t * tile, tile), tile)
        scores = dot_nt(qkv_ref[s, span, lo : lo + DH], keys)
        allowed = segc_ref[span, :] == segr_ref[...]
        exact = jnp.where(allowed, jnp.exp2(scores * (SCALE * LOG2E)), 0.0)
        inverse = 1.0 / jnp.sum(exact, axis=1, keepdims=True)
        context = dot_nn(exact.astype(BF16), values) * inverse
        ctx_ref[s, span, lo : lo + DH] = context.astype(BF16)
        inv_ref[s, span, head : head + 1] = inverse
        return carry

    lax.fori_loop(0, qkv_ref.shape[1] // tile, one_tile, 0)


def attend_kernel(x_ref, w_ref, b_ref, segc_ref, segr_ref, qkv_ref, ctx_ref, inv_ref, part_ref, *, cols, tile):
    block = pl.program_id(0)
    projected = dot_nn(x_ref[...], w_ref[0, :, : 3 * cols]) + b_ref[0]
    qkv_ref[0] = projected.astype(BF16)
    for head in range(cols // DH):
        attend_head(qkv_ref, ctx_ref, inv_ref, segc_ref, segr_ref, 0, head, cols, tile)
    part = dot_nt(ctx_ref[0], w_ref[0, :, 3 * cols : 4 * cols])

    @pl.when(block == 0)
    def _():
        part_ref[...] = part

    @pl.when(block > 0)
    def _():
        part_ref[...] += part


def attend(first_norm, weights, bias, segments, cols, tile):
    rows, width = first_norm.shape
    slots, _, lanes = weights.shape
    heads = cols // DH
    whole = lambda shape: pl.BlockSpec(shape, lambda s: (0,) * len(shape))
    each = lambda shape: pl.BlockSpec((1,) + shape, lambda s: (s, 0, 0))
    return pl.pallas_call(
        functools.partial(attend_kernel, cols=cols, tile=tile),
        grid=(slots,),
        in_specs=[
            whole((rows, width)),
            each((width, lanes)),
            each((1, 3 * cols)),
            whole((rows, 1)),
            whole((1, rows)),
        ],
        out_specs=[each((rows, 3 * cols)), each((rows, cols)), each((rows, heads)), whole((rows, width))],
        out_shape=[
            jax.ShapeDtypeStruct((slots, rows, 3 * cols), BF16),
            jax.ShapeDtypeStruct((slots, rows, cols), BF16),
            jax.ShapeDtypeStruct((slots, rows, heads), F32),
            jax.ShapeDtypeStruct((rows, width), F32),
        ],
        cost_estimate=pl.CostEstimate(
            flops=slots * (8 * rows * width * cols + 4 * rows * rows * 256 * heads),
            bytes_accessed=slots * width * lanes * 2 + rows * width * 10,
            transcendentals=slots * heads * rows * rows,
        ),
        name="attend",
    )(first_norm, weights, bias, segments[:, None], segments[None, :])


def attend_back_head(
    qkv_ref, ctx_ref, inv_ref, back_ref, segc_ref, segr_ref, grad_ref, bias_ref, key_acc, value_acc, s, head, cols, tile
):
    lo = head * DH
    rows = back_ref.shape[0]
    ones = jnp.ones((8, DH), F32)
    keys = qkv_ref[s, :, cols + lo : cols + lo + DH]
    values = qkv_ref[s, :, 2 * cols + lo : 2 * cols + lo + DH]
    key_acc[...] = jnp.zeros_like(key_acc)
    value_acc[...] = jnp.zeros_like(value_acc)

    def one_tile(t, query_total):
        span = pl.ds(pl.multiple_of(t * tile, tile), tile)
        queries = qkv_ref[s, span, lo : lo + DH]
        back = (back_ref[span, lo : lo + DH].astype(F32) * inv_ref[s, span, head : head + 1]).astype(BF16)
        along = back.astype(F32) * ctx_ref[s, span, lo : lo + DH].astype(F32)
        delta = lax.dot_general(
            ones, along, (((1,), (1,)), ((), ())), precision=lax.Precision.HIGHEST, preferred_element_type=F32
        )[:1]
        scores = dot_nt(keys, queries)
        allowed = segc_ref[...] == segr_ref[t]
        exact = jnp.where(allowed, jnp.exp2(scores * (SCALE * LOG2E)), 0.0)
        value_acc[...] += dot_nn(exact.astype(BF16), back)
        prob_grad = dot_nt(values, back)
        score_grad = (exact * (prob_grad - delta)).astype(BF16)
        key_acc[...] += dot_nn(score_grad, queries)
        query_grad = dot_tn(score_grad, keys) * SCALE
        grad_ref[span, lo : lo + DH] = query_grad.astype(BF16)
        return query_total + jnp.sum(query_grad, axis=0, keepdims=True)

    query_total = lax.fori_loop(0, rows // tile, one_tile, jnp.zeros((1, DH), F32))
    grad_ref[:, cols + lo : cols + lo + DH] = (key_acc[...] * SCALE).astype(BF16)
    grad_ref[:, 2 * cols + lo : 2 * cols + lo + DH] = value_acc[...].astype(BF16)
    bias_ref[s, 0:1, lo : lo + DH] = query_total
    bias_ref[s, 1:2, lo : lo + DH] = jnp.sum(value_acc[...], axis=0, keepdims=True)


def attend_back_kernel(
    r_ref, w_ref, qkv_ref, ctx_ref, inv_ref, segc_ref, segr_ref, grad_ref, bias_ref, back_ref, key_acc, value_acc, *, cols, tile
):
    back_ref[...] = dot_nn(r_ref[...], w_ref[0, :, 3 * cols : 4 * cols]).astype(BF16)
    for head in range(cols // DH):
        attend_back_head(
            qkv_ref, ctx_ref, inv_ref, back_ref, segc_ref, segr_ref, grad_ref.at[0], bias_ref, key_acc, value_acc, 0, head, cols, tile
        )


def attend_back(residual_half, weights, qkv, context, inverse, segments, cols, tile):
    rows, width = residual_half.shape
    slots, _, lanes = weights.shape
    heads = cols // DH
    whole = lambda shape: pl.BlockSpec(shape, lambda s: (0,) * len(shape))
    each = lambda shape: pl.BlockSpec((1,) + shape, lambda s: (s, 0, 0))
    return pl.pallas_call(
        functools.partial(attend_back_kernel, cols=cols, tile=tile),
        grid=(slots,),
        in_specs=[
            whole((rows, width)),
            each((width, lanes)),
            each((rows, 3 * cols)),
            each((rows, cols)),
            each((rows, heads)),
            whole((rows, 1)),
            whole((rows // tile, 1, tile)),
        ],
        out_specs=[each((rows, 3 * cols)), each((2, cols))],
        out_shape=[
            jax.ShapeDtypeStruct((slots, rows, 3 * cols), BF16),
            jax.ShapeDtypeStruct((slots, 2, cols), F32),
        ],
        scratch_shapes=[
            pltpu.VMEM((rows, cols), BF16),
            pltpu.VMEM((rows, DH), F32),
            pltpu.VMEM((rows, DH), F32),
        ],
        cost_estimate=pl.CostEstimate(
            flops=slots * (2 * rows * width * cols + 10 * rows * rows * 256 * heads),
            bytes_accessed=slots * width * lanes * 2 + rows * width * 10,
            transcendentals=slots * heads * rows * rows,
        ),
        name="attend_back",
    )(residual_half, weights, qkv, context, inverse, segments[:, None], segments.reshape(-1, 1, tile))


def plain_layer(shards, vectors, to_slot, from_slot, block_input, cotangent, gains, shifts, segments, owned, cols, units, parts):
    width, rows = block_input.shape[2], segments.shape[0]
    slots, slot = lax.axis_size("slot"), lax.axis_index("slot")
    main_units, in_lanes = shards[1].shape[1], 3 * cols
    rest = units - main_units
    spare = shards[0].shape[1] - in_lanes - cols - 2 * rest
    small_all, up_main, down_main = gather_weights(shards)
    vec_all = lax.all_gather(vectors, "slot", axis=0)
    grad_rows = jnp.where(owned[:, None], to_slot(cotangent), 0)
    upstream = grad_rows.astype(F32)
    x_float = to_slot(block_input).astype(F32)
    first_out, first_scaled, first_factor = norm_forward(x_float, gains[0], shifts[0])
    first_norm = first_out.astype(BF16)
    bias = vec_all[:, :1, :in_lanes].astype(F32) + vec_all[:, 1:2, :in_lanes].astype(F32)
    qkv, context, inverse, attention_part = attend(first_norm, small_all, bias, segments, cols, rows // 2)
    residual = x_float + part_sum(attention_part, parts) + shifts[2]
    second_out, second_scaled, second_factor = norm_forward(residual, gains[1], shifts[1])
    second_norm = second_out.astype(BF16)
    small_blocks = list(small_all)
    unit_all = vec_all[:, 2, :units].astype(F32)
    at = in_lanes + cols
    ups = list(up_main) + [b[:, at : at + rest] for b in small_blocks]
    downs = list(down_main) + [b[:, at + rest : at + 2 * rest] for b in small_blocks]
    unit_rows = list(unit_all[:, :main_units]) + list(unit_all[:, main_units:])
    pre_acts = [dot_nn(second_norm, w) + b for w, b in zip(ups, unit_rows)]
    hiddens = [gelu(p).astype(BF16) for p in pre_acts]
    output = (residual + part_sum(sum_products(hiddens, downs), parts) + shifts[3]).astype(BF16)
    down_sums = [dot_tn(grad_rows, h).astype(BF16) for h in hiddens]
    pre_grads = [gelu_back(p, dot_nn(grad_rows, w)) for p, w in zip(pre_acts, downs)]
    pre_halves = [p.astype(BF16) for p in pre_grads]
    unit_sums = [jnp.sum(p, axis=0) for p in pre_grads]
    up_sums = [dot_tn(second_norm, p).astype(BF16) for p in pre_halves]
    second_grad = part_sum(sum_products(pre_halves, ups), parts)
    residual_grad = upstream + norm_backward(second_grad, second_scaled, second_factor, gains[1])
    residual_half = residual_grad.astype(BF16)
    triple, bias_sum = attend_back(residual_half, small_all, qkv, context, inverse, segments, cols, rows // 2)
    first_part = sum_products(list(triple), [b[:, :in_lanes] for b in small_blocks])
    first_grad = part_sum(first_part, parts)
    input_grad = residual_grad + norm_backward(first_grad, first_scaled, first_factor, gains[0])
    blank = jnp.zeros((width, spare), BF16)
    small_sums = [
        jnp.concatenate(
            [
                dot_tn(first_norm, triple[s]).astype(BF16),
                dot_tn(residual_half, context[s]).astype(BF16),
                up_sums[slots + s],
                down_sums[slots + s],
                blank,
            ],
            axis=1,
        )
        for s in range(slots)
    ]
    down_grad, up_grad, small_grad = scatter_grads(
        [jnp.stack(down_sums[:slots]), jnp.stack(up_sums[:slots]), jnp.stack(small_sums)]
    )
    rows_sum = jnp.stack(
        [
            jnp.sum(first_grad * first_scaled, axis=0),
            jnp.sum(second_grad * second_scaled, axis=0),
            jnp.sum(first_grad, axis=0),
            jnp.sum(second_grad, axis=0),
            jnp.sum(residual_grad, axis=0),
            jnp.sum(upstream, axis=0),
        ]
    )
    unit_sum = jnp.stack([jnp.concatenate([unit_sums[s], unit_sums[slots + s]]) for s in range(slots)])
    rows_total, bias_total, unit_total = lax.psum((rows_sum, bias_sum, unit_sum), ("slot",) + FSDP)
    bias_grad = lax.dynamic_index_in_dim(bias_total, slot, 0, keepdims=False)
    unit_grad = lax.dynamic_index_in_dim(unit_total, slot, 0, keepdims=False)
    return (
        from_slot(output, owned), from_slot(input_grad.astype(BF16), owned), rows_total, bias_grad, unit_grad,
        down_grad, up_grad, small_grad,
    )


def on_device(
    block_input,
    segment_ids,
    norm_gains,
    row_biases,
    in_projection,
    query_value_bias,
    out_projection,
    up_weight,
    unit_bias,
    down_weight,
    cotangent,
):
    local, rows_each, width = block_input.shape
    rows_mb = segment_ids.shape[1]
    cols = in_projection.shape[2]
    units = up_weight.shape[1]
    shard_rows = up_weight.shape[0]
    slots, parts = lax.axis_size("slot"), lax.axis_size("part")
    slot, part = lax.axis_index("slot"), lax.axis_index("part")
    fsdp_index = lax.axis_index("fy") * lax.axis_size("fx") + lax.axis_index("fx")
    batch, image = slot % local, slot // local
    late = image == 1

    half_rows = rows_mb // IMG_MB
    padding = rows_mb - IMG_MB * IMG
    edge = round_up(max(half_rows - IMG, padding - (half_rows - IMG)), 16)
    tail = round_up(padding, 16)
    rows = round_up(half_rows + edge + tail, 128)
    filler = rows - half_rows - edge - tail
    paired = lax.axis_size("fy") == 2 and lax.axis_size("fx") == 2 and slots == 4 and parts == 2
    paired = paired and shard_rows % 32 == 0 and filler == 0

    def edges(main):
        near = jnp.where(late, main[:edge], main[half_rows - edge :])
        far = main[half_rows - tail :]
        return jnp.concatenate([near, far])

    def to_slot(value):
        mine = lax.dynamic_index_in_dim(value, batch, 0, keepdims=False)
        send = lax.dynamic_index_in_dim(value, 1 - batch, 0, keepdims=False)
        other = slot_swap(send, 1, slots)
        pair = jnp.where(batch == 0, jnp.stack([mine, other]), jnp.stack([other, mine]))
        main = part_gather(pair, parts).swapaxes(0, 1).reshape(half_rows, width)
        beyond = slot_swap(edges(main), local, slots)
        return jnp.concatenate([main, beyond, jnp.zeros((filler, width), value.dtype)])

    def from_slot(value, owned):
        main = value[:half_rows]
        beyond = slot_swap(value[half_rows : half_rows + edge + tail], local, slots)
        keep = owned[:half_rows, None]
        near, far = beyond[:edge], beyond[edge:]
        blank = lambda count: jnp.zeros((count, width), value.dtype)
        early_fill = jnp.concatenate([blank(half_rows - edge), near])
        late_fill = jnp.concatenate([near, blank(half_rows - edge - tail), far])
        main = jnp.where(keep, main, jnp.where(late, late_fill, early_fill))
        main = main.reshape(local, parts, rows_each, width)
        mine = lax.dynamic_index_in_dim(main, part, 1, keepdims=False)
        stay = lax.dynamic_index_in_dim(mine, batch, 0, keepdims=False)
        other = slot_swap(lax.dynamic_index_in_dim(mine, 1 - batch, 0, keepdims=False), 1, slots)
        return jnp.where(batch == 0, jnp.stack([stay, other]), jnp.stack([other, stay]))

    ids = jnp.where(batch == 0, segment_ids[:1], segment_ids[1:])
    filler_ids = lambda count: jnp.full((1, count), -2, jnp.int32)
    early_ids = jnp.concatenate([ids[:, : half_rows + edge], ids[:, rows_mb - tail :], filler_ids(filler)], axis=1)
    late_ids = jnp.concatenate(
        [ids[:, half_rows:], ids[:, half_rows - edge : half_rows], filler_ids(tail + filler)], axis=1
    )
    segr = jnp.where(late, late_ids, early_ids)
    segc = segr.reshape(rows, 1)

    main_units = units // 128 * 128
    rest = units - main_units
    in_lanes = 3 * cols
    small = in_lanes + cols + 2 * rest
    lanes = round_up(small, 128)
    gains, shifts = norm_gains, row_biases
    if paired:
        (
            small_all, up_main, down_main, gd, x_half, cot, first_norm, qkv, context, inverse, residual, second_norm,
            hidden, slope, hidden_rest, slope_rest, rest_up, rest_down,
        ) = forward_stage(
            (in_projection.swapaxes(1, 2), out_projection, up_weight, down_weight.T), (query_value_bias, unit_bias),
            block_input, cotangent, gains, shifts, segc, segr, cols, units, lanes, edge, tail,
        )
        gu, down_sum, rest_sums, residual_half, residual_grad, y_rows, sums, unit_sums, unit_rest_sums = middle_stage(
            down_main, up_main, gd, hidden, slope, hidden_rest, slope_rest, rest_up, rest_down, cot, second_norm, residual,
            gains, shifts, cols, rest, lanes - small,
        )
        in_grad, out_grad, up_grad, down_grad, input_grad, output, gain_grad, shift_grad, bias_grad, unit_grad = backward_stage(
            small_all, gu, rest_sums, residual_half, first_norm, qkv, context, inverse, segc, segr, x_half, residual_grad,
            y_rows, gains, down_sum, sums, unit_sums, unit_rest_sums, cols, rest, edge, tail, rows_each,
        )
        in_grad, down_grad = in_grad.swapaxes(1, 2), down_grad.T
    else:
        segments = segc[:, 0]
        image_id = (fsdp_index * local + batch) * IMG_MB + image
        owned = (segments == image_id) | (jnp.logical_not(late) & (segments == -1))
        down_t = down_weight.T
        small_shard = jnp.concatenate(
            [
                in_projection.transpose(1, 0, 2).reshape(shard_rows, in_lanes),
                out_projection.T,
                up_weight[:, main_units:],
                down_t[:, main_units:],
                jnp.zeros((shard_rows, lanes - small), BF16),
            ],
            axis=1,
        )
        shards = [small_shard, up_weight[:, :main_units], down_t[:, :main_units]]
        triple_bias = jnp.concatenate([query_value_bias[0], jnp.zeros((cols,), F32), query_value_bias[1]])
        high = triple_bias.astype(BF16)
        low = (triple_bias - high.astype(F32)).astype(BF16)
        wide = round_up(max(in_lanes, units), 128)
        vectors = [jnp.pad(v, (0, wide - v.shape[0])) for v in (high, low, unit_bias)]
        vectors = jnp.concatenate([jnp.stack(vectors), jnp.zeros((13, wide), BF16)])
        output, input_grad, rows_total, bias_grad, unit_grad, down_grad, up_grad, small_grad = plain_layer(
            shards, vectors, to_slot, from_slot, block_input, cotangent, gains, shifts, segments, owned, cols, units, parts
        )
        in_grad = small_grad[:, :in_lanes].reshape(shard_rows, 3, cols).transpose(1, 0, 2)
        out_grad = small_grad[:, in_lanes : in_lanes + cols].T
        at = in_lanes + cols
        up_grad = jnp.concatenate([up_grad, small_grad[:, at : at + rest]], axis=1)
        down_grad = jnp.concatenate([down_grad, small_grad[:, at + rest : at + 2 * rest]], axis=1).T
        gain_grad, shift_grad = rows_total[:2], rows_total[2:]
    return (
        output,
        input_grad.astype(F32),
        gain_grad,
        shift_grad,
        in_grad,
        bias_grad,
        out_grad,
        up_grad,
        unit_grad,
        down_grad,
    )


def solution(mesh):
    fsdp, tensor = mesh.shape["fsdp"], mesh.shape["tensor"]

    def layer(*arrays):
        local = arrays[0].shape[0] // fsdp
        slots = local * IMG_MB
        assert local == 2 and slots == 4 and tensor % slots == 0 and fsdp % 2 == 0
        grid = Mesh(
            mesh.devices.reshape(fsdp // 2, 2, slots, tensor // slots), ("fy", "fx", "slot", "part")
        )
        tens = ("slot", "part")
        return jax.shard_map(
            on_device,
            mesh=grid,
            in_specs=(
                P(FSDP, tens, None),
                P(FSDP, None),
                P(),
                P(),
                P(None, FSDP, tens),
                P(None, tens),
                P(tens, FSDP),
                P(FSDP, tens),
                P(tens),
                P(tens, FSDP),
                P(FSDP, tens, None),
            ),
            out_specs=(
                P(FSDP, tens, None),
                P(FSDP, tens, None),
                P(),
                P(),
                P(None, FSDP, tens),
                P(None, tens),
                P(tens, FSDP),
                P(FSDP, tens),
                P(tens),
                P(tens, FSDP),
            ),
            check_vma=False,
        )(*arrays)

    return layer
```
